16 devices in a mesh: tp: 2 (over z), dp: 8 (over y, x, core).
Axes of the slice: x: 2, y: 2, z: 2, core: 2. Of those that a mesh axis runs over, the one named last changes fastest.
Arguments:
- a_mat: bfloat16 [4096, 32768], P(('dp', 'tp'))
- b_mat: bfloat16 [32768, 14336], P(('dp', 'tp'))
Outputs:
- output: bfloat16 [4096, 14336], P(('dp', 'tp'))
All inputs are finite; a program needn't handle non-finite values.
Results may differ from the reference program's by a relative error of at most 0.001.
Values are sent between devices in bfloat16 or wider.
A program may use at most 1 GiB of HBM per device.

```python
import jax
import jax.numpy as jnp

D_MODEL = 4096
D_FF = 14336
TOKENS_DEV = 2048
DEVICES = 16
TOKENS = TOKENS_DEV * DEVICES


def setup_inputs(seed: int = 0) -> dict:
    root_key = jax.random.key(seed)
    key_a, key_b = jax.random.split(root_key)
    acts_t = jax.random.normal(key_a, (D_MODEL, TOKENS), jnp.float32)
    grads = jax.random.normal(key_b, (TOKENS, D_FF), jnp.float32) * (TOKENS ** -0.5)
    return {"a_mat": acts_t.astype(jnp.bfloat16), "b_mat": grads.astype(jnp.bfloat16)}


def reference(a_mat, b_mat):
    prod = jnp.dot(a_mat, b_mat, preferred_element_type=jnp.float32)
    return prod.astype(jnp.bfloat16)
```

```python
import functools

import jax
import jax.numpy as jnp
from jax import lax
from jax.experimental import pallas as pl
from jax.experimental.pallas import tpu as pltpu
from jax.sharding import PartitionSpec as P

MESH = pl.DeviceIdType.MESH
W = 128
G = 3
LOOK = 4


def bits_of(d):
    return (d // 4, (d // 2) % 2, d % 2)


def kernel(a_hbm, b_hbm, c_hbm, bx_hbm, a_v, b_v, p_v, r1_v, s2_v, r2_v, s3_v, r3_v, o_v,
           a_send, a_recv, a_loc, bx_send, bx_recv, b_sem, s1_sem, r1_sem, s2_sem, r2_sem, s3_sem, r3_sem, o_sem, credit):
    rows = a_hbm.shape[0]
    depth, columns = b_hbm.shape
    strips = columns // W
    rem = strips % G
    tiles = (strips + G - 1) // G
    lead = (G - rem) % G

    dp, tp = lax.axis_index("dp"), lax.axis_index("tp")
    core, x, y, z = dp % 2, (dp // 2) % 2, dp // 4, tp

    def flip(v, bit):
        return v + bit - 2 * v * bit

    def device(bits, other=0):
        return {"dp": flip(y, bits[1]) * 4 + flip(x, bits[0]) * 2 + flip(core, other), "tp": flip(z, bits[2])}

    axis_nbr = [device((1, 0, 0)), device((0, 1, 0)), device((0, 0, 1))]
    partner = device((0, 0, 0), 1)

    barrier = pltpu.get_barrier_semaphore()
    for d in range(1, 8):
        pl.semaphore_signal(barrier, inc=1, device_id=device(bits_of(d)), device_id_type=MESH)
    pl.semaphore_signal(barrier, inc=1, device_id=partner, device_id_type=MESH)

    def past_first(t):
        return (t + tiles) // (tiles + 1)

    def tile_col(t):
        return pl.multiple_of((t * G - lead * past_first(t)) * W, W)

    def a_copy(d, h):
        to = device(bits_of(d), h)
        col = pl.multiple_of((to["dp"] * 2 + to["tp"]) * depth, depth)
        src = a_hbm.at[:, pl.ds(col, depth)]
        dst = a_v.at[d, :, pl.ds(h * depth, depth)]
        if d == 0:
            return pltpu.make_async_copy(src, dst, a_loc.at[h])
        return pltpu.make_async_remote_copy(
            src_ref=src, dst_ref=dst, send_sem=a_send.at[d, h], recv_sem=a_recv.at[d, h],
            device_id=device(bits_of(d)), device_id_type=MESH)

    def bx_copy(t):
        cols = pl.ds(tile_col(t), G * W)
        return pltpu.make_async_remote_copy(
            src_ref=b_hbm.at[:, cols], dst_ref=bx_hbm.at[t], send_sem=bx_send.at[t], recv_sem=bx_recv.at[t],
            device_id=partner, device_id_type=MESH)

    def b_copies(t):
        slot = t % 2
        cols = pl.ds(tile_col(t), G * W)
        return (pltpu.make_async_copy(b_hbm.at[:, cols], b_v.at[slot, pl.ds(0, depth), :], b_sem.at[slot, 0]),
                pltpu.make_async_copy(bx_hbm.at[t], b_v.at[slot, pl.ds(depth, depth), :], b_sem.at[slot, 1]))

    def b_fetch(t):
        bx_copy(t).wait_recv()
        for copy in b_copies(t):
            copy.start()

    for copy in (a_copy(0, 0), a_copy(0, 1)):
        copy.start()
    pl.semaphore_wait(barrier, 8)
    bx_copy(0).start()

    groups = ((7,), (6, 1), (5, 2), (3, 4))
    halves = [[a_copy(d, h) for d in group] for group in groups for h in range(2)]
    for i, half in enumerate(halves):
        if i >= 2:
            for copy in halves[i - 2]:
                copy.wait_recv()
        for copy in half:
            copy.start()
        if i == 1:
            for t in range(1, min(LOOK, tiles)):
                bx_copy(t).start()
            b_fetch(0)
    for copy in (a_copy(0, 0), a_copy(0, 1)):
        copy.wait()
    for half in halves[-2:]:
        for copy in half:
            copy.wait_recv()

    def send(src, dst, send_sem, recv_sem, axis):
        return pltpu.make_async_remote_copy(
            src_ref=src, dst_ref=dst, send_sem=send_sem, recv_sem=recv_sem, device_id=axis_nbr[axis], device_id_type=MESH)

    def send1(t, g):
        s = t % 2
        return send(p_v.at[s, g, 1], r1_v.at[s, g], s1_sem.at[s, g], r1_sem.at[s, g], g)

    def send2(t, g):
        s = t % 2
        return send(s2_v.at[s, g, pl.ds(2, 2)], r2_v.at[s, g], s2_sem.at[s, g], r2_sem.at[s, g], (g + 1) % 3)

    def send3(t, g):
        s = t % 2
        return send(s3_v.at[s, g, 1], r3_v.at[s, g], s3_sem.at[s, g], r3_sem.at[s, g], (g + 2) % 3)

    def out_copy(t, g):
        s = t % 2
        col = tile_col(t) + g * W
        return pltpu.make_async_copy(o_v.at[s, g], c_hbm.at[:, pl.ds(pl.multiple_of(col, W), W)], o_sem.at[s, g])

    def first(g):
        return 0 if rem == 0 or g < rem else 1

    def when(t, low, high, fn):
        pl.when(jnp.logical_and(t >= low, t < high))(fn)

    def start_with_credit(t, g, phase, copy):
        when(t, first(g) + 2, tiles, lambda: pl.semaphore_wait(credit.at[phase, g], 1))
        when(t, first(g), tiles, lambda: copy(t, g).start())

    def give_credit(t, g, phase):
        when(t, first(g), tiles - 2, lambda: pl.semaphore_signal(
            credit.at[phase, g], inc=1, device_id=axis_nbr[(g + phase) % 3], device_id_type=MESH))

    def free(t, g, copy):
        when(t, first(g) + 2, tiles + 2, lambda: copy(t - 2, g).wait_send())

    def partials(t):
        s = t % 2

        def body(d, carry):
            b = bits_of(d)
            part = jnp.dot(a_v[d], b_v[s], preferred_element_type=jnp.float32)
            for g in range(G):
                p_v[s, g, b[g], b[(g + 1) % 3] * 2 + b[(g + 2) % 3]] = part[:, g * W:(g + 1) * W]
            return carry

        lax.fori_loop(0, 8, body, 0)

    def step(i, carry):
        t = i
        when(t, 0, tiles - LOOK, lambda: bx_copy(t + LOOK).start())
        when(t, 0, tiles - 1, lambda: b_fetch(t + 1))
        for g in range(G):
            free(t, g, send1)

        def products():
            for copy in b_copies(t):
                copy.wait()
            partials(t)

        when(t, 0, tiles, products)
        for g in range(G):
            start_with_credit(t, g, 0, send1)

        t1 = i - 1
        for g in range(G):
            free(t1, g, send2)

            def add1(g=g):
                s = t1 % 2
                send1(t1, g).wait_recv()
                s2_v[s, g] = p_v[s, g, 0] + r1_v[s, g]

            when(t1, first(g), tiles, add1)
            give_credit(t1, g, 0)
            start_with_credit(t1, g, 1, send2)

        t2 = i - 2
        for g in range(G):
            free(t2, g, send3)

            def add2(g=g):
                s = t2 % 2
                send2(t2, g).wait_recv()
                s3_v[s, g] = s2_v[s, g, 0:2] + r2_v[s, g]

            when(t2, first(g), tiles, add2)
            give_credit(t2, g, 1)
            start_with_credit(t2, g, 2, send3)

        t3 = i - 3
        for g in range(G):
            when(t3, first(g) + 2, tiles + 2, lambda g=g: out_copy(t3 - 2, g).wait())

            def add3(g=g):
                s = t3 % 2
                send3(t3, g).wait_recv()
                o_v[s, g] = (s3_v[s, g, 0] + r3_v[s, g]).astype(jnp.bfloat16)
                out_copy(t3, g).start()

            when(t3, first(g), tiles, add3)
            give_credit(t3, g, 2)
        return carry

    lax.fori_loop(0, tiles + 5, step, 0)

    for half in halves:
        for copy in half:
            copy.wait_send()

    def drain(t, carry):
        bx_copy(t).wait_send()
        return carry

    lax.fori_loop(0, tiles, drain, 0)


def solution(mesh):
    spec_rows = P(("dp", "tp"), None)

    def local_block(a_rows, b_rows):
        rows, inner = a_rows.shape
        depth, columns = b_rows.shape
        tiles = -(-columns // (G * W))
        f32, bf16 = jnp.float32, jnp.bfloat16
        dma = pltpu.SemaphoreType.DMA
        out = pl.pallas_call(
            kernel,
            name="matmul_reduce_scatter",
            out_shape=(jax.ShapeDtypeStruct((rows, columns), bf16), jax.ShapeDtypeStruct((tiles, depth, G * W), bf16)),
            in_specs=[pl.BlockSpec(memory_space=pl.ANY)] * 2,
            out_specs=(pl.BlockSpec(memory_space=pl.ANY),) * 2,
            scratch_shapes=[
                pltpu.VMEM((8, rows, 2 * depth), bf16),
                pltpu.VMEM((2, 2 * depth, G * W), bf16),
                pltpu.VMEM((2, G, 2, 4, rows, W), f32),
                pltpu.VMEM((2, G, 4, rows, W), f32),
                pltpu.VMEM((2, G, 4, rows, W), f32),
                pltpu.VMEM((2, G, 2, rows, W), f32),
                pltpu.VMEM((2, G, 2, rows, W), f32),
                pltpu.VMEM((2, G, rows, W), f32),
                pltpu.VMEM((2, G, rows, W), bf16),
                dma((8, 2)), dma((8, 2)), dma((2,)),
                dma((tiles,)), dma((tiles,)), dma((2, 2)),
                dma((2, G)), dma((2, G)), dma((2, G)), dma((2, G)), dma((2, G)), dma((2, G)), dma((2, G)),
                pltpu.SemaphoreType.REGULAR((3, G)),
            ],
            compiler_params=pltpu.CompilerParams(
                collective_id=0, has_side_effects=True, vmem_limit_bytes=60 * 1024 * 1024),
            cost_estimate=pl.CostEstimate(
                flops=2 * 8 * rows * 2 * depth * columns, bytes_accessed=6 * depth * columns, transcendentals=0),
        )(a_rows, b_rows)
        return out[0]

    return jax.shard_map(local_block, mesh=mesh, in_specs=(spec_rows, spec_rows), out_specs=spec_rows, check_vma=False)
```

```python
import functools

import jax
import jax.numpy as jnp
from jax import lax
from jax.experimental import pallas as pl
from jax.experimental.pallas import tpu as pltpu
from jax.sharding import PartitionSpec as P

MESH = pl.DeviceIdType.MESH
W = 128
G = 3
LOOK = 4


def bits_of(d):
    return (d // 4, (d // 2) % 2, d % 2)


def kernel(a_hbm, b_hbm, c_hbm, bx_hbm, a_v, relay, b_v, p_v, r1_v, s2_v, r2_v, s3_v, r3_v, o_v,
           a_send, a_recv, a_loc, bx_send, bx_recv, b_sem, s1_sem, r1_sem, s2_sem, r2_sem, s3_sem, r3_sem, o_sem, credit):
    rows = a_hbm.shape[0]
    depth, columns = b_hbm.shape
    strips = columns // W
    rem = strips % G
    tiles = (strips + G - 1) // G
    lead = (G - rem) % G

    dp, tp = lax.axis_index("dp"), lax.axis_index("tp")
    core, x, y, z = dp % 2, (dp // 2) % 2, dp // 4, tp

    def flip(v, bit):
        return v + bit - 2 * v * bit

    def device(bits, other=0):
        return {"dp": flip(y, bits[1]) * 4 + flip(x, bits[0]) * 2 + flip(core, other), "tp": flip(z, bits[2])}

    axis_nbr = [device((1, 0, 0)), device((0, 1, 0)), device((0, 0, 1))]
    partner = device((0, 0, 0), 1)

    barrier = pltpu.get_barrier_semaphore()
    for nbr in (*axis_nbr, partner):
        pl.semaphore_signal(barrier, inc=1, device_id=nbr, device_id_type=MESH)

    def past_first(t):
        return (t + tiles) // (tiles + 1)

    def tile_col(t):
        return pl.multiple_of((t * G - lead * past_first(t)) * W, W)

    def a_cols(d, h):
        to = device(bits_of(d), h)
        return a_hbm.at[:, pl.ds(pl.multiple_of((to["dp"] * 2 + to["tp"]) * depth, depth), depth)]

    def block(ref, i, h):
        return ref.at[i, :, pl.ds(h * depth, depth)]

    def hop(n, h, src, dst, axis):
        return pltpu.make_async_remote_copy(
            src_ref=src, dst_ref=dst, send_sem=a_send.at[n, h], recv_sem=a_recv.at[n, h],
            device_id=axis_nbr[axis], device_id_type=MESH)

    def hops(h):
        return (
            (hop(0, h, a_cols(7, h), block(relay, 0, h), 0),
             hop(1, h, a_cols(6, h), block(relay, 1, h), 1),
             hop(2, h, a_cols(5, h), block(relay, 2, h), 2)),
            (hop(3, h, block(relay, 1, h), block(a_v, 6, h), 0),
             hop(4, h, block(relay, 0, h), block(relay, 3, h), 1),
             hop(5, h, a_cols(3, h), block(relay, 4, h), 2)),
            (hop(6, h, block(relay, 2, h), block(a_v, 5, h), 0),
             hop(7, h, block(relay, 4, h), block(a_v, 3, h), 1),
             hop(8, h, block(relay, 3, h), block(a_v, 7, h), 2)),
            (hop(9, h, a_cols(4, h), block(a_v, 4, h), 0),
             hop(10, h, a_cols(2, h), block(a_v, 2, h), 1),
             hop(11, h, a_cols(1, h), block(a_v, 1, h), 2)))

    def a_own(h):
        return pltpu.make_async_copy(a_cols(0, h), block(a_v, 0, h), a_loc.at[h])

    def bx_copy(t):
        cols = pl.ds(tile_col(t), G * W)
        return pltpu.make_async_remote_copy(
            src_ref=b_hbm.at[:, cols], dst_ref=bx_hbm.at[t], send_sem=bx_send.at[t], recv_sem=bx_recv.at[t],
            device_id=partner, device_id_type=MESH)

    def b_copies(t):
        slot = t % 2
        cols = pl.ds(tile_col(t), G * W)
        return (pltpu.make_async_copy(b_hbm.at[:, cols], b_v.at[slot, pl.ds(0, depth), :], b_sem.at[slot, 0]),
                pltpu.make_async_copy(bx_hbm.at[t], b_v.at[slot, pl.ds(depth, depth), :], b_sem.at[slot, 1]))

    def b_fetch(t):
        bx_copy(t).wait_recv()
        for copy in b_copies(t):
            copy.start()

    def send(src, dst, send_sem, recv_sem, axis):
        return pltpu.make_async_remote_copy(
            src_ref=src, dst_ref=dst, send_sem=send_sem, recv_sem=recv_sem, device_id=axis_nbr[axis], device_id_type=MESH)

    def send1(t, g):
        s = t % 2
        return send(p_v.at[s, g, 1], r1_v.at[s, g], s1_sem.at[s, g], r1_sem.at[s, g], g)

    def send2(t, g):
        s = t % 2
        return send(s2_v.at[s, g, pl.ds(2, 2)], r2_v.at[s, g], s2_sem.at[s, g], r2_sem.at[s, g], (g + 1) % 3)

    def send3(t, g):
        s = t % 2
        return send(s3_v.at[s, g, 1], r3_v.at[s, g], s3_sem.at[s, g], r3_sem.at[s, g], (g + 2) % 3)

    def out_copy(t, g):
        s = t % 2
        col = tile_col(t) + g * W
        return pltpu.make_async_copy(o_v.at[s, g], c_hbm.at[:, pl.ds(pl.multiple_of(col, W), W)], o_sem.at[s, g])

    def first(g):
        return 0 if rem == 0 or g < rem else 1

    def when(t, low, high, fn):
        pl.when(jnp.logical_and(t >= low, t < high))(fn)

    def start_with_credit(t, g, phase, copy):
        when(t, first(g) + 2, tiles, lambda: pl.semaphore_wait(credit.at[phase, g], 1))
        when(t, first(g), tiles, lambda: copy(t, g).start())

    def give_credit(t, g, phase):
        when(t, first(g), tiles - 2, lambda: pl.semaphore_signal(
            credit.at[phase, g], inc=1, device_id=axis_nbr[(g + phase) % 3], device_id_type=MESH))

    def free(t, g, copy):
        when(t, first(g) + 2, tiles + 2, lambda: copy(t - 2, g).wait_send())

    def partial(t, d):
        s = t % 2
        b = bits_of(d)
        part = jnp.dot(a_v[d], b_v[s], preferred_element_type=jnp.float32)
        for g in range(G):
            p_v[s, g, b[g], b[(g + 1) % 3] * 2 + b[(g + 2) % 3]] = part[:, g * W:(g + 1) * W]

    def partials(t):
        def body(d, carry):
            partial(t, d)
            return carry

        lax.fori_loop(0, 8, body, 0)

    slots = [hops(0), hops(1)]
    for h in range(2):
        a_own(h).start()
    pl.semaphore_wait(barrier, 4)
    bx_copy(0).start()
    for h in range(2):
        for copy in slots[h][0]:
            copy.start()
    for t in range(1, min(LOOK, tiles)):
        bx_copy(t).start()
    for t in range(2):
        b_fetch(t)
    for h in range(2):
        slots[h][0][0].wait_recv()
        slots[h][0][1].wait_recv()
        for copy in slots[h][1]:
            copy.start()
    for t in range(2):
        for copy in b_copies(t):
            copy.wait()
    for h in range(2):
        a_own(h).wait()
    partial(0, 0)
    partial(1, 0)
    for h in range(2):
        slots[h][0][2].wait_recv()
        slots[h][1][1].wait_recv()
        slots[h][1][2].wait_recv()
        for copy in slots[h][2]:
            copy.start()
    for h in range(2):
        for copy in slots[h][3]:
            copy.start()
    for h in range(2):
        slots[h][1][0].wait_recv()
    partial(0, 6)
    partial(1, 6)
    for h in range(2):
        for copy in slots[h][2]:
            copy.wait_recv()
    for t in range(2):
        for d in (3, 5, 7):
            partial(t, d)
    for h in range(2):
        for copy in slots[h][3]:
            copy.wait_recv()
    for d in (1, 2, 4):
        partial(0, d)

    def step(i, carry):
        t = i
        when(t, 0, tiles - LOOK, lambda: bx_copy(t + LOOK).start())
        when(t, 1, tiles - 1, lambda: b_fetch(t + 1))
        for g in range(G):
            free(t, g, send1)

        def products():
            for copy in b_copies(t):
                copy.wait()
            partials(t)

        when(t, 2, tiles, products)

        def rest():
            for d in (1, 2, 4):
                partial(1, d)

        when(t, 1, 2, rest)
        for g in range(G):
            start_with_credit(t, g, 0, send1)

        t1 = i - 1
        for g in range(G):
            free(t1, g, send2)

            def add1(g=g):
                s = t1 % 2
                send1(t1, g).wait_recv()
                s2_v[s, g] = p_v[s, g, 0] + r1_v[s, g]

            when(t1, first(g), tiles, add1)
            give_credit(t1, g, 0)
            start_with_credit(t1, g, 1, send2)

        t2 = i - 2
        for g in range(G):
            free(t2, g, send3)

            def add2(g=g):
                s = t2 % 2
                send2(t2, g).wait_recv()
                s3_v[s, g] = s2_v[s, g, 0:2] + r2_v[s, g]

            when(t2, first(g), tiles, add2)
            give_credit(t2, g, 1)
            start_with_credit(t2, g, 2, send3)

        t3 = i - 3
        for g in range(G):
            when(t3, first(g) + 2, tiles + 2, lambda g=g: out_copy(t3 - 2, g).wait())

            def add3(g=g):
                s = t3 % 2
                send3(t3, g).wait_recv()
                o_v[s, g] = (s3_v[s, g, 0] + r3_v[s, g]).astype(jnp.bfloat16)
                out_copy(t3, g).start()

            when(t3, first(g), tiles, add3)
            give_credit(t3, g, 2)
        return carry

    lax.fori_loop(0, tiles + 5, step, 0)

    for h in range(2):
        for slot in slots[h]:
            for copy in slot:
                copy.wait_send()

    def drain(t, carry):
        bx_copy(t).wait_send()
        return carry

    lax.fori_loop(0, tiles, drain, 0)


def solution(mesh):
    spec_rows = P(("dp", "tp"), None)

    def local_block(a_rows, b_rows):
        rows, inner = a_rows.shape
        depth, columns = b_rows.shape
        tiles = -(-columns // (G * W))
        f32, bf16 = jnp.float32, jnp.bfloat16
        dma = pltpu.SemaphoreType.DMA
        out = pl.pallas_call(
            kernel,
            name="matmul_reduce_scatter",
            out_shape=(jax.ShapeDtypeStruct((rows, columns), bf16), jax.ShapeDtypeStruct((tiles, depth, G * W), bf16)),
            in_specs=[pl.BlockSpec(memory_space=pl.ANY)] * 2,
            out_specs=(pl.BlockSpec(memory_space=pl.ANY),) * 2,
            scratch_shapes=[
                pltpu.VMEM((8, rows, 2 * depth), bf16),
                pltpu.VMEM((5, rows, 2 * depth), bf16),
                pltpu.VMEM((2, 2 * depth, G * W), bf16),
                pltpu.VMEM((2, G, 2, 4, rows, W), f32),
                pltpu.VMEM((2, G, 4, rows, W), f32),
                pltpu.VMEM((2, G, 4, rows, W), f32),
                pltpu.VMEM((2, G, 2, rows, W), f32),
                pltpu.VMEM((2, G, 2, rows, W), f32),
                pltpu.VMEM((2, G, rows, W), f32),
                pltpu.VMEM((2, G, rows, W), bf16),
                dma((12, 2)), dma((12, 2)), dma((2,)),
                dma((tiles,)), dma((tiles,)), dma((2, 2)),
                dma((2, G)), dma((2, G)), dma((2, G)), dma((2, G)), dma((2, G)), dma((2, G)), dma((2, G)),
                pltpu.SemaphoreType.REGULAR((3, G)),
            ],
            compiler_params=pltpu.CompilerParams(
                collective_id=0, has_side_effects=True, vmem_limit_bytes=60 * 1024 * 1024),
            cost_estimate=pl.CostEstimate(
                flops=2 * 8 * rows * 2 * depth * columns, bytes_accessed=6 * depth * columns, transcendentals=0),
        )(a_rows, b_rows)
        return out[0]

    return jax.shard_map(local_block, mesh=mesh, in_specs=(spec_rows, spec_rows), out_specs=spec_rows, check_vma=False)
```

```python
import jax
import jax.numpy as jnp
from jax import lax
from jax.experimental import pallas as pl
from jax.experimental.pallas import tpu as pltpu
from jax.sharding import PartitionSpec as P

MESH = pl.DeviceIdType.MESH
W = 128
C = 2 * W
LOOK = 4
D3 = 6
DO = 6
AX, AY, AZ = 0, 1, 2


def bits_of(d):
    return (d // 4, (d // 2) % 2, d % 2)


def counts(columns):
    paired = columns // C // 4
    return columns // C - 2 * paired, paired


def kernel(a_hbm, b_hbm, c_hbm, bx_hbm, bz_hbm, bxz_hbm, relay,
           a_v, b_v, p_v, r1_v, s2_v, r2_v, s3_v, r3_v, o_v, q_v,
           hop_send, hop_recv, own_sem, bx_send, bx_recv, bxz_send, bxz_recv, ch_send, ch_recv, b_sem,
           s1_sem, r1_sem, s2_sem, r2_sem, s3_sem, r3_sem, o_sem, ql_sem, qs_sem, qr_sem, credit):
    depth, columns = b_hbm.shape
    plain, paired = counts(columns)
    tiles = plain + paired
    half = depth // 2
    chunks = 16 + 2 * paired
    rate = max(120, -(-1800 // plain), -(-100 * (16 + 2 * paired) // (tiles - 1)))

    dp, tp = lax.axis_index("dp"), lax.axis_index("tp")
    core, x, y, z = dp % 2, (dp // 2) % 2, dp // 4, tp

    def flip(v, bit):
        return v + bit - 2 * v * bit

    def device(bits, other=0):
        return {"dp": flip(y, bits[1]) * 4 + flip(x, bits[0]) * 2 + flip(core, other), "tp": flip(z, bits[2])}

    axis_nbr = [device((1, 0, 0)), device((0, 1, 0)), device((0, 0, 1))]
    partner = device((0, 0, 0), 1)

    barrier = pltpu.get_barrier_semaphore()
    for nbr in (*axis_nbr, partner):
        pl.semaphore_signal(barrier, inc=1, device_id=nbr, device_id_type=MESH)

    def send(src, dst, send_sem, recv_sem, to):
        return pltpu.make_async_remote_copy(
            src_ref=src, dst_ref=dst, send_sem=send_sem, recv_sem=recv_sem, device_id=to, device_id_type=MESH)

    def when(t, low, high, fn):
        pl.when(jnp.logical_and(t >= low, t < high))(fn)

    def is_paired(t):
        return (t + tiles - plain) // tiles

    def tile_cols(t, g=None):
        col = t * C + is_paired(t) * ((t - plain) * C + z * C)
        if g is None:
            return pl.ds(pl.multiple_of(col, W), C)
        return pl.ds(pl.multiple_of(col + g * W, W), W)

    def their_cols(q):
        return pl.ds(pl.multiple_of((plain + 2 * q + 1 - z) * C, W), C)

    def a_cols(bits, h):
        to = device(bits, h)
        return a_hbm.at[:, pl.ds(pl.multiple_of((to["dp"] * 2 + to["tp"]) * depth, depth), depth)]

    def near(d, h):
        return a_v.at[d, :, pl.ds(h * depth, depth)]

    def far(d, h):
        return a_v.at[d, :, pl.ds((2 + h) * depth, depth)]

    def held(i, h):
        return relay.at[i, :, pl.ds(h * depth, depth)]

    def hop(n, h, src, dst, axis):
        return send(src, dst, hop_send.at[n, h], hop_recv.at[n, h], axis_nbr[axis])

    both = range(2)
    x_far = [hop(0, h, a_cols((1, 0, 1), h), far(4, h), AX) for h in both]
    y_far = [hop(1, h, a_cols((0, 1, 1), h), far(2, h), AY) for h in both]
    z_own = [hop(2, h, a_cols((0, 0, 1), h), near(1, h), AZ) for h in both]
    xy_far1 = [hop(3, h, a_cols((1, 1, 1), h), held(0, h), AX) for h in both]
    yx_near1 = [hop(4, h, a_cols((1, 1, 0), h), held(1, h), AY) for h in both]
    z_x = [hop(5, h, far(4, h), near(5, h), AZ) for h in both]
    z_y = [hop(6, h, far(2, h), near(3, h), AZ) for h in both]
    yx_near2 = [hop(7, h, held(1, h), near(6, h), AX) for h in both]
    xy_far2 = [hop(8, h, held(0, h), far(6, h), AY) for h in both]
    x_near = [hop(9, h, a_cols((1, 0, 0), h), near(4, h), AX) for h in both]
    y_near = [hop(10, h, a_cols((0, 1, 0), h), near(2, h), AY) for h in both]
    z_xy = [hop(11, h, far(6, h), near(7, h), AZ) for h in both]
    all_hops = (x_far, y_far, z_own, xy_far1, yx_near1, z_x, z_y, yx_near2, xy_far2, x_near, y_near, z_xy)
    own = [pltpu.make_async_copy(a_cols((0, 0, 0), h), near(0, h), own_sem.at[h]) for h in both]
    own += [pltpu.make_async_copy(a_cols((0, 0, 1), h), far(0, h), own_sem.at[2 + h]) for h in both]

    def a_chunk(n):
        d, k = (n // 4) * 2, n % 4
        return send(a_v.at[d, :, pl.ds(pl.multiple_of(k * half, half), half)],
                    a_v.at[d + 1, :, pl.ds(pl.multiple_of(2 * depth + k * half, half), half)],
                    ch_send.at[n], ch_recv.at[n], axis_nbr[AZ])

    def b_chunk(q, h):
        rows = pl.ds(pl.multiple_of(h * half, half), half)
        n = 16 + 2 * q + h
        return send(b_hbm.at[rows, their_cols(q)], bz_hbm.at[q, rows], ch_send.at[n], ch_recv.at[n], axis_nbr[AZ])

    def start_chunks(i):
        def body(n, carry):
            when(n, 0, 16, lambda: a_chunk(n).start())
            when(n, 16, chunks, lambda: b_chunk((n - 16) // 2, (n - 16) % 2).start())
            return carry

        lax.fori_loop(rate * i // 100, rate * (i + 1) // 100, body, 0)

    def bx_copy(t):
        return send(b_hbm.at[:, tile_cols(t)], bx_hbm.at[t], bx_send.at[t], bx_recv.at[t], partner)

    def bxz_copy(q):
        return send(bz_hbm.at[q], bxz_hbm.at[q], bxz_send.at[q], bxz_recv.at[q], partner)

    def b_piece(t, k):
        src = (b_hbm.at[:, tile_cols(t)], bx_hbm.at[t], bz_hbm.at[t - plain], bxz_hbm.at[t - plain])[k]
        return pltpu.make_async_copy(src, b_v.at[t % 2, pl.ds(k * depth, depth)], b_sem.at[t % 2, k])

    def fetch_near(t):
        b_piece(t, 0).start()
        bx_copy(t).wait_recv()
        b_piece(t, 1).start()

    def fetch_far(t):
        for h in both:
            b_chunk(t - plain, h).wait_recv()
        bxz_copy(t - plain).start()
        b_piece(t, 2).start()

    def fetch_last(t):
        bxz_copy(t - plain).wait_recv()
        b_piece(t, 3).start()

    def partial(t, d, k):
        s = t % 2
        dx, dy, dz = bits_of(d)
        part = jnp.dot(a_v[d, :, 0:k * depth], b_v[s, 0:k * depth], preferred_element_type=jnp.float32)
        p_v[s, 0, dx, dy * 2 + dz] = part[:, 0:W]
        p_v[s, 1, dy, dx * 2 + dz] = part[:, W:C]

    def partials(t, k, n=8, order=lambda j: j):
        def body(j, carry):
            partial(t, order(j), k)
            return carry

        lax.fori_loop(0, n, body, 0)

    def first_two(n, order):
        def body(j, carry):
            partial(j // n, order(j % n), 2)
            return carry

        lax.fori_loop(0, 2 * n, body, 0)

    def send1(t, g):
        s = t % 2
        return send(p_v.at[s, g, 1], r1_v.at[s, g], s1_sem.at[s, g], r1_sem.at[s, g], axis_nbr[g])

    def send2(t, g):
        s = t % 2
        return send(s2_v.at[s, g, pl.ds(2, 2)], r2_v.at[s, g], s2_sem.at[s, g], r2_sem.at[s, g], axis_nbr[1 - g])

    def send3(t, g):
        s = t % D3
        return send(s3_v.at[s, g, 1], r3_v.at[s, g], s3_sem.at[s, g], r3_sem.at[s, g], axis_nbr[AZ])

    def out_copy(t, g):
        return pltpu.make_async_copy(o_v.at[t % 2, g], c_hbm.at[:, tile_cols(t, g)], o_sem.at[t % 2, g])

    def pair_here(t, g):
        s = t % DO
        return pltpu.make_async_copy(q_v.at[s, g, 0], c_hbm.at[:, tile_cols(t, g)], ql_sem.at[s, g])

    def pair_there(t, g):
        s = t % DO
        return send(q_v.at[s, g, 1], c_hbm.at[:, tile_cols(t, g)], qs_sem.at[s, g], qr_sem.at[t - plain, g], axis_nbr[AZ])

    def take(t, g, phase, slots, high):
        when(t, slots, high, lambda: pl.semaphore_wait(credit.at[phase, g], 1))

    def give(t, g, phase, axis, slots, high):
        when(t, 0, high - slots, lambda: pl.semaphore_signal(
            credit.at[phase, g], inc=1, device_id=axis_nbr[axis], device_id_type=MESH))

    for copy in own:
        copy.start()
    pl.semaphore_wait(barrier, 4)
    bx_copy(0).start()
    bx_copy(1).start()
    for group in (x_far, y_far, z_own):
        for copy in group:
            copy.start()
    for group in (xy_far1, yx_near1):
        for copy in group:
            copy.start()
    for t in range(2, min(LOOK, tiles)):
        bx_copy(t).start()
    for t in range(2):
        fetch_near(t)
    for h in both:
        x_far[h].wait_recv()
        z_x[h].start()
    for h in both:
        y_far[h].wait_recv()
        z_y[h].start()
    for h in both:
        yx_near1[h].wait_recv()
        yx_near2[h].start()
        xy_far1[h].wait_recv()
        xy_far2[h].start()
    for copy in x_near + y_near:
        copy.start()
    for t in range(2):
        for k in range(2):
            b_piece(t, k).wait()
    for copy in own:
        copy.wait()
    for copy in z_own + z_x:
        copy.wait_recv()
    first_two(3, lambda j: (3 * j * j - j) // 2)
    for h in both:
        xy_far2[h].wait_recv()
        z_xy[h].start()
    for copy in z_y + yx_near2:
        copy.wait_recv()
    first_two(2, lambda j: 3 + 3 * j)
    for copy in x_near + y_near + z_xy:
        copy.wait_recv()

    def last_three(j):
        return 2 + 2 * j + j // 2

    def step(i, carry):
        t = i
        when(t, 0, tiles, lambda: start_chunks(t))
        when(t, 0, tiles - LOOK, lambda: bx_copy(t + LOOK).start())
        when(t, 1, tiles - 1, lambda: fetch_near(t + 1))
        for g in both:
            when(t, 2, tiles + 2, lambda g=g: send1(t - 2, g).wait_send())

        def wait_b(pieces):
            for k in range(pieces):
                b_piece(t, k).wait()

        def near_products():
            wait_b(2)
            partials(t, 2)

        def all_products():
            wait_b(4)
            partials(t, 4)

        def wait_far():
            def body(n, carry):
                a_chunk(n).wait_recv()
                return carry

            lax.fori_loop(0, 16, body, 0)

        when(t, 0, 2, lambda: partials(t, 2, 3, last_three))
        when(t, 2, plain, near_products)
        when(t, plain, plain + 1, wait_far)
        when(t, plain, tiles, all_products)
        for g in both:
            take(t, g, 0, 2, tiles)
            when(t, 0, tiles, lambda g=g: send1(t, g).start())
        when(t, plain - 1, tiles - 1, lambda: fetch_far(t + 1))

        t1 = i - 1
        for g in both:
            when(t1, 2, tiles + 2, lambda g=g: send2(t1 - 2, g).wait_send())

            def add1(g=g):
                s = t1 % 2
                send1(t1, g).wait_recv()
                s2_v[s, g] = p_v[s, g, 0] + r1_v[s, g]

            when(t1, 0, tiles, add1)
            give(t1, g, 0, g, 2, tiles)
            take(t1, g, 1, 2, tiles)
            when(t1, 0, tiles, lambda g=g: send2(t1, g).start())

        t2 = i - 2
        for g in both:
            when(t2, D3, plain + D3, lambda g=g: send3(t2 - D3, g).wait_send())

            def add2(g=g):
                send2(t2, g).wait_recv()
                s3_v[t2 % D3, g] = s2_v[t2 % 2, g, 0:2] + r2_v[t2 % 2, g]

            def add2_paired(g=g):
                send2(t2, g).wait_recv()
                q_v[t2 % DO, g] = (s2_v[t2 % 2, g, 0:2] + r2_v[t2 % 2, g]).astype(jnp.bfloat16)

            def free_pair(g=g):
                pair_here(t2 - DO, g).wait()
                pair_there(t2 - DO, g).wait_send()

            def start_pair(g=g):
                pair_here(t2, g).start()
                pair_there(t2, g).start()

            when(t2, 0, plain, add2)
            when(t2, plain + DO, tiles, free_pair)
            when(t2, plain, tiles, add2_paired)
            give(t2, g, 1, 1 - g, 2, tiles)
            take(t2, g, 2, D3, plain)
            when(t2, 0, plain, lambda g=g: send3(t2, g).start())
            when(t2, plain, tiles, start_pair)

        t3 = i - 1 - D3
        for g in both:
            when(t3, 2, plain + 2, lambda g=g: out_copy(t3 - 2, g).wait())

            def add3(g=g):
                send3(t3, g).wait_recv()
                o_v[t3 % 2, g] = (s3_v[t3 % D3, g, 0] + r3_v[t3 % D3, g]).astype(jnp.bfloat16)
                out_copy(t3, g).start()

            when(t3, 0, plain, add3)
            give(t3, g, 2, AZ, D3, plain)
        when(t, plain - 1, tiles - 1, lambda: fetch_last(t + 1))
        return carry

    lax.fori_loop(0, max(tiles + 3, plain + D3 + 3), step, 0)

    for group in all_hops:
        for copy in group:
            copy.wait_send()

    def each(low, high, fn):
        def body(n, carry):
            fn(n)
            return carry

        lax.fori_loop(low, high, body, 0)

    each(0, tiles, lambda t: bx_copy(t).wait_send())
    each(0, paired, lambda q: bxz_copy(q).wait_send())
    each(0, 16, lambda n: a_chunk(n).wait_send())
    each(0, 2 * paired, lambda n: b_chunk(n // 2, n % 2).wait_send())
    for g in both:
        each(max(plain, tiles - DO), tiles, lambda t: pair_here(t, g).wait())
        each(max(plain, tiles - DO), tiles, lambda t: pair_there(t, g).wait_send())
        each(plain, tiles, lambda t: pair_there(t, g).wait_recv())


def solution(mesh):
    spec_rows = P(("dp", "tp"), None)

    def local_block(a_rows, b_rows):
        rows, inner = a_rows.shape
        depth, columns = b_rows.shape
        plain, paired = counts(columns)
        tiles = plain + paired
        f32, bf16 = jnp.float32, jnp.bfloat16
        dma = pltpu.SemaphoreType.DMA
        out = pl.pallas_call(
            kernel,
            name="matmul_reduce_scatter",
            out_shape=(
                jax.ShapeDtypeStruct((rows, columns), bf16),
                jax.ShapeDtypeStruct((tiles, depth, C), bf16),
                jax.ShapeDtypeStruct((paired, depth, C), bf16),
                jax.ShapeDtypeStruct((paired, depth, C), bf16),
                jax.ShapeDtypeStruct((2, rows, 2 * depth), bf16),
            ),
            in_specs=[pl.BlockSpec(memory_space=pl.ANY)] * 2,
            out_specs=(pl.BlockSpec(memory_space=pl.ANY),) * 5,
            scratch_shapes=[
                pltpu.VMEM((8, rows, 4 * depth), bf16),
                pltpu.VMEM((2, 4 * depth, C), bf16),
                pltpu.VMEM((2, 2, 2, 4, rows, W), f32),
                pltpu.VMEM((2, 2, 4, rows, W), f32),
                pltpu.VMEM((2, 2, 4, rows, W), f32),
                pltpu.VMEM((2, 2, 2, rows, W), f32),
                pltpu.VMEM((D3, 2, 2, rows, W), f32),
                pltpu.VMEM((D3, 2, rows, W), f32),
                pltpu.VMEM((2, 2, rows, W), bf16),
                pltpu.VMEM((DO, 2, 2, rows, W), bf16),
                dma((12, 2)), dma((12, 2)), dma((4,)),
                dma((tiles,)), dma((tiles,)), dma((paired,)), dma((paired,)),
                dma((16 + 2 * paired,)), dma((16 + 2 * paired,)), dma((2, 4)),
                dma((2, 2)), dma((2, 2)), dma((2, 2)), dma((2, 2)), dma((D3, 2)), dma((D3, 2)),
                dma((2, 2)), dma((DO, 2)), dma((DO, 2)), dma((paired, 2)),
                pltpu.SemaphoreType.REGULAR((3, 2)),
            ],
            compiler_params=pltpu.CompilerParams(
                collective_id=0, has_side_effects=True, vmem_limit_bytes=63 * 1024 * 1024),
            cost_estimate=pl.CostEstimate(
                flops=2 * 8 * rows * 2 * depth * columns, bytes_accessed=6 * depth * columns, transcendentals=0),
        )(a_rows, b_rows)
        return out[0]

    return jax.shard_map(local_block, mesh=mesh, in_specs=(spec_rows, spec_rows), out_specs=spec_rows, check_vma=False)
```

```python
import jax
import jax.numpy as jnp
from jax import lax
from jax.experimental import pallas as pl
from jax.experimental.pallas import tpu as pltpu
from jax.sharding import PartitionSpec as P

MESH = pl.DeviceIdType.MESH
W = 128
C = 2 * W
LOOK = 4
D3 = 6
DO = 6
AX, AY, AZ = 0, 1, 2


def bits_of(d):
    return (d // 4, (d // 2) % 2, d % 2)


def counts(columns):
    paired = columns // C // 4
    return columns // C - 2 * paired, paired


def kernel(a_hbm, b_hbm, c_v, bx_hbm, bz_hbm, bxz_hbm, relay,
           a_v, b_v, p_v, r1_v, s2_v, r2_v, s3_v, r3_v, q_v,
           hop_send, hop_recv, own_sem, bx_send, bx_recv, bxz_send, bxz_recv, ch_send, ch_recv, b_sem,
           s1_sem, r1_sem, s2_sem, r2_sem, s3_sem, r3_sem, qs_sem, qr_sem, credit):
    depth, columns = b_hbm.shape
    plain, paired = counts(columns)
    tiles = plain + paired
    half = depth // 2
    chunks = 16 + 2 * paired
    rate = max(120, -(-1800 // plain), -(-100 * (16 + 2 * paired) // (tiles - 1)))

    dp, tp = lax.axis_index("dp"), lax.axis_index("tp")
    core, x, y, z = dp % 2, (dp // 2) % 2, dp // 4, tp

    def flip(v, bit):
        return v + bit - 2 * v * bit

    def device(bits, other=0):
        return {"dp": flip(y, bits[1]) * 4 + flip(x, bits[0]) * 2 + flip(core, other), "tp": flip(z, bits[2])}

    axis_nbr = [device((1, 0, 0)), device((0, 1, 0)), device((0, 0, 1))]
    partner = device((0, 0, 0), 1)

    barrier = pltpu.get_barrier_semaphore()
    for nbr in (*axis_nbr, partner):
        pl.semaphore_signal(barrier, inc=1, device_id=nbr, device_id_type=MESH)

    def send(src, dst, send_sem, recv_sem, to):
        return pltpu.make_async_remote_copy(
            src_ref=src, dst_ref=dst, send_sem=send_sem, recv_sem=recv_sem, device_id=to, device_id_type=MESH)

    def when(t, low, high, fn):
        pl.when(jnp.logical_and(t >= low, t < high))(fn)

    def is_paired(t):
        return (t + tiles - plain) // tiles

    def tile_cols(t, g=None):
        col = t * C + is_paired(t) * ((t - plain) * C + z * C)
        if g is None:
            return pl.ds(pl.multiple_of(col, W), C)
        return pl.ds(pl.multiple_of(col + g * W, W), W)

    def their_cols(q):
        return pl.ds(pl.multiple_of((plain + 2 * q + 1 - z) * C, W), C)

    def a_cols(bits, h):
        to = device(bits, h)
        return a_hbm.at[:, pl.ds(pl.multiple_of((to["dp"] * 2 + to["tp"]) * depth, depth), depth)]

    def near(d, h):
        return a_v.at[d, :, pl.ds(h * depth, depth)]

    def far(d, h):
        return a_v.at[d, :, pl.ds((2 + h) * depth, depth)]

    def held(i, h):
        return relay.at[i, :, pl.ds(h * depth, depth)]

    def hop(n, h, src, dst, axis):
        return send(src, dst, hop_send.at[n, h], hop_recv.at[n, h], axis_nbr[axis])

    both = range(2)
    x_far = [hop(0, h, a_cols((1, 0, 1), h), far(4, h), AX) for h in both]
    y_far = [hop(1, h, a_cols((0, 1, 1), h), far(2, h), AY) for h in both]
    z_own = [hop(2, h, a_cols((0, 0, 1), h), near(1, h), AZ) for h in both]
    xy_far1 = [hop(3, h, a_cols((1, 1, 1), h), held(0, h), AX) for h in both]
    yx_near1 = [hop(4, h, a_cols((1, 1, 0), h), held(1, h), AY) for h in both]
    z_x = [hop(5, h, far(4, h), near(5, h), AZ) for h in both]
    z_y = [hop(6, h, far(2, h), near(3, h), AZ) for h in both]
    yx_near2 = [hop(7, h, held(1, h), near(6, h), AX) for h in both]
    xy_far2 = [hop(8, h, held(0, h), far(6, h), AY) for h in both]
    x_near = [hop(9, h, a_cols((1, 0, 0), h), near(4, h), AX) for h in both]
    y_near = [hop(10, h, a_cols((0, 1, 0), h), near(2, h), AY) for h in both]
    z_xy = [hop(11, h, far(6, h), near(7, h), AZ) for h in both]
    all_hops = (x_far, y_far, z_own, xy_far1, yx_near1, z_x, z_y, yx_near2, xy_far2, x_near, y_near, z_xy)
    own = [pltpu.make_async_copy(a_cols((0, 0, 0), h), near(0, h), own_sem.at[h]) for h in both]
    own += [pltpu.make_async_copy(a_cols((0, 0, 1), h), far(0, h), own_sem.at[2 + h]) for h in both]

    def a_chunk(n):
        d, k = (n // 4) * 2, n % 4
        return send(a_v.at[d, :, pl.ds(pl.multiple_of(k * half, half), half)],
                    a_v.at[d + 1, :, pl.ds(pl.multiple_of(2 * depth + k * half, half), half)],
                    ch_send.at[n], ch_recv.at[n], axis_nbr[AZ])

    def b_chunk(q, h):
        rows = pl.ds(pl.multiple_of(h * half, half), half)
        n = 16 + 2 * q + h
        return send(b_hbm.at[rows, their_cols(q)], bz_hbm.at[q, rows], ch_send.at[n], ch_recv.at[n], axis_nbr[AZ])

    def start_chunks(i):
        def body(n, carry):
            when(n, 0, 16, lambda: a_chunk(n).start())
            when(n, 16, chunks, lambda: b_chunk((n - 16) // 2, (n - 16) % 2).start())
            return carry

        lax.fori_loop(rate * i // 100, rate * (i + 1) // 100, body, 0)

    def bx_copy(t):
        return send(b_hbm.at[:, tile_cols(t)], bx_hbm.at[t], bx_send.at[t], bx_recv.at[t], partner)

    def bxz_copy(q):
        return send(bz_hbm.at[q], bxz_hbm.at[q], bxz_send.at[q], bxz_recv.at[q], partner)

    def b_piece(t, k):
        src = (b_hbm.at[:, tile_cols(t)], bx_hbm.at[t], bz_hbm.at[t - plain], bxz_hbm.at[t - plain])[k]
        return pltpu.make_async_copy(src, b_v.at[t % 2, pl.ds(k * depth, depth)], b_sem.at[t % 2, k])

    def fetch_near(t):
        b_piece(t, 0).start()
        bx_copy(t).wait_recv()
        b_piece(t, 1).start()

    def fetch_far(t):
        with jax.named_scope("b_chunk"):
            for h in both:
                b_chunk(t - plain, h).wait_recv()
        bxz_copy(t - plain).start()
        b_piece(t, 2).start()

    def fetch_last(t):
        with jax.named_scope("bxz"):
            bxz_copy(t - plain).wait_recv()
        b_piece(t, 3).start()

    def partial(t, d, k):
        s = t % 2
        dx, dy, dz = bits_of(d)
        part = jnp.dot(a_v[d, :, 0:k * depth], b_v[s, 0:k * depth], preferred_element_type=jnp.float32)
        p_v[s, 0, dx, dy * 2 + dz] = part[:, 0:W]
        p_v[s, 1, dy, dx * 2 + dz] = part[:, W:C]

    def partials(t, k, n=8, order=lambda j: j):
        def body(j, carry):
            partial(t, order(j), k)
            return carry

        lax.fori_loop(0, n, body, 0)

    def first_two(n, order):
        def body(j, carry):
            partial(j // n, order(j % n), 2)
            return carry

        lax.fori_loop(0, 2 * n, body, 0)

    def send1(t, g):
        s = t % 2
        return send(p_v.at[s, g, 1], r1_v.at[s, g], s1_sem.at[s, g], r1_sem.at[s, g], axis_nbr[g])

    def send2(t, g):
        s = t % 2
        return send(s2_v.at[s, g, pl.ds(2, 2)], r2_v.at[s, g], s2_sem.at[s, g], r2_sem.at[s, g], axis_nbr[1 - g])

    def send3(t, g):
        s = t % D3
        return send(s3_v.at[s, g, 1], r3_v.at[s, g], s3_sem.at[s, g], r3_sem.at[s, g], axis_nbr[AZ])

    def pair_there(t, g):
        s = t % DO
        return send(q_v.at[s, g], c_v.at[:, tile_cols(t, g)], qs_sem.at[s, g], qr_sem.at[t - plain, g], axis_nbr[AZ])

    def take(t, g, phase, slots, high):
        when(t, slots, high, lambda: pl.semaphore_wait(credit.at[phase, g], 1))

    def give(t, g, phase, axis, slots, high):
        when(t, 0, high - slots, lambda: pl.semaphore_signal(
            credit.at[phase, g], inc=1, device_id=axis_nbr[axis], device_id_type=MESH))

    for copy in own:
        copy.start()
    with jax.named_scope("barrier"):
        pl.semaphore_wait(barrier, 4)
    bx_copy(0).start()
    bx_copy(1).start()
    for group in (x_far, y_far, z_own):
        for copy in group:
            copy.start()
    for group in (xy_far1, yx_near1):
        for copy in group:
            copy.start()
    for t in range(2, min(LOOK, tiles)):
        bx_copy(t).start()
    for t in range(2):
        fetch_near(t)
    for h in both:
        with jax.named_scope("x_far"):
            x_far[h].wait_recv()
        z_x[h].start()
    for h in both:
        y_far[h].wait_recv()
        z_y[h].start()
    for h in both:
        with jax.named_scope("yx_near1"):
            yx_near1[h].wait_recv()
        yx_near2[h].start()
        xy_far1[h].wait_recv()
        xy_far2[h].start()
    for copy in x_near + y_near:
        copy.start()
    for t in range(2):
        for k in range(2):
            b_piece(t, k).wait()
    for copy in own:
        copy.wait()
    with jax.named_scope("z_x"):
        for copy in z_own + z_x:
            copy.wait_recv()
    first_two(3, lambda j: (3 * j * j - j) // 2)
    for h in both:
        with jax.named_scope("xy_far2"):
            xy_far2[h].wait_recv()
        z_xy[h].start()
    with jax.named_scope("z_y"):
        for copy in z_y + yx_near2:
            copy.wait_recv()
    first_two(2, lambda j: 3 + 3 * j)
    with jax.named_scope("x_near"):
        for copy in x_near + y_near:
            copy.wait_recv()
    with jax.named_scope("z_xy"):
        for copy in z_xy:
            copy.wait_recv()

    def last_three(j):
        return 2 + 2 * j + j // 2

    def step(i, carry):
        t = i
        when(t, 0, tiles, lambda: start_chunks(t))
        when(t, 0, tiles - LOOK, lambda: bx_copy(t + LOOK).start())
        when(t, 1, tiles - 1, lambda: fetch_near(t + 1))
        for g in both:
            when(t, 2, tiles + 2, lambda g=g: send1(t - 2, g).wait_send())

        def wait_b(pieces):
            for k in range(pieces):
                b_piece(t, k).wait()

        def near_products():
            with jax.named_scope("b_near"):
                wait_b(2)
            with jax.named_scope("dot_near"):
                partials(t, 2)

        def all_products():
            with jax.named_scope("b_all"):
                wait_b(4)
            with jax.named_scope("dot_all"):
                partials(t, 4)

        def wait_far():
            def body(n, carry):
                a_chunk(n).wait_recv()
                return carry

            with jax.named_scope("a_chunks"):
                lax.fori_loop(0, 16, body, 0)

        when(t, 0, 2, lambda: partials(t, 2, 3, last_three))
        when(t, 2, plain, near_products)
        when(t, plain, plain + 1, wait_far)
        when(t, plain, tiles, all_products)
        for g in both:
            take(t, g, 0, 2, tiles)
            when(t, 0, tiles, lambda g=g: send1(t, g).start())
        when(t, plain - 1, tiles - 1, lambda: fetch_far(t + 1))

        t1 = i - 1
        for g in both:
            when(t1, 2, tiles + 2, lambda g=g: send2(t1 - 2, g).wait_send())

            def add1(g=g):
                s = t1 % 2
                with jax.named_scope("recv1"):
                    send1(t1, g).wait_recv()
                s2_v[s, g] = p_v[s, g, 0] + r1_v[s, g]

            when(t1, 0, tiles, add1)
            give(t1, g, 0, g, 2, tiles)
            take(t1, g, 1, 2, tiles)
            when(t1, 0, tiles, lambda g=g: send2(t1, g).start())

        t2 = i - 2
        for g in both:
            when(t2, D3, plain + D3, lambda g=g: send3(t2 - D3, g).wait_send())

            def add2(g=g):
                with jax.named_scope("recv2"):
                    send2(t2, g).wait_recv()
                s3_v[t2 % D3, g] = s2_v[t2 % 2, g, 0:2] + r2_v[t2 % 2, g]

            def add2_paired(g=g):
                with jax.named_scope("recv2"):
                    send2(t2, g).wait_recv()
                both_sides = (s2_v[t2 % 2, g, 0:2] + r2_v[t2 % 2, g]).astype(jnp.bfloat16)
                q_v[t2 % DO, g] = both_sides[1]
                c_v[:, tile_cols(t2, g)] = both_sides[0]

            when(t2, 0, plain, add2)
            when(t2, plain + DO, tiles, lambda g=g: pair_there(t2 - DO, g).wait_send())
            when(t2, plain, tiles, add2_paired)
            give(t2, g, 1, 1 - g, 2, tiles)
            take(t2, g, 2, D3, plain)
            when(t2, 0, plain, lambda g=g: send3(t2, g).start())
            when(t2, plain, tiles, lambda g=g: pair_there(t2, g).start())

        t3 = i - 1 - D3
        for g in both:

            def add3(g=g):
                with jax.named_scope("recv3"):
                    send3(t3, g).wait_recv()
                c_v[:, tile_cols(t3, g)] = (s3_v[t3 % D3, g, 0] + r3_v[t3 % D3, g]).astype(jnp.bfloat16)

            when(t3, 0, plain, add3)
            give(t3, g, 2, AZ, D3, plain)
        when(t, plain - 1, tiles - 1, lambda: fetch_last(t + 1))
        return carry

    lax.fori_loop(0, max(tiles + 3, plain + D3 + 1), step, 0)

    for group in all_hops:
        for copy in group:
            copy.wait_send()

    def each(low, high, fn):
        def body(n, carry):
            fn(n)
            return carry

        lax.fori_loop(low, high, body, 0)

    each(0, tiles, lambda t: bx_copy(t).wait_send())
    each(0, paired, lambda q: bxz_copy(q).wait_send())
    each(0, 16, lambda n: a_chunk(n).wait_send())
    each(0, 2 * paired, lambda n: b_chunk(n // 2, n % 2).wait_send())
    for g in both:
        each(max(plain, tiles - DO), tiles, lambda t: pair_there(t, g).wait_send())
        each(plain, tiles, lambda t: pair_there(t, g).wait_recv())


def solution(mesh):
    spec_rows = P(("dp", "tp"), None)

    def local_block(a_rows, b_rows):
        rows, inner = a_rows.shape
        depth, columns = b_rows.shape
        plain, paired = counts(columns)
        tiles = plain + paired
        f32, bf16 = jnp.float32, jnp.bfloat16
        dma = pltpu.SemaphoreType.DMA
        out = pl.pallas_call(
            kernel,
            name="matmul_reduce_scatter",
            out_shape=(
                pltpu.VMEM((rows, columns), bf16),
                jax.ShapeDtypeStruct((tiles, depth, C), bf16),
                jax.ShapeDtypeStruct((paired, depth, C), bf16),
                jax.ShapeDtypeStruct((paired, depth, C), bf16),
                jax.ShapeDtypeStruct((2, rows, 2 * depth), bf16),
            ),
            in_specs=[pl.BlockSpec(memory_space=pl.ANY)] * 2,
            out_specs=(pl.BlockSpec(memory_space=pltpu.VMEM),) + (pl.BlockSpec(memory_space=pl.ANY),) * 4,
            scratch_shapes=[
                pltpu.VMEM((8, rows, 4 * depth), bf16),
                pltpu.VMEM((2, 4 * depth, C), bf16),
                pltpu.VMEM((2, 2, 2, 4, rows, W), f32),
                pltpu.VMEM((2, 2, 4, rows, W), f32),
                pltpu.VMEM((2, 2, 4, rows, W), f32),
                pltpu.VMEM((2, 2, 2, rows, W), f32),
                pltpu.VMEM((D3, 2, 2, rows, W), f32),
                pltpu.VMEM((D3, 2, rows, W), f32),
                pltpu.VMEM((DO, 2, rows, W), bf16),
                dma((12, 2)), dma((12, 2)), dma((4,)),
                dma((tiles,)), dma((tiles,)), dma((paired,)), dma((paired,)),
                dma((16 + 2 * paired,)), dma((16 + 2 * paired,)), dma((2, 4)),
                dma((2, 2)), dma((2, 2)), dma((2, 2)), dma((2, 2)), dma((D3, 2)), dma((D3, 2)),
                dma((DO, 2)), dma((paired, 2)),
                pltpu.SemaphoreType.REGULAR((3, 2)),
            ],
            compiler_params=pltpu.CompilerParams(
                collective_id=0, has_side_effects=True, vmem_limit_bytes=56 * 1024 * 1024),
            cost_estimate=pl.CostEstimate(
                flops=2 * 8 * rows * 2 * depth * columns, bytes_accessed=6 * depth * columns, transcendentals=0),
        )(a_rows, b_rows)
        return out[0]

    return jax.shard_map(local_block, mesh=mesh, in_specs=(spec_rows, spec_rows), out_specs=spec_rows, check_vma=False)
```

```python
import jax
import jax.numpy as jnp
from jax import lax
from jax.experimental import pallas as pl
from jax.experimental.pallas import tpu as pltpu
from jax.sharding import PartitionSpec as P

MESH = pl.DeviceIdType.MESH
W = 128
C = 2 * W
LOOK = 4
D3 = 6
DO = 6
LATE = 5
AHEAD = 2
AX, AY, AZ = 0, 1, 2


def bits_of(d):
    return (d // 4, (d // 2) % 2, d % 2)


def counts(columns):
    paired = columns // C * 27 // 100
    return columns // C - 2 * paired, paired


def kernel(a_hbm, b_hbm, c_v, bx_hbm, bz_hbm, bxz_hbm, relay,
           a_v, b_v, p_v, r1_v, s2_v, r2_v, s3_v, r3_v, q_v,
           hop_send, hop_recv, own_sem, bx_send, bx_recv, bxz_send, bxz_recv, ch_send, ch_recv, b_sem,
           s1_sem, r1_sem, s2_sem, r2_sem, s3_sem, r3_sem, qs_sem, qr_sem, credit):
    depth, columns = b_hbm.shape
    plain, paired = counts(columns)
    tiles = plain + paired
    half = depth // 2
    chunks = 16 + 2 * paired
    rate = max(116, -(-1600 // plain), -(-100 * (14 + 2 * paired) // (tiles - 2)))

    dp, tp = lax.axis_index("dp"), lax.axis_index("tp")
    core, x, y, z = dp % 2, (dp // 2) % 2, dp // 4, tp

    def flip(v, bit):
        return v + bit - 2 * v * bit

    def device(bits, other=0):
        return {"dp": flip(y, bits[1]) * 4 + flip(x, bits[0]) * 2 + flip(core, other), "tp": flip(z, bits[2])}

    axis_nbr = [device((1, 0, 0)), device((0, 1, 0)), device((0, 0, 1))]
    partner = device((0, 0, 0), 1)

    barrier = pltpu.get_barrier_semaphore()
    for nbr in (*axis_nbr, partner):
        pl.semaphore_signal(barrier, inc=1, device_id=nbr, device_id_type=MESH)

    def send(src, dst, send_sem, recv_sem, to):
        return pltpu.make_async_remote_copy(
            src_ref=src, dst_ref=dst, send_sem=send_sem, recv_sem=recv_sem, device_id=to, device_id_type=MESH)

    def when(t, low, high, fn):
        pl.when(jnp.logical_and(t >= low, t < high))(fn)

    def is_paired(t):
        return (t + tiles - plain) // tiles

    def tile_cols(t, g=None):
        col = t * C + is_paired(t) * ((t - plain) * C + z * C)
        if g is None:
            return pl.ds(pl.multiple_of(col, W), C)
        return pl.ds(pl.multiple_of(col + g * W, W), W)

    def their_cols(q):
        return pl.ds(pl.multiple_of((plain + 2 * q + 1 - z) * C, W), C)

    def a_cols(bits, h):
        to = device(bits, h)
        return a_hbm.at[:, pl.ds(pl.multiple_of((to["dp"] * 2 + to["tp"]) * depth, depth), depth)]

    def near(d, h):
        return a_v.at[d, :, pl.ds(h * depth, depth)]

    def far(d, h):
        return a_v.at[d, :, pl.ds((2 + h) * depth, depth)]

    def held(i, h):
        return relay.at[i, :, pl.ds(h * depth, depth)]

    def hop(n, h, src, dst, axis):
        return send(src, dst, hop_send.at[n, h], hop_recv.at[n, h], axis_nbr[axis])

    both = range(2)
    xy_far1 = [hop(0, h, a_cols((1, 1, 1), h), held(0, h), AX) for h in both]
    xy_near1 = [hop(1, h, a_cols((1, 1, 0), h), held(1, h), AX) for h in both]
    x_far = [hop(2, h, a_cols((1, 0, 1), h), far(4, h), AX) for h in both]
    x_near = [hop(3, h, a_cols((1, 0, 0), h), near(4, h), AX) for h in both]
    y_far = [hop(4, h, a_cols((0, 1, 1), h), far(2, h), AY) for h in both]
    xy_far2 = [hop(5, h, held(0, h), far(6, h), AY) for h in both]
    xy_near2 = [hop(6, h, held(1, h), near(6, h), AY) for h in both]
    y_near = [hop(7, h, a_cols((0, 1, 0), h), near(2, h), AY) for h in both]
    z_own = [hop(8, h, a_cols((0, 0, 1), h), near(1, h), AZ) for h in both]
    z_y = [hop(9, h, far(2, h), near(3, h), AZ) for h in both]
    z_xy = [hop(10, h, far(6, h), near(7, h), AZ) for h in both]
    z_x = [hop(11, h, far(4, h), near(5, h), AZ) for h in both]
    all_hops = (xy_far1, xy_near1, x_far, x_near, y_far, xy_far2, xy_near2, y_near, z_own, z_y, z_xy, z_x)
    own = [pltpu.make_async_copy(a_cols((0, 0, 0), h), near(0, h), own_sem.at[h]) for h in both]
    own += [pltpu.make_async_copy(a_cols((0, 0, 1), h), far(0, h), own_sem.at[2 + h]) for h in both]

    def a_chunk(n):
        d, k = (n // 4) * 2, n % 4
        return send(a_v.at[d, :, pl.ds(pl.multiple_of(k * half, half), half)],
                    a_v.at[d + 1, :, pl.ds(pl.multiple_of(2 * depth + k * half, half), half)],
                    ch_send.at[n], ch_recv.at[n], axis_nbr[AZ])

    def b_chunk(q, h):
        rows = pl.ds(pl.multiple_of(h * half, half), half)
        n = 16 + 2 * q + h
        return send(b_hbm.at[rows, their_cols(q)], bz_hbm.at[q, rows], ch_send.at[n], ch_recv.at[n], axis_nbr[AZ])

    def start_chunks(i):
        def body(n, carry):
            when(n, 0, 16, lambda: a_chunk(n).start())
            when(n, 16, chunks, lambda: b_chunk((n - 16) // 2, (n - 16) % 2).start())
            return carry

        lax.fori_loop(rate * i // 100 + AHEAD, rate * (i + 1) // 100 + AHEAD, body, 0)

    def bx_copy(t):
        return send(b_hbm.at[:, tile_cols(t)], bx_hbm.at[t], bx_send.at[t], bx_recv.at[t], partner)

    def bxz_copy(q):
        return send(bz_hbm.at[q], bxz_hbm.at[q], bxz_send.at[q], bxz_recv.at[q], partner)

    def b_piece(t, k):
        src = (b_hbm.at[:, tile_cols(t)], bx_hbm.at[t], bz_hbm.at[t - plain], bxz_hbm.at[t - plain])[k]
        return pltpu.make_async_copy(src, b_v.at[t % 2, pl.ds(k * depth, depth)], b_sem.at[t % 2, k])

    def fetch_near(t):
        b_piece(t, 0).start()
        bx_copy(t).wait_recv()
        b_piece(t, 1).start()

    def fetch_far(t):
        with jax.named_scope("b_chunk"):
            for h in both:
                b_chunk(t - plain, h).wait_recv()
        bxz_copy(t - plain).start()
        b_piece(t, 2).start()

    def fetch_last(t):
        with jax.named_scope("bxz"):
            bxz_copy(t - plain).wait_recv()
        b_piece(t, 3).start()

    def partial(t, d, k):
        s = t % 2
        dx, dy, dz = bits_of(d)
        part = jnp.dot(a_v[d, :, 0:k * depth], b_v[s, 0:k * depth], preferred_element_type=jnp.float32)
        p_v[s, 0, dx, dy * 2 + dz] = part[:, 0:W]
        p_v[s, 1, dy, dx * 2 + dz] = part[:, W:C]

    def partials(t, k, n=8, order=lambda j: j):
        def body(j, carry):
            partial(t, order(j), k)
            return carry

        lax.fori_loop(0, n, body, 0)

    def first_two(n, order):
        def body(j, carry):
            partial(j // n, order(j % n), 2)
            return carry

        lax.fori_loop(0, 2 * n, body, 0)

    def send1(t, g, k):
        s, blocks = t % 2, pl.ds(2 * k, 2)
        return send(p_v.at[s, g, 1, blocks], r1_v.at[s, g, blocks], s1_sem.at[s, g, k], r1_sem.at[s, g, k], axis_nbr[g])

    def send2(t, g, k):
        s = t % 2
        return send(s2_v.at[s, g, 2 + k], r2_v.at[s, g, k], s2_sem.at[s, g, k], r2_sem.at[s, g, k], axis_nbr[1 - g])

    def send3(t, g):
        s = t % D3
        return send(s3_v.at[s, g, 1], r3_v.at[s, g], s3_sem.at[s, g], r3_sem.at[s, g], axis_nbr[AZ])

    def pair_there(t, g):
        s = t % DO
        return send(q_v.at[s, g], c_v.at[:, tile_cols(t, g)], qs_sem.at[s, g], qr_sem.at[t - plain, g], axis_nbr[AZ])

    def take(t, g, phase, slots, high):
        when(t, slots, high, lambda: pl.semaphore_wait(credit.at[phase, g], 1))

    def give(t, g, phase, axis, slots, high):
        when(t, 0, high - slots, lambda: pl.semaphore_signal(
            credit.at[phase, g], inc=1, device_id=axis_nbr[axis], device_id_type=MESH))

    for copy in own:
        copy.start()
    with jax.named_scope("barrier"):
        pl.semaphore_wait(barrier, 4)
    for group in (xy_far1, y_far, z_own, xy_near1, x_far, x_near):
        for copy in group:
            copy.start()
    for t in range(min(LOOK, tiles)):
        bx_copy(t).start()
    for t in range(2):
        fetch_near(t)
    for h in both:
        with jax.named_scope("y_far"):
            y_far[h].wait_recv()
        z_y[h].start()
        with jax.named_scope("xy_far1"):
            xy_far1[h].wait_recv()
        xy_far2[h].start()
    for h in both:
        with jax.named_scope("xy_near1"):
            xy_near1[h].wait_recv()
        xy_near2[h].start()
        with jax.named_scope("xy_far2"):
            xy_far2[h].wait_recv()
        z_xy[h].start()
    for copy in y_near:
        copy.start()
    for t in range(2):
        for k in range(2):
            b_piece(t, k).wait()
    for copy in own:
        copy.wait()
    with jax.named_scope("z_y"):
        for copy in z_own + z_y:
            copy.wait_recv()
    first_two(3, lambda j: j + j // 2)
    for h in both:
        with jax.named_scope("x_far"):
            x_far[h].wait_recv()
        z_x[h].start()
    with jax.named_scope("z_xy"):
        for copy in xy_near2 + z_xy:
            copy.wait_recv()
    first_two(2, lambda j: 6 + j)
    for t in range(2):
        for g in both:
            send1(t, g, 1).start()
    with jax.named_scope("z_x"):
        for copy in x_near + y_near + z_x:
            copy.wait_recv()
    for n in range(AHEAD):
        a_chunk(n).start()

    def last_three(j):
        return 2 + (3 * j + 1) // 2

    def add3(t, g):
        with jax.named_scope("recv3"):
            send3(t, g).wait_recv()
        c_v[:, tile_cols(t, g)] = (s3_v[t % D3, g, 0] + r3_v[t % D3, g]).astype(jnp.bfloat16)

    def start_late():
        def body(t, carry):
            for g in both:
                when(t, D3, plain, lambda g=g: pl.semaphore_wait(credit.at[2, g], 1))
                send3(t, g).start()
            return carry

        lax.fori_loop(plain - LATE, plain, body, 0)

    def step(i, carry):
        t = i
        when(t, 0, tiles, lambda: start_chunks(t))
        when(t, 0, tiles - LOOK, lambda: bx_copy(t + LOOK).start())
        when(t, 1, tiles - 1, lambda: fetch_near(t + 1))
        for g in both:
            for k in both:
                when(t, 2, tiles + 2, lambda g=g, k=k: send1(t - 2, g, k).wait_send())

        def wait_b(pieces):
            for k in range(pieces):
                b_piece(t, k).wait()

        def near_products():
            with jax.named_scope("b_near"):
                wait_b(2)
            with jax.named_scope("dot_near"):
                partials(t, 2)

        def all_products():
            with jax.named_scope("b_all"):
                wait_b(4)
            with jax.named_scope("dot_all"):
                partials(t, 4)

        def wait_far():
            def body(n, carry):
                a_chunk(n).wait_recv()
                return carry

            with jax.named_scope("a_chunks"):
                lax.fori_loop(0, 16, body, 0)

        when(t, 0, 2, lambda: partials(t, 2, 3, last_three))
        when(t, 2, plain, near_products)
        when(t, plain, plain + 1, wait_far)
        when(t, plain, tiles, all_products)
        for g in both:
            take(t, g, 0, 2, tiles)
            when(t, 2, tiles, lambda g=g: send1(t, g, 1).start())
        for g in both:
            when(t, 0, tiles, lambda g=g: send1(t, g, 0).start())
        when(t, plain - 1, tiles - 1, lambda: fetch_far(t + 1))

        t1 = i - 1

        def add1(g, k):
            s, blocks = t1 % 2, pl.ds(2 * k, 2)
            with jax.named_scope("recv1"):
                send1(t1, g, k).wait_recv()
            s2_v[s, g, blocks] = p_v[s, g, 0, blocks] + r1_v[s, g, blocks]

        for g in both:
            for k in both:
                when(t1, 2, tiles + 2, lambda g=g, k=k: send2(t1 - 2, g, k).wait_send())
            when(t1, 0, tiles, lambda g=g: add1(g, 1))
            take(t1, g, 1, 2, tiles)
            for k in (1, 0):
                when(t1, 0, tiles, lambda g=g, k=k: send2(t1, g, k).start())
        for g in both:
            when(t1, 0, tiles, lambda g=g: add1(g, 0))
            give(t1, g, 0, g, 2, tiles)

        t2 = i - 2

        def sum2(g, k):
            with jax.named_scope("recv2"):
                send2(t2, g, k).wait_recv()
            return s2_v[t2 % 2, g, k] + r2_v[t2 % 2, g, k]

        def add2(g, k):
            s3_v[t2 % D3, g, k] = sum2(g, k)

        def add2_there(g):
            q_v[t2 % DO, g] = sum2(g, 1).astype(jnp.bfloat16)

        def add2_here(g):
            c_v[:, tile_cols(t2, g)] = sum2(g, 0).astype(jnp.bfloat16)

        for g in both:
            when(t2, D3, plain - LATE + D3, lambda g=g: send3(t2 - D3, g).wait_send())
            when(t2, plain + DO, tiles, lambda g=g: pair_there(t2 - DO, g).wait_send())
            when(t2, 0, plain, lambda g=g: add2(g, 1))
            when(t2, plain, tiles, lambda g=g: add2_there(g))
            take(t2, g, 2, D3, plain - LATE)
            when(t2, 0, plain - LATE, lambda g=g: send3(t2, g).start())
            when(t2, plain, tiles, lambda g=g: pair_there(t2, g).start())
        for g in both:
            when(t2, 0, plain, lambda g=g: add2(g, 0))
            when(t2, plain, tiles, lambda g=g: add2_here(g))
            give(t2, g, 1, 1 - g, 2, tiles)

        t3 = i - 1 - D3
        for g in both:
            when(t3, 0, plain - LATE, lambda g=g: add3(t3, g))
            give(t3, g, 2, AZ, D3, plain)
        when(t, tiles - 2, tiles - 1, start_late)
        when(t, plain - 1, tiles - 1, lambda: fetch_last(t + 1))
        return carry

    lax.fori_loop(0, tiles + 3, step, 0)

    for group in all_hops:
        for copy in group:
            copy.wait_send()

    def each(low, high, fn):
        def body(n, carry):
            fn(n)
            return carry

        lax.fori_loop(low, high, body, 0)

    for g in both:
        each(plain - LATE, plain, lambda t: add3(t, g))
        each(plain - LATE, plain, lambda t: send3(t, g).wait_send())
    each(0, tiles, lambda t: bx_copy(t).wait_send())
    each(0, paired, lambda q: bxz_copy(q).wait_send())
    each(0, 16, lambda n: a_chunk(n).wait_send())
    each(0, 2 * paired, lambda n: b_chunk(n // 2, n % 2).wait_send())
    for g in both:
        each(max(plain, tiles - DO), tiles, lambda t: pair_there(t, g).wait_send())
        each(plain, tiles, lambda t: pair_there(t, g).wait_recv())


def solution(mesh):
    spec_rows = P(("dp", "tp"), None)

    def local_block(a_rows, b_rows):
        rows, inner = a_rows.shape
        depth, columns = b_rows.shape
        plain, paired = counts(columns)
        tiles = plain + paired
        f32, bf16 = jnp.float32, jnp.bfloat16
        dma = pltpu.SemaphoreType.DMA
        out = pl.pallas_call(
            kernel,
            name="matmul_reduce_scatter",
            out_shape=(
                pltpu.VMEM((rows, columns), bf16),
                jax.ShapeDtypeStruct((tiles, depth, C), bf16),
                jax.ShapeDtypeStruct((paired, depth, C), bf16),
                jax.ShapeDtypeStruct((paired, depth, C), bf16),
                jax.ShapeDtypeStruct((2, rows, 2 * depth), bf16),
            ),
            in_specs=[pl.BlockSpec(memory_space=pl.ANY)] * 2,
            out_specs=(pl.BlockSpec(memory_space=pltpu.VMEM),) + (pl.BlockSpec(memory_space=pl.ANY),) * 4,
            scratch_shapes=[
                pltpu.VMEM((8, rows, 4 * depth), bf16),
                pltpu.VMEM((2, 4 * depth, C), bf16),
                pltpu.VMEM((2, 2, 2, 4, rows, W), f32),
                pltpu.VMEM((2, 2, 4, rows, W), f32),
                pltpu.VMEM((2, 2, 4, rows, W), f32),
                pltpu.VMEM((2, 2, 2, rows, W), f32),
                pltpu.VMEM((D3, 2, 2, rows, W), f32),
                pltpu.VMEM((D3, 2, rows, W), f32),
                pltpu.VMEM((DO, 2, rows, W), bf16),
                dma((12, 2)), dma((12, 2)), dma((4,)),
                dma((tiles,)), dma((tiles,)), dma((paired,)), dma((paired,)),
                dma((16 + 2 * paired,)), dma((16 + 2 * paired,)), dma((2, 4)),
                dma((2, 2, 2)), dma((2, 2, 2)), dma((2, 2, 2)), dma((2, 2, 2)), dma((D3, 2)), dma((D3, 2)),
                dma((DO, 2)), dma((paired, 2)),
                pltpu.SemaphoreType.REGULAR((3, 2)),
            ],
            compiler_params=pltpu.CompilerParams(
                collective_id=0, has_side_effects=True, vmem_limit_bytes=56 * 1024 * 1024),
            cost_estimate=pl.CostEstimate(
                flops=2 * 8 * rows * 2 * depth * columns, bytes_accessed=6 * depth * columns, transcendentals=0),
        )(a_rows, b_rows)
        return out[0]

    return jax.shard_map(local_block, mesh=mesh, in_specs=(spec_rows, spec_rows), out_specs=spec_rows, check_vma=False)
```

```python
import jax
import jax.numpy as jnp
from jax import lax
from jax.experimental import pallas as pl
from jax.experimental.pallas import tpu as pltpu
from jax.sharding import PartitionSpec as P

MESH = pl.DeviceIdType.MESH
W = 128
C = 2 * W
LOOK = 4
D3 = 6
DO = 6
LATE = 4
AHEAD = 2
AX, AY, AZ = 0, 1, 2


def bits_of(d):
    return (d // 4, (d // 2) % 2, d % 2)


def counts(columns):
    paired = columns // C // 4
    return columns // C - 2 * paired - 1, paired


def kernel(a_hbm, b_hbm, c_v, bx_hbm, bz_hbm, bxz_hbm, relay,
           a_v, b_v, p_v, r1_v, s2_v, r2_v, s3_v, r3_v, q_v,
           hop_send, hop_recv, own_sem, bx_send, bx_recv, bxz_send, bxz_recv, ch_send, ch_recv, b_sem,
           s1_sem, r1_sem, s2_sem, r2_sem, s3_sem, r3_sem, qs_sem, qr_sem, credit):
    depth, columns = b_hbm.shape
    plain, paired = counts(columns)
    tiles = plain + paired
    rows, upper = a_hbm.shape[0], a_hbm.shape[0] // 2
    half = depth // 2
    chunks = 16 + 2 * paired
    last = plain + paired
    rate = max(114, -(-1600 // plain), -(-100 * (15 + 2 * paired) // (tiles - 1)))

    dp, tp = lax.axis_index("dp"), lax.axis_index("tp")
    core, x, y, z = dp % 2, (dp // 2) % 2, dp // 4, tp

    def flip(v, bit):
        return v + bit - 2 * v * bit

    def device(bits, other=0):
        return {"dp": flip(y, bits[1]) * 4 + flip(x, bits[0]) * 2 + flip(core, other), "tp": flip(z, bits[2])}

    axis_nbr = [device((1, 0, 0)), device((0, 1, 0)), device((0, 0, 1))]
    partner = device((0, 0, 0), 1)

    barrier = pltpu.get_barrier_semaphore()
    for nbr in (*axis_nbr, partner):
        pl.semaphore_signal(barrier, inc=1, device_id=nbr, device_id_type=MESH)

    def send(src, dst, send_sem, recv_sem, to):
        return pltpu.make_async_remote_copy(
            src_ref=src, dst_ref=dst, send_sem=send_sem, recv_sem=recv_sem, device_id=to, device_id_type=MESH)

    def when(t, low, high, fn):
        pl.when(jnp.logical_and(t >= low, t < high))(fn)

    def is_paired(t):
        return (t + tiles - plain) // tiles

    def tile_cols(t, g=None):
        col = t * C + is_paired(t) * ((t - plain) * C + z * C)
        if g is None:
            return pl.ds(pl.multiple_of(col, W), C)
        return pl.ds(pl.multiple_of(col + g * W, W), W)

    def their_cols(q):
        return pl.ds(pl.multiple_of((plain + 2 * q + 1 - z) * C, W), C)

    def last_cols(side):
        return pl.ds(pl.multiple_of((plain + 2 * paired) * C + side * W, W), W)

    def a_cols(bits, h):
        to = device(bits, h)
        return a_hbm.at[:, pl.ds(pl.multiple_of((to["dp"] * 2 + to["tp"]) * depth, depth), depth)]

    def near(d, h):
        return a_v.at[d, :, pl.ds(h * depth, depth)]

    def far(d, h):
        return a_v.at[d, :, pl.ds((2 + h) * depth, depth)]

    def held(i, h):
        return relay.at[i, :, pl.ds(h * depth, depth)]

    def hop(n, h, src, dst, axis):
        return send(src, dst, hop_send.at[n, h], hop_recv.at[n, h], axis_nbr[axis])

    both = range(2)
    xy_far1 = [hop(0, h, a_cols((1, 1, 1), h), held(0, h), AX) for h in both]
    xy_near1 = [hop(1, h, a_cols((1, 1, 0), h), held(1, h), AX) for h in both]
    x_far = [hop(2, h, a_cols((1, 0, 1), h), far(4, h), AX) for h in both]
    x_near = [hop(3, h, a_cols((1, 0, 0), h), near(4, h), AX) for h in both]
    y_far = [hop(4, h, a_cols((0, 1, 1), h), far(2, h), AY) for h in both]
    xy_far2 = [hop(5, h, held(0, h), far(6, h), AY) for h in both]
    xy_near2 = [hop(6, h, held(1, h), near(6, h), AY) for h in both]
    y_near = [hop(7, h, a_cols((0, 1, 0), h), near(2, h), AY) for h in both]
    z_own = [hop(8, h, a_cols((0, 0, 1), h), near(1, h), AZ) for h in both]
    z_y = [hop(9, h, far(2, h), near(3, h), AZ) for h in both]
    z_xy = [hop(10, h, far(6, h), near(7, h), AZ) for h in both]
    z_x = [hop(11, h, far(4, h), near(5, h), AZ) for h in both]
    all_hops = (xy_far1, xy_near1, x_far, x_near, y_far, xy_far2, xy_near2, y_near, z_own, z_y, z_xy, z_x)
    own = [pltpu.make_async_copy(a_cols((0, 0, 0), h), near(0, h), own_sem.at[h]) for h in both]
    own += [pltpu.make_async_copy(a_cols((0, 0, 1), h), far(0, h), own_sem.at[2 + h]) for h in both]

    def a_chunk(n):
        d, k = (n // 4) * 2, n % 4
        return send(a_v.at[d, :, pl.ds(pl.multiple_of(k * half, half), half)],
                    a_v.at[d + 1, :, pl.ds(pl.multiple_of(2 * depth + k * half, half), half)],
                    ch_send.at[n], ch_recv.at[n], axis_nbr[AZ])

    def b_chunk(q, h):
        rows = pl.ds(pl.multiple_of(h * half, half), half)
        n = 16 + 2 * q + h
        return send(b_hbm.at[rows, their_cols(q)], bz_hbm.at[q, rows], ch_send.at[n], ch_recv.at[n], axis_nbr[AZ])

    def last_chunk():
        return send(b_hbm.at[:, last_cols(1 - z)], bz_hbm.at[paired, :, 0:W], ch_send.at[chunks], ch_recv.at[chunks], axis_nbr[AZ])

    def start_chunks(i):
        def body(n, carry):
            when(n, 0, 16, lambda: a_chunk(n).start())
            when(n, 16, chunks, lambda: b_chunk((n - 16) // 2, (n - 16) % 2).start())
            when(n, chunks, chunks + 1, lambda: last_chunk().start())
            return carry

        lax.fori_loop(rate * i // 100 + AHEAD, rate * (i + 1) // 100 + AHEAD, body, 0)

    def bx_copy(t):
        return send(b_hbm.at[:, tile_cols(t)], bx_hbm.at[t], bx_send.at[t], bx_recv.at[t], partner)

    def bxz_copy(q):
        return send(bz_hbm.at[q], bxz_hbm.at[q], bxz_send.at[q], bxz_recv.at[q], partner)

    def last_bx():
        return send(b_hbm.at[:, last_cols(z)], bx_hbm.at[last, :, 0:W], bx_send.at[last], bx_recv.at[last], partner)

    def last_bxz():
        return send(bz_hbm.at[paired, :, 0:W], bxz_hbm.at[paired, :, 0:W], bxz_send.at[paired], bxz_recv.at[paired], partner)

    def last_piece(k):
        src = (b_hbm.at[:, last_cols(z)], bx_hbm.at[last, :, 0:W], bz_hbm.at[paired, :, 0:W], bxz_hbm.at[paired, :, 0:W])[k]
        return pltpu.make_async_copy(src, b_v.at[last % 2, pl.ds(k * depth, depth), 0:W], b_sem.at[last % 2, k])

    def b_piece(t, k):
        src = (b_hbm.at[:, tile_cols(t)], bx_hbm.at[t], bz_hbm.at[t - plain], bxz_hbm.at[t - plain])[k]
        return pltpu.make_async_copy(src, b_v.at[t % 2, pl.ds(k * depth, depth)], b_sem.at[t % 2, k])

    def fetch_near(t):
        b_piece(t, 0).start()
        bx_copy(t).wait_recv()
        b_piece(t, 1).start()

    def fetch_far(t):
        with jax.named_scope("b_chunk"):
            for h in both:
                b_chunk(t - plain, h).wait_recv()
        bxz_copy(t - plain).start()
        b_piece(t, 2).start()

    def fetch_last(t):
        with jax.named_scope("bxz"):
            bxz_copy(t - plain).wait_recv()
        b_piece(t, 3).start()

    def last_near():
        last_piece(0).start()
        last_bx().wait_recv()
        last_piece(1).start()

    def last_far():
        with jax.named_scope("last_chunk"):
            last_chunk().wait_recv()
        last_bxz().start()
        last_piece(2).start()

    def last_fetch():
        last_bxz().wait_recv()
        last_piece(3).start()

    def partial(t, d, k):
        s = t % 2
        dx, dy, dz = bits_of(d)
        part = jnp.dot(a_v[d, :, 0:k * depth], b_v[s, 0:k * depth], preferred_element_type=jnp.float32)
        p_v[s, 0, dx, dy * 2 + dz] = part[:, 0:W]
        p_v[s, 1, dy, dx * 2 + dz] = part[:, W:C]

    def last_partials():
        s = last % 2

        def body(d, carry):
            dx, dy, dz = bits_of(d)
            part = jnp.dot(a_v[d], b_v[s, :, 0:W], preferred_element_type=jnp.float32)
            p_v[s, 0, dx, dy * 2 + dz, 0:upper] = part[0:upper]
            p_v[s, 1, dy, dx * 2 + dz, 0:upper] = part[upper:rows]
            return carry

        lax.fori_loop(0, 8, body, 0)

    def partials(t, k, n=8, order=lambda j: j):
        def body(j, carry):
            partial(t, order(j), k)
            return carry

        lax.fori_loop(0, n, body, 0)

    def first_two(n, order):
        def body(j, carry):
            partial(j // n, order(j % n), 2)
            return carry

        lax.fori_loop(0, 2 * n, body, 0)

    def send1(t, g, k, n=rows):
        s, blocks, part = t % 2, pl.ds(2 * k, 2), pl.ds(0, n)
        return send(p_v.at[s, g, 1, blocks, part], r1_v.at[s, g, blocks, part],
                    s1_sem.at[s, g, k], r1_sem.at[s, g, k], axis_nbr[g])

    def send2(t, g, k, n=rows):
        s, part = t % 2, pl.ds(0, n)
        return send(s2_v.at[s, g, 2 + k, part], r2_v.at[s, g, k, part],
                    s2_sem.at[s, g, k], r2_sem.at[s, g, k], axis_nbr[1 - g])

    def send3(t, g):
        s = t % D3
        return send(s3_v.at[s, g, 1], r3_v.at[s, g], s3_sem.at[s, g], r3_sem.at[s, g], axis_nbr[AZ])

    def pair_there(t, g):
        s = t % DO
        return send(q_v.at[s, g], c_v.at[:, tile_cols(t, g)], qs_sem.at[s, g], qr_sem.at[t - plain, g], axis_nbr[AZ])

    def last_there(g):
        s = last % DO
        return send(q_v.at[s, g, pl.ds(0, upper)], c_v.at[pl.ds(g * upper, upper), last_cols(z)],
                    qs_sem.at[s, g], qr_sem.at[paired, g], axis_nbr[AZ])

    def take(t, g, phase, slots, high):
        when(t, slots, high, lambda: pl.semaphore_wait(credit.at[phase, g], 1))

    def give(t, g, phase, axis, slots, high):
        when(t, 0, high - slots, lambda: pl.semaphore_signal(
            credit.at[phase, g], inc=1, device_id=axis_nbr[axis], device_id_type=MESH))

    for copy in own:
        copy.start()
    with jax.named_scope("barrier"):
        pl.semaphore_wait(barrier, 4)
    for group in (xy_far1, y_far, z_own, xy_near1, x_far, x_near):
        for copy in group:
            copy.start()
    for t in range(min(LOOK, tiles)):
        bx_copy(t).start()
    for t in range(2):
        fetch_near(t)
    for h in both:
        with jax.named_scope("y_far"):
            y_far[h].wait_recv()
        z_y[h].start()
        with jax.named_scope("xy_far1"):
            xy_far1[h].wait_recv()
        xy_far2[h].start()
    for h in both:
        with jax.named_scope("xy_near1"):
            xy_near1[h].wait_recv()
        xy_near2[h].start()
        with jax.named_scope("xy_far2"):
            xy_far2[h].wait_recv()
        z_xy[h].start()
    for copy in y_near:
        copy.start()
    for t in range(2):
        for k in range(2):
            b_piece(t, k).wait()
    for copy in own:
        copy.wait()
    with jax.named_scope("z_y"):
        for copy in z_own + z_y:
            copy.wait_recv()
    first_two(3, lambda j: j + j // 2)
    for h in both:
        with jax.named_scope("x_far"):
            x_far[h].wait_recv()
        z_x[h].start()
    with jax.named_scope("z_xy"):
        for copy in xy_near2 + z_xy:
            copy.wait_recv()
    first_two(2, lambda j: 6 + j)
    for t in range(2):
        for g in both:
            send1(t, g, 1).start()
    with jax.named_scope("z_x"):
        for copy in x_near + y_near + z_x:
            copy.wait_recv()
    for n in range(AHEAD):
        a_chunk(n).start()

    def last_three(j):
        return 2 + (3 * j + 1) // 2

    def add3(t, g):
        with jax.named_scope("recv3"):
            send3(t, g).wait_recv()
        c_v[:, tile_cols(t, g)] = (s3_v[t % D3, g, 0] + r3_v[t % D3, g]).astype(jnp.bfloat16)

    def start_late():
        def body(t, carry):
            for g in both:
                when(t, D3, plain, lambda g=g: pl.semaphore_wait(credit.at[2, g], 1))
                send3(t, g).start()
            return carry

        lax.fori_loop(plain - LATE, plain, body, 0)

    def step(i, carry):
        t = i
        when(t, 0, tiles, lambda: start_chunks(t))
        when(t, 0, tiles - LOOK, lambda: bx_copy(t + LOOK).start())
        when(t, tiles - LOOK, tiles - LOOK + 1, lambda: last_bx().start())
        when(t, 1, tiles - 1, lambda: fetch_near(t + 1))
        when(t, tiles - 1, tiles, last_near)
        for g in both:
            for k in both:
                when(t, 2, tiles + 2, lambda g=g, k=k: send1(t - 2, g, k).wait_send())

        def wait_b(pieces):
            for k in range(pieces):
                b_piece(t, k).wait()

        def near_products():
            with jax.named_scope("b_near"):
                wait_b(2)
            with jax.named_scope("dot_near"):
                partials(t, 2)

        def all_products():
            with jax.named_scope("b_all"):
                wait_b(4)
            with jax.named_scope("dot_all"):
                partials(t, 4)

        def last_products():
            with jax.named_scope("b_last"):
                for k in range(4):
                    last_piece(k).wait()
            with jax.named_scope("dot_last"):
                last_partials()
            for g in both:
                pl.semaphore_wait(credit.at[0, g], 1)
                send1(last, g, 1, upper).start()
            for g in both:
                send1(last, g, 0, upper).start()

        def wait_far():
            def body(n, carry):
                a_chunk(n).wait_recv()
                return carry

            with jax.named_scope("a_chunks"):
                lax.fori_loop(0, 16, body, 0)

        when(t, 0, 2, lambda: partials(t, 2, 3, last_three))
        when(t, 2, plain, near_products)
        when(t, plain, plain + 1, wait_far)
        when(t, plain, tiles, all_products)
        when(t, last, last + 1, last_products)
        for g in both:
            take(t, g, 0, 2, tiles)
            when(t, 2, tiles, lambda g=g: send1(t, g, 1).start())
        for g in both:
            when(t, 0, tiles, lambda g=g: send1(t, g, 0).start())
        when(t, plain - 1, tiles - 1, lambda: fetch_far(t + 1))
        when(t, tiles - 1, tiles, last_far)

        t1 = i - 1

        def add1(g, k, n=rows):
            s, blocks, part = t1 % 2, pl.ds(2 * k, 2), pl.ds(0, n)
            with jax.named_scope("recv1"):
                send1(t1, g, k, n).wait_recv()
            s2_v[s, g, blocks, part] = p_v[s, g, 0, blocks, part] + r1_v[s, g, blocks, part]

        def last1():
            for g in both:
                add1(g, 1, upper)
                pl.semaphore_wait(credit.at[1, g], 1)
                for k in (1, 0):
                    send2(last, g, k, upper).start()
            for g in both:
                add1(g, 0, upper)

        for g in both:
            for k in both:
                when(t1, 2, tiles + 2, lambda g=g, k=k: send2(t1 - 2, g, k).wait_send())
            when(t1, 0, tiles, lambda g=g: add1(g, 1))
            take(t1, g, 1, 2, tiles)
            for k in (1, 0):
                when(t1, 0, tiles, lambda g=g, k=k: send2(t1, g, k).start())
        for g in both:
            when(t1, 0, tiles, lambda g=g: add1(g, 0))
            give(t1, g, 0, g, 2, last + 1)
        when(t1, last, last + 1, last1)

        t2 = i - 2

        def sum2(g, k, n=rows):
            part = pl.ds(0, n)
            with jax.named_scope("recv2"):
                send2(t2, g, k, n).wait_recv()
            return s2_v[t2 % 2, g, k, part] + r2_v[t2 % 2, g, k, part]

        def last2():
            for g in both:
                q_v[last % DO, g, pl.ds(0, upper)] = sum2(g, 1, upper).astype(jnp.bfloat16)
                last_there(g).start()
            for g in both:
                c_v[pl.ds(g * upper, upper), last_cols(z)] = sum2(g, 0, upper).astype(jnp.bfloat16)

        def add2(g, k):
            s3_v[t2 % D3, g, k] = sum2(g, k)

        def add2_there(g):
            q_v[t2 % DO, g] = sum2(g, 1).astype(jnp.bfloat16)

        def add2_here(g):
            c_v[:, tile_cols(t2, g)] = sum2(g, 0).astype(jnp.bfloat16)

        for g in both:
            when(t2, D3, plain - LATE + D3, lambda g=g: send3(t2 - D3, g).wait_send())
            when(t2, plain + DO, last + 1, lambda g=g: pair_there(t2 - DO, g).wait_send())
            when(t2, 0, plain, lambda g=g: add2(g, 1))
            when(t2, plain, tiles, lambda g=g: add2_there(g))
            take(t2, g, 2, D3, plain - LATE)
            when(t2, 0, plain - LATE, lambda g=g: send3(t2, g).start())
            when(t2, plain, tiles, lambda g=g: pair_there(t2, g).start())
        for g in both:
            when(t2, 0, plain, lambda g=g: add2(g, 0))
            when(t2, plain, tiles, lambda g=g: add2_here(g))
            give(t2, g, 1, 1 - g, 2, last + 1)
        when(t2, last, last + 1, last2)

        t3 = i - 1 - D3
        for g in both:
            when(t3, 0, plain - LATE, lambda g=g: add3(t3, g))
            give(t3, g, 2, AZ, D3, plain)
        when(t, last - 1, last, start_late)
        when(t, plain - 1, tiles - 1, lambda: fetch_last(t + 1))
        when(t, tiles - 1, tiles, last_fetch)
        return carry

    lax.fori_loop(0, tiles + 3, step, 0)

    for group in all_hops:
        for copy in group:
            copy.wait_send()

    def each(low, high, fn):
        def body(n, carry):
            fn(n)
            return carry

        lax.fori_loop(low, high, body, 0)

    for g in both:
        each(plain - LATE, plain, lambda t: add3(t, g))
        each(plain - LATE, plain, lambda t: send3(t, g).wait_send())
    for g in both:
        for k in both:
            send1(last, g, k, upper).wait_send()
            send2(last, g, k, upper).wait_send()
        last_there(g).wait_send()
        last_there(g).wait_recv()
    last_bx().wait_send()
    last_bxz().wait_send()
    last_chunk().wait_send()
    each(0, tiles, lambda t: bx_copy(t).wait_send())
    each(0, paired, lambda q: bxz_copy(q).wait_send())
    each(0, 16, lambda n: a_chunk(n).wait_send())
    each(0, 2 * paired, lambda n: b_chunk(n // 2, n % 2).wait_send())
    for g in both:
        each(max(plain, last + 1 - DO), tiles, lambda t: pair_there(t, g).wait_send())
        each(plain, tiles, lambda t: pair_there(t, g).wait_recv())


def solution(mesh):
    spec_rows = P(("dp", "tp"), None)

    def local_block(a_rows, b_rows):
        rows, inner = a_rows.shape
        depth, columns = b_rows.shape
        plain, paired = counts(columns)
        tiles = plain + paired
        f32, bf16 = jnp.float32, jnp.bfloat16
        dma = pltpu.SemaphoreType.DMA
        out = pl.pallas_call(
            kernel,
            name="matmul_reduce_scatter",
            out_shape=(
                pltpu.VMEM((rows, columns), bf16),
                jax.ShapeDtypeStruct((tiles + 1, depth, C), bf16),
                jax.ShapeDtypeStruct((paired + 1, depth, C), bf16),
                jax.ShapeDtypeStruct((paired + 1, depth, C), bf16),
                jax.ShapeDtypeStruct((2, rows, 2 * depth), bf16),
            ),
            in_specs=[pl.BlockSpec(memory_space=pl.ANY)] * 2,
            out_specs=(pl.BlockSpec(memory_space=pltpu.VMEM),) + (pl.BlockSpec(memory_space=pl.ANY),) * 4,
            scratch_shapes=[
                pltpu.VMEM((8, rows, 4 * depth), bf16),
                pltpu.VMEM((2, 4 * depth, C), bf16),
                pltpu.VMEM((2, 2, 2, 4, rows, W), f32),
                pltpu.VMEM((2, 2, 4, rows, W), f32),
                pltpu.VMEM((2, 2, 4, rows, W), f32),
                pltpu.VMEM((2, 2, 2, rows, W), f32),
                pltpu.VMEM((D3, 2, 2, rows, W), f32),
                pltpu.VMEM((D3, 2, rows, W), f32),
                pltpu.VMEM((DO, 2, rows, W), bf16),
                dma((12, 2)), dma((12, 2)), dma((4,)),
                dma((tiles + 1,)), dma((tiles + 1,)), dma((paired + 1,)), dma((paired + 1,)),
                dma((17 + 2 * paired,)), dma((17 + 2 * paired,)), dma((2, 4)),
                dma((2, 2, 2)), dma((2, 2, 2)), dma((2, 2, 2)), dma((2, 2, 2)), dma((D3, 2)), dma((D3, 2)),
                dma((DO, 2)), dma((paired + 1, 2)),
                pltpu.SemaphoreType.REGULAR((3, 2)),
            ],
            compiler_params=pltpu.CompilerParams(
                collective_id=0, has_side_effects=True, vmem_limit_bytes=56 * 1024 * 1024),
            cost_estimate=pl.CostEstimate(
                flops=2 * 8 * rows * 2 * depth * columns, bytes_accessed=6 * depth * columns, transcendentals=0),
        )(a_rows, b_rows)
        return out[0]

    return jax.shard_map(local_block, mesh=mesh, in_specs=(spec_rows, spec_rows), out_specs=spec_rows, check_vma=False)
```

```python
import jax
import jax.numpy as jnp
from jax import lax
from jax.experimental import pallas as pl
from jax.experimental.pallas import tpu as pltpu
from jax.sharding import PartitionSpec as P

MESH = pl.DeviceIdType.MESH
W = 128
C = 2 * W
LOOK = 4
D3 = 6
DO = 6
LATE = 4
AHEAD = 2
LAG = 5
AX, AY, AZ = 0, 1, 2


def bits_of(d):
    return (d // 4, (d // 2) % 2, d % 2)


def counts(columns):
    paired = columns // C // 4
    return columns // C - 2 * paired - 1, paired


def kernel(a_hbm, b_hbm, c_v, bx_hbm, bz_hbm, bxz_hbm, relay,
           a_v, b_v, p_v, r1_v, s2_v, r2_v, s3_v, r3_v, q_v,
           hop_send, hop_recv, own_sem, bx_send, bx_recv, bxz_send, bxz_recv, ch_send, ch_recv, b_sem,
           s1_sem, r1_sem, s2_sem, r2_sem, s3_sem, r3_sem, qs_sem, qr_sem, credit):
    depth, columns = b_hbm.shape
    plain, paired = counts(columns)
    tiles = plain + paired
    rows, upper = a_hbm.shape[0], a_hbm.shape[0] // 2
    half = depth // 2
    chunks = 16 + 2 * paired
    last = plain + paired
    rate = max(114, -(-1600 // plain), -(-100 * (15 + 2 * paired) // (tiles - 1)))

    dp, tp = lax.axis_index("dp"), lax.axis_index("tp")
    core, x, y, z = dp % 2, (dp // 2) % 2, dp // 4, tp

    def flip(v, bit):
        return v + bit - 2 * v * bit

    def device(bits, other=0):
        return {"dp": flip(y, bits[1]) * 4 + flip(x, bits[0]) * 2 + flip(core, other), "tp": flip(z, bits[2])}

    axis_nbr = [device((1, 0, 0)), device((0, 1, 0)), device((0, 0, 1))]
    partner = device((0, 0, 0), 1)

    barrier = pltpu.get_barrier_semaphore()
    for nbr in (*axis_nbr, partner):
        pl.semaphore_signal(barrier, inc=1, device_id=nbr, device_id_type=MESH)

    def send(src, dst, send_sem, recv_sem, to):
        return pltpu.make_async_remote_copy(
            src_ref=src, dst_ref=dst, send_sem=send_sem, recv_sem=recv_sem, device_id=to, device_id_type=MESH)

    def when(t, low, high, fn):
        pl.when(jnp.logical_and(t >= low, t < high))(fn)

    def is_paired(t):
        return (t + tiles - plain) // tiles

    def tile_cols(t, g=None):
        col = t * C + is_paired(t) * ((t - plain) * C + z * C)
        if g is None:
            return pl.ds(pl.multiple_of(col, W), C)
        return pl.ds(pl.multiple_of(col + g * W, W), W)

    def their_cols(q):
        return pl.ds(pl.multiple_of((plain + 2 * q + 1 - z) * C, W), C)

    def last_cols(side):
        return pl.ds(pl.multiple_of((plain + 2 * paired) * C + side * W, W), W)

    def a_cols(bits, h):
        to = device(bits, h)
        return a_hbm.at[:, pl.ds(pl.multiple_of((to["dp"] * 2 + to["tp"]) * depth, depth), depth)]

    def near(d, h):
        return a_v.at[d, :, pl.ds(h * depth, depth)]

    def far(d, h):
        return a_v.at[d, :, pl.ds((2 + h) * depth, depth)]

    def held(i, h):
        return relay.at[i, :, pl.ds(h * depth, depth)]

    def hop(n, h, src, dst, axis):
        return send(src, dst, hop_send.at[n, h], hop_recv.at[n, h], axis_nbr[axis])

    both = range(2)
    xy_far1 = [hop(0, h, a_cols((1, 1, 1), h), held(0, h), AX) for h in both]
    xy_near1 = [hop(1, h, a_cols((1, 1, 0), h), held(1, h), AX) for h in both]
    x_far = [hop(2, h, a_cols((1, 0, 1), h), far(4, h), AX) for h in both]
    x_near = [hop(3, h, a_cols((1, 0, 0), h), near(4, h), AX) for h in both]
    y_far = [hop(4, h, a_cols((0, 1, 1), h), far(2, h), AY) for h in both]
    xy_far2 = [hop(5, h, held(0, h), far(6, h), AY) for h in both]
    xy_near2 = [hop(6, h, held(1, h), near(6, h), AY) for h in both]
    y_near = [hop(7, h, a_cols((0, 1, 0), h), near(2, h), AY) for h in both]
    z_own = [hop(8, h, a_cols((0, 0, 1), h), near(1, h), AZ) for h in both]
    z_y = [hop(9, h, far(2, h), near(3, h), AZ) for h in both]
    z_xy = [hop(10, h, far(6, h), near(7, h), AZ) for h in both]
    z_x = [hop(11, h, far(4, h), near(5, h), AZ) for h in both]
    all_hops = (xy_far1, xy_near1, x_far, x_near, y_far, xy_far2, xy_near2, y_near, z_own, z_y, z_xy, z_x)
    own = [pltpu.make_async_copy(a_cols((0, 0, 0), h), near(0, h), own_sem.at[h]) for h in both]
    own += [pltpu.make_async_copy(a_cols((0, 0, 1), h), far(0, h), own_sem.at[2 + h]) for h in both]

    def a_chunk(n):
        d, k = (n // 4) * 2, n % 4
        return send(a_v.at[d, :, pl.ds(pl.multiple_of(k * half, half), half)],
                    a_v.at[d + 1, :, pl.ds(pl.multiple_of(2 * depth + k * half, half), half)],
                    ch_send.at[n], ch_recv.at[n], axis_nbr[AZ])

    def b_chunk(q, h):
        rows = pl.ds(pl.multiple_of(h * half, half), half)
        n = 16 + 2 * q + h
        return send(b_hbm.at[rows, their_cols(q)], bz_hbm.at[q, rows], ch_send.at[n], ch_recv.at[n], axis_nbr[AZ])

    def last_chunk():
        return send(b_hbm.at[:, last_cols(1 - z)], bz_hbm.at[paired, :, 0:W], ch_send.at[chunks], ch_recv.at[chunks], axis_nbr[AZ])

    def start_chunks(i):
        def body(n, carry):
            when(n, 0, 16, lambda: a_chunk(n).start())
            when(n, 16, chunks, lambda: b_chunk((n - 16) // 2, (n - 16) % 2).start())
            when(n, chunks, chunks + 1, lambda: last_chunk().start())
            return carry

        lax.fori_loop(rate * i // 100 + AHEAD, rate * (i + 1) // 100 + AHEAD, body, 0)

    def end_chunks(i):
        def body(n, carry):
            when(n, 0, 16, lambda: a_chunk(n).wait_send())
            when(n, 16, chunks, lambda: b_chunk((n - 16) // 2, (n - 16) % 2).wait_send())
            when(n, chunks, chunks + 1, lambda: last_chunk().wait_send())
            return carry

        lax.fori_loop(rate * i // 100 + AHEAD, rate * (i + 1) // 100 + AHEAD, body, 0)

    def bx_copy(t):
        return send(b_hbm.at[:, tile_cols(t)], bx_hbm.at[t], bx_send.at[t], bx_recv.at[t], partner)

    def bxz_copy(q):
        return send(bz_hbm.at[q], bxz_hbm.at[q], bxz_send.at[q], bxz_recv.at[q], partner)

    def last_bx():
        return send(b_hbm.at[:, last_cols(z)], bx_hbm.at[last, :, 0:W], bx_send.at[last], bx_recv.at[last], partner)

    def last_bxz():
        return send(bz_hbm.at[paired, :, 0:W], bxz_hbm.at[paired, :, 0:W], bxz_send.at[paired], bxz_recv.at[paired], partner)

    def last_piece(k):
        src = (b_hbm.at[:, last_cols(z)], bx_hbm.at[last, :, 0:W], bz_hbm.at[paired, :, 0:W], bxz_hbm.at[paired, :, 0:W])[k]
        return pltpu.make_async_copy(src, b_v.at[last % 2, pl.ds(k * depth, depth), 0:W], b_sem.at[last % 2, k])

    def b_piece(t, k):
        src = (b_hbm.at[:, tile_cols(t)], bx_hbm.at[t], bz_hbm.at[t - plain], bxz_hbm.at[t - plain])[k]
        return pltpu.make_async_copy(src, b_v.at[t % 2, pl.ds(k * depth, depth)], b_sem.at[t % 2, k])

    def fetch_near(t):
        b_piece(t, 0).start()
        bx_copy(t).wait_recv()
        b_piece(t, 1).start()

    def fetch_far(t):
        with jax.named_scope("b_chunk"):
            for h in both:
                b_chunk(t - plain, h).wait_recv()
        bxz_copy(t - plain).start()
        b_piece(t, 2).start()

    def fetch_last(t):
        with jax.named_scope("bxz"):
            bxz_copy(t - plain).wait_recv()
        b_piece(t, 3).start()

    def last_near():
        last_piece(0).start()
        last_bx().wait_recv()
        last_piece(1).start()

    def last_far():
        with jax.named_scope("last_chunk"):
            last_chunk().wait_recv()
        last_bxz().start()
        last_piece(2).start()

    def last_fetch():
        last_bxz().wait_recv()
        last_piece(3).start()

    def partial(t, d, k):
        s = t % 2
        dx, dy, dz = bits_of(d)
        part = jnp.dot(a_v[d, :, 0:k * depth], b_v[s, 0:k * depth], preferred_element_type=jnp.float32)
        p_v[s, 0, dx, dy * 2 + dz] = part[:, 0:W]
        p_v[s, 1, dy, dx * 2 + dz] = part[:, W:C]

    def last_partials():
        s = last % 2

        def body(d, carry):
            dx, dy, dz = bits_of(d)
            part = jnp.dot(a_v[d], b_v[s, :, 0:W], preferred_element_type=jnp.float32)
            p_v[s, 0, dx, dy * 2 + dz, 0:upper] = part[0:upper]
            p_v[s, 1, dy, dx * 2 + dz, 0:upper] = part[upper:rows]
            return carry

        lax.fori_loop(0, 8, body, 0)

    def partials(t, k, n=8, order=lambda j: j):
        def body(j, carry):
            partial(t, order(j), k)
            return carry

        lax.fori_loop(0, n, body, 0)

    def first_two(n, order):
        def body(j, carry):
            partial(j // n, order(j % n), 2)
            return carry

        lax.fori_loop(0, 2 * n, body, 0)

    def send1(t, g, k, n=rows):
        s, blocks, part = t % 2, pl.ds(2 * k, 2), pl.ds(0, n)
        return send(p_v.at[s, g, 1, blocks, part], r1_v.at[s, g, blocks, part],
                    s1_sem.at[s, g, k], r1_sem.at[s, g, k], axis_nbr[g])

    def send2(t, g, k, n=rows):
        s, part = t % 2, pl.ds(0, n)
        return send(s2_v.at[s, g, 2 + k, part], r2_v.at[s, g, k, part],
                    s2_sem.at[s, g, k], r2_sem.at[s, g, k], axis_nbr[1 - g])

    def send3(t, g):
        s = t % D3
        return send(s3_v.at[s, g, 1], r3_v.at[s, g], s3_sem.at[s, g], r3_sem.at[s, g], axis_nbr[AZ])

    def pair_there(t, g):
        s = t % DO
        return send(q_v.at[s, g], c_v.at[:, tile_cols(t, g)], qs_sem.at[s, g], qr_sem.at[t - plain, g], axis_nbr[AZ])

    def last_there(g):
        s = last % DO
        return send(q_v.at[s, g, pl.ds(0, upper)], c_v.at[pl.ds(g * upper, upper), last_cols(z)],
                    qs_sem.at[s, g], qr_sem.at[paired, g], axis_nbr[AZ])

    def take(t, g, phase, slots, high):
        when(t, slots, high, lambda: pl.semaphore_wait(credit.at[phase, g], 1))

    def give(t, g, phase, axis, slots, high):
        when(t, 0, high - slots, lambda: pl.semaphore_signal(
            credit.at[phase, g], inc=1, device_id=axis_nbr[axis], device_id_type=MESH))

    for copy in own:
        copy.start()
    with jax.named_scope("barrier"):
        pl.semaphore_wait(barrier, 4)
    for group in (xy_far1, y_far, z_own, xy_near1, x_far, x_near):
        for copy in group:
            copy.start()
    for t in range(min(LOOK, tiles)):
        bx_copy(t).start()
    for t in range(2):
        fetch_near(t)
    for h in both:
        with jax.named_scope("y_far"):
            y_far[h].wait_recv()
        z_y[h].start()
        with jax.named_scope("xy_far1"):
            xy_far1[h].wait_recv()
        xy_far2[h].start()
    for h in both:
        with jax.named_scope("xy_near1"):
            xy_near1[h].wait_recv()
        xy_near2[h].start()
        with jax.named_scope("xy_far2"):
            xy_far2[h].wait_recv()
        z_xy[h].start()
    for copy in y_near:
        copy.start()
    for t in range(2):
        for k in range(2):
            b_piece(t, k).wait()
    for copy in own:
        copy.wait()
    with jax.named_scope("z_y"):
        for copy in z_own + z_y:
            copy.wait_recv()
    first_two(3, lambda j: j + j // 2)
    for h in both:
        with jax.named_scope("x_far"):
            x_far[h].wait_recv()
        z_x[h].start()
    with jax.named_scope("z_xy"):
        for copy in xy_near2 + z_xy:
            copy.wait_recv()
    first_two(2, lambda j: 6 + j)
    for t in range(2):
        for g in both:
            send1(t, g, 1).start()
    with jax.named_scope("z_x"):
        for copy in x_near + y_near + z_x:
            copy.wait_recv()
    for n in range(AHEAD):
        a_chunk(n).start()

    def last_three(j):
        return 2 + (3 * j + 1) // 2

    def add3(t, g):
        with jax.named_scope("recv3"):
            send3(t, g).wait_recv()
        c_v[:, tile_cols(t, g)] = (s3_v[t % D3, g, 0] + r3_v[t % D3, g]).astype(jnp.bfloat16)

    def start_late():
        def body(t, carry):
            for g in both:
                when(t, D3, plain, lambda g=g: pl.semaphore_wait(credit.at[2, g], 1))
                send3(t, g).start()
            return carry

        lax.fori_loop(plain - LATE, plain, body, 0)

    def end_hops():
        for group in all_hops:
            for copy in group:
                copy.wait_send()
        for n in range(AHEAD):
            a_chunk(n).wait_send()

    def step(i, carry):
        t = i
        when(t, 0, tiles, lambda: start_chunks(t))
        when(t, LAG, tiles + 3, lambda: end_chunks(t - LAG))
        when(t, 1, tiles + 1, lambda: bx_copy(t - 1).wait_send())
        when(t, plain + 1, tiles + 1, lambda: bxz_copy(t - 1 - plain).wait_send())
        when(t, LAG, LAG + 1, end_hops)
        for g in both:
            when(t, plain + LAG, tiles + 3, lambda g=g: pair_there(t - LAG, g).wait_recv())
        when(t, 0, tiles - LOOK, lambda: bx_copy(t + LOOK).start())
        when(t, tiles - LOOK, tiles - LOOK + 1, lambda: last_bx().start())
        when(t, 1, tiles - 1, lambda: fetch_near(t + 1))
        when(t, tiles - 1, tiles, last_near)
        for g in both:
            for k in both:
                when(t, 2, tiles + 2, lambda g=g, k=k: send1(t - 2, g, k).wait_send())

        def wait_b(pieces):
            for k in range(pieces):
                b_piece(t, k).wait()

        def near_products():
            with jax.named_scope("b_near"):
                wait_b(2)
            with jax.named_scope("dot_near"):
                partials(t, 2)

        def all_products():
            with jax.named_scope("b_all"):
                wait_b(4)
            with jax.named_scope("dot_all"):
                partials(t, 4)

        def last_products():
            with jax.named_scope("b_last"):
                for k in range(4):
                    last_piece(k).wait()
            with jax.named_scope("dot_last"):
                last_partials()
            for g in both:
                pl.semaphore_wait(credit.at[0, g], 1)
                send1(last, g, 1, upper).start()
            for g in both:
                send1(last, g, 0, upper).start()

        def wait_far():
            def body(n, carry):
                a_chunk(n).wait_recv()
                return carry

            with jax.named_scope("a_chunks"):
                lax.fori_loop(0, 16, body, 0)

        when(t, 0, 2, lambda: partials(t, 2, 3, last_three))
        when(t, 2, plain, near_products)
        when(t, plain, plain + 1, wait_far)
        when(t, plain, tiles, all_products)
        when(t, last, last + 1, last_products)
        for g in both:
            take(t, g, 0, 2, tiles)
            when(t, 2, tiles, lambda g=g: send1(t, g, 1).start())
        for g in both:
            when(t, 0, tiles, lambda g=g: send1(t, g, 0).start())
        when(t, plain - 1, tiles - 1, lambda: fetch_far(t + 1))
        when(t, tiles - 1, tiles, last_far)

        t1 = i - 1

        def add1(g, k, n=rows):
            s, blocks, part = t1 % 2, pl.ds(2 * k, 2), pl.ds(0, n)
            with jax.named_scope("recv1"):
                send1(t1, g, k, n).wait_recv()
            s2_v[s, g, blocks, part] = p_v[s, g, 0, blocks, part] + r1_v[s, g, blocks, part]

        def last1():
            for g in both:
                add1(g, 1, upper)
                pl.semaphore_wait(credit.at[1, g], 1)
                for k in (1, 0):
                    send2(last, g, k, upper).start()
            for g in both:
                add1(g, 0, upper)

        for g in both:
            for k in both:
                when(t1, 2, tiles + 2, lambda g=g, k=k: send2(t1 - 2, g, k).wait_send())
            when(t1, 0, tiles, lambda g=g: add1(g, 1))
            take(t1, g, 1, 2, tiles)
            for k in (1, 0):
                when(t1, 0, tiles, lambda g=g, k=k: send2(t1, g, k).start())
        for g in both:
            when(t1, 0, tiles, lambda g=g: add1(g, 0))
            give(t1, g, 0, g, 2, last + 1)
        when(t1, last, last + 1, last1)

        t2 = i - 2

        def sum2(g, k, n=rows):
            part = pl.ds(0, n)
            with jax.named_scope("recv2"):
                send2(t2, g, k, n).wait_recv()
            return s2_v[t2 % 2, g, k, part] + r2_v[t2 % 2, g, k, part]

        def last2():
            for g in both:
                q_v[last % DO, g, pl.ds(0, upper)] = sum2(g, 1, upper).astype(jnp.bfloat16)
                last_there(g).start()
            for g in both:
                c_v[pl.ds(g * upper, upper), last_cols(z)] = sum2(g, 0, upper).astype(jnp.bfloat16)

        def add2(g, k):
            s3_v[t2 % D3, g, k] = sum2(g, k)

        def add2_there(g):
            q_v[t2 % DO, g] = sum2(g, 1).astype(jnp.bfloat16)

        def add2_here(g):
            c_v[:, tile_cols(t2, g)] = sum2(g, 0).astype(jnp.bfloat16)

        for g in both:
            when(t2, D3, plain - LATE + D3, lambda g=g: send3(t2 - D3, g).wait_send())
            when(t2, plain + DO, last + 1, lambda g=g: pair_there(t2 - DO, g).wait_send())
            when(t2, 0, plain, lambda g=g: add2(g, 1))
            when(t2, plain, tiles, lambda g=g: add2_there(g))
            take(t2, g, 2, D3, plain - LATE)
            when(t2, 0, plain - LATE, lambda g=g: send3(t2, g).start())
            when(t2, plain, tiles, lambda g=g: pair_there(t2, g).start())
        for g in both:
            when(t2, 0, plain, lambda g=g: add2(g, 0))
            when(t2, plain, tiles, lambda g=g: add2_here(g))
            give(t2, g, 1, 1 - g, 2, last + 1)
        when(t2, last, last + 1, last2)

        t3 = i - 1 - D3
        for g in both:
            when(t3, 0, plain - LATE, lambda g=g: add3(t3, g))
            give(t3, g, 2, AZ, D3, plain)
        when(t, last - 1, last, start_late)
        when(t, plain - 1, tiles - 1, lambda: fetch_last(t + 1))
        when(t, tiles - 1, tiles, last_fetch)
        return carry

    lax.fori_loop(0, tiles + 3, step, 0)

    def each(low, high, fn):
        def body(n, carry):
            fn(n)
            return carry

        lax.fori_loop(low, high, body, 0)

    for g in both:
        each(plain - LATE, plain, lambda t: add3(t, g))
        each(plain - LATE, plain, lambda t: send3(t, g).wait_send())
    for g in both:
        for k in both:
            send1(last, g, k, upper).wait_send()
            send2(last, g, k, upper).wait_send()
        last_there(g).wait_send()
        last_there(g).wait_recv()
    last_bx().wait_send()
    last_bxz().wait_send()
    each(tiles + 3 - LAG, tiles, end_chunks)
    for g in both:
        each(max(plain, last + 1 - DO), tiles, lambda t: pair_there(t, g).wait_send())
        each(max(plain, tiles + 3 - LAG), tiles, lambda t: pair_there(t, g).wait_recv())


def solution(mesh):
    spec_rows = P(("dp", "tp"), None)

    def local_block(a_rows, b_rows):
        rows, inner = a_rows.shape
        depth, columns = b_rows.shape
        plain, paired = counts(columns)
        tiles = plain + paired
        f32, bf16 = jnp.float32, jnp.bfloat16
        dma = pltpu.SemaphoreType.DMA
        out = pl.pallas_call(
            kernel,
            name="matmul_reduce_scatter",
            out_shape=(
                pltpu.VMEM((rows, columns), bf16),
                jax.ShapeDtypeStruct((tiles + 1, depth, C), bf16),
                jax.ShapeDtypeStruct((paired + 1, depth, C), bf16),
                jax.ShapeDtypeStruct((paired + 1, depth, C), bf16),
                jax.ShapeDtypeStruct((2, rows, 2 * depth), bf16),
            ),
            in_specs=[pl.BlockSpec(memory_space=pl.ANY)] * 2,
            out_specs=(pl.BlockSpec(memory_space=pltpu.VMEM),) + (pl.BlockSpec(memory_space=pl.ANY),) * 4,
            scratch_shapes=[
                pltpu.VMEM((8, rows, 4 * depth), bf16),
                pltpu.VMEM((2, 4 * depth, C), bf16),
                pltpu.VMEM((2, 2, 2, 4, rows, W), f32),
                pltpu.VMEM((2, 2, 4, rows, W), f32),
                pltpu.VMEM((2, 2, 4, rows, W), f32),
                pltpu.VMEM((2, 2, 2, rows, W), f32),
                pltpu.VMEM((D3, 2, 2, rows, W), f32),
                pltpu.VMEM((D3, 2, rows, W), f32),
                pltpu.VMEM((DO, 2, rows, W), bf16),
                dma((12, 2)), dma((12, 2)), dma((4,)),
                dma((tiles + 1,)), dma((tiles + 1,)), dma((paired + 1,)), dma((paired + 1,)),
                dma((17 + 2 * paired,)), dma((17 + 2 * paired,)), dma((2, 4)),
                dma((2, 2, 2)), dma((2, 2, 2)), dma((2, 2, 2)), dma((2, 2, 2)), dma((D3, 2)), dma((D3, 2)),
                dma((DO, 2)), dma((paired + 1, 2)),
                pltpu.SemaphoreType.REGULAR((3, 2)),
            ],
            compiler_params=pltpu.CompilerParams(
                collective_id=0, has_side_effects=True, vmem_limit_bytes=56 * 1024 * 1024),
            cost_estimate=pl.CostEstimate(
                flops=2 * 8 * rows * 2 * depth * columns, bytes_accessed=6 * depth * columns, transcendentals=0),
        )(a_rows, b_rows)
        return out[0]

    return jax.shard_map(local_block, mesh=mesh, in_specs=(spec_rows, spec_rows), out_specs=spec_rows, check_vma=False)
```

```python
import jax
import jax.numpy as jnp
from jax import lax
from jax.experimental import pallas as pl
from jax.experimental.pallas import tpu as pltpu
from jax.sharding import PartitionSpec as P

MESH = pl.DeviceIdType.MESH
W = 128
C = 2 * W
LOOK = 4
D3 = 6
DO = 6
LATE = 4
AHEAD = 2
LAG = 5
AX, AY, AZ = 0, 1, 2


def bits_of(d):
    return (d // 4, (d // 2) % 2, d % 2)


def counts(columns):
    paired = columns // C // 4
    return columns // C - 2 * paired - 1, paired


def kernel(a_hbm, b_hbm, c_v, bx_hbm, bz_hbm, bxz_hbm, relay,
           a_v, b_v, p_v, r1_v, s2_v, r2_v, s3_v, r3_v, q_v,
           hop_send, hop_recv, own_sem, bx_send, bx_recv, bxz_send, bxz_recv, ch_send, ch_recv, b_sem,
           s1_sem, r1_sem, s2_sem, r2_sem, s3_sem, r3_sem, qs_sem, qr_sem, credit):
    depth, columns = b_hbm.shape
    plain, paired = counts(columns)
    tiles = plain + paired
    rows, upper = a_hbm.shape[0], a_hbm.shape[0] // 2
    half = depth // 2
    chunks = 16 + 2 * paired
    last = plain + paired
    rate = max(114, -(-1600 // plain), -(-100 * (15 + 2 * paired) // (tiles - 1)))

    dp, tp = lax.axis_index("dp"), lax.axis_index("tp")
    core, x, y, z = dp % 2, (dp // 2) % 2, dp // 4, tp

    def flip(v, bit):
        return v + bit - 2 * v * bit

    def device(bits, other=0):
        return {"dp": flip(y, bits[1]) * 4 + flip(x, bits[0]) * 2 + flip(core, other), "tp": flip(z, bits[2])}

    axis_nbr = [device((1, 0, 0)), device((0, 1, 0)), device((0, 0, 1))]
    partner = device((0, 0, 0), 1)

    barrier = pltpu.get_barrier_semaphore()
    for nbr in (*axis_nbr, partner):
        pl.semaphore_signal(barrier, inc=1, device_id=nbr, device_id_type=MESH)

    def send(src, dst, send_sem, recv_sem, to):
        return pltpu.make_async_remote_copy(
            src_ref=src, dst_ref=dst, send_sem=send_sem, recv_sem=recv_sem, device_id=to, device_id_type=MESH)

    def when(t, low, high, fn):
        pl.when(jnp.logical_and(t >= low, t < high))(fn)

    def is_paired(t):
        return (t + tiles - plain) // tiles

    def tile_cols(t, g=None):
        col = t * C + is_paired(t) * ((t - plain) * C + z * C)
        if g is None:
            return pl.ds(pl.multiple_of(col, W), C)
        return pl.ds(pl.multiple_of(col + g * W, W), W)

    def their_cols(q):
        return pl.ds(pl.multiple_of((plain + 2 * q + 1 - z) * C, W), C)

    def last_cols(side):
        return pl.ds(pl.multiple_of((plain + 2 * paired) * C + side * W, W), W)

    def a_cols(bits, h):
        to = device(bits, h)
        return a_hbm.at[:, pl.ds(pl.multiple_of((to["dp"] * 2 + to["tp"]) * depth, depth), depth)]

    def near(d, h):
        return a_v.at[d, :, pl.ds(h * depth, depth)]

    def far(d, h):
        return a_v.at[d, :, pl.ds((2 + h) * depth, depth)]

    def held(i, h):
        return relay.at[i, :, pl.ds(h * depth, depth)]

    def hop(n, h, src, dst, axis):
        return send(src, dst, hop_send.at[n, h], hop_recv.at[n, h], axis_nbr[axis])

    both = range(2)
    xy_far1 = [hop(0, h, a_cols((1, 1, 1), h), held(0, h), AX) for h in both]
    xy_near1 = [hop(1, h, a_cols((1, 1, 0), h), held(1, h), AX) for h in both]
    x_far = [hop(2, h, a_cols((1, 0, 1), h), far(4, h), AX) for h in both]
    x_near = [hop(3, h, a_cols((1, 0, 0), h), near(4, h), AX) for h in both]
    y_far = [hop(4, h, a_cols((0, 1, 1), h), far(2, h), AY) for h in both]
    xy_far2 = [hop(5, h, held(0, h), far(6, h), AY) for h in both]
    xy_near2 = [hop(6, h, held(1, h), near(6, h), AY) for h in both]
    y_near = [hop(7, h, a_cols((0, 1, 0), h), near(2, h), AY) for h in both]
    z_own = [hop(8, h, a_cols((0, 0, 1), h), near(1, h), AZ) for h in both]
    z_y = [hop(9, h, far(2, h), near(3, h), AZ) for h in both]
    z_xy = [hop(10, h, far(6, h), near(7, h), AZ) for h in both]
    z_x = [hop(11, h, far(4, h), near(5, h), AZ) for h in both]
    all_hops = (xy_far1, xy_near1, x_far, x_near, y_far, xy_far2, xy_near2, y_near, z_own, z_y, z_xy, z_x)
    own = [pltpu.make_async_copy(a_cols((0, 0, 0), h), near(0, h), own_sem.at[h]) for h in both]
    own += [pltpu.make_async_copy(a_cols((0, 0, 1), h), far(0, h), own_sem.at[2 + h]) for h in both]

    def a_chunk(n):
        d, k = (n // 4) * 2, n % 4
        return send(a_v.at[d, :, pl.ds(pl.multiple_of(k * half, half), half)],
                    a_v.at[d + 1, :, pl.ds(pl.multiple_of(2 * depth + k * half, half), half)],
                    ch_send.at[n], ch_recv.at[n], axis_nbr[AZ])

    def b_chunk(q, h):
        rows = pl.ds(pl.multiple_of(h * half, half), half)
        n = 16 + 2 * q + h
        return send(b_hbm.at[rows, their_cols(q)], bz_hbm.at[q, rows], ch_send.at[n], ch_recv.at[n], axis_nbr[AZ])

    def last_chunk():
        return send(b_hbm.at[:, last_cols(1 - z)], bz_hbm.at[paired, :, 0:W], ch_send.at[chunks], ch_recv.at[chunks], axis_nbr[AZ])

    def start_chunks(i):
        def body(n, carry):
            when(n, 0, 16, lambda: a_chunk(n).start())
            when(n, 16, chunks, lambda: b_chunk((n - 16) // 2, (n - 16) % 2).start())
            when(n, chunks, chunks + 1, lambda: last_chunk().start())
            return carry

        lax.fori_loop(rate * i // 100 + AHEAD, rate * (i + 1) // 100 + AHEAD, body, 0)

    def end_chunks(i):
        def body(n, carry):
            when(n, 0, 16, lambda: a_chunk(n).wait_send())
            when(n, 16, chunks, lambda: b_chunk((n - 16) // 2, (n - 16) % 2).wait_send())
            when(n, chunks, chunks + 1, lambda: last_chunk().wait_send())
            return carry

        lax.fori_loop(rate * i // 100 + AHEAD, rate * (i + 1) // 100 + AHEAD, body, 0)

    def bx_copy(t):
        return send(b_hbm.at[:, tile_cols(t)], bx_hbm.at[t], bx_send.at[t], bx_recv.at[t], partner)

    def bxz_copy(q):
        return send(bz_hbm.at[q], bxz_hbm.at[q], bxz_send.at[q], bxz_recv.at[q], partner)

    def last_bx():
        return send(b_hbm.at[:, last_cols(z)], bx_hbm.at[last, :, 0:W], bx_send.at[last], bx_recv.at[last], partner)

    def last_bxz():
        return send(bz_hbm.at[paired, :, 0:W], bxz_hbm.at[paired, :, 0:W], bxz_send.at[paired], bxz_recv.at[paired], partner)

    def last_piece(k):
        src = (b_hbm.at[:, last_cols(z)], bx_hbm.at[last, :, 0:W], bz_hbm.at[paired, :, 0:W], bxz_hbm.at[paired, :, 0:W])[k]
        return pltpu.make_async_copy(src, b_v.at[last % 2, pl.ds(k * depth, depth), 0:W], b_sem.at[last % 2, k])

    def b_piece(t, k):
        src = (b_hbm.at[:, tile_cols(t)], bx_hbm.at[t], bz_hbm.at[t - plain], bxz_hbm.at[t - plain])[k]
        return pltpu.make_async_copy(src, b_v.at[t % 2, pl.ds(k * depth, depth)], b_sem.at[t % 2, k])

    def fetch_near(t):
        b_piece(t, 0).start()
        bx_copy(t).wait_recv()
        b_piece(t, 1).start()

    def fetch_far(t):
        with jax.named_scope("b_chunk"):
            for h in both:
                b_chunk(t - plain, h).wait_recv()
        bxz_copy(t - plain).start()
        b_piece(t, 2).start()

    def fetch_last(t):
        with jax.named_scope("bxz"):
            bxz_copy(t - plain).wait_recv()
        b_piece(t, 3).start()

    def last_near():
        last_piece(0).start()
        last_bx().wait_recv()
        last_piece(1).start()

    def last_far():
        with jax.named_scope("last_chunk"):
            last_chunk().wait_recv()
        last_bxz().start()
        last_piece(2).start()

    def last_fetch():
        last_bxz().wait_recv()
        last_piece(3).start()

    def partial(t, d, k):
        s = t % 2
        dx, dy, dz = bits_of(d)
        part = jnp.dot(a_v[d, :, 0:k * depth], b_v[s, 0:k * depth], preferred_element_type=jnp.float32)
        p_v[s, 0, dx, dy * 2 + dz] = part[:, 0:W]
        p_v[s, 1, dy, dx * 2 + dz] = part[:, W:C]

    def last_partials():
        s = last % 2

        def body(d, carry):
            dx, dy, dz = bits_of(d)
            part = jnp.dot(a_v[d], b_v[s, :, 0:W], preferred_element_type=jnp.float32)
            p_v[s, 0, dx, dy * 2 + dz, 0:upper] = part[0:upper]
            p_v[s, 1, dy, dx * 2 + dz, 0:upper] = part[upper:rows]
            return carry

        lax.fori_loop(0, 8, body, 0)

    def partials(t, k, n=8, order=lambda j: j):
        def body(j, carry):
            partial(t, order(j), k)
            return carry

        lax.fori_loop(0, n, body, 0)

    def first_two(n, order):
        def body(j, carry):
            partial(j // n, order(j % n), 2)
            return carry

        lax.fori_loop(0, 2 * n, body, 0)

    def send1(t, g, k, n=rows):
        s, blocks, part = t % 2, pl.ds(2 * k, 2), pl.ds(0, n)
        return send(p_v.at[s, g, 1, blocks, part], r1_v.at[s, g, blocks, part],
                    s1_sem.at[s, g, k], r1_sem.at[s, g, k], axis_nbr[g])

    def send2(t, g, k, n=rows):
        s, part = t % 2, pl.ds(0, n)
        return send(s2_v.at[s, g, 2 + k, part], r2_v.at[s, g, k, part],
                    s2_sem.at[s, g, k], r2_sem.at[s, g, k], axis_nbr[1 - g])

    def send3(t, g):
        s = t % D3
        return send(s3_v.at[s, g, 1], r3_v.at[s, g], s3_sem.at[s, g], r3_sem.at[s, g], axis_nbr[AZ])

    def pair_there(t, g):
        s = t % DO
        return send(q_v.at[s, g], c_v.at[:, tile_cols(t, g)], qs_sem.at[s, g], qr_sem.at[t - plain, g], axis_nbr[AZ])

    def last_there(g):
        s = last % DO
        return send(q_v.at[s, g, pl.ds(0, upper)], c_v.at[pl.ds(g * upper, upper), last_cols(z)],
                    qs_sem.at[s, g], qr_sem.at[paired, g], axis_nbr[AZ])

    def take(t, g, phase, slots, high):
        when(t, slots, high, lambda: pl.semaphore_wait(credit.at[phase, g], 1))

    def give(t, g, phase, axis, slots, high):
        when(t, 0, high - slots, lambda: pl.semaphore_signal(
            credit.at[phase, g], inc=1, device_id=axis_nbr[axis], device_id_type=MESH))

    for copy in own:
        copy.start()
    with jax.named_scope("barrier"):
        pl.semaphore_wait(barrier, 4)
    for group in (xy_far1, y_far, z_own, xy_near1, x_far, x_near):
        for copy in group:
            copy.start()
    for t in range(min(LOOK, tiles)):
        bx_copy(t).start()
    for t in range(2):
        fetch_near(t)
    for h in both:
        with jax.named_scope("y_far"):
            y_far[h].wait_recv()
        z_y[h].start()
        with jax.named_scope("xy_far1"):
            xy_far1[h].wait_recv()
        xy_far2[h].start()
    for h in both:
        with jax.named_scope("xy_near1"):
            xy_near1[h].wait_recv()
        xy_near2[h].start()
        with jax.named_scope("xy_far2"):
            xy_far2[h].wait_recv()
        z_xy[h].start()
    for copy in y_near:
        copy.start()
    for t in range(2):
        for k in range(2):
            b_piece(t, k).wait()
    for copy in own:
        copy.wait()
    with jax.named_scope("z_y"):
        for copy in z_own + z_y:
            copy.wait_recv()
    first_two(3, lambda j: j + j // 2)
    for h in both:
        with jax.named_scope("x_far"):
            x_far[h].wait_recv()
        z_x[h].start()
    with jax.named_scope("z_xy"):
        for copy in xy_near2 + z_xy:
            copy.wait_recv()
    first_two(2, lambda j: 6 + j)
    for t in range(2):
        for g in both:
            send1(t, g, 1).start()
    with jax.named_scope("z_x"):
        for copy in x_near + y_near + z_x:
            copy.wait_recv()
    for n in range(AHEAD):
        a_chunk(n).start()

    def last_three(j):
        return 2 + (3 * j + 1) // 2

    def add3(t, g):
        with jax.named_scope("recv3"):
            send3(t, g).wait_recv()
        c_v[:, tile_cols(t, g)] = (s3_v[t % D3, g, 0] + r3_v[t % D3, g]).astype(jnp.bfloat16)

    def start_late():
        def body(t, carry):
            for g in both:
                when(t, D3, plain, lambda g=g: pl.semaphore_wait(credit.at[2, g], 1))
                send3(t, g).start()
            return carry

        lax.fori_loop(plain - LATE, plain, body, 0)

    def end_hops():
        for group in all_hops:
            for copy in group:
                copy.wait_send()
        for n in range(AHEAD):
            a_chunk(n).wait_send()

    def step(i, carry):
        t = i
        when(t, 0, tiles, lambda: start_chunks(t))
        when(t, LAG, tiles + 3, lambda: end_chunks(t - LAG))
        when(t, 1, tiles + 1, lambda: bx_copy(t - 1).wait_send())
        when(t, plain + 1, tiles + 1, lambda: bxz_copy(t - 1 - plain).wait_send())
        when(t, LAG, LAG + 1, end_hops)
        when(t, 0, tiles - LOOK, lambda: bx_copy(t + LOOK).start())
        when(t, tiles - LOOK, tiles - LOOK + 1, lambda: last_bx().start())
        when(t, 1, tiles - 1, lambda: fetch_near(t + 1))
        when(t, tiles - 1, tiles, last_near)
        for g in both:
            for k in both:
                when(t, 2, tiles + 2, lambda g=g, k=k: send1(t - 2, g, k).wait_send())

        def wait_b(pieces):
            for k in range(pieces):
                b_piece(t, k).wait()

        def near_products():
            with jax.named_scope("b_near"):
                wait_b(2)
            with jax.named_scope("dot_near"):
                partials(t, 2)

        def all_products():
            with jax.named_scope("b_all"):
                wait_b(4)
            with jax.named_scope("dot_all"):
                partials(t, 4)

        def last_products():
            with jax.named_scope("b_last"):
                for k in range(4):
                    last_piece(k).wait()
            with jax.named_scope("dot_last"):
                last_partials()
            for g in both:
                pl.semaphore_wait(credit.at[0, g], 1)
                send1(last, g, 1, upper).start()
            for g in both:
                send1(last, g, 0, upper).start()

        def wait_far():
            def body(n, carry):
                a_chunk(n).wait_recv()
                return carry

            with jax.named_scope("a_chunks"):
                lax.fori_loop(0, 16, body, 0)

        when(t, 0, 2, lambda: partials(t, 2, 3, last_three))
        when(t, 2, plain, near_products)
        when(t, plain, plain + 1, wait_far)
        when(t, plain, tiles, all_products)
        when(t, last, last + 1, last_products)
        for g in both:
            take(t, g, 0, 2, tiles)
            when(t, 2, tiles, lambda g=g: send1(t, g, 1).start())
        for g in both:
            when(t, 0, tiles, lambda g=g: send1(t, g, 0).start())
        when(t, plain - 1, tiles - 1, lambda: fetch_far(t + 1))
        when(t, tiles - 1, tiles, last_far)

        t1 = i - 1

        def add1(g, k, n=rows):
            s, blocks, part = t1 % 2, pl.ds(2 * k, 2), pl.ds(0, n)
            with jax.named_scope("recv1"):
                send1(t1, g, k, n).wait_recv()
            s2_v[s, g, blocks, part] = p_v[s, g, 0, blocks, part] + r1_v[s, g, blocks, part]

        def last1():
            for g in both:
                add1(g, 1, upper)
                pl.semaphore_wait(credit.at[1, g], 1)
                for k in (1, 0):
                    send2(last, g, k, upper).start()
            for g in both:
                add1(g, 0, upper)

        for g in both:
            for k in both:
                when(t1, 2, tiles + 2, lambda g=g, k=k: send2(t1 - 2, g, k).wait_send())
            when(t1, 0, tiles, lambda g=g: add1(g, 1))
            take(t1, g, 1, 2, tiles)
            for k in (1, 0):
                when(t1, 0, tiles, lambda g=g, k=k: send2(t1, g, k).start())
        for g in both:
            when(t1, 0, tiles, lambda g=g: add1(g, 0))
            give(t1, g, 0, g, 2, last + 1)
        when(t1, last, last + 1, last1)

        t2 = i - 2

        def sum2(g, k, n=rows):
            part = pl.ds(0, n)
            with jax.named_scope("recv2"):
                send2(t2, g, k, n).wait_recv()
            return s2_v[t2 % 2, g, k, part] + r2_v[t2 % 2, g, k, part]

        def last2():
            for g in both:
                q_v[last % DO, g, pl.ds(0, upper)] = sum2(g, 1, upper).astype(jnp.bfloat16)
                last_there(g).start()
            for g in both:
                c_v[pl.ds(g * upper, upper), last_cols(z)] = sum2(g, 0, upper).astype(jnp.bfloat16)

        def add2(g, k):
            s3_v[t2 % D3, g, k] = sum2(g, k)

        def add2_there(g):
            q_v[t2 % DO, g] = sum2(g, 1).astype(jnp.bfloat16)

        def add2_here(g):
            c_v[:, tile_cols(t2, g)] = sum2(g, 0).astype(jnp.bfloat16)

        for g in both:
            when(t2, D3, plain - LATE + D3, lambda g=g: send3(t2 - D3, g).wait_send())
            when(t2, plain + DO, last + 1, lambda g=g: pair_there(t2 - DO, g).wait_send())
            when(t2, 0, plain, lambda g=g: add2(g, 1))
            when(t2, plain, tiles, lambda g=g: add2_there(g))
            take(t2, g, 2, D3, plain - LATE)
            when(t2, 0, plain - LATE, lambda g=g: send3(t2, g).start())
            when(t2, plain, tiles, lambda g=g: pair_there(t2, g).start())
        for g in both:
            when(t2, 0, plain, lambda g=g: add2(g, 0))
            when(t2, plain, tiles, lambda g=g: add2_here(g))
            give(t2, g, 1, 1 - g, 2, last + 1)
        when(t2, last, last + 1, last2)

        t3 = i - 1 - D3
        for g in both:
            when(t3, 0, plain - LATE, lambda g=g: add3(t3, g))
            give(t3, g, 2, AZ, D3, plain)
        when(t, last - 1, last, start_late)
        when(t, plain - 1, tiles - 1, lambda: fetch_last(t + 1))
        when(t, tiles - 1, tiles, last_fetch)
        return carry

    lax.fori_loop(0, tiles + 3, step, 0)

    def each(low, high, fn):
        def body(n, carry):
            fn(n)
            return carry

        lax.fori_loop(low, high, body, 0)

    for g in both:
        each(plain - LATE, plain, lambda t: add3(t, g))
    with jax.named_scope("end_late"):
        for g in both:
            each(plain - LATE, plain, lambda t: send3(t, g).wait_send())
    with jax.named_scope("end_chunks"):
        each(tiles + 3 - LAG, tiles, end_chunks)
    with jax.named_scope("end_pairs"):
        for g in both:
            each(max(plain, last + 1 - DO), tiles, lambda t: pair_there(t, g).wait_send())
    with jax.named_scope("end_pairs_recv"):
        for g in both:
            each(plain, tiles, lambda t: pair_there(t, g).wait_recv())
    with jax.named_scope("end_last"):
        for g in both:
            for k in both:
                send1(last, g, k, upper).wait_send()
                send2(last, g, k, upper).wait_send()
        last_bx().wait_send()
        last_bxz().wait_send()
    with jax.named_scope("end_last_send"):
        for g in both:
            last_there(g).wait_send()
    with jax.named_scope("end_last_recv"):
        for g in both:
            last_there(g).wait_recv()


def solution(mesh):
    spec_rows = P(("dp", "tp"), None)

    def local_block(a_rows, b_rows):
        rows, inner = a_rows.shape
        depth, columns = b_rows.shape
        plain, paired = counts(columns)
        tiles = plain + paired
        f32, bf16 = jnp.float32, jnp.bfloat16
        dma = pltpu.SemaphoreType.DMA
        out = pl.pallas_call(
            kernel,
            name="matmul_reduce_scatter",
            out_shape=(
                pltpu.VMEM((rows, columns), bf16),
                jax.ShapeDtypeStruct((tiles + 1, depth, C), bf16),
                jax.ShapeDtypeStruct((paired + 1, depth, C), bf16),
                jax.ShapeDtypeStruct((paired + 1, depth, C), bf16),
                jax.ShapeDtypeStruct((2, rows, 2 * depth), bf16),
            ),
            in_specs=[pl.BlockSpec(memory_space=pl.ANY)] * 2,
            out_specs=(pl.BlockSpec(memory_space=pltpu.VMEM),) + (pl.BlockSpec(memory_space=pl.ANY),) * 4,
            scratch_shapes=[
                pltpu.VMEM((8, rows, 4 * depth), bf16),
                pltpu.VMEM((2, 4 * depth, C), bf16),
                pltpu.VMEM((2, 2, 2, 4, rows, W), f32),
                pltpu.VMEM((2, 2, 4, rows, W), f32),
                pltpu.VMEM((2, 2, 4, rows, W), f32),
                pltpu.VMEM((2, 2, 2, rows, W), f32),
                pltpu.VMEM((D3, 2, 2, rows, W), f32),
                pltpu.VMEM((D3, 2, rows, W), f32),
                pltpu.VMEM((DO, 2, rows, W), bf16),
                dma((12, 2)), dma((12, 2)), dma((4,)),
                dma((tiles + 1,)), dma((tiles + 1,)), dma((paired + 1,)), dma((paired + 1,)),
                dma((17 + 2 * paired,)), dma((17 + 2 * paired,)), dma((2, 4)),
                dma((2, 2, 2)), dma((2, 2, 2)), dma((2, 2, 2)), dma((2, 2, 2)), dma((D3, 2)), dma((D3, 2)),
                dma((DO, 2)), dma((paired + 1, 2)),
                pltpu.SemaphoreType.REGULAR((3, 2)),
            ],
            compiler_params=pltpu.CompilerParams(
                collective_id=0, has_side_effects=True, vmem_limit_bytes=56 * 1024 * 1024),
            cost_estimate=pl.CostEstimate(
                flops=2 * 8 * rows * 2 * depth * columns, bytes_accessed=6 * depth * columns, transcendentals=0),
        )(a_rows, b_rows)
        return out[0]

    return jax.shard_map(local_block, mesh=mesh, in_specs=(spec_rows, spec_rows), out_specs=spec_rows, check_vma=False)
```

```python
import jax
import jax.numpy as jnp
from jax import lax
from jax.experimental import pallas as pl
from jax.experimental.pallas import tpu as pltpu
from jax.sharding import PartitionSpec as P

MESH = pl.DeviceIdType.MESH
W = 128
C = 2 * W
LOOK = 4
D3 = 6
DO = 6
LATE = 4
AHEAD = 2
LAG = 5
RX, RZ, RC = 2 * LOOK, LOOK + 1, 8
AX, AY, AZ = 0, 1, 2


def bits_of(d):
    return (d // 4, (d // 2) % 2, d % 2)


def counts(columns):
    paired = columns // C // 4
    return columns // C - 2 * paired - 1, paired


def kernel(a_hbm, b_hbm, c_v, bx_hbm, bz_hbm, bxz_hbm, relay,
           a_v, b_v, p_v, r1_v, s2_v, r2_v, s3_v, r3_v, q_v,
           hop_send, hop_recv, own_sem, bx_send, bx_recv, bxz_send, bxz_recv, ch_send, ch_recv, b_sem,
           s1_sem, r1_sem, s2_sem, r2_sem, s3_sem, r3_sem, qs_sem, qr_sem, credit):
    depth, columns = b_hbm.shape
    plain, paired = counts(columns)
    tiles = plain + paired
    rows, upper = a_hbm.shape[0], a_hbm.shape[0] // 2
    half = depth // 2
    chunks = 16 + 2 * paired
    last = plain + paired
    rate = max(114, -(-1600 // plain), -(-100 * (15 + 2 * paired) // (tiles - 1)))

    dp, tp = lax.axis_index("dp"), lax.axis_index("tp")
    core, x, y, z = dp % 2, (dp // 2) % 2, dp // 4, tp

    def flip(v, bit):
        return v + bit - 2 * v * bit

    def device(bits, other=0):
        return {"dp": flip(y, bits[1]) * 4 + flip(x, bits[0]) * 2 + flip(core, other), "tp": flip(z, bits[2])}

    axis_nbr = [device((1, 0, 0)), device((0, 1, 0)), device((0, 0, 1))]
    partner = device((0, 0, 0), 1)

    barrier = pltpu.get_barrier_semaphore()
    for nbr in (*axis_nbr, partner):
        pl.semaphore_signal(barrier, inc=1, device_id=nbr, device_id_type=MESH)

    def send(src, dst, send_sem, recv_sem, to):
        return pltpu.make_async_remote_copy(
            src_ref=src, dst_ref=dst, send_sem=send_sem, recv_sem=recv_sem, device_id=to, device_id_type=MESH)

    def wait_bytes(ref, sem):
        pltpu.make_async_copy(ref, ref, sem).wait()

    def when(t, low, high, fn):
        pl.when(jnp.logical_and(t >= low, t < high))(fn)

    def is_paired(t):
        return (t + tiles - plain) // tiles

    def tile_cols(t, g=None):
        col = t * C + is_paired(t) * ((t - plain) * C + z * C)
        if g is None:
            return pl.ds(pl.multiple_of(col, W), C)
        return pl.ds(pl.multiple_of(col + g * W, W), W)

    def their_cols(q):
        return pl.ds(pl.multiple_of((plain + 2 * q + 1 - z) * C, W), C)

    def last_cols(side):
        return pl.ds(pl.multiple_of((plain + 2 * paired) * C + side * W, W), W)

    def a_cols(bits, h):
        to = device(bits, h)
        return a_hbm.at[:, pl.ds(pl.multiple_of((to["dp"] * 2 + to["tp"]) * depth, depth), depth)]

    def near(d, h):
        return a_v.at[d, :, pl.ds(h * depth, depth)]

    def far(d, h):
        return a_v.at[d, :, pl.ds((2 + h) * depth, depth)]

    def held(i, h):
        return relay.at[i, :, pl.ds(h * depth, depth)]

    def hop(n, h, src, dst, axis):
        return send(src, dst, hop_send, hop_recv.at[-n - 1 if n < 0 else 3 + 2 * n + h], axis_nbr[axis])

    both = range(2)
    xy_far1 = [hop(0, h, a_cols((1, 1, 1), h), held(0, h), AX) for h in both]
    xy_near1 = [hop(1, h, a_cols((1, 1, 0), h), held(1, h), AX) for h in both]
    x_far = [hop(2, h, a_cols((1, 0, 1), h), far(4, h), AX) for h in both]
    y_far = [hop(3, h, a_cols((0, 1, 1), h), far(2, h), AY) for h in both]
    xy_far2 = [hop(4, h, held(0, h), far(6, h), AY) for h in both]
    z_own = [hop(-1, h, a_cols((0, 0, 1), h), near(1, h), AZ) for h in both]
    z_y = [hop(-1, h, far(2, h), near(3, h), AZ) for h in both]
    xy_near2 = [hop(-2, h, held(1, h), near(6, h), AY) for h in both]
    z_xy = [hop(-2, h, far(6, h), near(7, h), AZ) for h in both]
    x_near = [hop(-3, h, a_cols((1, 0, 0), h), near(4, h), AX) for h in both]
    y_near = [hop(-3, h, a_cols((0, 1, 0), h), near(2, h), AY) for h in both]
    z_x = [hop(-3, h, far(4, h), near(5, h), AZ) for h in both]
    hops = 24

    def end_group(n, copies):
        wait_bytes(a_v.at[pl.ds(0, copies // 2), :, pl.ds(0, 2 * depth)], hop_recv.at[n - 1])

    own = [pltpu.make_async_copy(a_cols((0, 0, 0), h), near(0, h), own_sem) for h in both]
    own += [pltpu.make_async_copy(a_cols((0, 0, 1), h), far(0, h), own_sem) for h in both]

    def a_chunk(n):
        d, k = (n // 4) * 2, n % 4
        return send(a_v.at[d, :, pl.ds(pl.multiple_of(k * half, half), half)],
                    a_v.at[d + 1, :, pl.ds(pl.multiple_of(2 * depth + k * half, half), half)],
                    ch_send.at[n % RC], ch_recv.at[0], axis_nbr[AZ])

    def b_chunk(q, h):
        rows = pl.ds(pl.multiple_of(h * half, half), half)
        n = 16 + 2 * q + h
        return send(b_hbm.at[rows, their_cols(q)], bz_hbm.at[q, rows], ch_send.at[n % RC], ch_recv.at[1 + q], axis_nbr[AZ])

    def last_chunk():
        return send(b_hbm.at[:, last_cols(1 - z)], bz_hbm.at[paired, :, 0:W], ch_send.at[chunks % RC], ch_recv.at[1 + paired], axis_nbr[AZ])

    def start_chunks(i):
        def body(n, carry):
            when(n, 0, 16, lambda: a_chunk(n).start())
            when(n, 16, chunks, lambda: b_chunk((n - 16) // 2, (n - 16) % 2).start())
            when(n, chunks, chunks + 1, lambda: last_chunk().start())
            return carry

        lax.fori_loop(rate * i // 100 + AHEAD, rate * (i + 1) // 100 + AHEAD, body, 0)

    def end_chunks(i):
        def body(n, carry):
            when(n, 0, 16, lambda: a_chunk(n).wait_send())
            when(n, 16, chunks, lambda: b_chunk((n - 16) // 2, (n - 16) % 2).wait_send())
            when(n, chunks, chunks + 1, lambda: last_chunk().wait_send())
            return carry

        lax.fori_loop(rate * i // 100 + AHEAD, rate * (i + 1) // 100 + AHEAD, body, 0)

    def bx_copy(t):
        return send(b_hbm.at[:, tile_cols(t)], bx_hbm.at[t], bx_send.at[t % RX], bx_recv.at[t % RX], partner)

    def bxz_copy(q):
        return send(bz_hbm.at[q], bxz_hbm.at[q], bxz_send.at[q % RZ], bxz_recv.at[q % RZ], partner)

    def last_bx():
        return send(b_hbm.at[:, last_cols(z)], bx_hbm.at[last, :, 0:W], bx_send.at[last % RX], bx_recv.at[last % RX], partner)

    def last_bxz():
        return send(bz_hbm.at[paired, :, 0:W], bxz_hbm.at[paired, :, 0:W], bxz_send.at[paired % RZ], bxz_recv.at[paired % RZ], partner)

    def last_piece(k):
        src = (b_hbm.at[:, last_cols(z)], bx_hbm.at[last, :, 0:W], bz_hbm.at[paired, :, 0:W], bxz_hbm.at[paired, :, 0:W])[k]
        return pltpu.make_async_copy(src, b_v.at[last % 2, pl.ds(k * depth, depth), 0:W], b_sem.at[last % 2])

    def b_piece(t, k):
        src = (b_hbm.at[:, tile_cols(t)], bx_hbm.at[t], bz_hbm.at[t - plain], bxz_hbm.at[t - plain])[k]
        return pltpu.make_async_copy(src, b_v.at[t % 2, pl.ds(k * depth, depth)], b_sem.at[t % 2])

    def fetch_near(t):
        b_piece(t, 0).start()
        bx_copy(t).wait_recv()
        b_piece(t, 1).start()

    def fetch_far(t):
        with jax.named_scope("b_chunk"):
            wait_bytes(bz_hbm.at[t - plain], ch_recv.at[1 + t - plain])
        bxz_copy(t - plain).start()
        b_piece(t, 2).start()

    def fetch_last(t):
        with jax.named_scope("bxz"):
            bxz_copy(t - plain).wait_recv()
        b_piece(t, 3).start()

    def last_near():
        last_piece(0).start()
        last_bx().wait_recv()
        last_piece(1).start()

    def last_far():
        with jax.named_scope("last_chunk"):
            last_chunk().wait_recv()
        last_bxz().start()
        last_piece(2).start()

    def last_fetch():
        last_bxz().wait_recv()
        last_piece(3).start()

    def partial(t, d, k):
        s = t % 2
        dx, dy, dz = bits_of(d)
        part = jnp.dot(a_v[d, :, 0:k * depth], b_v[s, 0:k * depth], preferred_element_type=jnp.float32)
        p_v[s, 0, dx, dy * 2 + dz] = part[:, 0:W]
        p_v[s, 1, dy, dx * 2 + dz] = part[:, W:C]

    def last_partials():
        s = last % 2

        def body(d, carry):
            dx, dy, dz = bits_of(d)
            part = jnp.dot(a_v[d], b_v[s, :, 0:W], preferred_element_type=jnp.float32)
            p_v[s, 0, dx, dy * 2 + dz, 0:upper] = part[0:upper]
            p_v[s, 1, dy, dx * 2 + dz, 0:upper] = part[upper:rows]
            return carry

        lax.fori_loop(0, 8, body, 0)

    def partials(t, k, n=8, order=lambda j: j):
        def body(j, carry):
            partial(t, order(j), k)
            return carry

        lax.fori_loop(0, n, body, 0)

    def first_two(n, order):
        def body(j, carry):
            partial(j // n, order(j % n), 2)
            return carry

        lax.fori_loop(0, 2 * n, body, 0)

    def send1(t, g, k, n=rows):
        s, blocks, part = t % 2, pl.ds(2 * k, 2), pl.ds(0, n)
        return send(p_v.at[s, g, 1, blocks, part], r1_v.at[s, g, blocks, part],
                    s1_sem.at[s, g], r1_sem.at[s, g, k], axis_nbr[g])

    def send2(t, g, k, n=rows):
        s, part = t % 2, pl.ds(0, n)
        return send(s2_v.at[s, g, 2 + k, part], r2_v.at[s, g, k, part],
                    s2_sem.at[s, g], r2_sem.at[s, g, k], axis_nbr[1 - g])

    def sent1(t, g, n=rows):
        wait_bytes(p_v.at[t % 2, g, 1, :, pl.ds(0, n)], s1_sem.at[t % 2, g])

    def sent2(t, g, n=rows):
        wait_bytes(r2_v.at[t % 2, g, :, pl.ds(0, n)], s2_sem.at[t % 2, g])

    def send3(t, g):
        s = t % D3
        return send(s3_v.at[s, g, 1], r3_v.at[s, g], s3_sem.at[s], r3_sem.at[s], axis_nbr[AZ])

    def pair_there(t, g):
        s = t % DO
        return send(q_v.at[s, g], c_v.at[:, tile_cols(t, g)], qs_sem.at[s], qr_sem, axis_nbr[AZ])

    def last_there(g):
        s = last % DO
        return send(q_v.at[s, g, pl.ds(0, upper)], c_v.at[pl.ds(g * upper, upper), last_cols(z)],
                    qs_sem.at[s], qr_sem, axis_nbr[AZ])

    def sent3(t):
        wait_bytes(r3_v.at[t % D3], s3_sem.at[t % D3])

    def got3(t):
        with jax.named_scope("recv3"):
            wait_bytes(r3_v.at[t % D3], r3_sem.at[t % D3])

    def pair_sent(t):
        wait_bytes(q_v.at[t % DO], qs_sem.at[t % DO])

    def take(t, g, phase, slots, high):
        when(t, slots, high, lambda: pl.semaphore_wait(credit.at[phase, g], 1))

    def give(t, g, phase, axis, slots, high):
        when(t, 0, high - slots, lambda: pl.semaphore_signal(
            credit.at[phase, g], inc=1, device_id=axis_nbr[axis], device_id_type=MESH))

    for copy in own:
        copy.start()
    with jax.named_scope("barrier"):
        pl.semaphore_wait(barrier, 4)
    for group in (xy_far1, y_far, z_own, xy_near1, x_far, x_near):
        for copy in group:
            copy.start()
    for t in range(min(LOOK, tiles)):
        bx_copy(t).start()
    for t in range(2):
        fetch_near(t)
    for h in both:
        with jax.named_scope("y_far"):
            y_far[h].wait_recv()
        z_y[h].start()
        with jax.named_scope("xy_far1"):
            xy_far1[h].wait_recv()
        xy_far2[h].start()
    for h in both:
        with jax.named_scope("xy_near1"):
            xy_near1[h].wait_recv()
        xy_near2[h].start()
        with jax.named_scope("xy_far2"):
            xy_far2[h].wait_recv()
        z_xy[h].start()
    for copy in y_near:
        copy.start()
    for t in range(2):
        wait_bytes(b_v.at[t, pl.ds(0, 2 * depth)], b_sem.at[t])
    wait_bytes(a_v.at[0], own_sem)
    with jax.named_scope("z_y"):
        end_group(1, 4)
    first_two(3, lambda j: j + j // 2)
    for h in both:
        with jax.named_scope("x_far"):
            x_far[h].wait_recv()
        z_x[h].start()
    with jax.named_scope("z_xy"):
        end_group(2, 4)
    first_two(2, lambda j: 6 + j)
    for t in range(2):
        for g in both:
            send1(t, g, 1).start()
    with jax.named_scope("z_x"):
        end_group(3, 6)
    for n in range(AHEAD):
        a_chunk(n).start()

    def last_three(j):
        return 2 + (3 * j + 1) // 2

    def add3(t, g):
        c_v[:, tile_cols(t, g)] = (s3_v[t % D3, g, 0] + r3_v[t % D3, g]).astype(jnp.bfloat16)

    def start_late():
        def body(t, carry):
            for g in both:
                when(t, D3, plain, lambda g=g: pl.semaphore_wait(credit.at[2, g], 1))
                send3(t, g).start()
            return carry

        lax.fori_loop(plain - LATE, plain, body, 0)

    def end_hops():
        wait_bytes(a_v.at[pl.ds(0, hops // 4)], hop_send)
        for n in range(AHEAD):
            a_chunk(n).wait_send()

    def step(i, carry):
        t = i
        when(t, 0, tiles, lambda: start_chunks(t))
        when(t, LAG, tiles + 3, lambda: end_chunks(t - LAG))
        when(t, 1, tiles + 1, lambda: bx_copy(t - 1).wait_send())
        when(t, plain + 1, tiles + 1, lambda: bxz_copy(t - 1 - plain).wait_send())
        when(t, LAG, LAG + 1, end_hops)
        when(t, 0, tiles - LOOK, lambda: bx_copy(t + LOOK).start())
        when(t, tiles - LOOK, tiles - LOOK + 1, lambda: last_bx().start())
        when(t, 1, tiles - 1, lambda: fetch_near(t + 1))
        when(t, tiles - 1, tiles, last_near)
        for g in both:
            when(t, 2, tiles + 2, lambda g=g: sent1(t - 2, g))

        def wait_b(pieces):
            wait_bytes(b_v.at[t % 2, pl.ds(0, pieces * depth)], b_sem.at[t % 2])

        def near_products():
            with jax.named_scope("b_near"):
                wait_b(2)
            with jax.named_scope("dot_near"):
                partials(t, 2)

        def all_products():
            with jax.named_scope("b_all"):
                wait_b(4)
            with jax.named_scope("dot_all"):
                partials(t, 4)

        def last_products():
            with jax.named_scope("b_last"):
                wait_bytes(b_v.at[last % 2, :, 0:W], b_sem.at[last % 2])
            with jax.named_scope("dot_last"):
                last_partials()
            for g in both:
                pl.semaphore_wait(credit.at[0, g], 1)
                send1(last, g, 1, upper).start()
            for g in both:
                send1(last, g, 0, upper).start()

        def wait_far():
            with jax.named_scope("a_chunks"):
                wait_bytes(a_v.at[pl.ds(0, 4), :, pl.ds(2 * depth, 2 * depth)], ch_recv.at[0])

        when(t, 0, 2, lambda: partials(t, 2, 3, last_three))
        when(t, 2, plain, near_products)
        when(t, plain, plain + 1, wait_far)
        when(t, plain, tiles, all_products)
        when(t, last, last + 1, last_products)
        for g in both:
            take(t, g, 0, 2, tiles)
            when(t, 2, tiles, lambda g=g: send1(t, g, 1).start())
        for g in both:
            when(t, 0, tiles, lambda g=g: send1(t, g, 0).start())
        when(t, plain - 1, tiles - 1, lambda: fetch_far(t + 1))
        when(t, tiles - 1, tiles, last_far)

        t1 = i - 1

        def add1(g, k, n=rows):
            s, blocks, part = t1 % 2, pl.ds(2 * k, 2), pl.ds(0, n)
            with jax.named_scope("recv1"):
                send1(t1, g, k, n).wait_recv()
            s2_v[s, g, blocks, part] = p_v[s, g, 0, blocks, part] + r1_v[s, g, blocks, part]

        def last1():
            for g in both:
                add1(g, 1, upper)
                pl.semaphore_wait(credit.at[1, g], 1)
                for k in (1, 0):
                    send2(last, g, k, upper).start()
            for g in both:
                add1(g, 0, upper)

        for g in both:
            when(t1, 2, tiles + 2, lambda g=g: sent2(t1 - 2, g))
            when(t1, 0, tiles, lambda g=g: add1(g, 1))
            take(t1, g, 1, 2, tiles)
            for k in (1, 0):
                when(t1, 0, tiles, lambda g=g, k=k: send2(t1, g, k).start())
        for g in both:
            when(t1, 0, tiles, lambda g=g: add1(g, 0))
            give(t1, g, 0, g, 2, last + 1)
        when(t1, last, last + 1, last1)

        t2 = i - 2

        def sum2(g, k, n=rows):
            part = pl.ds(0, n)
            with jax.named_scope("recv2"):
                send2(t2, g, k, n).wait_recv()
            return s2_v[t2 % 2, g, k, part] + r2_v[t2 % 2, g, k, part]

        def last2():
            for g in both:
                q_v[last % DO, g, pl.ds(0, upper)] = sum2(g, 1, upper).astype(jnp.bfloat16)
                last_there(g).start()
            for g in both:
                c_v[pl.ds(g * upper, upper), last_cols(z)] = sum2(g, 0, upper).astype(jnp.bfloat16)

        def add2(g, k):
            s3_v[t2 % D3, g, k] = sum2(g, k)

        def add2_there(g):
            q_v[t2 % DO, g] = sum2(g, 1).astype(jnp.bfloat16)

        def add2_here(g):
            c_v[:, tile_cols(t2, g)] = sum2(g, 0).astype(jnp.bfloat16)

        when(t2, D3, plain - LATE + D3, lambda: sent3(t2 - D3))
        when(t2, plain + DO, last + 1, lambda: pair_sent(t2 - DO))
        for g in both:
            when(t2, 0, plain, lambda g=g: add2(g, 1))
            when(t2, plain, tiles, lambda g=g: add2_there(g))
            take(t2, g, 2, D3, plain - LATE)
            when(t2, 0, plain - LATE, lambda g=g: send3(t2, g).start())
            when(t2, plain, tiles, lambda g=g: pair_there(t2, g).start())
        for g in both:
            when(t2, 0, plain, lambda g=g: add2(g, 0))
            when(t2, plain, tiles, lambda g=g: add2_here(g))
            give(t2, g, 1, 1 - g, 2, last + 1)
        when(t2, last, last + 1, last2)

        t3 = i - 1 - D3
        when(t3, 0, plain - LATE, lambda: got3(t3))
        for g in both:
            when(t3, 0, plain - LATE, lambda g=g: add3(t3, g))
            give(t3, g, 2, AZ, D3, plain)
        when(t, last - 1, last, start_late)
        when(t, plain - 1, tiles - 1, lambda: fetch_last(t + 1))
        when(t, tiles - 1, tiles, last_fetch)
        return carry

    lax.fori_loop(0, tiles + 3, step, 0)

    def each(low, high, fn):
        def body(n, carry):
            fn(n)
            return carry

        lax.fori_loop(low, high, body, 0)

    each(plain - LATE, plain, got3)
    for g in both:
        each(plain - LATE, plain, lambda t: add3(t, g))
    each(plain - LATE, plain, sent3)
    each(tiles + 3 - LAG, tiles, end_chunks)
    each(max(plain, last + 1 - DO), tiles, pair_sent)
    for g in both:
        sent1(last, g, upper)
        sent2(last, g, upper)
    last_bx().wait_send()
    last_bxz().wait_send()
    wait_bytes(q_v.at[last % DO, :, pl.ds(0, upper)], qs_sem.at[last % DO])
    with jax.named_scope("end"):
        wait_bytes(c_v.at[:, pl.ds(0, paired * C + W)], qr_sem)


def solution(mesh):
    spec_rows = P(("dp", "tp"), None)

    def local_block(a_rows, b_rows):
        rows, inner = a_rows.shape
        depth, columns = b_rows.shape
        plain, paired = counts(columns)
        tiles = plain + paired
        f32, bf16 = jnp.float32, jnp.bfloat16
        dma = pltpu.SemaphoreType.DMA
        out = pl.pallas_call(
            kernel,
            name="matmul_reduce_scatter",
            out_shape=(
                pltpu.VMEM((rows, columns), bf16),
                jax.ShapeDtypeStruct((tiles + 1, depth, C), bf16),
                jax.ShapeDtypeStruct((paired + 1, depth, C), bf16),
                jax.ShapeDtypeStruct((paired + 1, depth, C), bf16),
                jax.ShapeDtypeStruct((2, rows, 2 * depth), bf16),
            ),
            in_specs=[pl.BlockSpec(memory_space=pl.ANY)] * 2,
            out_specs=(pl.BlockSpec(memory_space=pltpu.VMEM),) + (pl.BlockSpec(memory_space=pl.ANY),) * 4,
            scratch_shapes=[
                pltpu.VMEM((8, rows, 4 * depth), bf16),
                pltpu.VMEM((2, 4 * depth, C), bf16),
                pltpu.VMEM((2, 2, 2, 4, rows, W), f32),
                pltpu.VMEM((2, 2, 4, rows, W), f32),
                pltpu.VMEM((2, 2, 4, rows, W), f32),
                pltpu.VMEM((2, 2, 2, rows, W), f32),
                pltpu.VMEM((D3, 2, 2, rows, W), f32),
                pltpu.VMEM((D3, 2, rows, W), f32),
                pltpu.VMEM((DO, 2, rows, W), bf16),
                dma, dma((13,)), dma, dma((RX,)), dma((RX,)), dma((RZ,)), dma((RZ,)), dma((RC,)), dma((2 + paired,)), dma((2,)),
                dma((2, 2)), dma((2, 2, 2)), dma((2, 2)), dma((2, 2, 2)), dma((D3,)), dma((D3,)), dma((DO,)), dma,
                pltpu.SemaphoreType.REGULAR((3, 2)),
            ],
            compiler_params=pltpu.CompilerParams(
                collective_id=0, has_side_effects=True, vmem_limit_bytes=56 * 1024 * 1024),
            cost_estimate=pl.CostEstimate(
                flops=2 * 8 * rows * 2 * depth * columns, bytes_accessed=6 * depth * columns, transcendentals=0),
        )(a_rows, b_rows)
        return out[0]

    return jax.shard_map(local_block, mesh=mesh, in_specs=(spec_rows, spec_rows), out_specs=spec_rows, check_vma=False)
```

```python
import jax
import jax.numpy as jnp
from jax import lax
from jax.experimental import pallas as pl
from jax.experimental.pallas import tpu as pltpu
from jax.sharding import PartitionSpec as P

MESH = pl.DeviceIdType.MESH
W = 128
C = 2 * W
LOOK = 4
D3 = 6
DO = 6
LATE = 4
AHEAD = 2
LAG = 5
RX, RZ, RC = 2 * LOOK, LOOK + 1, 8
AX, AY, AZ = 0, 1, 2


def bits_of(d):
    return (d // 4, (d // 2) % 2, d % 2)


def counts(columns):
    paired = columns // C // 4
    return columns // C - 2 * paired - 1, paired


def kernel(a_hbm, b_hbm, c_v, bx_hbm, bz_hbm, bxz_hbm, relay,
           a_v, b_v, p_v, r1_v, s2_v, r2_v, s3_v, r3_v, q_v,
           hop_send, hop_recv, own_sem, bx_send, bx_recv, bxz_send, bxz_recv, ch_send, ch_recv, b_sem,
           s1_sem, r1_sem, s2_sem, r2_sem, s3_sem, r3_sem, qs_sem, qr_sem, credit):
    depth, columns = b_hbm.shape
    plain, paired = counts(columns)
    tiles = plain + paired
    rows, upper = a_hbm.shape[0], a_hbm.shape[0] // 2
    half = depth // 2
    chunks = 16 + 2 * paired
    last = plain + paired
    rate = max(114, -(-1600 // plain), -(-100 * (15 + 2 * paired) // (tiles - 1)))

    dp, tp = lax.axis_index("dp"), lax.axis_index("tp")
    core, x, y, z = dp % 2, (dp // 2) % 2, dp // 4, tp

    def flip(v, bit):
        return v + bit - 2 * v * bit

    def device(bits, other=0):
        return {"dp": flip(y, bits[1]) * 4 + flip(x, bits[0]) * 2 + flip(core, other), "tp": flip(z, bits[2])}

    axis_nbr = [device((1, 0, 0)), device((0, 1, 0)), device((0, 0, 1))]
    partner = device((0, 0, 0), 1)

    barrier = pltpu.get_barrier_semaphore()
    for nbr in (*axis_nbr, partner):
        pl.semaphore_signal(barrier, inc=1, device_id=nbr, device_id_type=MESH)

    def send(src, dst, send_sem, recv_sem, to):
        return pltpu.make_async_remote_copy(
            src_ref=src, dst_ref=dst, send_sem=send_sem, recv_sem=recv_sem, device_id=to, device_id_type=MESH)

    def wait_bytes(ref, sem):
        pltpu.make_async_copy(ref, ref, sem).wait()

    def when(t, low, high, fn):
        pl.when(jnp.logical_and(t >= low, t < high))(fn)

    def is_paired(t):
        return (t + tiles - plain) // tiles

    def tile_cols(t, g=None):
        col = t * C + is_paired(t) * ((t - plain) * C + z * C)
        if g is None:
            return pl.ds(pl.multiple_of(col, W), C)
        return pl.ds(pl.multiple_of(col + g * W, W), W)

    def their_cols(q):
        return pl.ds(pl.multiple_of((plain + 2 * q + 1 - z) * C, W), C)

    def last_cols(side):
        return pl.ds(pl.multiple_of((plain + 2 * paired) * C + side * W, W), W)

    def a_cols(bits, h):
        to = device(bits, h)
        return a_hbm.at[:, pl.ds(pl.multiple_of((to["dp"] * 2 + to["tp"]) * depth, depth), depth)]

    def near(d, h):
        return a_v.at[d, :, pl.ds(h * depth, depth)]

    def far(d, h):
        return a_v.at[d, :, pl.ds((2 + h) * depth, depth)]

    def held(i, h):
        return relay.at[i, :, pl.ds(h * depth, depth)]

    def hop(n, h, src, dst, axis):
        return send(src, dst, hop_send, hop_recv.at[-n - 1 if n < 0 else 3 + 2 * n + h], axis_nbr[axis])

    both = range(2)
    xy_far1 = [hop(0, h, a_cols((1, 1, 1), h), held(0, h), AX) for h in both]
    xy_near1 = [hop(1, h, a_cols((1, 1, 0), h), held(1, h), AX) for h in both]
    x_far = [hop(2, h, a_cols((1, 0, 1), h), far(4, h), AX) for h in both]
    y_far = [hop(3, h, a_cols((0, 1, 1), h), far(2, h), AY) for h in both]
    xy_far2 = [hop(4, h, held(0, h), far(6, h), AY) for h in both]
    z_own = [hop(-1, h, a_cols((0, 0, 1), h), near(1, h), AZ) for h in both]
    z_y = [hop(-1, h, far(2, h), near(3, h), AZ) for h in both]
    xy_near2 = [hop(-2, h, held(1, h), near(6, h), AY) for h in both]
    z_xy = [hop(-2, h, far(6, h), near(7, h), AZ) for h in both]
    x_near = [hop(-3, h, a_cols((1, 0, 0), h), near(4, h), AX) for h in both]
    y_near = [hop(-3, h, a_cols((0, 1, 0), h), near(2, h), AY) for h in both]
    z_x = [hop(-3, h, far(4, h), near(5, h), AZ) for h in both]
    hops = 24

    def end_group(n, copies):
        wait_bytes(a_v.at[pl.ds(0, copies // 2), :, pl.ds(0, 2 * depth)], hop_recv.at[n - 1])

    own = [pltpu.make_async_copy(a_cols((0, 0, 0), h), near(0, h), own_sem) for h in both]
    own += [pltpu.make_async_copy(a_cols((0, 0, 1), h), far(0, h), own_sem) for h in both]

    def a_chunk(n):
        d, k = (n // 4) * 2, n % 4
        return send(a_v.at[d, :, pl.ds(pl.multiple_of(k * half, half), half)],
                    a_v.at[d + 1, :, pl.ds(pl.multiple_of(2 * depth + k * half, half), half)],
                    ch_send.at[n % RC], ch_recv.at[0], axis_nbr[AZ])

    def b_chunk(q, h):
        rows = pl.ds(pl.multiple_of(h * half, half), half)
        n = 16 + 2 * q + h
        return send(b_hbm.at[rows, their_cols(q)], bz_hbm.at[q, rows], ch_send.at[n % RC], ch_recv.at[1 + q], axis_nbr[AZ])

    def last_chunk():
        return send(b_hbm.at[:, last_cols(1 - z)], bz_hbm.at[paired, :, 0:W], ch_send.at[chunks % RC], ch_recv.at[1 + paired], axis_nbr[AZ])

    def start_chunks(i):
        def body(n, carry):
            when(n, 0, 16, lambda: a_chunk(n).start())
            when(n, 16, chunks, lambda: b_chunk((n - 16) // 2, (n - 16) % 2).start())
            when(n, chunks, chunks + 1, lambda: last_chunk().start())
            return carry

        lax.fori_loop(rate * i // 100 + AHEAD, rate * (i + 1) // 100 + AHEAD, body, 0)

    def end_chunks(i):
        def body(n, carry):
            when(n, 0, 16, lambda: a_chunk(n).wait_send())
            when(n, 16, chunks, lambda: b_chunk((n - 16) // 2, (n - 16) % 2).wait_send())
            when(n, chunks, chunks + 1, lambda: last_chunk().wait_send())
            return carry

        lax.fori_loop(rate * i // 100 + AHEAD, rate * (i + 1) // 100 + AHEAD, body, 0)

    def bx_copy(t):
        return send(b_hbm.at[:, tile_cols(t)], bx_hbm.at[t], bx_send.at[t % RX], bx_recv.at[t % RX], partner)

    def bxz_copy(q):
        return send(bz_hbm.at[q], bxz_hbm.at[q], bxz_send.at[q % RZ], bxz_recv.at[q % RZ], partner)

    def last_bx():
        return send(b_hbm.at[:, last_cols(z)], bx_hbm.at[last, :, 0:W], bx_send.at[last % RX], bx_recv.at[last % RX], partner)

    def last_bxz():
        return send(bz_hbm.at[paired, :, 0:W], bxz_hbm.at[paired, :, 0:W], bxz_send.at[paired % RZ], bxz_recv.at[paired % RZ], partner)

    def last_piece(k):
        src = (b_hbm.at[:, last_cols(z)], bx_hbm.at[last, :, 0:W], bz_hbm.at[paired, :, 0:W], bxz_hbm.at[paired, :, 0:W])[k]
        return pltpu.make_async_copy(src, b_v.at[last % 2, pl.ds(k * depth, depth), 0:W], b_sem.at[last % 2])

    def b_piece(t, k):
        src = (b_hbm.at[:, tile_cols(t)], bx_hbm.at[t], bz_hbm.at[t - plain], bxz_hbm.at[t - plain])[k]
        return pltpu.make_async_copy(src, b_v.at[t % 2, pl.ds(k * depth, depth)], b_sem.at[t % 2])

    def fetch_near(t):
        b_piece(t, 0).start()
        bx_copy(t).wait_recv()
        b_piece(t, 1).start()

    def fetch_far(t):
        with jax.named_scope("b_chunk"):
            wait_bytes(bz_hbm.at[t - plain], ch_recv.at[1 + t - plain])
        bxz_copy(t - plain).start()
        b_piece(t, 2).start()

    def fetch_last(t):
        with jax.named_scope("bxz"):
            bxz_copy(t - plain).wait_recv()
        b_piece(t, 3).start()

    def last_near():
        last_piece(0).start()
        last_bx().wait_recv()
        last_piece(1).start()

    def last_far():
        with jax.named_scope("last_chunk"):
            last_chunk().wait_recv()
        last_bxz().start()
        last_piece(2).start()

    def last_fetch():
        last_bxz().wait_recv()
        last_piece(3).start()

    def partial(t, d, k):
        s = t % 2
        dx, dy, dz = bits_of(d)
        part = jnp.dot(a_v[d, :, 0:k * depth], b_v[s, 0:k * depth], preferred_element_type=jnp.float32)
        p_v[s, 0, dx, dy * 2 + dz] = part[:, 0:W]
        p_v[s, 1, dy, dx * 2 + dz] = part[:, W:C]

    def last_partials():
        s = last % 2

        def body(d, carry):
            dx, dy, dz = bits_of(d)
            part = jnp.dot(a_v[d], b_v[s, :, 0:W], preferred_element_type=jnp.float32)
            p_v[s, 0, dx, dy * 2 + dz, 0:upper] = part[0:upper]
            p_v[s, 1, dy, dx * 2 + dz, 0:upper] = part[upper:rows]
            return carry

        lax.fori_loop(0, 8, body, 0)

    def partials(t, k, n=8, order=lambda j: j):
        def body(j, carry):
            partial(t, order(j), k)
            return carry

        lax.fori_loop(0, n, body, 0)

    def first_two(n, order):
        def body(j, carry):
            partial(j // n, order(j % n), 2)
            return carry

        lax.fori_loop(0, 2 * n, body, 0)

    def send1(t, g, k, n=rows):
        s, blocks, part = t % 2, pl.ds(2 * k, 2), pl.ds(0, n)
        return send(p_v.at[s, g, 1, blocks, part], r1_v.at[s, g, blocks, part],
                    s1_sem.at[s, g], r1_sem.at[s, g, k], axis_nbr[g])

    def send2(t, g, k, n=rows):
        s, part = t % 2, pl.ds(0, n)
        return send(s2_v.at[s, g, 2 + k, part], r2_v.at[s, g, k, part],
                    s2_sem.at[s, g], r2_sem.at[s, g, k], axis_nbr[1 - g])

    def sent1(t, g, n=rows):
        wait_bytes(p_v.at[t % 2, g, 1, :, pl.ds(0, n)], s1_sem.at[t % 2, g])

    def sent2(t, g, n=rows):
        wait_bytes(r2_v.at[t % 2, g, :, pl.ds(0, n)], s2_sem.at[t % 2, g])

    def send3(t, g):
        s = t % D3
        return send(s3_v.at[s, g, 1], r3_v.at[s, g], s3_sem.at[s], r3_sem.at[s], axis_nbr[AZ])

    def pair_there(t, g):
        s = t % DO
        return send(q_v.at[s, g], c_v.at[:, tile_cols(t, g)], qs_sem.at[s], qr_sem, axis_nbr[AZ])

    def last_there(g):
        s = last % DO
        return send(q_v.at[s, g, pl.ds(0, upper)], c_v.at[pl.ds(g * upper, upper), last_cols(z)],
                    qs_sem.at[s], qr_sem, axis_nbr[AZ])

    def sent3(t):
        wait_bytes(r3_v.at[t % D3], s3_sem.at[t % D3])

    def got3(t):
        with jax.named_scope("recv3"):
            wait_bytes(r3_v.at[t % D3], r3_sem.at[t % D3])

    def pair_sent(t):
        wait_bytes(q_v.at[t % DO], qs_sem.at[t % DO])

    def take(t, g, phase, slots, high):
        when(t, slots, high, lambda: pl.semaphore_wait(credit.at[phase, g], 1))

    def give(t, g, phase, axis, slots, high):
        when(t, 0, high - slots, lambda: pl.semaphore_signal(
            credit.at[phase, g], inc=1, device_id=axis_nbr[axis], device_id_type=MESH))

    for copy in own:
        copy.start()
    with jax.named_scope("barrier"):
        pl.semaphore_wait(barrier, 4)
    for group in (xy_far1, y_far, z_own, xy_near1, x_far, x_near):
        for copy in group:
            copy.start()
    for t in range(min(LOOK, tiles)):
        bx_copy(t).start()
    for t in range(2):
        fetch_near(t)
    for h in both:
        with jax.named_scope("y_far"):
            y_far[h].wait_recv()
        z_y[h].start()
        with jax.named_scope("xy_far1"):
            xy_far1[h].wait_recv()
        xy_far2[h].start()
    for h in both:
        with jax.named_scope("xy_near1"):
            xy_near1[h].wait_recv()
        xy_near2[h].start()
        with jax.named_scope("xy_far2"):
            xy_far2[h].wait_recv()
        z_xy[h].start()
    for copy in y_near:
        copy.start()
    for t in range(2):
        wait_bytes(b_v.at[t, pl.ds(0, 2 * depth)], b_sem.at[t])
    wait_bytes(a_v.at[0], own_sem)
    with jax.named_scope("z_y"):
        end_group(1, 4)
    first_two(3, lambda j: j + j // 2)
    for h in both:
        with jax.named_scope("x_far"):
            x_far[h].wait_recv()
        z_x[h].start()
    with jax.named_scope("z_xy"):
        end_group(2, 4)
    first_two(2, lambda j: 6 + j)
    for t in range(2):
        for g in both:
            send1(t, g, 1).start()
    with jax.named_scope("z_x"):
        end_group(3, 6)
    for n in range(AHEAD):
        a_chunk(n).start()

    def last_three(j):
        return 2 + (3 * j + 1) // 2

    def add3(t, g):
        c_v[:, tile_cols(t, g)] = (s3_v[t % D3, g, 0] + r3_v[t % D3, g]).astype(jnp.bfloat16)

    def start_late():
        def body(t, carry):
            for g in both:
                when(t, D3, plain, lambda g=g: pl.semaphore_wait(credit.at[2, g], 1))
                send3(t, g).start()
            return carry

        lax.fori_loop(plain - LATE, plain, body, 0)

    def each(low, high, fn):
        def body(n, carry):
            fn(n)
            return carry

        lax.fori_loop(low, high, body, 0)

    def end_hops():
        wait_bytes(a_v.at[pl.ds(0, hops // 4)], hop_send)
        for n in range(AHEAD):
            a_chunk(n).wait_send()

    def step(i, carry):
        t = i
        when(t, 0, tiles, lambda: start_chunks(t))
        when(t, LAG, tiles + 3, lambda: end_chunks(t - LAG))
        when(t, 1, tiles + 1, lambda: bx_copy(t - 1).wait_send())
        when(t, plain + 1, tiles + 1, lambda: bxz_copy(t - 1 - plain).wait_send())
        when(t, LAG, LAG + 1, end_hops)
        when(t, 0, tiles - LOOK, lambda: bx_copy(t + LOOK).start())
        when(t, tiles - LOOK, tiles - LOOK + 1, lambda: last_bx().start())
        when(t, 1, tiles - 1, lambda: fetch_near(t + 1))
        when(t, tiles - 1, tiles, last_near)
        for g in both:
            when(t, 2, tiles + 2, lambda g=g: sent1(t - 2, g))

        def wait_b(pieces):
            wait_bytes(b_v.at[t % 2, pl.ds(0, pieces * depth)], b_sem.at[t % 2])

        def near_products():
            with jax.named_scope("b_near"):
                wait_b(2)
            with jax.named_scope("dot_near"):
                partials(t, 2)

        def all_products():
            with jax.named_scope("b_all"):
                wait_b(4)
            with jax.named_scope("dot_all"):
                partials(t, 4)

        def last_products():
            with jax.named_scope("b_last"):
                wait_bytes(b_v.at[last % 2, :, 0:W], b_sem.at[last % 2])
            with jax.named_scope("dot_last"):
                last_partials()
            for g in both:
                pl.semaphore_wait(credit.at[0, g], 1)
                send1(last, g, 1, upper).start()
            for g in both:
                send1(last, g, 0, upper).start()

        def wait_far():
            with jax.named_scope("a_chunks"):
                wait_bytes(a_v.at[pl.ds(0, 4), :, pl.ds(2 * depth, 2 * depth)], ch_recv.at[0])

        when(t, 0, 2, lambda: partials(t, 2, 3, last_three))
        when(t, 2, plain, near_products)
        when(t, plain, plain + 1, wait_far)
        when(t, plain, tiles, all_products)
        when(t, last, last + 1, last_products)
        for g in both:
            take(t, g, 0, 2, tiles)
            when(t, 2, tiles, lambda g=g: send1(t, g, 1).start())
        for g in both:
            when(t, 0, tiles, lambda g=g: send1(t, g, 0).start())
        when(t, plain - 1, tiles - 1, lambda: fetch_far(t + 1))
        when(t, tiles - 1, tiles, last_far)

        t1 = i - 1

        def add1(g, k, n=rows):
            s, blocks, part = t1 % 2, pl.ds(2 * k, 2), pl.ds(0, n)
            with jax.named_scope("recv1"):
                send1(t1, g, k, n).wait_recv()
            s2_v[s, g, blocks, part] = p_v[s, g, 0, blocks, part] + r1_v[s, g, blocks, part]

        def last1():
            for g in both:
                add1(g, 1, upper)
                pl.semaphore_wait(credit.at[1, g], 1)
                send2(last, g, 1, upper).start()
            for g in both:
                send2(last - 1, g, 0).start()
            for g in both:
                send2(last, g, 0, upper).start()
            for g in both:
                add1(g, 0, upper)

        for g in both:
            when(t1, 2, tiles + 1, lambda g=g: sent2(t1 - 2, g))
            when(t1, 0, tiles, lambda g=g: add1(g, 1))
            take(t1, g, 1, 2, tiles)
            when(t1, 0, tiles, lambda g=g: send2(t1, g, 1).start())
            when(t1, 0, tiles - 1, lambda g=g: send2(t1, g, 0).start())
        for g in both:
            when(t1, 0, tiles, lambda g=g: add1(g, 0))
            give(t1, g, 0, g, 2, last + 1)
        when(t1, last, last + 1, last1)

        t2 = i - 2

        def sum2(t, g, k, n=rows):
            part = pl.ds(0, n)
            with jax.named_scope("recv2"):
                send2(t, g, k, n).wait_recv()
            return s2_v[t % 2, g, k, part] + r2_v[t % 2, g, k, part]

        def last2():
            for g in both:
                q_v[last % DO, g, pl.ds(0, upper)] = sum2(last, g, 1, upper).astype(jnp.bfloat16)
                last_there(g).start()
            each(plain - LATE, plain, got3)
            for g in both:
                each(plain - LATE, plain, lambda t: add3(t, g))
            each(plain - LATE, plain, sent3)
            each(tiles + 3 - LAG, tiles, end_chunks)
            each(max(plain, last + 1 - DO), tiles - 1, pair_sent)
            last_bx().wait_send()
            last_bxz().wait_send()
            for g in both:
                sent1(last, g, upper)
            for g in both:
                add2_here(last - 1, g)
            for g in both:
                c_v[pl.ds(g * upper, upper), last_cols(z)] = sum2(last, g, 0, upper).astype(jnp.bfloat16)

        def add2(g, k):
            s3_v[t2 % D3, g, k] = sum2(t2, g, k)

        def add2_there(g):
            q_v[t2 % DO, g] = sum2(t2, g, 1).astype(jnp.bfloat16)

        def add2_here(t, g):
            c_v[:, tile_cols(t, g)] = sum2(t, g, 0).astype(jnp.bfloat16)

        when(t2, D3, plain - LATE + D3, lambda: sent3(t2 - D3))
        when(t2, plain + DO, last + 1, lambda: pair_sent(t2 - DO))
        for g in both:
            when(t2, 0, plain, lambda g=g: add2(g, 1))
            when(t2, plain, tiles, lambda g=g: add2_there(g))
            take(t2, g, 2, D3, plain - LATE)
            when(t2, 0, plain - LATE, lambda g=g: send3(t2, g).start())
            when(t2, plain, tiles, lambda g=g: pair_there(t2, g).start())
        for g in both:
            when(t2, 0, plain, lambda g=g: add2(g, 0))
            when(t2, plain, tiles - 1, lambda g=g: add2_here(t2, g))
            give(t2, g, 1, 1 - g, 2, last + 1)
        when(t2, last, last + 1, last2)

        t3 = i - 1 - D3
        when(t3, 0, plain - LATE, lambda: got3(t3))
        for g in both:
            when(t3, 0, plain - LATE, lambda g=g: add3(t3, g))
            give(t3, g, 2, AZ, D3, plain)
        when(t, last - 1, last, start_late)
        when(t, plain - 1, tiles - 1, lambda: fetch_last(t + 1))
        when(t, tiles - 1, tiles, last_fetch)
        return carry

    lax.fori_loop(0, tiles + 3, step, 0)

    each(max(plain, tiles - 1), tiles, pair_sent)
    for g in both:
        sent2(last - 1, g)
        sent2(last, g, upper)
    wait_bytes(q_v.at[last % DO, :, pl.ds(0, upper)], qs_sem.at[last % DO])
    with jax.named_scope("end"):
        wait_bytes(c_v.at[:, pl.ds(0, paired * C + W)], qr_sem)


def solution(mesh):
    spec_rows = P(("dp", "tp"), None)

    def local_block(a_rows, b_rows):
        rows, inner = a_rows.shape
        depth, columns = b_rows.shape
        plain, paired = counts(columns)
        tiles = plain + paired
        f32, bf16 = jnp.float32, jnp.bfloat16
        dma = pltpu.SemaphoreType.DMA
        out = pl.pallas_call(
            kernel,
            name="matmul_reduce_scatter",
            out_shape=(
                pltpu.VMEM((rows, columns), bf16),
                jax.ShapeDtypeStruct((tiles + 1, depth, C), bf16),
                jax.ShapeDtypeStruct((paired + 1, depth, C), bf16),
                jax.ShapeDtypeStruct((paired + 1, depth, C), bf16),
                jax.ShapeDtypeStruct((2, rows, 2 * depth), bf16),
            ),
            in_specs=[pl.BlockSpec(memory_space=pl.ANY)] * 2,
            out_specs=(pl.BlockSpec(memory_space=pltpu.VMEM),) + (pl.BlockSpec(memory_space=pl.ANY),) * 4,
            scratch_shapes=[
                pltpu.VMEM((8, rows, 4 * depth), bf16),
                pltpu.VMEM((2, 4 * depth, C), bf16),
                pltpu.VMEM((2, 2, 2, 4, rows, W), f32),
                pltpu.VMEM((2, 2, 4, rows, W), f32),
                pltpu.VMEM((2, 2, 4, rows, W), f32),
                pltpu.VMEM((2, 2, 2, rows, W), f32),
                pltpu.VMEM((D3, 2, 2, rows, W), f32),
                pltpu.VMEM((D3, 2, rows, W), f32),
                pltpu.VMEM((DO, 2, rows, W), bf16),
                dma, dma((13,)), dma, dma((RX,)), dma((RX,)), dma((RZ,)), dma((RZ,)), dma((RC,)), dma((2 + paired,)), dma((2,)),
                dma((2, 2)), dma((2, 2, 2)), dma((2, 2)), dma((2, 2, 2)), dma((D3,)), dma((D3,)), dma((DO,)), dma,
                pltpu.SemaphoreType.REGULAR((3, 2)),
            ],
            compiler_params=pltpu.CompilerParams(
                collective_id=0, has_side_effects=True, vmem_limit_bytes=56 * 1024 * 1024),
            cost_estimate=pl.CostEstimate(
                flops=2 * 8 * rows * 2 * depth * columns, bytes_accessed=6 * depth * columns, transcendentals=0),
        )(a_rows, b_rows)
        return out[0]

    return jax.shard_map(local_block, mesh=mesh, in_specs=(spec_rows, spec_rows), out_specs=spec_rows, check_vma=False)
```

```python
import jax
import jax.numpy as jnp
from jax import lax
from jax.experimental import pallas as pl
from jax.experimental.pallas import tpu as pltpu
from jax.sharding import PartitionSpec as P

MESH = pl.DeviceIdType.MESH
W = 128
C = 2 * W
LOOK = 2
D3 = 6
DO = 6
LATE = 4
AHEAD = 2
LAG = 5
RX, RZ, RC = 2 * LOOK, LOOK + 1, 8
AX, AY, AZ = 0, 1, 2


def bits_of(d):
    return (d // 4, (d // 2) % 2, d % 2)


def counts(columns):
    paired = columns // C // 4
    return columns // C - 2 * paired - 1, paired


def kernel(a_hbm, b_hbm, c_v, bx_hbm, bz_hbm, bxz_hbm, relay,
           a_v, b_v, p_v, r1_v, s2_v, r2_v, s3_v, r3_v, q_v,
           hop_send, own_sem, bx_send, bx_recv, bxz_send, bxz_recv, ch_send, ch_recv, b_sem,
           s1_sem, r1_sem, s2_sem, r2_sem, s3_sem, r3_sem, qs_sem, qr_sem, credit):
    depth, columns = b_hbm.shape
    plain, paired = counts(columns)
    tiles = plain + paired
    rows, upper = a_hbm.shape[0], a_hbm.shape[0] // 2
    half = depth // 2
    chunks = 16 + 2 * paired
    last = plain + paired
    rate = max(114, -(-1600 // plain), -(-100 * (15 + 2 * paired) // (tiles - 1)))

    dp, tp = lax.axis_index("dp"), lax.axis_index("tp")
    core, x, y, z = dp % 2, (dp // 2) % 2, dp // 4, tp

    def flip(v, bit):
        return v + bit - 2 * v * bit

    def device(bits, other=0):
        return {"dp": flip(y, bits[1]) * 4 + flip(x, bits[0]) * 2 + flip(core, other), "tp": flip(z, bits[2])}

    axis_nbr = [device((1, 0, 0)), device((0, 1, 0)), device((0, 0, 1))]
    partner = device((0, 0, 0), 1)

    barrier = pltpu.get_barrier_semaphore()
    for nbr in (*axis_nbr, partner):
        pl.semaphore_signal(barrier, inc=1, device_id=nbr, device_id_type=MESH)

    def send(src, dst, send_sem, recv_sem, to):
        return pltpu.make_async_remote_copy(
            src_ref=src, dst_ref=dst, send_sem=send_sem, recv_sem=recv_sem, device_id=to, device_id_type=MESH)

    def wait_bytes(ref, sem):
        pltpu.make_async_copy(ref, ref, sem).wait()

    def when(t, low, high, fn):
        pl.when(jnp.logical_and(t >= low, t < high))(fn)

    def is_paired(t):
        return (t + tiles - plain) // tiles

    def tile_cols(t, g=None):
        col = t * C + is_paired(t) * ((t - plain) * C + z * C)
        if g is None:
            return pl.ds(pl.multiple_of(col, W), C)
        return pl.ds(pl.multiple_of(col + g * W, W), W)

    def their_cols(q):
        return pl.ds(pl.multiple_of((plain + 2 * q + 1 - z) * C, W), C)

    def last_cols(side):
        return pl.ds(pl.multiple_of((plain + 2 * paired) * C + side * W, W), W)

    def a_cols(bits, h):
        to = device(bits, h)
        return a_hbm.at[:, pl.ds(pl.multiple_of((to["dp"] * 2 + to["tp"]) * depth, depth), depth)]

    def near(d, h):
        return a_v.at[d, :, pl.ds(h * depth, depth)]

    def far(d, h):
        return a_v.at[d, :, pl.ds((2 + h) * depth, depth)]

    def held(i, h):
        return relay.at[i, :, pl.ds(h * depth, depth)]

    def hop(n, h, src, dst, axis):
        return send(src, dst, hop_send, ch_recv.at[-n if n < 0 else 4 + 2 * n + h], axis_nbr[axis])

    both = range(2)
    xy_far1 = [hop(0, h, a_cols((1, 1, 1), h), held(0, h), AX) for h in both]
    xy_near1 = [hop(1, h, a_cols((1, 1, 0), h), held(1, h), AX) for h in both]
    x_far = [hop(2, h, a_cols((1, 0, 1), h), far(4, h), AX) for h in both]
    y_far = [hop(3, h, a_cols((0, 1, 1), h), far(2, h), AY) for h in both]
    xy_far2 = [hop(4, h, held(0, h), far(6, h), AY) for h in both]
    z_own = [hop(-1, h, a_cols((0, 0, 1), h), near(1, h), AZ) for h in both]
    z_y = [hop(-1, h, far(2, h), near(3, h), AZ) for h in both]
    xy_near2 = [hop(-2, h, held(1, h), near(6, h), AY) for h in both]
    z_xy = [hop(-2, h, far(6, h), near(7, h), AZ) for h in both]
    x_near = [hop(-3, h, a_cols((1, 0, 0), h), near(4, h), AX) for h in both]
    y_near = [hop(-3, h, a_cols((0, 1, 0), h), near(2, h), AY) for h in both]
    z_x = [hop(-3, h, far(4, h), near(5, h), AZ) for h in both]
    hops = 24

    def end_group(n, copies):
        wait_bytes(a_v.at[pl.ds(0, copies // 2), :, pl.ds(0, 2 * depth)], ch_recv.at[n])

    own = [pltpu.make_async_copy(a_cols((0, 0, 0), h), near(0, h), own_sem) for h in both]
    own += [pltpu.make_async_copy(a_cols((0, 0, 1), h), far(0, h), own_sem) for h in both]

    def a_chunk(n):
        d, k = (n // 4) * 2, n % 4
        return send(a_v.at[d, :, pl.ds(pl.multiple_of(k * half, half), half)],
                    a_v.at[d + 1, :, pl.ds(pl.multiple_of(2 * depth + k * half, half), half)],
                    ch_send.at[n % RC], ch_recv.at[0], axis_nbr[AZ])

    def b_chunk(q, h):
        rows = pl.ds(pl.multiple_of(h * half, half), half)
        n = 16 + 2 * q + h
        return send(b_hbm.at[rows, their_cols(q)], bz_hbm.at[q, rows], ch_send.at[n % RC], ch_recv.at[1 + q], axis_nbr[AZ])

    def last_chunk():
        return send(b_hbm.at[:, last_cols(1 - z)], bz_hbm.at[paired, :, 0:W], ch_send.at[chunks % RC], ch_recv.at[1 + paired], axis_nbr[AZ])

    def start_chunks(i):
        def body(n, carry):
            when(n, 0, 16, lambda: a_chunk(n).start())
            when(n, 16, chunks, lambda: b_chunk((n - 16) // 2, (n - 16) % 2).start())
            when(n, chunks, chunks + 1, lambda: last_chunk().start())
            return carry

        lax.fori_loop(rate * i // 100 + AHEAD, rate * (i + 1) // 100 + AHEAD, body, 0)

    def end_chunks(i):
        def body(n, carry):
            when(n, 0, 16, lambda: a_chunk(n).wait_send())
            when(n, 16, chunks, lambda: b_chunk((n - 16) // 2, (n - 16) % 2).wait_send())
            when(n, chunks, chunks + 1, lambda: last_chunk().wait_send())
            return carry

        lax.fori_loop(rate * i // 100 + AHEAD, rate * (i + 1) // 100 + AHEAD, body, 0)

    def bx_copy(t):
        return send(b_hbm.at[:, tile_cols(t)], bx_hbm.at[t], bx_send.at[t % RX], bx_recv.at[t % RX], partner)

    def bxz_copy(q):
        return send(bz_hbm.at[q], bxz_hbm.at[q], bxz_send.at[q % RZ], bxz_recv.at[q % RZ], partner)

    def last_bx():
        return send(b_hbm.at[:, last_cols(z)], bx_hbm.at[last, :, 0:W], bx_send.at[last % RX], bx_recv.at[last % RX], partner)

    def last_bxz():
        return send(bz_hbm.at[paired, :, 0:W], bxz_hbm.at[paired, :, 0:W], bxz_send.at[paired % RZ], bxz_recv.at[paired % RZ], partner)

    def last_piece(k):
        src = (b_hbm.at[:, last_cols(z)], bx_hbm.at[last, :, 0:W], bz_hbm.at[paired, :, 0:W], bxz_hbm.at[paired, :, 0:W])[k]
        return pltpu.make_async_copy(src, b_v.at[last % 2, pl.ds(k * depth, depth), 0:W], b_sem.at[last % 2])

    def b_piece(t, k):
        src = (b_hbm.at[:, tile_cols(t)], bx_hbm.at[t], bz_hbm.at[t - plain], bxz_hbm.at[t - plain])[k]
        return pltpu.make_async_copy(src, b_v.at[t % 2, pl.ds(k * depth, depth)], b_sem.at[t % 2])

    def fetch_near(t):
        b_piece(t, 0).start()
        bx_copy(t).wait_recv()
        b_piece(t, 1).start()

    def fetch_far(t):
        wait_bytes(bz_hbm.at[t - plain], ch_recv.at[1 + t - plain])
        bxz_copy(t - plain).start()
        b_piece(t, 2).start()

    def fetch_last(t):
        bxz_copy(t - plain).wait_recv()
        b_piece(t, 3).start()

    def last_near():
        last_piece(0).start()
        last_bx().wait_recv()
        last_piece(1).start()

    def last_far():
        last_chunk().wait_recv()
        last_bxz().start()
        last_piece(2).start()

    def last_fetch():
        last_bxz().wait_recv()
        last_piece(3).start()

    def partial(t, d, k):
        s = t % 2
        dx, dy, dz = bits_of(d)
        part = jnp.dot(a_v[d, :, 0:k * depth], b_v[s, 0:k * depth], preferred_element_type=jnp.float32)
        p_v[s, 0, dx, dy * 2 + dz] = part[:, 0:W]
        p_v[s, 1, dy, dx * 2 + dz] = part[:, W:C]

    def last_partials():
        s = last % 2

        def body(d, carry):
            dx, dy, dz = bits_of(d)
            part = jnp.dot(a_v[d], b_v[s, :, 0:W], preferred_element_type=jnp.float32)
            p_v[s, 0, dx, dy * 2 + dz, 0:upper] = part[0:upper]
            p_v[s, 1, dy, dx * 2 + dz, 0:upper] = part[upper:rows]
            return carry

        lax.fori_loop(0, 8, body, 0)

    def partials(t, k, n=8, order=lambda j: j):
        def body(j, carry):
            partial(t, order(j), k)
            return carry

        lax.fori_loop(0, n, body, 0)

    def first_two(n, order):
        def body(j, carry):
            partial(j // n, order(j % n), 2)
            return carry

        lax.fori_loop(0, 2 * n, body, 0)

    def send1(t, g, k, n=rows):
        s, blocks, part = t % 2, pl.ds(2 * k, 2), pl.ds(0, n)
        return send(p_v.at[s, g, 1, blocks, part], r1_v.at[s, g, blocks, part],
                    s1_sem.at[s, g], r1_sem.at[s, g, k], axis_nbr[g])

    def send2(t, g, k, n=rows):
        s, part = t % 2, pl.ds(0, n)
        return send(s2_v.at[s, g, 2 + k, part], r2_v.at[s, g, k, part],
                    s2_sem.at[s, g], r2_sem.at[s, g, k], axis_nbr[1 - g])

    def sent1(t, g, n=rows):
        wait_bytes(p_v.at[t % 2, g, 1, :, pl.ds(0, n)], s1_sem.at[t % 2, g])

    def sent2(t, g, n=rows):
        wait_bytes(r2_v.at[t % 2, g, :, pl.ds(0, n)], s2_sem.at[t % 2, g])

    def send3(t, g):
        s = t % D3
        return send(s3_v.at[s, g, 1], r3_v.at[s, g], s3_sem.at[s], r3_sem.at[s], axis_nbr[AZ])

    def pair_there(t, g):
        s = t % DO
        return send(q_v.at[s, g], c_v.at[:, tile_cols(t, g)], qs_sem.at[s], qr_sem, axis_nbr[AZ])

    def last_there(g):
        s = last % DO
        return send(q_v.at[s, g, pl.ds(0, upper)], c_v.at[pl.ds(g * upper, upper), last_cols(z)],
                    qs_sem.at[s], qr_sem, axis_nbr[AZ])

    def sent3(t):
        wait_bytes(r3_v.at[t % D3], s3_sem.at[t % D3])

    def got3(t):
        wait_bytes(r3_v.at[t % D3], r3_sem.at[t % D3])

    def pair_sent(t):
        wait_bytes(q_v.at[t % DO], qs_sem.at[t % DO])

    def take(t, g, phase, slots, high):
        when(t, slots, high, lambda: pl.semaphore_wait(credit.at[phase, g], 1))

    def give(t, g, phase, axis, slots, high):
        when(t, 0, high - slots, lambda: pl.semaphore_signal(
            credit.at[phase, g], inc=1, device_id=axis_nbr[axis], device_id_type=MESH))

    for copy in own:
        copy.start()
    pl.semaphore_wait(barrier, 4)
    for group in (xy_far1, y_far, z_own, xy_near1, x_far, x_near):
        for copy in group:
            copy.start()
    for t in range(min(LOOK, tiles)):
        bx_copy(t).start()
    for t in range(2):
        fetch_near(t)
    for h in both:
        y_far[h].wait_recv()
        z_y[h].start()
        xy_far1[h].wait_recv()
        xy_far2[h].start()
    for h in both:
        xy_near1[h].wait_recv()
        xy_near2[h].start()
        xy_far2[h].wait_recv()
        z_xy[h].start()
    for copy in y_near:
        copy.start()
    for t in range(2):
        wait_bytes(b_v.at[t, pl.ds(0, 2 * depth)], b_sem.at[t])
    wait_bytes(a_v.at[0], own_sem)
    end_group(1, 4)
    first_two(3, lambda j: j + j // 2)
    for h in both:
        x_far[h].wait_recv()
        z_x[h].start()
    for n in range(AHEAD):
        a_chunk(n).start()
    end_group(2, 4)
    first_two(2, lambda j: 6 + j)
    for t in range(2):
        for g in both:
            send1(t, g, 1).start()
    end_group(3, 6)

    def last_three(j):
        return 2 + (3 * j + 1) // 2

    def add3(t, g):
        c_v[:, tile_cols(t, g)] = (s3_v[t % D3, g, 0] + r3_v[t % D3, g]).astype(jnp.bfloat16)

    def start_late():
        def body(t, carry):
            for g in both:
                when(t, D3, plain, lambda g=g: pl.semaphore_wait(credit.at[2, g], 1))
                send3(t, g).start()
            return carry

        lax.fori_loop(plain - LATE, plain, body, 0)

    def each(low, high, fn):
        def body(n, carry):
            fn(n)
            return carry

        lax.fori_loop(low, high, body, 0)

    def end_hops():
        wait_bytes(a_v.at[pl.ds(0, hops // 4)], hop_send)
        for n in range(AHEAD):
            a_chunk(n).wait_send()

    def step(i, carry):
        t = i
        when(t, 0, tiles, lambda: start_chunks(t))
        when(t, LAG, tiles + 3, lambda: end_chunks(t - LAG))
        when(t, 1, tiles + 1, lambda: bx_copy(t - 1).wait_send())
        when(t, plain + 1, tiles + 1, lambda: bxz_copy(t - 1 - plain).wait_send())
        when(t, LAG, LAG + 1, end_hops)
        when(t, 0, tiles - LOOK, lambda: bx_copy(t + LOOK).start())
        when(t, tiles - LOOK, tiles - LOOK + 1, lambda: last_bx().start())
        when(t, 1, tiles - 1, lambda: fetch_near(t + 1))
        when(t, tiles - 1, tiles, last_near)
        for g in both:
            when(t, 2, tiles + 2, lambda g=g: sent1(t - 2, g))

        def wait_b(pieces):
            wait_bytes(b_v.at[t % 2, pl.ds(0, pieces * depth)], b_sem.at[t % 2])

        def near_products():
            wait_b(2)
            partials(t, 2)

        def all_products():
            wait_b(4)
            partials(t, 4)

        def last_products():
            wait_bytes(b_v.at[last % 2, :, 0:W], b_sem.at[last % 2])
            last_partials()
            for g in both:
                pl.semaphore_wait(credit.at[0, g], 1)
                send1(last, g, 1, upper).start()
            for g in both:
                send1(last, g, 0, upper).start()

        def wait_far():
            wait_bytes(a_v.at[pl.ds(0, 4), :, pl.ds(2 * depth, 2 * depth)], ch_recv.at[0])

        when(t, 0, 2, lambda: partials(t, 2, 3, last_three))
        when(t, 2, plain, near_products)
        when(t, plain, plain + 1, wait_far)
        when(t, plain, tiles, all_products)
        when(t, last, last + 1, last_products)
        for g in both:
            take(t, g, 0, 2, tiles)
            when(t, 2, tiles, lambda g=g: send1(t, g, 1).start())
        for g in both:
            when(t, 0, tiles, lambda g=g: send1(t, g, 0).start())
        when(t, plain - 1, tiles - 1, lambda: fetch_far(t + 1))
        when(t, tiles - 1, tiles, last_far)

        t1 = i - 1

        def add1(g, k, n=rows):
            s, blocks, part = t1 % 2, pl.ds(2 * k, 2), pl.ds(0, n)
            send1(t1, g, k, n).wait_recv()
            s2_v[s, g, blocks, part] = p_v[s, g, 0, blocks, part] + r1_v[s, g, blocks, part]

        def last1():
            for g in both:
                add1(g, 1, upper)
                pl.semaphore_wait(credit.at[1, g], 1)
                send2(last, g, 1, upper).start()
            for g in both:
                send2(last - 1, g, 0).start()
            for g in both:
                send2(last, g, 0, upper).start()
            for g in both:
                add1(g, 0, upper)

        for g in both:
            when(t1, 2, tiles + 1, lambda g=g: sent2(t1 - 2, g))
            when(t1, 0, tiles, lambda g=g: add1(g, 1))
            take(t1, g, 1, 2, tiles)
            when(t1, 0, tiles, lambda g=g: send2(t1, g, 1).start())
            when(t1, 0, tiles - 1, lambda g=g: send2(t1, g, 0).start())
        for g in both:
            when(t1, 0, tiles, lambda g=g: add1(g, 0))
            give(t1, g, 0, g, 2, last + 1)
        when(t1, last, last + 1, last1)

        t2 = i - 2

        def sum2(t, g, k, n=rows):
            part = pl.ds(0, n)
            send2(t, g, k, n).wait_recv()
            return s2_v[t % 2, g, k, part] + r2_v[t % 2, g, k, part]

        def last2():
            for g in both:
                q_v[last % DO, g, pl.ds(0, upper)] = sum2(last, g, 1, upper).astype(jnp.bfloat16)
                last_there(g).start()
            each(plain - LATE, plain, got3)
            for g in both:
                each(plain - LATE, plain, lambda t: add3(t, g))
            each(plain - LATE, plain, sent3)
            each(tiles + 3 - LAG, tiles, end_chunks)
            each(max(plain, last + 1 - DO), tiles - 1, pair_sent)
            last_bx().wait_send()
            last_bxz().wait_send()
            for g in both:
                sent1(last, g, upper)
            for g in both:
                add2_here(last - 1, g)
            for g in both:
                c_v[pl.ds(g * upper, upper), last_cols(z)] = sum2(last, g, 0, upper).astype(jnp.bfloat16)

        def add2(g, k):
            s3_v[t2 % D3, g, k] = sum2(t2, g, k)

        def add2_there(g):
            q_v[t2 % DO, g] = sum2(t2, g, 1).astype(jnp.bfloat16)

        def add2_here(t, g):
            c_v[:, tile_cols(t, g)] = sum2(t, g, 0).astype(jnp.bfloat16)

        when(t2, D3, plain - LATE + D3, lambda: sent3(t2 - D3))
        when(t2, plain + DO, last + 1, lambda: pair_sent(t2 - DO))
        for g in both:
            when(t2, 0, plain, lambda g=g: add2(g, 1))
            when(t2, plain, tiles, lambda g=g: add2_there(g))
            take(t2, g, 2, D3, plain - LATE)
            when(t2, 0, plain - LATE, lambda g=g: send3(t2, g).start())
            when(t2, plain, tiles, lambda g=g: pair_there(t2, g).start())
        for g in both:
            when(t2, 0, plain, lambda g=g: add2(g, 0))
            when(t2, plain, tiles - 1, lambda g=g: add2_here(t2, g))
            give(t2, g, 1, 1 - g, 2, last + 1)
        when(t2, last, last + 1, last2)

        t3 = i - 1 - D3
        when(t3, 0, plain - LATE, lambda: got3(t3))
        for g in both:
            when(t3, 0, plain - LATE, lambda g=g: add3(t3, g))
            give(t3, g, 2, AZ, D3, plain)
        when(t, last - 1, last, start_late)
        when(t, plain - 1, tiles - 1, lambda: fetch_last(t + 1))
        when(t, tiles - 1, tiles, last_fetch)
        return carry

    lax.fori_loop(0, tiles + 3, step, 0)

    each(max(plain, tiles - 1), tiles, pair_sent)
    for g in both:
        sent2(last - 1, g)
        sent2(last, g, upper)
    wait_bytes(q_v.at[last % DO, :, pl.ds(0, upper)], qs_sem.at[last % DO])
    wait_bytes(c_v.at[:, pl.ds(0, paired * C + W)], qr_sem)


def solution(mesh):
    spec_rows = P(("dp", "tp"), None)

    def local_block(a_rows, b_rows):
        rows, inner = a_rows.shape
        depth, columns = b_rows.shape
        plain, paired = counts(columns)
        tiles = plain + paired
        f32, bf16 = jnp.float32, jnp.bfloat16
        dma = pltpu.SemaphoreType.DMA
        out = pl.pallas_call(
            kernel,
            name="matmul_reduce_scatter",
            out_shape=(
                pltpu.VMEM((rows, columns), bf16),
                jax.ShapeDtypeStruct((tiles + 1, depth, C), bf16),
                jax.ShapeDtypeStruct((paired + 1, depth, C), bf16),
                jax.ShapeDtypeStruct((paired + 1, depth, C), bf16),
                jax.ShapeDtypeStruct((2, rows, 2 * depth), bf16),
            ),
            in_specs=[pl.BlockSpec(memory_space=pl.ANY)] * 2,
            out_specs=(pl.BlockSpec(memory_space=pltpu.VMEM),) + (pl.BlockSpec(memory_space=pl.ANY),) * 4,
            scratch_shapes=[
                pltpu.VMEM((8, rows, 4 * depth), bf16),
                pltpu.VMEM((2, 4 * depth, C), bf16),
                pltpu.VMEM((2, 2, 2, 4, rows, W), f32),
                pltpu.VMEM((2, 2, 4, rows, W), f32),
                pltpu.VMEM((2, 2, 4, rows, W), f32),
                pltpu.VMEM((2, 2, 2, rows, W), f32),
                pltpu.VMEM((D3, 2, 2, rows, W), f32),
                pltpu.VMEM((D3, 2, rows, W), f32),
                pltpu.VMEM((DO, 2, rows, W), bf16),
                dma, dma, dma((RX,)), dma((RX,)), dma((RZ,)), dma((RZ,)), dma((RC,)), dma((max(2 + paired, 14),)), dma((2,)),
                dma((2, 2)), dma((2, 2, 2)), dma((2, 2)), dma((2, 2, 2)), dma((D3,)), dma((D3,)), dma((DO,)), dma,
                pltpu.SemaphoreType.REGULAR((3, 2)),
            ],
            compiler_params=pltpu.CompilerParams(
                collective_id=0, has_side_effects=True, vmem_limit_bytes=56 * 1024 * 1024),
            cost_estimate=pl.CostEstimate(
                flops=2 * 8 * rows * 2 * depth * columns, bytes_accessed=6 * depth * columns, transcendentals=0),
        )(a_rows, b_rows)
        return out[0]

    return jax.shard_map(local_block, mesh=mesh, in_specs=(spec_rows, spec_rows), out_specs=spec_rows, check_vma=False)
```

```python
import jax
import jax.numpy as jnp
from jax import lax
from jax.experimental import pallas as pl
from jax.experimental.pallas import tpu as pltpu
from jax.sharding import PartitionSpec as P

MESH = pl.DeviceIdType.MESH
W = 128
C = 2 * W
LOOK = 2
D3 = 6
DO = 6
LATE = 4
AHEAD = 2
LAG = 5
RX, RZ, RC = 2 * LOOK, LOOK + 1, 8
AX, AY, AZ = 0, 1, 2


def bits_of(d):
    return (d // 4, (d // 2) % 2, d % 2)


def counts(columns):
    paired = columns // C // 4
    return columns // C - 2 * paired - 1, paired


def kernel(a_hbm, b_hbm, c_v, bx_hbm, bz_hbm, bxz_hbm, relay,
           a_v, b_v, p_v, r1_v, s2_v, r2_v, s3_v, r3_v, q_v,
           hop_send, own_sem, bx_send, bx_recv, bxz_send, bxz_recv, ch_send, ch_recv, b_sem,
           s1_sem, r1_sem, s2_sem, r2_sem, s3_sem, r3_sem, qs_sem, qr_sem, credit):
    depth, columns = b_hbm.shape
    plain, paired = counts(columns)
    tiles = plain + paired
    rows, upper = a_hbm.shape[0], a_hbm.shape[0] // 2
    half = depth // 2
    chunks = 16 + 2 * paired
    last = plain + paired
    rate = max(114, -(-1600 // plain), -(-100 * (15 + 2 * paired) // (tiles - 1)))

    dp, tp = lax.axis_index("dp"), lax.axis_index("tp")
    core, x, y, z = dp % 2, (dp // 2) % 2, dp // 4, tp

    def flip(v, bit):
        return v + bit - 2 * v * bit

    def device(bits, other=0):
        return {"dp": flip(y, bits[1]) * 4 + flip(x, bits[0]) * 2 + flip(core, other), "tp": flip(z, bits[2])}

    axis_nbr = [device((1, 0, 0)), device((0, 1, 0)), device((0, 0, 1))]
    partner = device((0, 0, 0), 1)

    barrier = pltpu.get_barrier_semaphore()
    for nbr in (*axis_nbr, partner):
        pl.semaphore_signal(barrier, inc=1, device_id=nbr, device_id_type=MESH)

    def send(src, dst, send_sem, recv_sem, to):
        return pltpu.make_async_remote_copy(
            src_ref=src, dst_ref=dst, send_sem=send_sem, recv_sem=recv_sem, device_id=to, device_id_type=MESH)

    def wait_bytes(ref, sem):
        pltpu.make_async_copy(ref, ref, sem).wait()

    def when(t, low, high, fn):
        pl.when(jnp.logical_and(t >= low, t < high))(fn)

    def is_paired(t):
        return (t + tiles - plain) // tiles

    def tile_cols(t, g=None):
        col = t * C + is_paired(t) * ((t - plain) * C + z * C)
        if g is None:
            return pl.ds(pl.multiple_of(col, W), C)
        return pl.ds(pl.multiple_of(col + g * W, W), W)

    def their_cols(q):
        return pl.ds(pl.multiple_of((plain + 2 * q + 1 - z) * C, W), C)

    def last_cols(side):
        return pl.ds(pl.multiple_of((plain + 2 * paired) * C + side * W, W), W)

    def a_cols(bits, h):
        to = device(bits, h)
        return a_hbm.at[:, pl.ds(pl.multiple_of((to["dp"] * 2 + to["tp"]) * depth, depth), depth)]

    def near(d, h):
        return a_v.at[d, :, pl.ds(h * depth, depth)]

    def far(d, h):
        return a_v.at[d, :, pl.ds((2 + h) * depth, depth)]

    def held(i, h):
        return relay.at[i, :, pl.ds(h * depth, depth)]

    def hop(n, h, src, dst, axis):
        return send(src, dst, hop_send, ch_recv.at[-n if n < 0 else 4 + 2 * n + h], axis_nbr[axis])

    both = range(2)
    xy_far1 = [hop(0, h, a_cols((1, 1, 1), h), held(0, h), AX) for h in both]
    xy_near1 = [hop(1, h, a_cols((1, 1, 0), h), held(1, h), AX) for h in both]
    x_far = [hop(2, h, a_cols((1, 0, 1), h), far(4, h), AX) for h in both]
    y_far = [hop(3, h, a_cols((0, 1, 1), h), far(2, h), AY) for h in both]
    xy_far2 = [hop(4, h, held(0, h), far(6, h), AY) for h in both]
    z_own = [hop(-1, h, a_cols((0, 0, 1), h), near(1, h), AZ) for h in both]
    z_y = [hop(-1, h, far(2, h), near(3, h), AZ) for h in both]
    xy_near2 = [hop(-2, h, held(1, h), near(6, h), AY) for h in both]
    z_xy = [hop(-2, h, far(6, h), near(7, h), AZ) for h in both]
    x_near = [hop(-3, h, a_cols((1, 0, 0), h), near(4, h), AX) for h in both]
    y_near = [hop(-3, h, a_cols((0, 1, 0), h), near(2, h), AY) for h in both]
    z_x = [hop(-3, h, far(4, h), near(5, h), AZ) for h in both]
    hops = 24

    def end_group(n, copies):
        wait_bytes(a_v.at[pl.ds(0, copies // 2), :, pl.ds(0, 2 * depth)], ch_recv.at[n])

    own = [pltpu.make_async_copy(a_cols((0, 0, 0), h), near(0, h), own_sem) for h in both]
    own += [pltpu.make_async_copy(a_cols((0, 0, 1), h), far(0, h), own_sem) for h in both]

    def a_chunk(n):
        d, k = (n // 4) * 2, n % 4
        return send(a_v.at[d, :, pl.ds(pl.multiple_of(k * half, half), half)],
                    a_v.at[d + 1, :, pl.ds(pl.multiple_of(2 * depth + k * half, half), half)],
                    ch_send.at[n % RC], ch_recv.at[0], axis_nbr[AZ])

    def b_chunk(q, h):
        rows = pl.ds(pl.multiple_of(h * half, half), half)
        n = 16 + 2 * q + h
        return send(b_hbm.at[rows, their_cols(q)], bz_hbm.at[q, rows], ch_send.at[n % RC], ch_recv.at[1 + q], axis_nbr[AZ])

    def last_chunk():
        return send(b_hbm.at[:, last_cols(1 - z)], bz_hbm.at[paired, :, 0:W], ch_send.at[chunks % RC], ch_recv.at[1 + paired], axis_nbr[AZ])

    def start_chunks(i):
        def body(n, carry):
            when(n, 0, 16, lambda: a_chunk(n).start())
            when(n, 16, chunks, lambda: b_chunk((n - 16) // 2, (n - 16) % 2).start())
            when(n, chunks, chunks + 1, lambda: last_chunk().start())
            return carry

        lax.fori_loop(rate * i // 100 + AHEAD, rate * (i + 1) // 100 + AHEAD, body, 0)

    def end_chunks(i):
        def body(n, carry):
            when(n, 0, 16, lambda: a_chunk(n).wait_send())
            when(n, 16, chunks, lambda: b_chunk((n - 16) // 2, (n - 16) % 2).wait_send())
            when(n, chunks, chunks + 1, lambda: last_chunk().wait_send())
            return carry

        lax.fori_loop(rate * i // 100 + AHEAD, rate * (i + 1) // 100 + AHEAD, body, 0)

    def bx_copy(t):
        return send(b_hbm.at[:, tile_cols(t)], bx_hbm.at[t], bx_send.at[t % RX], bx_recv.at[t % RX], partner)

    def bxz_copy(q):
        return send(bz_hbm.at[q], bxz_hbm.at[q], bxz_send.at[q % RZ], bxz_recv.at[q % RZ], partner)

    def last_bx():
        return send(b_hbm.at[:, last_cols(z)], bx_hbm.at[last, :, 0:W], bx_send.at[last % RX], bx_recv.at[last % RX], partner)

    def last_bxz():
        return send(bz_hbm.at[paired, :, 0:W], bxz_hbm.at[paired, :, 0:W], bxz_send.at[paired % RZ], bxz_recv.at[paired % RZ], partner)

    def last_piece(k):
        src = (b_hbm.at[:, last_cols(z)], bx_hbm.at[last, :, 0:W], bz_hbm.at[paired, :, 0:W], bxz_hbm.at[paired, :, 0:W])[k]
        return pltpu.make_async_copy(src, b_v.at[last % 2, pl.ds(k * depth, depth), 0:W], b_sem.at[last % 2])

    def b_piece(t, k):
        src = (b_hbm.at[:, tile_cols(t)], bx_hbm.at[t], bz_hbm.at[t - plain], bxz_hbm.at[t - plain])[k]
        return pltpu.make_async_copy(src, b_v.at[t % 2, pl.ds(k * depth, depth)], b_sem.at[t % 2])

    def fetch_near(t):
        b_piece(t, 0).start()
        bx_copy(t).wait_recv()
        b_piece(t, 1).start()

    def fetch_far(t):
        wait_bytes(bz_hbm.at[t - plain], ch_recv.at[1 + t - plain])
        bxz_copy(t - plain).start()
        b_piece(t, 2).start()

    def fetch_last(t):
        bxz_copy(t - plain).wait_recv()
        b_piece(t, 3).start()

    def last_near():
        last_piece(0).start()
        last_bx().wait_recv()
        last_piece(1).start()

    def last_far():
        last_chunk().wait_recv()
        last_bxz().start()
        last_piece(2).start()

    def last_fetch():
        last_bxz().wait_recv()
        last_piece(3).start()

    def partial(t, d, k):
        s = t % 2
        dx, dy, dz = bits_of(d)
        part = jnp.dot(a_v[d, :, 0:k * depth], b_v[s, 0:k * depth], preferred_element_type=jnp.float32)
        p_v[s, 0, dx, dy * 2 + dz] = part[:, 0:W]
        p_v[s, 1, dy, dx * 2 + dz] = part[:, W:C]

    def last_partials():
        s = last % 2

        def body(d, carry):
            dx, dy, dz = bits_of(d)
            part = jnp.dot(a_v[d], b_v[s, :, 0:W], preferred_element_type=jnp.float32)
            p_v[s, 0, dx, dy * 2 + dz, 0:upper] = part[0:upper]
            p_v[s, 1, dy, dx * 2 + dz, 0:upper] = part[upper:rows]
            return carry

        lax.fori_loop(0, 8, body, 0)

    def partials(t, k, n=8, order=lambda j: j):
        def body(j, carry):
            partial(t, order(j), k)
            return carry

        lax.fori_loop(0, n, body, 0)

    def first_two(n, order):
        def body(j, carry):
            partial(j // n, order(j % n), 2)
            return carry

        lax.fori_loop(0, 2 * n, body, 0)

    def send1(t, g, k, n=rows):
        s, blocks, part = t % 2, pl.ds(2 * k, 2), pl.ds(0, n)
        return send(p_v.at[s, g, 1, blocks, part], r1_v.at[s, g, blocks, part],
                    s1_sem.at[s, g], r1_sem.at[s, g, k], axis_nbr[g])

    def send2(t, g, k, n=rows):
        s, part = t % 2, pl.ds(0, n)
        return send(s2_v.at[s, g, 2 + k, part], r2_v.at[s, g, k, part],
                    s2_sem.at[s, g], r2_sem.at[s, g, k], axis_nbr[1 - g])

    def sent1(t, g, n=rows):
        wait_bytes(p_v.at[t % 2, g, 1, :, pl.ds(0, n)], s1_sem.at[t % 2, g])

    def sent2(t, g, n=rows):
        wait_bytes(r2_v.at[t % 2, g, :, pl.ds(0, n)], s2_sem.at[t % 2, g])

    def send3(t, g):
        s = t % D3
        return send(s3_v.at[s, g, 1], r3_v.at[s, g], s3_sem.at[s], r3_sem.at[s], axis_nbr[AZ])

    def pair_there(t, g):
        s = t % DO
        return send(q_v.at[s, g], c_v.at[:, tile_cols(t, g)], qs_sem.at[s], qr_sem, axis_nbr[AZ])

    def last_there(g):
        s = last % DO
        return send(q_v.at[s, g, pl.ds(0, upper)], c_v.at[pl.ds(g * upper, upper), last_cols(z)],
                    qs_sem.at[s], qr_sem, axis_nbr[AZ])

    def sent3(t):
        wait_bytes(r3_v.at[t % D3], s3_sem.at[t % D3])

    def got3(t):
        wait_bytes(r3_v.at[t % D3], r3_sem.at[t % D3])

    def pair_sent(t):
        wait_bytes(q_v.at[t % DO], qs_sem.at[t % DO])

    def take(t, g, phase, slots, high):
        when(t, slots, high, lambda: pl.semaphore_wait(credit.at[phase, g], 1))

    def give(t, g, phase, axis, slots, high):
        when(t, 0, high - slots, lambda: pl.semaphore_signal(
            credit.at[phase, g], inc=1, device_id=axis_nbr[axis], device_id_type=MESH))

    for copy in own:
        copy.start()
    pl.semaphore_wait(barrier, 4)
    for group in (xy_far1, y_far, z_own, xy_near1, x_far, x_near):
        for copy in group:
            copy.start()
    for t in range(min(LOOK, tiles)):
        bx_copy(t).start()
    for t in range(2):
        fetch_near(t)
    for h in both:
        y_far[h].wait_recv()
        z_y[h].start()
        xy_far1[h].wait_recv()
        xy_far2[h].start()
    for h in both:
        xy_near1[h].wait_recv()
        xy_near2[h].start()
        xy_far2[h].wait_recv()
        z_xy[h].start()
    for copy in y_near:
        copy.start()
    for t in range(2):
        wait_bytes(b_v.at[t, pl.ds(0, 2 * depth)], b_sem.at[t])
    wait_bytes(a_v.at[0], own_sem)
    end_group(1, 4)
    first_two(3, lambda j: j + j // 2)
    for h in both:
        x_far[h].wait_recv()
        z_x[h].start()
    for n in range(AHEAD):
        a_chunk(n).start()
    end_group(2, 4)
    first_two(2, lambda j: 6 + j)
    for t in range(2):
        for g in both:
            send1(t, g, 1).start()
    end_group(3, 6)

    def last_three(j):
        return 2 + (3 * j + 1) // 2

    def add3(t, g):
        c_v[:, tile_cols(t, g)] = (s3_v[t % D3, g, 0] + r3_v[t % D3, g]).astype(jnp.bfloat16)

    def start_late():
        def body(t, carry):
            for g in both:
                when(t, D3, plain, lambda g=g: pl.semaphore_wait(credit.at[2, g], 1))
                send3(t, g).start()
            return carry

        lax.fori_loop(plain - LATE, plain, body, 0)

    def each(low, high, fn):
        def body(n, carry):
            fn(n)
            return carry

        lax.fori_loop(low, high, body, 0)

    def end_hops():
        wait_bytes(a_v.at[pl.ds(0, hops // 4)], hop_send)
        for n in range(AHEAD):
            a_chunk(n).wait_send()

    def step(i, carry):
        t = i
        when(t, 0, tiles, lambda: start_chunks(t))
        when(t, LAG, tiles + 3, lambda: end_chunks(t - LAG))
        when(t, 1, tiles + 1, lambda: bx_copy(t - 1).wait_send())
        when(t, plain + 1, tiles + 1, lambda: bxz_copy(t - 1 - plain).wait_send())
        when(t, LAG, LAG + 1, end_hops)
        when(t, 0, tiles - LOOK, lambda: bx_copy(t + LOOK).start())
        when(t, tiles - LOOK, tiles - LOOK + 1, lambda: last_bx().start())
        when(t, 1, tiles - 1, lambda: fetch_near(t + 1))
        when(t, tiles - 1, tiles, last_near)
        for g in both:
            when(t, 2, tiles + 2, lambda g=g: sent1(t - 2, g))

        def wait_b(pieces):
            wait_bytes(b_v.at[t % 2, pl.ds(0, pieces * depth)], b_sem.at[t % 2])

        def near_products():
            wait_b(2)
            partials(t, 2)

        def all_products():
            wait_b(4)
            partials(t, 4)

        def last_products():
            wait_bytes(b_v.at[last % 2, :, 0:W], b_sem.at[last % 2])
            last_partials()

        def start_last():
            for g in both:
                pl.semaphore_wait(credit.at[0, g], 1)
                send1(last, g, 1, upper).start()
            for g in both:
                send1(last, g, 0, upper).start()

        def wait_far():
            wait_bytes(a_v.at[pl.ds(0, 4), :, pl.ds(2 * depth, 2 * depth)], ch_recv.at[0])

        when(t, 0, 2, lambda: partials(t, 2, 3, last_three))
        when(t, 2, plain, near_products)
        when(t, plain, plain + 1, wait_far)
        when(t, plain, tiles, all_products)
        when(t, last, last + 1, last_products)
        for g in both:
            take(t, g, 0, 2, tiles)
            when(t, 2, tiles, lambda g=g: send1(t, g, 1).start())
        for g in both:
            when(t, 0, tiles, lambda g=g: send1(t, g, 0).start())
        when(t, plain - 1, tiles - 1, lambda: fetch_far(t + 1))
        when(t, tiles - 1, tiles, last_far)

        t1 = i - 1

        def add1(g, k, n=rows):
            s, blocks, part = t1 % 2, pl.ds(2 * k, 2), pl.ds(0, n)
            send1(t1, g, k, n).wait_recv()
            s2_v[s, g, blocks, part] = p_v[s, g, 0, blocks, part] + r1_v[s, g, blocks, part]

        def last1():
            for g in both:
                add1(g, 1, upper)
                pl.semaphore_wait(credit.at[1, g], 1)
                send2(last, g, 1, upper).start()
            for g in both:
                send2(last - 1, g, 0).start()
            for g in both:
                send2(last, g, 0, upper).start()
            for g in both:
                add1(g, 0, upper)

        for g in both:
            when(t1, 2, tiles + 1, lambda g=g: sent2(t1 - 2, g))
            when(t1, 0, tiles, lambda g=g: add1(g, 1))
            take(t1, g, 1, 2, tiles)
            when(t1, 0, tiles, lambda g=g: send2(t1, g, 1).start())
            when(t1, 0, tiles - 1, lambda g=g: send2(t1, g, 0).start())
        when(t, last, last + 1, start_last)
        for g in both:
            when(t1, 0, tiles, lambda g=g: add1(g, 0))
            give(t1, g, 0, g, 2, last + 1)
        when(t1, last, last + 1, last1)

        t2 = i - 2

        def sum2(t, g, k, n=rows):
            part = pl.ds(0, n)
            send2(t, g, k, n).wait_recv()
            return s2_v[t % 2, g, k, part] + r2_v[t % 2, g, k, part]

        def last2():
            for g in both:
                q_v[last % DO, g, pl.ds(0, upper)] = sum2(last, g, 1, upper).astype(jnp.bfloat16)
                last_there(g).start()
            each(plain - LATE, plain, got3)
            for g in both:
                each(plain - LATE, plain, lambda t: add3(t, g))
            each(plain - LATE, plain, sent3)
            each(tiles + 3 - LAG, tiles, end_chunks)
            each(max(plain, last + 1 - DO), tiles - 1, pair_sent)
            last_bx().wait_send()
            last_bxz().wait_send()
            for g in both:
                sent1(last, g, upper)
            for g in both:
                add2_here(last - 1, g)
            for g in both:
                c_v[pl.ds(g * upper, upper), last_cols(z)] = sum2(last, g, 0, upper).astype(jnp.bfloat16)

        def add2(g, k):
            s3_v[t2 % D3, g, k] = sum2(t2, g, k)

        def add2_there(g):
            q_v[t2 % DO, g] = sum2(t2, g, 1).astype(jnp.bfloat16)

        def add2_here(t, g):
            c_v[:, tile_cols(t, g)] = sum2(t, g, 0).astype(jnp.bfloat16)

        when(t2, D3, plain - LATE + D3, lambda: sent3(t2 - D3))
        when(t2, plain + DO, last + 1, lambda: pair_sent(t2 - DO))
        for g in both:
            when(t2, 0, plain, lambda g=g: add2(g, 1))
            when(t2, plain, tiles, lambda g=g: add2_there(g))
            take(t2, g, 2, D3, plain - LATE)
            when(t2, 0, plain - LATE, lambda g=g: send3(t2, g).start())
            when(t2, plain, tiles, lambda g=g: pair_there(t2, g).start())
        for g in both:
            when(t2, 0, plain, lambda g=g: add2(g, 0))
            when(t2, plain, tiles - 1, lambda g=g: add2_here(t2, g))
            give(t2, g, 1, 1 - g, 2, last + 1)
        when(t2, last, last + 1, last2)

        t3 = i - 1 - D3
        when(t3, 0, plain - LATE, lambda: got3(t3))
        for g in both:
            when(t3, 0, plain - LATE, lambda g=g: add3(t3, g))
            give(t3, g, 2, AZ, D3, plain)
        when(t, last - 1, last, start_late)
        when(t, plain - 1, tiles - 1, lambda: fetch_last(t + 1))
        when(t, tiles - 1, tiles, last_fetch)
        return carry

    lax.fori_loop(0, tiles + 3, step, 0)

    each(max(plain, tiles - 1), tiles, pair_sent)
    for g in both:
        sent2(last - 1, g)
        sent2(last, g, upper)
    wait_bytes(q_v.at[last % DO, :, pl.ds(0, upper)], qs_sem.at[last % DO])
    wait_bytes(c_v.at[:, pl.ds(0, paired * C + W)], qr_sem)


def solution(mesh):
    spec_rows = P(("dp", "tp"), None)

    def local_block(a_rows, b_rows):
        rows, inner = a_rows.shape
        depth, columns = b_rows.shape
        plain, paired = counts(columns)
        tiles = plain + paired
        f32, bf16 = jnp.float32, jnp.bfloat16
        dma = pltpu.SemaphoreType.DMA
        out = pl.pallas_call(
            kernel,
            name="matmul_reduce_scatter",
            out_shape=(
                pltpu.VMEM((rows, columns), bf16),
                jax.ShapeDtypeStruct((tiles + 1, depth, C), bf16),
                jax.ShapeDtypeStruct((paired + 1, depth, C), bf16),
                jax.ShapeDtypeStruct((paired + 1, depth, C), bf16),
                jax.ShapeDtypeStruct((2, rows, 2 * depth), bf16),
            ),
            in_specs=[pl.BlockSpec(memory_space=pl.ANY)] * 2,
            out_specs=(pl.BlockSpec(memory_space=pltpu.VMEM),) + (pl.BlockSpec(memory_space=pl.ANY),) * 4,
            scratch_shapes=[
                pltpu.VMEM((8, rows, 4 * depth), bf16),
                pltpu.VMEM((2, 4 * depth, C), bf16),
                pltpu.VMEM((2, 2, 2, 4, rows, W), f32),
                pltpu.VMEM((2, 2, 4, rows, W), f32),
                pltpu.VMEM((2, 2, 4, rows, W), f32),
                pltpu.VMEM((2, 2, 2, rows, W), f32),
                pltpu.VMEM((D3, 2, 2, rows, W), f32),
                pltpu.VMEM((D3, 2, rows, W), f32),
                pltpu.VMEM((DO, 2, rows, W), bf16),
                dma, dma, dma((RX,)), dma((RX,)), dma((RZ,)), dma((RZ,)), dma((RC,)), dma((max(2 + paired, 14),)), dma((2,)),
                dma((2, 2)), dma((2, 2, 2)), dma((2, 2)), dma((2, 2, 2)), dma((D3,)), dma((D3,)), dma((DO,)), dma,
                pltpu.SemaphoreType.REGULAR((3, 2)),
            ],
            compiler_params=pltpu.CompilerParams(
                collective_id=0, has_side_effects=True, vmem_limit_bytes=56 * 1024 * 1024),
            cost_estimate=pl.CostEstimate(
                flops=2 * 8 * rows * 2 * depth * columns, bytes_accessed=6 * depth * columns, transcendentals=0),
        )(a_rows, b_rows)
        return out[0]

    return jax.shard_map(local_block, mesh=mesh, in_specs=(spec_rows, spec_rows), out_specs=spec_rows, check_vma=False)
```

```python
import jax
import jax.numpy as jnp
from jax import lax
from jax.experimental import pallas as pl
from jax.experimental.pallas import tpu as pltpu
from jax.sharding import PartitionSpec as P

MESH = pl.DeviceIdType.MESH
W = 128
C = 2 * W
LOOK = 2
D3 = 6
DO = 6
LATE = 4
AHEAD = 2
LAG = 5
RX, RZ, RC = 2 * LOOK, LOOK + 1, 8
AX, AY, AZ = 0, 1, 2


def bits_of(d):
    return (d // 4, (d // 2) % 2, d % 2)


def counts(columns):
    paired = columns // C // 4
    return columns // C - 2 * paired - 1, paired


def kernel(a_hbm, b_hbm, c_v, bx_hbm, bz_hbm, bxz_hbm, relay,
           a_v, b_v, p_v, r1_v, s2_v, r2_v, s3_v, r3_v, q_v,
           hop_send, own_sem, bx_send, bx_recv, bxz_send, bxz_recv, ch_send, ch_recv, b_sem,
           s1_sem, r1_sem, s2_sem, r2_sem, s3_sem, r3_sem, qs_sem, qr_sem, credit):
    depth, columns = b_hbm.shape
    plain, paired = counts(columns)
    tiles = plain + paired
    rows, upper = a_hbm.shape[0], a_hbm.shape[0] // 2
    half = depth // 2
    chunks = 16 + 2 * paired
    last = plain + paired
    rate = max(114, -(-1600 // plain), -(-100 * (15 + 2 * paired) // (tiles - 1)))

    dp, tp = lax.axis_index("dp"), lax.axis_index("tp")
    core, x, y, z = dp % 2, (dp // 2) % 2, dp // 4, tp

    def flip(v, bit):
        return v + bit - 2 * v * bit

    def device(bits, other=0):
        return {"dp": flip(y, bits[1]) * 4 + flip(x, bits[0]) * 2 + flip(core, other), "tp": flip(z, bits[2])}

    axis_nbr = [device((1, 0, 0)), device((0, 1, 0)), device((0, 0, 1))]
    partner = device((0, 0, 0), 1)

    barrier = pltpu.get_barrier_semaphore()
    for nbr in (*axis_nbr, partner):
        pl.semaphore_signal(barrier, inc=1, device_id=nbr, device_id_type=MESH)

    def send(src, dst, send_sem, recv_sem, to):
        return pltpu.make_async_remote_copy(
            src_ref=src, dst_ref=dst, send_sem=send_sem, recv_sem=recv_sem, device_id=to, device_id_type=MESH)

    def wait_bytes(ref, sem):
        pltpu.make_async_copy(ref, ref, sem).wait()

    def when(t, low, high, fn):
        pl.when(jnp.logical_and(t >= low, t < high))(fn)

    def is_paired(t):
        return (t + tiles - plain) // tiles

    def tile_cols(t, g=None):
        col = t * C + is_paired(t) * ((t - plain) * C + z * C)
        if g is None:
            return pl.ds(pl.multiple_of(col, W), C)
        return pl.ds(pl.multiple_of(col + g * W, W), W)

    def their_cols(q):
        return pl.ds(pl.multiple_of((plain + 2 * q + 1 - z) * C, W), C)

    def last_cols(side):
        return pl.ds(pl.multiple_of((plain + 2 * paired) * C + side * W, W), W)

    def a_cols(bits, h):
        to = device(bits, h)
        return a_hbm.at[:, pl.ds(pl.multiple_of((to["dp"] * 2 + to["tp"]) * depth, depth), depth)]

    def near(d, h):
        return a_v.at[d, :, pl.ds(h * depth, depth)]

    def far(d, h):
        return a_v.at[d, :, pl.ds((2 + h) * depth, depth)]

    def held(i, h):
        return relay.at[i, :, pl.ds(h * depth, depth)]

    def hop(n, h, src, dst, axis):
        return send(src, dst, hop_send, ch_recv.at[-n if n < 0 else 4 + 2 * n + h], axis_nbr[axis])

    both = range(2)
    xy_far1 = [hop(0, h, a_cols((1, 1, 1), h), held(0, h), AX) for h in both]
    xy_near1 = [hop(1, h, a_cols((1, 1, 0), h), held(1, h), AX) for h in both]
    x_far = [hop(2, h, a_cols((1, 0, 1), h), far(4, h), AX) for h in both]
    y_far = [hop(3, h, a_cols((0, 1, 1), h), far(2, h), AY) for h in both]
    xy_far2 = [hop(4, h, held(0, h), far(6, h), AY) for h in both]
    z_own = [hop(-1, h, a_cols((0, 0, 1), h), near(1, h), AZ) for h in both]
    z_y = [hop(-1, h, far(2, h), near(3, h), AZ) for h in both]
    xy_near2 = [hop(-2, h, held(1, h), near(6, h), AY) for h in both]
    z_xy = [hop(-2, h, far(6, h), near(7, h), AZ) for h in both]
    x_near = [hop(-3, h, a_cols((1, 0, 0), h), near(4, h), AX) for h in both]
    y_near = [hop(-3, h, a_cols((0, 1, 0), h), near(2, h), AY) for h in both]
    z_x = [hop(-3, h, far(4, h), near(5, h), AZ) for h in both]
    hops = 24

    def end_group(n, copies):
        wait_bytes(a_v.at[pl.ds(0, copies // 2), :, pl.ds(0, 2 * depth)], ch_recv.at[n])

    own = [pltpu.make_async_copy(a_cols((0, 0, 0), h), near(0, h), own_sem) for h in both]
    own += [pltpu.make_async_copy(a_cols((0, 0, 1), h), far(0, h), own_sem) for h in both]

    def a_chunk(n):
        d, k = (n // 4) * 2, n % 4
        return send(a_v.at[d, :, pl.ds(pl.multiple_of(k * half, half), half)],
                    a_v.at[d + 1, :, pl.ds(pl.multiple_of(2 * depth + k * half, half), half)],
                    ch_send.at[n % RC], ch_recv.at[0], axis_nbr[AZ])

    def b_chunk(q, h):
        rows = pl.ds(pl.multiple_of(h * half, half), half)
        n = 16 + 2 * q + h
        return send(b_hbm.at[rows, their_cols(q)], bz_hbm.at[q, rows], ch_send.at[n % RC], ch_recv.at[1 + q], axis_nbr[AZ])

    def last_chunk():
        return send(b_hbm.at[:, last_cols(1 - z)], bz_hbm.at[paired, :, 0:W], ch_send.at[chunks % RC], ch_recv.at[1 + paired], axis_nbr[AZ])

    def start_chunks(i):
        def body(n, carry):
            when(n, 0, 16, lambda: a_chunk(n).start())
            when(n, 16, chunks, lambda: b_chunk((n - 16) // 2, (n - 16) % 2).start())
            when(n, chunks, chunks + 1, lambda: last_chunk().start())
            return carry

        lax.fori_loop(rate * i // 100 + AHEAD, rate * (i + 1) // 100 + AHEAD, body, 0)

    def end_chunks(i):
        def body(n, carry):
            when(n, 0, 16, lambda: a_chunk(n).wait_send())
            when(n, 16, chunks, lambda: b_chunk((n - 16) // 2, (n - 16) % 2).wait_send())
            when(n, chunks, chunks + 1, lambda: last_chunk().wait_send())
            return carry

        lax.fori_loop(rate * i // 100 + AHEAD, rate * (i + 1) // 100 + AHEAD, body, 0)

    def bx_copy(t):
        return send(b_hbm.at[:, tile_cols(t)], bx_hbm.at[t], bx_send.at[t % RX], bx_recv.at[t % RX], partner)

    def bxz_copy(q):
        return send(bz_hbm.at[q], bxz_hbm.at[q], bxz_send.at[q % RZ], bxz_recv.at[q % RZ], partner)

    def last_bx():
        return send(b_hbm.at[:, last_cols(z)], bx_hbm.at[last, :, 0:W], bx_send.at[last % RX], bx_recv.at[last % RX], partner)

    def last_bxz():
        return send(bz_hbm.at[paired, :, 0:W], bxz_hbm.at[paired, :, 0:W], bxz_send.at[paired % RZ], bxz_recv.at[paired % RZ], partner)

    def last_piece(k):
        src = (b_hbm.at[:, last_cols(z)], bx_hbm.at[last, :, 0:W], bz_hbm.at[paired, :, 0:W], bxz_hbm.at[paired, :, 0:W])[k]
        return pltpu.make_async_copy(src, b_v.at[last % 2, pl.ds(k * depth, depth), 0:W], b_sem.at[last % 2])

    def b_piece(t, k):
        src = (b_hbm.at[:, tile_cols(t)], bx_hbm.at[t], bz_hbm.at[t - plain], bxz_hbm.at[t - plain])[k]
        return pltpu.make_async_copy(src, b_v.at[t % 2, pl.ds(k * depth, depth)], b_sem.at[t % 2])

    def fetch_near(t):
        b_piece(t, 0).start()
        bx_copy(t).wait_recv()
        b_piece(t, 1).start()

    def fetch_far(t):
        wait_bytes(bz_hbm.at[t - plain], ch_recv.at[1 + t - plain])
        bxz_copy(t - plain).start()
        b_piece(t, 2).start()

    def fetch_last(t):
        bxz_copy(t - plain).wait_recv()
        b_piece(t, 3).start()

    def last_near():
        last_piece(0).start()
        last_bx().wait_recv()
        last_piece(1).start()

    def last_far():
        last_chunk().wait_recv()
        last_bxz().start()
        last_piece(2).start()

    def last_fetch():
        last_bxz().wait_recv()
        last_piece(3).start()

    def partial(t, d, k):
        s = t % 2
        dx, dy, dz = bits_of(d)
        part = jnp.dot(a_v[d, :, 0:k * depth], b_v[s, 0:k * depth], preferred_element_type=jnp.float32)
        p_v[s, 0, dx, dy * 2 + dz] = part[:, 0:W]
        p_v[s, 1, dy, dx * 2 + dz] = part[:, W:C]

    def last_partials():
        s = last % 2

        def body(d, carry):
            dx, dy, dz = bits_of(d)
            part = jnp.dot(a_v[d], b_v[s, :, 0:W], preferred_element_type=jnp.float32)
            p_v[s, 0, dx, dy * 2 + dz, 0:upper] = part[0:upper]
            p_v[s, 1, dy, dx * 2 + dz, 0:upper] = part[upper:rows]
            return carry

        lax.fori_loop(0, 8, body, 0)

    def partials(t, k, n=8, order=lambda j: j):
        def body(j, carry):
            partial(t, order(j), k)
            return carry

        lax.fori_loop(0, n, body, 0)

    def first_two(n, order):
        def body(j, carry):
            partial(j // n, order(j % n), 2)
            return carry

        lax.fori_loop(0, 2 * n, body, 0)

    def send1(t, g, k, n=rows):
        s, blocks, part = t % 2, pl.ds(2 * k, 2), pl.ds(0, n)
        return send(p_v.at[s, g, 1, blocks, part], r1_v.at[s, g, blocks, part],
                    s1_sem.at[s, g], r1_sem.at[s, g, k], axis_nbr[g])

    def send2(t, g, k, n=rows):
        s, part = t % 2, pl.ds(0, n)
        return send(s2_v.at[s, g, 2 + k, part], r2_v.at[s, g, k, part],
                    s2_sem.at[s, g], r2_sem.at[s, g, k], axis_nbr[1 - g])

    def sent1(t, g, n=rows):
        wait_bytes(p_v.at[t % 2, g, 1, :, pl.ds(0, n)], s1_sem.at[t % 2, g])

    def sent2(t, g, n=rows):
        wait_bytes(r2_v.at[t % 2, g, :, pl.ds(0, n)], s2_sem.at[t % 2, g])

    def send3(t, g):
        s = t % D3
        return send(s3_v.at[s, g, 1], r3_v.at[s, g], s3_sem.at[s], r3_sem.at[s], axis_nbr[AZ])

    def pair_there(t, g):
        s = t % DO
        return send(q_v.at[s, g], c_v.at[:, tile_cols(t, g)], qs_sem.at[s], qr_sem, axis_nbr[AZ])

    def last_there(g):
        s = last % DO
        return send(q_v.at[s, g, pl.ds(0, upper)], c_v.at[pl.ds(g * upper, upper), last_cols(z)],
                    qs_sem.at[s], qr_sem, axis_nbr[AZ])

    def sent3(t):
        wait_bytes(r3_v.at[t % D3], s3_sem.at[t % D3])

    def got3(t):
        wait_bytes(r3_v.at[t % D3], r3_sem.at[t % D3])

    def pair_sent(t):
        wait_bytes(q_v.at[t % DO], qs_sem.at[t % DO])

    def take(t, g, phase, slots, high):
        when(t, slots, high, lambda: pl.semaphore_wait(credit.at[phase, g], 1))

    def give(t, g, phase, axis, slots, high):
        when(t, 0, high - slots, lambda: pl.semaphore_signal(
            credit.at[phase, g], inc=1, device_id=axis_nbr[axis], device_id_type=MESH))

    for copy in own:
        copy.start()
    pl.semaphore_wait(barrier, 4)
    for group in (xy_far1, y_far, z_own, xy_near1, x_far, x_near):
        for copy in group:
            copy.start()
    for t in range(min(LOOK, tiles)):
        bx_copy(t).start()
    for t in range(2):
        fetch_near(t)
    for h in both:
        y_far[h].wait_recv()
        z_y[h].start()
        xy_far1[h].wait_recv()
        xy_far2[h].start()
    for h in both:
        xy_near1[h].wait_recv()
        xy_near2[h].start()
        xy_far2[h].wait_recv()
        z_xy[h].start()
    for copy in y_near:
        copy.start()
    for t in range(2):
        wait_bytes(b_v.at[t, pl.ds(0, 2 * depth)], b_sem.at[t])
    wait_bytes(a_v.at[0], own_sem)
    end_group(1, 4)
    first_two(3, lambda j: j + j // 2)
    for h in both:
        x_far[h].wait_recv()
        z_x[h].start()
    for n in range(AHEAD):
        a_chunk(n).start()
    end_group(2, 4)
    first_two(2, lambda j: 6 + j)
    for t in range(2):
        for g in both:
            send1(t, g, 1).start()
    end_group(3, 6)

    def last_three(j):
        return 2 + (3 * j + 1) // 2

    def add3(t, g):
        c_v[:, tile_cols(t, g)] = (s3_v[t % D3, g, 0] + r3_v[t % D3, g]).astype(jnp.bfloat16)

    def start_late():
        def body(t, carry):
            for g in both:
                when(t, D3, plain, lambda g=g: pl.semaphore_wait(credit.at[2, g], 1))
                send3(t, g).start()
            return carry

        lax.fori_loop(plain - LATE, plain, body, 0)

    def each(low, high, fn):
        def body(n, carry):
            fn(n)
            return carry

        lax.fori_loop(low, high, body, 0)

    def end_hops():
        wait_bytes(a_v.at[pl.ds(0, hops // 4)], hop_send)
        for n in range(AHEAD):
            a_chunk(n).wait_send()

    def step(i, carry):
        t = i
        when(t, 0, tiles, lambda: start_chunks(t))
        when(t, LAG, tiles + 3, lambda: end_chunks(t - LAG))
        when(t, 1, tiles + 1, lambda: bx_copy(t - 1).wait_send())
        when(t, plain + 1, tiles + 1, lambda: bxz_copy(t - 1 - plain).wait_send())
        when(t, LAG, LAG + 1, end_hops)
        when(t, 0, tiles - LOOK, lambda: bx_copy(t + LOOK).start())
        when(t, tiles - LOOK, tiles - LOOK + 1, lambda: last_bx().start())
        when(t, 1, tiles - 1, lambda: fetch_near(t + 1))
        when(t, tiles - 1, tiles, last_near)
        for g in both:
            when(t, 2, tiles + 2, lambda g=g: sent1(t - 2, g))

        def wait_b(pieces):
            wait_bytes(b_v.at[t % 2, pl.ds(0, pieces * depth)], b_sem.at[t % 2])

        def near_products():
            wait_b(2)
            partials(t, 2)

        def all_products():
            wait_b(4)
            partials(t, 4)

        def last_products():
            wait_bytes(b_v.at[last % 2, :, 0:W], b_sem.at[last % 2])
            last_partials()

        def start_last():
            for g in both:
                pl.semaphore_wait(credit.at[0, g], 1)
                send1(last, g, 1, upper).start()
            for g in both:
                send1(last, g, 0, upper).start()

        def wait_far():
            wait_bytes(a_v.at[pl.ds(0, 4), :, pl.ds(2 * depth, 2 * depth)], ch_recv.at[0])

        when(t, 0, 2, lambda: partials(t, 2, 3, last_three))
        when(t, 2, plain, near_products)
        when(t, plain, plain + 1, wait_far)
        when(t, plain, tiles, all_products)
        when(t, last, last + 1, last_products)
        for g in both:
            take(t, g, 0, 2, tiles)
            when(t, 2, tiles, lambda g=g: send1(t, g, 1).start())
        for g in both:
            when(t, 0, tiles, lambda g=g: send1(t, g, 0).start())
        when(t, plain - 1, tiles - 1, lambda: fetch_far(t + 1))
        when(t, tiles - 1, tiles, last_far)

        t1 = i - 1

        def add1(t, g, k, n=rows):
            s, blocks, part = t % 2, pl.ds(2 * k, 2), pl.ds(0, n)
            send1(t, g, k, n).wait_recv()
            s2_v[s, g, blocks, part] = p_v[s, g, 0, blocks, part] + r1_v[s, g, blocks, part]

        def last1():
            for g in both:
                add1(last, g, 1, upper)
                pl.semaphore_wait(credit.at[1, g], 1)
                send2(last, g, 1, upper).start()
            for g in both:
                send2(last - 1, g, 0).start()
            for g in both:
                send2(last, g, 0, upper).start()

        for g in both:
            when(t1, 2, tiles + 1, lambda g=g: sent2(t1 - 2, g))
            when(t1, 0, tiles, lambda g=g: add1(t1, g, 1))
            take(t1, g, 1, 2, tiles)
            when(t1, 0, tiles, lambda g=g: send2(t1, g, 1).start())
            when(t1, 0, tiles - 1, lambda g=g: send2(t1, g, 0).start())
        when(t, last, last + 1, start_last)
        for g in both:
            when(t1, 0, tiles, lambda g=g: add1(t1, g, 0))
            give(t1, g, 0, g, 2, last + 1)
        when(t1, last, last + 1, last1)

        t2 = i - 2

        def sum2(t, g, k, n=rows):
            part = pl.ds(0, n)
            send2(t, g, k, n).wait_recv()
            return s2_v[t % 2, g, k, part] + r2_v[t % 2, g, k, part]

        def last2():
            for g in both:
                add1(last, g, 0, upper)
            for g in both:
                q_v[last % DO, g, pl.ds(0, upper)] = sum2(last, g, 1, upper).astype(jnp.bfloat16)
                last_there(g).start()
            each(plain - LATE, plain, got3)
            for g in both:
                each(plain - LATE, plain, lambda t: add3(t, g))
            each(plain - LATE, plain, sent3)
            each(tiles + 3 - LAG, tiles, end_chunks)
            each(max(plain, last + 1 - DO), tiles - 1, pair_sent)
            last_bx().wait_send()
            last_bxz().wait_send()
            for g in both:
                sent1(last, g, upper)
            for g in both:
                add2_here(last - 1, g)
            for g in both:
                c_v[pl.ds(g * upper, upper), last_cols(z)] = sum2(last, g, 0, upper).astype(jnp.bfloat16)

        def add2(g, k):
            s3_v[t2 % D3, g, k] = sum2(t2, g, k)

        def add2_there(g):
            q_v[t2 % DO, g] = sum2(t2, g, 1).astype(jnp.bfloat16)

        def add2_here(t, g):
            c_v[:, tile_cols(t, g)] = sum2(t, g, 0).astype(jnp.bfloat16)

        when(t2, D3, plain - LATE + D3, lambda: sent3(t2 - D3))
        when(t2, plain + DO, last + 1, lambda: pair_sent(t2 - DO))
        for g in both:
            when(t2, 0, plain, lambda g=g: add2(g, 1))
            when(t2, plain, tiles, lambda g=g: add2_there(g))
            take(t2, g, 2, D3, plain - LATE)
            when(t2, 0, plain - LATE, lambda g=g: send3(t2, g).start())
            when(t2, plain, tiles, lambda g=g: pair_there(t2, g).start())
        for g in both:
            when(t2, 0, plain, lambda g=g: add2(g, 0))
            when(t2, plain, tiles - 1, lambda g=g: add2_here(t2, g))
            give(t2, g, 1, 1 - g, 2, last + 1)
        when(t2, last, last + 1, last2)

        t3 = i - 1 - D3
        when(t3, 0, plain - LATE, lambda: got3(t3))
        for g in both:
            when(t3, 0, plain - LATE, lambda g=g: add3(t3, g))
            give(t3, g, 2, AZ, D3, plain)
        when(t, last - 1, last, start_late)
        when(t, plain - 1, tiles - 1, lambda: fetch_last(t + 1))
        when(t, tiles - 1, tiles, last_fetch)
        return carry

    lax.fori_loop(0, tiles + 3, step, 0)

    each(max(plain, tiles - 1), tiles, pair_sent)
    for g in both:
        sent2(last - 1, g)
        sent2(last, g, upper)
    wait_bytes(q_v.at[last % DO, :, pl.ds(0, upper)], qs_sem.at[last % DO])
    wait_bytes(c_v.at[:, pl.ds(0, paired * C + W)], qr_sem)


def solution(mesh):
    spec_rows = P(("dp", "tp"), None)

    def local_block(a_rows, b_rows):
        rows, inner = a_rows.shape
        depth, columns = b_rows.shape
        plain, paired = counts(columns)
        tiles = plain + paired
        f32, bf16 = jnp.float32, jnp.bfloat16
        dma = pltpu.SemaphoreType.DMA
        out = pl.pallas_call(
            kernel,
            name="matmul_reduce_scatter",
            out_shape=(
                pltpu.VMEM((rows, columns), bf16),
                jax.ShapeDtypeStruct((tiles + 1, depth, C), bf16),
                jax.ShapeDtypeStruct((paired + 1, depth, C), bf16),
                jax.ShapeDtypeStruct((paired + 1, depth, C), bf16),
                jax.ShapeDtypeStruct((2, rows, 2 * depth), bf16),
            ),
            in_specs=[pl.BlockSpec(memory_space=pl.ANY)] * 2,
            out_specs=(pl.BlockSpec(memory_space=pltpu.VMEM),) + (pl.BlockSpec(memory_space=pl.ANY),) * 4,
            scratch_shapes=[
                pltpu.VMEM((8, rows, 4 * depth), bf16),
                pltpu.VMEM((2, 4 * depth, C), bf16),
                pltpu.VMEM((2, 2, 2, 4, rows, W), f32),
                pltpu.VMEM((2, 2, 4, rows, W), f32),
                pltpu.VMEM((2, 2, 4, rows, W), f32),
                pltpu.VMEM((2, 2, 2, rows, W), f32),
                pltpu.VMEM((D3, 2, 2, rows, W), f32),
                pltpu.VMEM((D3, 2, rows, W), f32),
                pltpu.VMEM((DO, 2, rows, W), bf16),
                dma, dma, dma((RX,)), dma((RX,)), dma((RZ,)), dma((RZ,)), dma((RC,)), dma((max(2 + paired, 14),)), dma((2,)),
                dma((2, 2)), dma((2, 2, 2)), dma((2, 2)), dma((2, 2, 2)), dma((D3,)), dma((D3,)), dma((DO,)), dma,
                pltpu.SemaphoreType.REGULAR((3, 2)),
            ],
            compiler_params=pltpu.CompilerParams(
                collective_id=0, has_side_effects=True, vmem_limit_bytes=56 * 1024 * 1024),
            cost_estimate=pl.CostEstimate(
                flops=2 * 8 * rows * 2 * depth * columns, bytes_accessed=6 * depth * columns, transcendentals=0),
        )(a_rows, b_rows)
        return out[0]

    return jax.shard_map(local_block, mesh=mesh, in_specs=(spec_rows, spec_rows), out_specs=spec_rows, check_vma=False)
```

```python
import jax
import jax.numpy as jnp
from jax import lax
from jax.experimental import pallas as pl
from jax.experimental.pallas import tpu as pltpu
from jax.sharding import PartitionSpec as P

MESH = pl.DeviceIdType.MESH
W = 128
C = 2 * W
LOOK = 2
D3 = 6
DO = 6
LATE = 4
AHEAD = 2
LAG = 5
RX, RZ, RC = 2 * LOOK, LOOK + 1, 8
AX, AY, AZ = 0, 1, 2


def bits_of(d):
    return (d // 4, (d // 2) % 2, d % 2)


def counts(columns):
    paired = columns // C // 4
    return columns // C - 2 * paired - 1, paired


def kernel(a_hbm, b_hbm, c_v, bx_hbm, bz_hbm, bxz_hbm, relay,
           a_v, b_v, p_v, r1_v, s2_v, r2_v, s3_v, r3_v, q_v,
           hop_send, own_sem, bx_send, bx_recv, bxz_send, bxz_recv, ch_send, ch_recv, b_sem,
           s1_sem, r1_sem, s2_sem, r2_sem, s3_sem, r3_sem, qs_sem, qr_sem, credit):
    depth, columns = b_hbm.shape
    plain, paired = counts(columns)
    tiles = plain + paired
    rows, upper = a_hbm.shape[0], a_hbm.shape[0] // 2
    half = depth // 2
    chunks = 16 + 2 * paired
    last = plain + paired
    rate = max(114, -(-1600 // plain), -(-100 * (15 + 2 * paired) // (tiles - 1)))

    dp, tp = lax.axis_index("dp"), lax.axis_index("tp")
    core, x, y, z = dp % 2, (dp // 2) % 2, dp // 4, tp

    def flip(v, bit):
        return v + bit - 2 * v * bit

    def device(bits, other=0):
        return {"dp": flip(y, bits[1]) * 4 + flip(x, bits[0]) * 2 + flip(core, other), "tp": flip(z, bits[2])}

    axis_nbr = [device((1, 0, 0)), device((0, 1, 0)), device((0, 0, 1))]
    partner = device((0, 0, 0), 1)

    barrier = pltpu.get_barrier_semaphore()
    for nbr in (*axis_nbr, partner):
        pl.semaphore_signal(barrier, inc=1, device_id=nbr, device_id_type=MESH)

    def send(src, dst, send_sem, recv_sem, to):
        return pltpu.make_async_remote_copy(
            src_ref=src, dst_ref=dst, send_sem=send_sem, recv_sem=recv_sem, device_id=to, device_id_type=MESH)

    def wait_bytes(ref, sem):
        pltpu.make_async_copy(ref, ref, sem).wait()

    def when(t, low, high, fn):
        pl.when(jnp.logical_and(t >= low, t < high))(fn)

    def is_paired(t):
        return (t + tiles - plain) // tiles

    def tile_cols(t, g=None):
        col = t * C + is_paired(t) * ((t - plain) * C + z * C)
        if g is None:
            return pl.ds(pl.multiple_of(col, W), C)
        return pl.ds(pl.multiple_of(col + g * W, W), W)

    def their_cols(q):
        return pl.ds(pl.multiple_of((plain + 2 * q + 1 - z) * C, W), C)

    def last_cols(side):
        return pl.ds(pl.multiple_of((plain + 2 * paired) * C + side * W, W), W)

    def a_cols(bits, h):
        to = device(bits, h)
        return a_hbm.at[:, pl.ds(pl.multiple_of((to["dp"] * 2 + to["tp"]) * depth, depth), depth)]

    def near(d, h):
        return a_v.at[d, :, pl.ds(h * depth, depth)]

    def far(d, h):
        return a_v.at[d, :, pl.ds((2 + h) * depth, depth)]

    def held(i, h):
        return relay.at[i, :, pl.ds(h * depth, depth)]

    def hop(n, h, src, dst, axis):
        return send(src, dst, hop_send, ch_recv.at[-n if n < 0 else 4 + 2 * n + h], axis_nbr[axis])

    both = range(2)
    xy_far1 = [hop(0, h, a_cols((1, 1, 1), h), held(0, h), AX) for h in both]
    xy_near1 = [hop(1, h, a_cols((1, 1, 0), h), held(1, h), AX) for h in both]
    x_far = [hop(2, h, a_cols((1, 0, 1), h), far(4, h), AX) for h in both]
    y_far = [hop(3, h, a_cols((0, 1, 1), h), far(2, h), AY) for h in both]
    xy_far2 = [hop(4, h, held(0, h), far(6, h), AY) for h in both]
    z_own = [hop(-1, h, a_cols((0, 0, 1), h), near(1, h), AZ) for h in both]
    z_y = [hop(-1, h, far(2, h), near(3, h), AZ) for h in both]
    xy_near2 = [hop(-2, h, held(1, h), near(6, h), AY) for h in both]
    z_xy = [hop(-2, h, far(6, h), near(7, h), AZ) for h in both]
    x_near = [hop(-3, h, a_cols((1, 0, 0), h), near(4, h), AX) for h in both]
    y_near = [hop(-3, h, a_cols((0, 1, 0), h), near(2, h), AY) for h in both]
    z_x = [hop(-3, h, far(4, h), near(5, h), AZ) for h in both]
    hops = 24

    def end_group(n, copies):
        wait_bytes(a_v.at[pl.ds(0, copies // 2), :, pl.ds(0, 2 * depth)], ch_recv.at[n])

    own = [pltpu.make_async_copy(a_cols((0, 0, 0), h), near(0, h), own_sem) for h in both]
    own += [pltpu.make_async_copy(a_cols((0, 0, 1), h), far(0, h), own_sem) for h in both]

    def a_chunk(n):
        d, k = (n // 4) * 2, n % 4
        return send(a_v.at[d, :, pl.ds(pl.multiple_of(k * half, half), half)],
                    a_v.at[d + 1, :, pl.ds(pl.multiple_of(2 * depth + k * half, half), half)],
                    ch_send.at[n % RC], ch_recv.at[0], axis_nbr[AZ])

    def b_chunk(q, h):
        rows = pl.ds(pl.multiple_of(h * half, half), half)
        n = 16 + 2 * q + h
        return send(b_hbm.at[rows, their_cols(q)], bz_hbm.at[q, rows], ch_send.at[n % RC], ch_recv.at[1 + q], axis_nbr[AZ])

    def last_chunk():
        return send(b_hbm.at[:, last_cols(1 - z)], bz_hbm.at[paired, :, 0:W], ch_send.at[chunks % RC], ch_recv.at[1 + paired], axis_nbr[AZ])

    def start_chunks(i):
        def body(n, carry):
            when(n, 0, 16, lambda: a_chunk(n).start())
            when(n, 16, chunks, lambda: b_chunk((n - 16) // 2, (n - 16) % 2).start())
            when(n, chunks, chunks + 1, lambda: last_chunk().start())
            return carry

        lax.fori_loop(rate * i // 100 + AHEAD, rate * (i + 1) // 100 + AHEAD, body, 0)

    def end_chunks(i):
        def body(n, carry):
            when(n, 0, 16, lambda: a_chunk(n).wait_send())
            when(n, 16, chunks, lambda: b_chunk((n - 16) // 2, (n - 16) % 2).wait_send())
            when(n, chunks, chunks + 1, lambda: last_chunk().wait_send())
            return carry

        lax.fori_loop(rate * i // 100 + AHEAD, rate * (i + 1) // 100 + AHEAD, body, 0)

    def bx_copy(t):
        return send(b_hbm.at[:, tile_cols(t)], bx_hbm.at[t], bx_send.at[t % RX], bx_recv.at[t % RX], partner)

    def bxz_copy(q):
        return send(bz_hbm.at[q], bxz_hbm.at[q], bxz_send.at[q % RZ], bxz_recv.at[q % RZ], partner)

    def last_bx():
        return send(b_hbm.at[:, last_cols(z)], bx_hbm.at[last, :, 0:W], bx_send.at[last % RX], bx_recv.at[last % RX], partner)

    def last_bxz():
        return send(bz_hbm.at[paired, :, 0:W], bxz_hbm.at[paired, :, 0:W], bxz_send.at[paired % RZ], bxz_recv.at[paired % RZ], partner)

    def last_piece(k):
        src = (b_hbm.at[:, last_cols(z)], bx_hbm.at[last, :, 0:W], bz_hbm.at[paired, :, 0:W], bxz_hbm.at[paired, :, 0:W])[k]
        return pltpu.make_async_copy(src, b_v.at[last % 2, pl.ds(k * depth, depth), 0:W], b_sem.at[last % 2])

    def b_piece(t, k):
        src = (b_hbm.at[:, tile_cols(t)], bx_hbm.at[t], bz_hbm.at[t - plain], bxz_hbm.at[t - plain])[k]
        return pltpu.make_async_copy(src, b_v.at[t % 2, pl.ds(k * depth, depth)], b_sem.at[t % 2])

    def fetch_near(t):
        b_piece(t, 0).start()
        bx_copy(t).wait_recv()
        b_piece(t, 1).start()

    def fetch_far(t):
        wait_bytes(bz_hbm.at[t - plain], ch_recv.at[1 + t - plain])
        bxz_copy(t - plain).start()
        b_piece(t, 2).start()

    def fetch_last(t):
        bxz_copy(t - plain).wait_recv()
        b_piece(t, 3).start()

    def last_near():
        last_piece(0).start()
        last_bx().wait_recv()
        last_piece(1).start()

    def last_far():
        last_chunk().wait_recv()
        last_bxz().start()
        last_piece(2).start()

    def last_fetch():
        last_bxz().wait_recv()
        last_piece(3).start()

    def partial(t, d, k):
        s = t % 2
        dx, dy, dz = bits_of(d)
        part = jnp.dot(a_v[d, :, 0:k * depth], b_v[s, 0:k * depth], preferred_element_type=jnp.float32)
        p_v[s, 0, dx, dy * 2 + dz] = part[:, 0:W]
        p_v[s, 1, dy, dx * 2 + dz] = part[:, W:C]

    def last_partials():
        s = last % 2

        def body(d, carry):
            dx, dy, dz = bits_of(d)
            part = jnp.dot(a_v[d], b_v[s, :, 0:W], preferred_element_type=jnp.float32)
            p_v[s, 0, dx, dy * 2 + dz, 0:upper] = part[0:upper]
            p_v[s, 1, dy, dx * 2 + dz, 0:upper] = part[upper:rows]
            return carry

        lax.fori_loop(0, 8, body, 0)

    def partials(t, k, n=8, order=lambda j: j):
        def body(j, carry):
            partial(t, order(j), k)
            return carry

        lax.fori_loop(0, n, body, 0)

    def first_two(n, order):
        def body(j, carry):
            partial(j // n, order(j % n), 2)
            return carry

        lax.fori_loop(0, 2 * n, body, 0)

    def send1(t, g, k, n=rows):
        s, blocks, part = t % 2, pl.ds(2 * k, 2), pl.ds(0, n)
        return send(p_v.at[s, g, 1, blocks, part], r1_v.at[s, g, blocks, part],
                    s1_sem.at[s, g], r1_sem.at[s, g, k], axis_nbr[g])

    def send2(t, g, k, n=rows):
        s, part = t % 2, pl.ds(0, n)
        return send(s2_v.at[s, g, 2 + k, part], r2_v.at[s, g, k, part],
                    s2_sem.at[s, g], r2_sem.at[s, g, k], axis_nbr[1 - g])

    def sent1(t, g, n=rows):
        wait_bytes(p_v.at[t % 2, g, 1, :, pl.ds(0, n)], s1_sem.at[t % 2, g])

    def sent2(t, g, n=rows):
        wait_bytes(r2_v.at[t % 2, g, :, pl.ds(0, n)], s2_sem.at[t % 2, g])

    def send3(t, g):
        s = t % D3
        return send(s3_v.at[s, g, 1], r3_v.at[s, g], s3_sem.at[s], r3_sem.at[s], axis_nbr[AZ])

    def pair_there(t, g):
        s = t % DO
        return send(q_v.at[s, g], c_v.at[:, tile_cols(t, g)], qs_sem.at[s], qr_sem, axis_nbr[AZ])

    def last_there(g):
        s = last % DO
        return send(q_v.at[s, g, pl.ds(0, upper)], c_v.at[pl.ds(g * upper, upper), last_cols(z)],
                    qs_sem.at[s], qr_sem, axis_nbr[AZ])

    def sent3(t):
        wait_bytes(r3_v.at[t % D3], s3_sem.at[t % D3])

    def got3(t):
        wait_bytes(r3_v.at[t % D3], r3_sem.at[t % D3])

    def pair_sent(t):
        wait_bytes(q_v.at[t % DO], qs_sem.at[t % DO])

    def take(t, g, phase, slots, high):
        when(t, slots, high, lambda: pl.semaphore_wait(credit.at[phase, g], 1))

    def give(t, g, phase, axis, slots, high):
        when(t, 0, high - slots, lambda: pl.semaphore_signal(
            credit.at[phase, g], inc=1, device_id=axis_nbr[axis], device_id_type=MESH))

    for copy in own:
        copy.start()
    pl.semaphore_wait(barrier, 4)
    for group in (xy_far1, y_far, z_own, xy_near1, x_far, x_near):
        for copy in group:
            copy.start()
    for t in range(min(LOOK, tiles)):
        bx_copy(t).start()
    for t in range(2):
        fetch_near(t)
    for h in both:
        y_far[h].wait_recv()
        z_y[h].start()
        xy_far1[h].wait_recv()
        xy_far2[h].start()
    for h in both:
        xy_near1[h].wait_recv()
        xy_near2[h].start()
        xy_far2[h].wait_recv()
        z_xy[h].start()
    for copy in y_near:
        copy.start()
    for t in range(2):
        wait_bytes(b_v.at[t, pl.ds(0, 2 * depth)], b_sem.at[t])
    wait_bytes(a_v.at[0], own_sem)
    end_group(1, 4)
    first_two(3, lambda j: j + j // 2)
    for h in both:
        x_far[h].wait_recv()
        z_x[h].start()
    for n in range(AHEAD):
        a_chunk(n).start()
    end_group(2, 4)
    first_two(2, lambda j: 6 + j)
    for t in range(2):
        for g in both:
            send1(t, g, 1).start()
    end_group(3, 6)

    def last_three(j):
        return 2 + (3 * j + 1) // 2

    def add3(t, g):
        c_v[:, tile_cols(t, g)] = (s3_v[t % D3, g, 0] + r3_v[t % D3, g]).astype(jnp.bfloat16)

    def start_late():
        def body(t, carry):
            for g in both:
                when(t, D3, plain, lambda g=g: pl.semaphore_wait(credit.at[2, g], 1))
                send3(t, g).start()
            return carry

        lax.fori_loop(plain - LATE, plain, body, 0)

    def each(low, high, fn):
        def body(n, carry):
            fn(n)
            return carry

        lax.fori_loop(low, high, body, 0)

    def end_hops():
        wait_bytes(a_v.at[pl.ds(0, hops // 4)], hop_send)
        for n in range(AHEAD):
            a_chunk(n).wait_send()

    def step(i, carry):
        t = i
        when(t, 0, tiles, lambda: start_chunks(t))
        when(t, LAG, tiles + 3, lambda: end_chunks(t - LAG))
        when(t, 1, tiles + 1, lambda: bx_copy(t - 1).wait_send())
        when(t, plain + 1, tiles + 1, lambda: bxz_copy(t - 1 - plain).wait_send())
        when(t, LAG, LAG + 1, end_hops)
        when(t, 0, tiles - LOOK, lambda: bx_copy(t + LOOK).start())
        when(t, tiles - LOOK, tiles - LOOK + 1, lambda: last_bx().start())
        when(t, 1, tiles - 1, lambda: fetch_near(t + 1))
        when(t, tiles - 1, tiles, last_near)
        for g in both:
            when(t, 2, tiles + 2, lambda g=g: sent1(t - 2, g))

        def wait_b(pieces):
            wait_bytes(b_v.at[t % 2, pl.ds(0, pieces * depth)], b_sem.at[t % 2])

        def near_products():
            wait_b(2)
            partials(t, 2)

        def all_products():
            wait_b(4)
            partials(t, 4)

        def last_products():
            wait_bytes(b_v.at[last % 2, :, 0:W], b_sem.at[last % 2])
            last_partials()

        def start_last():
            for g in both:
                pl.semaphore_wait(credit.at[0, g], 1)
                send1(last, g, 1, upper).start()
            for g in both:
                send1(last, g, 0, upper).start()

        def wait_far():
            wait_bytes(a_v.at[pl.ds(0, 4), :, pl.ds(2 * depth, 2 * depth)], ch_recv.at[0])

        when(t, 0, 2, lambda: partials(t, 2, 3, last_three))
        when(t, 2, plain, near_products)
        when(t, plain, plain + 1, wait_far)
        when(t, plain, tiles, all_products)
        when(t, last, last + 1, last_products)
        for g in both:
            take(t, g, 0, 2, tiles)
            when(t, 2, tiles, lambda g=g: send1(t, g, 1).start())
        for g in both:
            when(t, 0, tiles, lambda g=g: send1(t, g, 0).start())
        when(t, plain - 1, tiles - 1, lambda: fetch_far(t + 1))
        when(t, tiles - 1, tiles, last_far)

        t1 = i - 1

        def add1(t, g, k, n=rows):
            s, blocks, part = t % 2, pl.ds(2 * k, 2), pl.ds(0, n)
            send1(t, g, k, n).wait_recv()
            s2_v[s, g, blocks, part] = p_v[s, g, 0, blocks, part] + r1_v[s, g, blocks, part]

        def last1():
            for g in both:
                add1(last, g, 1, upper)
                pl.semaphore_wait(credit.at[1, g], 1)
                send2(last, g, 1, upper).start()
            for g in both:
                send2(last - 1, g, 0).start()
            for g in both:
                send2(last, g, 0, upper).start()

        for g in both:
            when(t1, 2, tiles + 1, lambda g=g: sent2(t1 - 2, g))
            when(t1, 0, tiles, lambda g=g: add1(t1, g, 1))
            take(t1, g, 1, 2, tiles)
            when(t1, 0, tiles, lambda g=g: send2(t1, g, 1).start())
            when(t1, 0, tiles - 1, lambda g=g: send2(t1, g, 0).start())
        when(t, last, last + 1, start_last)
        for g in both:
            when(t1, 0, tiles, lambda g=g: add1(t1, g, 0))
            give(t1, g, 0, g, 2, last + 1)
        when(t1, last, last + 1, last1)

        t2 = i - 2

        def sum2(t, g, k, n=rows):
            part = pl.ds(0, n)
            send2(t, g, k, n).wait_recv()
            return s2_v[t % 2, g, k, part] + r2_v[t % 2, g, k, part]

        def last2():
            for g in both:
                add1(last, g, 0, upper)
            for g in both:
                q_v[last % DO, g, pl.ds(0, upper)] = sum2(last, g, 1, upper).astype(jnp.bfloat16)
                last_there(g).start()
            each(plain - LATE, plain, got3)
            for g in both:
                each(plain - LATE, plain, lambda t: add3(t, g))
            each(plain - LATE, plain, sent3)
            each(tiles + 3 - LAG, tiles, end_chunks)
            each(max(plain, last + 1 - DO), tiles - 1, pair_sent)
            last_bx().wait_send()
            last_bxz().wait_send()
            for g in both:
                sent1(last, g, upper)
            for g in both:
                add2_here(last - 1, g)
            for g in both:
                c_v[pl.ds(g * upper, upper), last_cols(z)] = sum2(last, g, 0, upper).astype(jnp.bfloat16)

        def add2(g, k):
            s3_v[t2 % D3, g, k] = sum2(t2, g, k)

        def add2_there(g):
            q_v[t2 % DO, g] = sum2(t2, g, 1).astype(jnp.bfloat16)

        def add2_here(t, g):
            c_v[:, tile_cols(t, g)] = sum2(t, g, 0).astype(jnp.bfloat16)

        when(t2, D3, plain - LATE + D3, lambda: sent3(t2 - D3))
        when(t2, plain + DO, last + 1, lambda: pair_sent(t2 - DO))
        for g in both:
            when(t2, 0, plain, lambda g=g: add2(g, 1))
            when(t2, plain, tiles, lambda g=g: add2_there(g))
            take(t2, g, 2, D3, plain - LATE)
            when(t2, 0, plain - LATE, lambda g=g: send3(t2, g).start())
            when(t2, plain, tiles, lambda g=g: pair_there(t2, g).start())
        for g in both:
            when(t2, 0, plain, lambda g=g: add2(g, 0))
            when(t2, plain, tiles - 1, lambda g=g: add2_here(t2, g))
            give(t2, g, 1, 1 - g, 2, last + 1)
        when(t2, last, last + 1, last2)

        t3 = i - 1 - D3
        when(t3, 0, plain - LATE, lambda: got3(t3))
        for g in both:
            when(t3, 0, plain - LATE, lambda g=g: add3(t3, g))
            give(t3, g, 2, AZ, D3, plain)
        when(t, last - 2, last - 1, start_late)
        when(t, plain - 1, tiles - 1, lambda: fetch_last(t + 1))
        when(t, tiles - 1, tiles, last_fetch)
        return carry

    lax.fori_loop(0, tiles + 3, step, 0)

    each(max(plain, tiles - 1), tiles, pair_sent)
    for g in both:
        sent2(last - 1, g)
        sent2(last, g, upper)
    wait_bytes(q_v.at[last % DO, :, pl.ds(0, upper)], qs_sem.at[last % DO])
    wait_bytes(c_v.at[:, pl.ds(0, paired * C + W)], qr_sem)


def solution(mesh):
    spec_rows = P(("dp", "tp"), None)

    def local_block(a_rows, b_rows):
        rows, inner = a_rows.shape
        depth, columns = b_rows.shape
        plain, paired = counts(columns)
        tiles = plain + paired
        f32, bf16 = jnp.float32, jnp.bfloat16
        dma = pltpu.SemaphoreType.DMA
        out = pl.pallas_call(
            kernel,
            name="matmul_reduce_scatter",
            out_shape=(
                pltpu.VMEM((rows, columns), bf16),
                jax.ShapeDtypeStruct((tiles + 1, depth, C), bf16),
                jax.ShapeDtypeStruct((paired + 1, depth, C), bf16),
                jax.ShapeDtypeStruct((paired + 1, depth, C), bf16),
                jax.ShapeDtypeStruct((2, rows, 2 * depth), bf16),
            ),
            in_specs=[pl.BlockSpec(memory_space=pl.ANY)] * 2,
            out_specs=(pl.BlockSpec(memory_space=pltpu.VMEM),) + (pl.BlockSpec(memory_space=pl.ANY),) * 4,
            scratch_shapes=[
                pltpu.VMEM((8, rows, 4 * depth), bf16),
                pltpu.VMEM((2, 4 * depth, C), bf16),
                pltpu.VMEM((2, 2, 2, 4, rows, W), f32),
                pltpu.VMEM((2, 2, 4, rows, W), f32),
                pltpu.VMEM((2, 2, 4, rows, W), f32),
                pltpu.VMEM((2, 2, 2, rows, W), f32),
                pltpu.VMEM((D3, 2, 2, rows, W), f32),
                pltpu.VMEM((D3, 2, rows, W), f32),
                pltpu.VMEM((DO, 2, rows, W), bf16),
                dma, dma, dma((RX,)), dma((RX,)), dma((RZ,)), dma((RZ,)), dma((RC,)), dma((max(2 + paired, 14),)), dma((2,)),
                dma((2, 2)), dma((2, 2, 2)), dma((2, 2)), dma((2, 2, 2)), dma((D3,)), dma((D3,)), dma((DO,)), dma,
                pltpu.SemaphoreType.REGULAR((3, 2)),
            ],
            compiler_params=pltpu.CompilerParams(
                collective_id=0, has_side_effects=True, vmem_limit_bytes=56 * 1024 * 1024),
            cost_estimate=pl.CostEstimate(
                flops=2 * 8 * rows * 2 * depth * columns, bytes_accessed=6 * depth * columns, transcendentals=0),
        )(a_rows, b_rows)
        return out[0]

    return jax.shard_map(local_block, mesh=mesh, in_specs=(spec_rows, spec_rows), out_specs=spec_rows, check_vma=False)
```

```python
import jax
import jax.numpy as jnp
from jax import lax
from jax.experimental import pallas as pl
from jax.experimental.pallas import tpu as pltpu
from jax.sharding import PartitionSpec as P

MESH = pl.DeviceIdType.MESH
W = 128
C = 2 * W
LOOK = 2
D3 = 6
DO = 6
LATE = 4
AHEAD = 2
LAG = 5
RX, RZ, RC = 2 * LOOK, LOOK + 1, 8
AX, AY, AZ = 0, 1, 2


def bits_of(d):
    return (d // 4, (d // 2) % 2, d % 2)


def counts(columns):
    paired = columns // C // 4
    return columns // C - 2 * paired - 1, paired


def kernel(a_hbm, b_hbm, c_v, bx_hbm, bz_hbm, bxz_hbm, relay,
           a_v, b_v, p_v, r1_v, s2_v, r2_v, s3_v, r3_v, q_v,
           hop_send, own_sem, bx_send, bx_recv, bxz_send, bxz_recv, ch_send, ch_recv, b_sem,
           s1_sem, r1_sem, s2_sem, r2_sem, s3_sem, r3_sem, qs_sem, qr_sem, credit):
    depth, columns = b_hbm.shape
    plain, paired = counts(columns)
    tiles = plain + paired
    rows, upper = a_hbm.shape[0], a_hbm.shape[0] // 2
    half = depth // 2
    chunks = 16 + 2 * paired
    last = plain + paired
    rate = max(114, -(-1600 // plain), -(-100 * (15 + 2 * paired) // (tiles - 1)))

    dp, tp = lax.axis_index("dp"), lax.axis_index("tp")
    core, x, y, z = dp % 2, (dp // 2) % 2, dp // 4, tp

    def flip(v, bit):
        return v + bit - 2 * v * bit

    def device(bits, other=0):
        return {"dp": flip(y, bits[1]) * 4 + flip(x, bits[0]) * 2 + flip(core, other), "tp": flip(z, bits[2])}

    axis_nbr = [device((1, 0, 0)), device((0, 1, 0)), device((0, 0, 1))]
    partner = device((0, 0, 0), 1)

    barrier = pltpu.get_barrier_semaphore()
    for nbr in (*axis_nbr, partner):
        pl.semaphore_signal(barrier, inc=1, device_id=nbr, device_id_type=MESH)

    def send(src, dst, send_sem, recv_sem, to):
        return pltpu.make_async_remote_copy(
            src_ref=src, dst_ref=dst, send_sem=send_sem, recv_sem=recv_sem, device_id=to, device_id_type=MESH)

    def wait_bytes(ref, sem):
        pltpu.make_async_copy(ref, ref, sem).wait()

    def when(t, low, high, fn):
        pl.when(jnp.logical_and(t >= low, t < high))(fn)

    def is_paired(t):
        return (t + tiles - plain) // tiles

    def tile_cols(t, g=None):
        col = t * C + is_paired(t) * ((t - plain) * C + z * C)
        if g is None:
            return pl.ds(pl.multiple_of(col, W), C)
        return pl.ds(pl.multiple_of(col + g * W, W), W)

    def their_cols(q):
        return pl.ds(pl.multiple_of((plain + 2 * q + 1 - z) * C, W), C)

    def last_cols(side):
        return pl.ds(pl.multiple_of((plain + 2 * paired) * C + side * W, W), W)

    def a_cols(bits, h):
        to = device(bits, h)
        return a_hbm.at[:, pl.ds(pl.multiple_of((to["dp"] * 2 + to["tp"]) * depth, depth), depth)]

    def near(d, h):
        return a_v.at[d, :, pl.ds(h * depth, depth)]

    def far(d, h):
        return a_v.at[d, :, pl.ds((2 + h) * depth, depth)]

    def held(i, h):
        return relay.at[i, :, pl.ds(h * depth, depth)]

    def hop(n, h, src, dst, axis):
        return send(src, dst, hop_send, ch_recv.at[-n if n < 0 else 4 + 2 * n + h], axis_nbr[axis])

    both = range(2)
    xy_far1 = [hop(0, h, a_cols((1, 1, 1), h), held(0, h), AX) for h in both]
    xy_near1 = [hop(1, h, a_cols((1, 1, 0), h), held(1, h), AX) for h in both]
    x_far = [hop(2, h, a_cols((1, 0, 1), h), far(4, h), AX) for h in both]
    y_far = [hop(3, h, a_cols((0, 1, 1), h), far(2, h), AY) for h in both]
    xy_far2 = [hop(4, h, held(0, h), far(6, h), AY) for h in both]
    z_own = [hop(-1, h, a_cols((0, 0, 1), h), near(1, h), AZ) for h in both]
    z_y = [hop(-1, h, far(2, h), near(3, h), AZ) for h in both]
    xy_near2 = [hop(-2, h, held(1, h), near(6, h), AY) for h in both]
    z_xy = [hop(-2, h, far(6, h), near(7, h), AZ) for h in both]
    x_near = [hop(-3, h, a_cols((1, 0, 0), h), near(4, h), AX) for h in both]
    y_near = [hop(-3, h, a_cols((0, 1, 0), h), near(2, h), AY) for h in both]
    z_x = [hop(-3, h, far(4, h), near(5, h), AZ) for h in both]
    hops = 24

    def end_group(n, copies):
        wait_bytes(a_v.at[pl.ds(0, copies // 2), :, pl.ds(0, 2 * depth)], ch_recv.at[n])

    own = [pltpu.make_async_copy(a_cols((0, 0, 0), h), near(0, h), own_sem) for h in both]
    own += [pltpu.make_async_copy(a_cols((0, 0, 1), h), far(0, h), own_sem) for h in both]

    def a_chunk(n):
        d, k = (n // 4) * 2, n % 4
        return send(a_v.at[d, :, pl.ds(pl.multiple_of(k * half, half), half)],
                    a_v.at[d + 1, :, pl.ds(pl.multiple_of(2 * depth + k * half, half), half)],
                    ch_send.at[n % RC], ch_recv.at[0], axis_nbr[AZ])

    def b_chunk(q, h):
        rows = pl.ds(pl.multiple_of(h * half, half), half)
        n = 16 + 2 * q + h
        return send(b_hbm.at[rows, their_cols(q)], bz_hbm.at[q, rows], ch_send.at[n % RC], ch_recv.at[1 + q], axis_nbr[AZ])

    def last_chunk():
        return send(b_hbm.at[:, last_cols(1 - z)], bz_hbm.at[paired, :, 0:W], ch_send.at[chunks % RC], ch_recv.at[1 + paired], axis_nbr[AZ])

    def start_chunks(i):
        def body(n, carry):
            when(n, 0, 16, lambda: a_chunk(n).start())
            when(n, 16, chunks, lambda: b_chunk((n - 16) // 2, (n - 16) % 2).start())
            when(n, chunks, chunks + 1, lambda: last_chunk().start())
            return carry

        lax.fori_loop(rate * i // 100 + AHEAD, rate * (i + 1) // 100 + AHEAD, body, 0)

    def end_chunks(i):
        def body(n, carry):
            when(n, 0, 16, lambda: a_chunk(n).wait_send())
            when(n, 16, chunks, lambda: b_chunk((n - 16) // 2, (n - 16) % 2).wait_send())
            when(n, chunks, chunks + 1, lambda: last_chunk().wait_send())
            return carry

        lax.fori_loop(rate * i // 100 + AHEAD, rate * (i + 1) // 100 + AHEAD, body, 0)

    def bx_copy(t):
        return send(b_hbm.at[:, tile_cols(t)], bx_hbm.at[t], bx_send.at[t % RX], bx_recv.at[t % RX], partner)

    def bxz_copy(q):
        return send(bz_hbm.at[q], bxz_hbm.at[q], bxz_send.at[q % RZ], bxz_recv.at[q % RZ], partner)

    def last_bx():
        return send(b_hbm.at[:, last_cols(z)], bx_hbm.at[last, :, 0:W], bx_send.at[last % RX], bx_recv.at[last % RX], partner)

    def last_bxz():
        return send(bz_hbm.at[paired, :, 0:W], bxz_hbm.at[paired, :, 0:W], bxz_send.at[paired % RZ], bxz_recv.at[paired % RZ], partner)

    def last_piece(k):
        src = (b_hbm.at[:, last_cols(z)], bx_hbm.at[last, :, 0:W], bz_hbm.at[paired, :, 0:W], bxz_hbm.at[paired, :, 0:W])[k]
        return pltpu.make_async_copy(src, b_v.at[last % 2, pl.ds(k * depth, depth), 0:W], b_sem.at[last % 2])

    def b_piece(t, k):
        src = (b_hbm.at[:, tile_cols(t)], bx_hbm.at[t], bz_hbm.at[t - plain], bxz_hbm.at[t - plain])[k]
        return pltpu.make_async_copy(src, b_v.at[t % 2, pl.ds(k * depth, depth)], b_sem.at[t % 2])

    def fetch_near(t):
        b_piece(t, 0).start()
        bx_copy(t).wait_recv()
        b_piece(t, 1).start()

    def fetch_far(t):
        wait_bytes(bz_hbm.at[t - plain], ch_recv.at[1 + t - plain])
        bxz_copy(t - plain).start()
        b_piece(t, 2).start()

    def fetch_last(t):
        bxz_copy(t - plain).wait_recv()
        b_piece(t, 3).start()

    def last_near():
        last_piece(0).start()
        last_bx().wait_recv()
        last_piece(1).start()

    def last_far():
        last_chunk().wait_recv()
        last_bxz().start()
        last_piece(2).start()

    def last_fetch():
        last_bxz().wait_recv()
        last_piece(3).start()

    def partial(t, d, k):
        s = t % 2
        dx, dy, dz = bits_of(d)
        part = jnp.dot(a_v[d, :, 0:k * depth], b_v[s, 0:k * depth], preferred_element_type=jnp.float32)
        p_v[s, 0, dx, dy * 2 + dz] = part[:, 0:W]
        p_v[s, 1, dy, dx * 2 + dz] = part[:, W:C]

    def last_partials():
        s = last % 2

        def body(d, carry):
            dx, dy, dz = bits_of(d)
            part = jnp.dot(a_v[d], b_v[s, :, 0:W], preferred_element_type=jnp.float32)
            p_v[s, 0, dx, dy * 2 + dz, 0:upper] = part[0:upper]
            p_v[s, 1, dy, dx * 2 + dz, 0:upper] = part[upper:rows]
            return carry

        lax.fori_loop(0, 8, body, 0)

    def partials(t, k, n=8, order=lambda j: j):
        def body(j, carry):
            partial(t, order(j), k)
            return carry

        lax.fori_loop(0, n, body, 0)

    def first_two(n, order):
        def body(j, carry):
            partial(j // n, order(j % n), 2)
            return carry

        lax.fori_loop(0, 2 * n, body, 0)

    def send1(t, g, k, n=rows):
        s, blocks, part = t % 2, pl.ds(2 * k, 2), pl.ds(0, n)
        return send(p_v.at[s, g, 1, blocks, part], r1_v.at[s, g, blocks, part],
                    s1_sem.at[s, g], r1_sem.at[s, g, k], axis_nbr[g])

    def send2(t, g, k, n=rows):
        s, part = t % 2, pl.ds(0, n)
        return send(s2_v.at[s, g, 2 + k, part], r2_v.at[s, g, k, part],
                    s2_sem.at[s, g], r2_sem.at[s, g, k], axis_nbr[1 - g])

    def sent1(t, g, n=rows):
        wait_bytes(p_v.at[t % 2, g, 1, :, pl.ds(0, n)], s1_sem.at[t % 2, g])

    def sent2(t, g, n=rows):
        wait_bytes(r2_v.at[t % 2, g, :, pl.ds(0, n)], s2_sem.at[t % 2, g])

    def send3(t, g):
        s = t % D3
        return send(s3_v.at[s, g, 1], r3_v.at[s, g], s3_sem.at[s], r3_sem.at[s], axis_nbr[AZ])

    def pair_there(t, g):
        s = t % DO
        return send(q_v.at[s, g], c_v.at[:, tile_cols(t, g)], qs_sem.at[s], qr_sem, axis_nbr[AZ])

    def last_there(g):
        s = last % DO
        return send(q_v.at[s, g, pl.ds(0, upper)], c_v.at[pl.ds(g * upper, upper), last_cols(z)],
                    qs_sem.at[s], qr_sem, axis_nbr[AZ])

    def sent3(t):
        wait_bytes(r3_v.at[t % D3], s3_sem.at[t % D3])

    def got3(t):
        wait_bytes(r3_v.at[t % D3], r3_sem.at[t % D3])

    def pair_sent(t):
        wait_bytes(q_v.at[t % DO], qs_sem.at[t % DO])

    def take(t, g, phase, slots, high):
        when(t, slots, high, lambda: pl.semaphore_wait(credit.at[phase, g], 1))

    def give(t, g, phase, axis, slots, high):
        when(t, 0, high - slots, lambda: pl.semaphore_signal(
            credit.at[phase, g], inc=1, device_id=axis_nbr[axis], device_id_type=MESH))

    for copy in own:
        copy.start()
    pl.semaphore_wait(barrier, 4)
    for h in both:
        for group in (xy_far1, y_far, z_own):
            group[h].start()
    for group in (xy_near1, x_far, x_near):
        for copy in group:
            copy.start()
    for t in range(min(LOOK, tiles)):
        bx_copy(t).start()
    for t in range(2):
        fetch_near(t)
    for h in both:
        y_far[h].wait_recv()
        z_y[h].start()
        xy_far1[h].wait_recv()
        xy_far2[h].start()
    for h in both:
        xy_near1[h].wait_recv()
        xy_near2[h].start()
        xy_far2[h].wait_recv()
        z_xy[h].start()
    for copy in y_near:
        copy.start()
    for t in range(2):
        wait_bytes(b_v.at[t, pl.ds(0, 2 * depth)], b_sem.at[t])
    wait_bytes(a_v.at[0], own_sem)
    end_group(1, 4)
    first_two(3, lambda j: j + j // 2)
    for h in both:
        x_far[h].wait_recv()
        z_x[h].start()
    for n in range(AHEAD):
        a_chunk(n).start()
    end_group(2, 4)
    first_two(2, lambda j: 6 + j)
    for t in range(2):
        for g in both:
            send1(t, g, 1).start()
    end_group(3, 6)

    def last_three(j):
        return 2 + (3 * j + 1) // 2

    def add3(t, g):
        c_v[:, tile_cols(t, g)] = (s3_v[t % D3, g, 0] + r3_v[t % D3, g]).astype(jnp.bfloat16)

    def start_late():
        def body(t, carry):
            for g in both:
                when(t, D3, plain, lambda g=g: pl.semaphore_wait(credit.at[2, g], 1))
                send3(t, g).start()
            return carry

        lax.fori_loop(plain - LATE, plain, body, 0)

    def each(low, high, fn):
        def body(n, carry):
            fn(n)
            return carry

        lax.fori_loop(low, high, body, 0)

    def end_hops():
        wait_bytes(a_v.at[pl.ds(0, hops // 4)], hop_send)
        for n in range(AHEAD):
            a_chunk(n).wait_send()

    def step(i, carry):
        t = i
        when(t, 0, tiles, lambda: start_chunks(t))
        when(t, LAG, tiles + 3, lambda: end_chunks(t - LAG))
        when(t, 1, tiles + 1, lambda: bx_copy(t - 1).wait_send())
        when(t, plain + 1, tiles + 1, lambda: bxz_copy(t - 1 - plain).wait_send())
        when(t, LAG, LAG + 1, end_hops)
        when(t, 0, tiles - LOOK, lambda: bx_copy(t + LOOK).start())
        when(t, tiles - LOOK, tiles - LOOK + 1, lambda: last_bx().start())
        when(t, 1, tiles - 1, lambda: fetch_near(t + 1))
        when(t, tiles - 1, tiles, last_near)
        for g in both:
            when(t, 2, tiles + 2, lambda g=g: sent1(t - 2, g))

        def wait_b(pieces):
            wait_bytes(b_v.at[t % 2, pl.ds(0, pieces * depth)], b_sem.at[t % 2])

        def near_products():
            wait_b(2)
            partials(t, 2)

        def all_products():
            wait_b(4)
            partials(t, 4)

        def last_products():
            wait_bytes(b_v.at[last % 2, :, 0:W], b_sem.at[last % 2])
            last_partials()

        def start_last():
            for g in both:
                pl.semaphore_wait(credit.at[0, g], 1)
                send1(last, g, 1, upper).start()
            for g in both:
                send1(last, g, 0, upper).start()

        def wait_far():
            wait_bytes(a_v.at[pl.ds(0, 4), :, pl.ds(2 * depth, 2 * depth)], ch_recv.at[0])

        when(t, 0, 2, lambda: partials(t, 2, 3, last_three))
        when(t, 2, plain, near_products)
        when(t, plain, plain + 1, wait_far)
        when(t, plain, tiles, all_products)
        when(t, last, last + 1, last_products)
        for g in both:
            take(t, g, 0, 2, tiles)
            when(t, 2, tiles, lambda g=g: send1(t, g, 1).start())
        for g in both:
            when(t, 0, tiles, lambda g=g: send1(t, g, 0).start())
        when(t, plain - 1, tiles - 1, lambda: fetch_far(t + 1))
        when(t, tiles - 1, tiles, last_far)

        t1 = i - 1

        def add1(t, g, k, n=rows):
            s, blocks, part = t % 2, pl.ds(2 * k, 2), pl.ds(0, n)
            send1(t, g, k, n).wait_recv()
            s2_v[s, g, blocks, part] = p_v[s, g, 0, blocks, part] + r1_v[s, g, blocks, part]

        def last1():
            for g in both:
                add1(last, g, 1, upper)
                pl.semaphore_wait(credit.at[1, g], 1)
                send2(last, g, 1, upper).start()
            for g in both:
                send2(last - 1, g, 0).start()
            for g in both:
                send2(last, g, 0, upper).start()

        for g in both:
            when(t1, 2, tiles + 1, lambda g=g: sent2(t1 - 2, g))
            when(t1, 0, tiles, lambda g=g: add1(t1, g, 1))
            take(t1, g, 1, 2, tiles)
            when(t1, 0, tiles, lambda g=g: send2(t1, g, 1).start())
            when(t1, 0, tiles - 1, lambda g=g: send2(t1, g, 0).start())
        when(t, last, last + 1, start_last)
        for g in both:
            when(t1, 0, tiles, lambda g=g: add1(t1, g, 0))
            give(t1, g, 0, g, 2, last + 1)
        when(t1, last, last + 1, last1)

        t2 = i - 2

        def sum2(t, g, k, n=rows):
            part = pl.ds(0, n)
            send2(t, g, k, n).wait_recv()
            return s2_v[t % 2, g, k, part] + r2_v[t % 2, g, k, part]

        def last2():
            for g in both:
                add1(last, g, 0, upper)
            for g in both:
                q_v[last % DO, g, pl.ds(0, upper)] = sum2(last, g, 1, upper).astype(jnp.bfloat16)
                last_there(g).start()
            each(plain - LATE, plain, got3)
            for g in both:
                each(plain - LATE, plain, lambda t: add3(t, g))
            each(plain - LATE, plain, sent3)
            each(tiles + 3 - LAG, tiles, end_chunks)
            each(max(plain, last + 1 - DO), tiles - 1, pair_sent)
            last_bx().wait_send()
            last_bxz().wait_send()
            for g in both:
                sent1(last, g, upper)
            for g in both:
                add2_here(last - 1, g)
            for g in both:
                c_v[pl.ds(g * upper, upper), last_cols(z)] = sum2(last, g, 0, upper).astype(jnp.bfloat16)

        def add2(g, k):
            s3_v[t2 % D3, g, k] = sum2(t2, g, k)

        def add2_there(g):
            q_v[t2 % DO, g] = sum2(t2, g, 1).astype(jnp.bfloat16)

        def add2_here(t, g):
            c_v[:, tile_cols(t, g)] = sum2(t, g, 0).astype(jnp.bfloat16)

        when(t2, D3, plain - LATE + D3, lambda: sent3(t2 - D3))
        when(t2, plain + DO, last + 1, lambda: pair_sent(t2 - DO))
        for g in both:
            when(t2, 0, plain, lambda g=g: add2(g, 1))
            when(t2, plain, tiles, lambda g=g: add2_there(g))
            take(t2, g, 2, D3, plain - LATE)
            when(t2, 0, plain - LATE, lambda g=g: send3(t2, g).start())
            when(t2, plain, tiles, lambda g=g: pair_there(t2, g).start())
        for g in both:
            when(t2, 0, plain, lambda g=g: add2(g, 0))
            when(t2, plain, tiles - 1, lambda g=g: add2_here(t2, g))
            give(t2, g, 1, 1 - g, 2, last + 1)
        when(t2, last, last + 1, last2)

        t3 = i - 1 - D3
        when(t3, 0, plain - LATE, lambda: got3(t3))
        for g in both:
            when(t3, 0, plain - LATE, lambda g=g: add3(t3, g))
            give(t3, g, 2, AZ, D3, plain)
        when(t, last - 2, last - 1, start_late)
        when(t, plain - 1, tiles - 1, lambda: fetch_last(t + 1))
        when(t, tiles - 1, tiles, last_fetch)
        return carry

    lax.fori_loop(0, tiles + 3, step, 0)

    each(max(plain, tiles - 1), tiles, pair_sent)
    for g in both:
        sent2(last - 1, g)
        sent2(last, g, upper)
    wait_bytes(q_v.at[last % DO, :, pl.ds(0, upper)], qs_sem.at[last % DO])
    wait_bytes(c_v.at[:, pl.ds(0, paired * C + W)], qr_sem)


def write_out(c_v, c_hbm, sem):
    rows = c_v.shape[0] // 8
    copies = [pltpu.make_async_copy(c_v.at[pl.ds(i * rows, rows)], c_hbm.at[pl.ds(i * rows, rows)], sem.at[i]) for i in range(8)]
    for copy in copies:
        copy.start()
    for copy in copies:
        copy.wait()


def solution(mesh):
    spec_rows = P(("dp", "tp"), None)

    def local_block(a_rows, b_rows):
        rows, inner = a_rows.shape
        depth, columns = b_rows.shape
        plain, paired = counts(columns)
        tiles = plain + paired
        f32, bf16 = jnp.float32, jnp.bfloat16
        dma = pltpu.SemaphoreType.DMA
        out = pl.pallas_call(
            kernel,
            name="matmul_reduce_scatter",
            out_shape=(
                pltpu.VMEM((rows, columns), bf16),
                jax.ShapeDtypeStruct((tiles + 1, depth, C), bf16),
                jax.ShapeDtypeStruct((paired + 1, depth, C), bf16),
                jax.ShapeDtypeStruct((paired + 1, depth, C), bf16),
                jax.ShapeDtypeStruct((2, rows, 2 * depth), bf16),
            ),
            in_specs=[pl.BlockSpec(memory_space=pl.ANY)] * 2,
            out_specs=(pl.BlockSpec(memory_space=pltpu.VMEM),) + (pl.BlockSpec(memory_space=pl.ANY),) * 4,
            scratch_shapes=[
                pltpu.VMEM((8, rows, 4 * depth), bf16),
                pltpu.VMEM((2, 4 * depth, C), bf16),
                pltpu.VMEM((2, 2, 2, 4, rows, W), f32),
                pltpu.VMEM((2, 2, 4, rows, W), f32),
                pltpu.VMEM((2, 2, 4, rows, W), f32),
                pltpu.VMEM((2, 2, 2, rows, W), f32),
                pltpu.VMEM((D3, 2, 2, rows, W), f32),
                pltpu.VMEM((D3, 2, rows, W), f32),
                pltpu.VMEM((DO, 2, rows, W), bf16),
                dma, dma, dma((RX,)), dma((RX,)), dma((RZ,)), dma((RZ,)), dma((RC,)), dma((max(2 + paired, 14),)), dma((2,)),
                dma((2, 2)), dma((2, 2, 2)), dma((2, 2)), dma((2, 2, 2)), dma((D3,)), dma((D3,)), dma((DO,)), dma,
                pltpu.SemaphoreType.REGULAR((3, 2)),
            ],
            compiler_params=pltpu.CompilerParams(
                collective_id=0, has_side_effects=True, vmem_limit_bytes=56 * 1024 * 1024),
            cost_estimate=pl.CostEstimate(
                flops=2 * 8 * rows * 2 * depth * columns, bytes_accessed=6 * depth * columns, transcendentals=0),
        )(a_rows, b_rows)
        return pl.pallas_call(
            write_out,
            name="write_out",
            out_shape=jax.ShapeDtypeStruct((rows, columns), bf16),
            in_specs=[pl.BlockSpec(memory_space=pltpu.VMEM)],
            out_specs=pl.BlockSpec(memory_space=pl.ANY),
            scratch_shapes=[dma((8,))],
            compiler_params=pltpu.CompilerParams(vmem_limit_bytes=1024 * 1024),
            cost_estimate=pl.CostEstimate(flops=0, bytes_accessed=4 * rows * columns, transcendentals=0),
        )(out[0])

    return jax.shard_map(local_block, mesh=mesh, in_specs=(spec_rows, spec_rows), out_specs=spec_rows, check_vma=False)
```

```python
import jax
import jax.numpy as jnp
from jax import lax
from jax.experimental import pallas as pl
from jax.experimental.pallas import tpu as pltpu
from jax.sharding import PartitionSpec as P

MESH = pl.DeviceIdType.MESH
W = 128
C = 2 * W
LOOK = 2
D3 = 6
DO = 6
LATE = 4
AHEAD = 2
LAG = 5
RX, RZ, RC = 2 * LOOK, LOOK + 1, 8
AX, AY, AZ = 0, 1, 2


def bits_of(d):
    return (d // 4, (d // 2) % 2, d % 2)


def counts(columns):
    paired = columns // C // 4
    return columns // C - 2 * paired - 1, paired


def kernel(a_hbm, b_hbm, c_v, bx_hbm, bz_hbm, bxz_hbm, relay,
           a_v, b_v, p_v, r1_v, s2_v, r2_v, s3_v, r3_v, q_v,
           hop_send, own_sem, bx_send, bx_recv, bxz_send, bxz_recv, ch_send, ch_recv, b_sem,
           s1_sem, r1_sem, rk_sem, s2_sem, r2_sem, s3_sem, r3_sem, qs_sem, qr_sem, credit):
    depth, columns = b_hbm.shape
    plain, paired = counts(columns)
    tiles = plain + paired
    rows, upper = a_hbm.shape[0], a_hbm.shape[0] // 2
    half = depth // 2
    chunks = 16 + 2 * paired
    last = plain + paired
    rate = max(114, -(-1600 // plain), -(-100 * (15 + 2 * paired) // (tiles - 1)))

    dp, tp = lax.axis_index("dp"), lax.axis_index("tp")
    core, x, y, z = dp % 2, (dp // 2) % 2, dp // 4, tp

    def flip(v, bit):
        return v + bit - 2 * v * bit

    def device(bits, other=0):
        return {"dp": flip(y, bits[1]) * 4 + flip(x, bits[0]) * 2 + flip(core, other), "tp": flip(z, bits[2])}

    axis_nbr = [device((1, 0, 0)), device((0, 1, 0)), device((0, 0, 1))]
    partner = device((0, 0, 0), 1)

    barrier = pltpu.get_barrier_semaphore()
    for nbr in (*axis_nbr, partner):
        pl.semaphore_signal(barrier, inc=1, device_id=nbr, device_id_type=MESH)

    def send(src, dst, send_sem, recv_sem, to):
        return pltpu.make_async_remote_copy(
            src_ref=src, dst_ref=dst, send_sem=send_sem, recv_sem=recv_sem, device_id=to, device_id_type=MESH)

    def wait_bytes(ref, sem):
        pltpu.make_async_copy(ref, ref, sem).wait()

    def when(t, low, high, fn):
        pl.when(jnp.logical_and(t >= low, t < high))(fn)

    def is_paired(t):
        return (t + tiles - plain) // tiles

    def tile_cols(t, g=None):
        col = t * C + is_paired(t) * ((t - plain) * C + z * C)
        if g is None:
            return pl.ds(pl.multiple_of(col, W), C)
        return pl.ds(pl.multiple_of(col + g * W, W), W)

    def their_cols(q):
        return pl.ds(pl.multiple_of((plain + 2 * q + 1 - z) * C, W), C)

    def last_cols(side):
        return pl.ds(pl.multiple_of((plain + 2 * paired) * C + side * W, W), W)

    def a_cols(bits, h):
        to = device(bits, h)
        return a_hbm.at[:, pl.ds(pl.multiple_of((to["dp"] * 2 + to["tp"]) * depth, depth), depth)]

    def near(d, h):
        return a_v.at[d, :, pl.ds(h * depth, depth)]

    def far(d, h):
        return a_v.at[d, :, pl.ds((2 + h) * depth, depth)]

    def held(i, h):
        return relay.at[i, :, pl.ds(h * depth, depth)]

    def hop(n, h, src, dst, axis):
        return send(src, dst, hop_send, ch_recv.at[-n if n < 0 else 4 + 2 * n + h], axis_nbr[axis])

    both = range(2)
    xy_far1 = [hop(0, h, a_cols((1, 1, 1), h), held(0, h), AX) for h in both]
    xy_near1 = [hop(1, h, a_cols((1, 1, 0), h), held(1, h), AX) for h in both]
    x_far = [hop(2, h, a_cols((1, 0, 1), h), far(4, h), AX) for h in both]
    y_far = [hop(3, h, a_cols((0, 1, 1), h), far(2, h), AY) for h in both]
    xy_far2 = [hop(4, h, held(0, h), far(6, h), AY) for h in both]
    z_own = [hop(-1, h, a_cols((0, 0, 1), h), near(1, h), AZ) for h in both]
    z_y = [hop(-1, h, far(2, h), near(3, h), AZ) for h in both]
    xy_near2 = [hop(-2, h, held(1, h), near(6, h), AY) for h in both]
    z_xy = [hop(-2, h, far(6, h), near(7, h), AZ) for h in both]
    x_near = [hop(-3, h, a_cols((1, 0, 0), h), near(4, h), AX) for h in both]
    y_near = [hop(-3, h, a_cols((0, 1, 0), h), near(2, h), AY) for h in both]
    z_x = [hop(-3, h, far(4, h), near(5, h), AZ) for h in both]
    hops = 24

    def end_group(n, copies):
        wait_bytes(a_v.at[pl.ds(0, copies // 2), :, pl.ds(0, 2 * depth)], ch_recv.at[n])

    own = [pltpu.make_async_copy(a_cols((0, 0, 0), h), near(0, h), own_sem) for h in both]
    own += [pltpu.make_async_copy(a_cols((0, 0, 1), h), far(0, h), own_sem) for h in both]

    def a_chunk(n):
        d, k = (n // 4) * 2, n % 4
        return send(a_v.at[d, :, pl.ds(pl.multiple_of(k * half, half), half)],
                    a_v.at[d + 1, :, pl.ds(pl.multiple_of(2 * depth + k * half, half), half)],
                    ch_send.at[n % RC], ch_recv.at[0], axis_nbr[AZ])

    def b_chunk(q, h):
        rows = pl.ds(pl.multiple_of(h * half, half), half)
        n = 16 + 2 * q + h
        return send(b_hbm.at[rows, their_cols(q)], bz_hbm.at[q, rows], ch_send.at[n % RC], ch_recv.at[1 + q], axis_nbr[AZ])

    def last_chunk():
        return send(b_hbm.at[:, last_cols(1 - z)], bz_hbm.at[paired, :, 0:W], ch_send.at[chunks % RC], ch_recv.at[1 + paired], axis_nbr[AZ])

    def start_chunks(i):
        def body(n, carry):
            when(n, 0, 16, lambda: a_chunk(n).start())
            when(n, 16, chunks, lambda: b_chunk((n - 16) // 2, (n - 16) % 2).start())
            when(n, chunks, chunks + 1, lambda: last_chunk().start())
            return carry

        lax.fori_loop(rate * i // 100 + AHEAD, rate * (i + 1) // 100 + AHEAD, body, 0)

    def end_chunks(i):
        def body(n, carry):
            when(n, 0, 16, lambda: a_chunk(n).wait_send())
            when(n, 16, chunks, lambda: b_chunk((n - 16) // 2, (n - 16) % 2).wait_send())
            when(n, chunks, chunks + 1, lambda: last_chunk().wait_send())
            return carry

        lax.fori_loop(rate * i // 100 + AHEAD, rate * (i + 1) // 100 + AHEAD, body, 0)

    def bx_copy(t):
        return send(b_hbm.at[:, tile_cols(t)], bx_hbm.at[t], bx_send.at[t % RX], bx_recv.at[t % RX], partner)

    def bxz_copy(q):
        return send(bz_hbm.at[q], bxz_hbm.at[q], bxz_send.at[q % RZ], bxz_recv.at[q % RZ], partner)

    def last_bx():
        return send(b_hbm.at[:, last_cols(z)], bx_hbm.at[last, :, 0:W], bx_send.at[last % RX], bx_recv.at[last % RX], partner)

    def last_bxz():
        return send(bz_hbm.at[paired, :, 0:W], bxz_hbm.at[paired, :, 0:W], bxz_send.at[paired % RZ], bxz_recv.at[paired % RZ], partner)

    def last_piece(k):
        src = (b_hbm.at[:, last_cols(z)], bx_hbm.at[last, :, 0:W], bz_hbm.at[paired, :, 0:W], bxz_hbm.at[paired, :, 0:W])[k]
        return pltpu.make_async_copy(src, b_v.at[last % 2, pl.ds(k * depth, depth), 0:W], b_sem.at[last % 2])

    def b_piece(t, k):
        src = (b_hbm.at[:, tile_cols(t)], bx_hbm.at[t], bz_hbm.at[t - plain], bxz_hbm.at[t - plain])[k]
        return pltpu.make_async_copy(src, b_v.at[t % 2, pl.ds(k * depth, depth)], b_sem.at[t % 2])

    def fetch_near(t):
        b_piece(t, 0).start()
        bx_copy(t).wait_recv()
        b_piece(t, 1).start()

    def fetch_far(t):
        wait_bytes(bz_hbm.at[t - plain], ch_recv.at[1 + t - plain])
        bxz_copy(t - plain).start()
        b_piece(t, 2).start()

    def fetch_last(t):
        bxz_copy(t - plain).wait_recv()
        b_piece(t, 3).start()

    def last_near():
        last_piece(0).start()
        last_bx().wait_recv()
        last_piece(1).start()

    def last_far():
        last_chunk().wait_recv()
        last_bxz().start()
        last_piece(2).start()

    def last_fetch():
        last_bxz().wait_recv()
        last_piece(3).start()

    def partial(t, d, k):
        s = t % 2
        dx, dy, dz = bits_of(d)
        part = jnp.dot(a_v[d, :, 0:k * depth], b_v[s, 0:k * depth], preferred_element_type=jnp.float32)
        p_v[s, 0, dx, dy * 2 + dz] = part[:, 0:W]
        p_v[s, 1, dy, dx * 2 + dz] = part[:, W:C]

    def last_partials():
        s = last % 2

        def body(d, carry):
            dx, dy, dz = bits_of(d)
            part = jnp.dot(a_v[d], b_v[s, :, 0:W], preferred_element_type=jnp.float32)
            p_v[s, 0, dx, dy * 2 + dz, 0:upper] = part[0:upper]
            p_v[s, 1, dy, dx * 2 + dz, 0:upper] = part[upper:rows]
            return carry

        lax.fori_loop(0, 8, body, 0)

    def partials(t, k, n=8, order=lambda j: j):
        def body(j, carry):
            partial(t, order(j), k)
            return carry

        lax.fori_loop(0, n, body, 0)

    def first_two(n, order):
        def body(j, carry):
            partial(j // n, order(j % n), 2)
            return carry

        lax.fori_loop(0, 2 * n, body, 0)

    def send1(t, g, k):
        s, blocks = t % 2, pl.ds(2 * k, 2)
        return send(p_v.at[s, g, 1, blocks], r1_v.at[s, g, blocks], s1_sem.at[s], r1_sem.at[s, k], axis_nbr[g])

    def got1(t, k):
        wait_bytes(r1_v.at[t % 2, :, pl.ds(2 * k, 2)], r1_sem.at[t % 2, k])

    def sent1(t):
        wait_bytes(r1_v.at[t % 2], s1_sem.at[t % 2])

    def send2(t, g, k, n=rows):
        s, part = t % 2, pl.ds(0, n)
        return send(s2_v.at[s, g, 2 + k, part], r2_v.at[s, g, k, part], s2_sem.at[s], r2_sem.at[s, k], axis_nbr[1 - g])

    def got2(t, k, n=rows):
        wait_bytes(r2_v.at[t % 2, :, k, pl.ds(0, n)], r2_sem.at[t % 2, k])

    def sent2(t, n=rows):
        wait_bytes(r2_v.at[t % 2, :, :, pl.ds(0, n)], s2_sem.at[t % 2])

    pieces = (pl.ds(2, 2), pl.ds(1, 1), pl.ds(0, 1))
    last_part = pl.ds(0, upper)

    def last_sem(k):
        return (r1_sem.at[last % 2, 1], rk_sem, r1_sem.at[last % 2, 0])[k]

    def last_send1(g, k):
        s = last % 2
        return send(p_v.at[s, g, 1, pieces[k], last_part], r1_v.at[s, g, pieces[k], last_part],
                    s1_sem.at[s], last_sem(k), axis_nbr[g])

    def last_add1(k):
        s = last % 2
        wait_bytes(r1_v.at[s, :, pieces[k], last_part], last_sem(k))
        for g in both:
            s2_v[s, g, pieces[k], last_part] = p_v[s, g, 0, pieces[k], last_part] + r1_v[s, g, pieces[k], last_part]

    def send3(t, g):
        s = t % D3
        return send(s3_v.at[s, g, 1], r3_v.at[s, g], s3_sem.at[s], r3_sem.at[s], axis_nbr[AZ])

    def pair_there(t, g):
        s = t % DO
        return send(q_v.at[s, g], c_v.at[:, tile_cols(t, g)], qs_sem.at[s], qr_sem, axis_nbr[AZ])

    def last_there(g):
        s = last % DO
        return send(q_v.at[s, g, pl.ds(0, upper)], c_v.at[pl.ds(g * upper, upper), last_cols(z)],
                    qs_sem.at[s], qr_sem, axis_nbr[AZ])

    def sent3(t):
        wait_bytes(r3_v.at[t % D3], s3_sem.at[t % D3])

    def got3(t):
        wait_bytes(r3_v.at[t % D3], r3_sem.at[t % D3])

    def pair_sent(t):
        wait_bytes(q_v.at[t % DO], qs_sem.at[t % DO])

    def take(t, g, phase, slots, high):
        when(t, slots, high, lambda: pl.semaphore_wait(credit.at[phase, g], 1))

    def give(t, g, phase, axis, slots, high):
        when(t, 0, high - slots, lambda: pl.semaphore_signal(
            credit.at[phase, g], inc=1, device_id=axis_nbr[axis], device_id_type=MESH))

    for copy in own:
        copy.start()
    pl.semaphore_wait(barrier, 4)
    for group in (xy_far1, y_far, z_own, xy_near1, x_far, x_near):
        for copy in group:
            copy.start()
    for t in range(min(LOOK, tiles)):
        bx_copy(t).start()
    for t in range(2):
        fetch_near(t)
    for h in both:
        y_far[h].wait_recv()
        z_y[h].start()
        xy_far1[h].wait_recv()
        xy_far2[h].start()
    for h in both:
        xy_near1[h].wait_recv()
        xy_near2[h].start()
        xy_far2[h].wait_recv()
        z_xy[h].start()
    for copy in y_near:
        copy.start()
    for t in range(2):
        wait_bytes(b_v.at[t, pl.ds(0, 2 * depth)], b_sem.at[t])
    wait_bytes(a_v.at[0], own_sem)
    end_group(1, 4)
    first_two(3, lambda j: j + j // 2)
    for h in both:
        x_far[h].wait_recv()
        z_x[h].start()
    for n in range(AHEAD):
        a_chunk(n).start()
    end_group(2, 4)
    first_two(2, lambda j: 6 + j)
    for t in range(2):
        for g in both:
            send1(t, g, 1).start()
    end_group(3, 6)

    def last_three(j):
        return 2 + (3 * j + 1) // 2

    def add3(t, g):
        c_v[:, tile_cols(t, g)] = (s3_v[t % D3, g, 0] + r3_v[t % D3, g]).astype(jnp.bfloat16)

    def start_late():
        def body(t, carry):
            for g in both:
                when(t, D3, plain, lambda g=g: pl.semaphore_wait(credit.at[2, g], 1))
                send3(t, g).start()
            return carry

        lax.fori_loop(plain - LATE, plain, body, 0)

    def each(low, high, fn):
        def body(n, carry):
            fn(n)
            return carry

        lax.fori_loop(low, high, body, 0)

    def end_hops():
        wait_bytes(a_v.at[pl.ds(0, hops // 4)], hop_send)
        for n in range(AHEAD):
            a_chunk(n).wait_send()

    def step(i, carry):
        t = i
        when(t, 0, tiles, lambda: start_chunks(t))
        when(t, LAG, tiles + 3, lambda: end_chunks(t - LAG))
        when(t, 1, tiles + 1, lambda: bx_copy(t - 1).wait_send())
        when(t, plain + 1, tiles + 1, lambda: bxz_copy(t - 1 - plain).wait_send())
        when(t, LAG, LAG + 1, end_hops)
        when(t, 0, tiles - LOOK, lambda: bx_copy(t + LOOK).start())
        when(t, tiles - LOOK, tiles - LOOK + 1, lambda: last_bx().start())
        when(t, 1, tiles - 1, lambda: fetch_near(t + 1))
        when(t, tiles - 1, tiles, last_near)
        when(t, 2, tiles + 2, lambda: sent1(t - 2))

        def wait_b(pieces):
            wait_bytes(b_v.at[t % 2, pl.ds(0, pieces * depth)], b_sem.at[t % 2])

        def near_products():
            wait_b(2)
            partials(t, 2)

        def all_products():
            wait_b(4)
            partials(t, 4)

        def last_products():
            wait_bytes(b_v.at[last % 2, :, 0:W], b_sem.at[last % 2])
            last_partials()

            for g in both:
                pl.semaphore_wait(credit.at[0, g], 1)
                last_send1(g, 0).start()

        def start_kept():
            for g in both:
                last_send1(g, 1).start()

        def wait_far():
            wait_bytes(a_v.at[pl.ds(0, 4), :, pl.ds(2 * depth, 2 * depth)], ch_recv.at[0])

        when(t, 0, 2, lambda: partials(t, 2, 3, last_three))
        when(t, 2, plain, near_products)
        when(t, plain, plain + 1, wait_far)
        when(t, plain, tiles, all_products)
        when(t, last, last + 1, last_products)
        for g in both:
            take(t, g, 0, 2, tiles)
            when(t, 2, tiles, lambda g=g: send1(t, g, 1).start())
        for g in both:
            when(t, 0, tiles, lambda g=g: send1(t, g, 0).start())
        when(t, plain - 1, tiles - 1, lambda: fetch_far(t + 1))
        when(t, tiles - 1, tiles, last_far)

        t1 = i - 1

        def add1(k):
            s, blocks = t1 % 2, pl.ds(2 * k, 2)
            got1(t1, k)
            for g in both:
                s2_v[s, g, blocks] = p_v[s, g, 0, blocks] + r1_v[s, g, blocks]

        def last1():
            last_add1(0)
            for g in both:
                pl.semaphore_wait(credit.at[1, g], 1)
                send2(last, g, 1, upper).start()
            for g in both:
                send2(last - 1, g, 0).start()
            for g in both:
                last_send1(g, 2).start()
            for g in both:
                send2(last, g, 0, upper).start()

        when(t1, 2, tiles + 1, lambda: sent2(t1 - 2))
        when(t1, 0, tiles, lambda: add1(1))
        for g in both:
            take(t1, g, 1, 2, tiles)
            when(t1, 0, tiles, lambda g=g: send2(t1, g, 1).start())
            when(t1, 0, tiles - 1, lambda g=g: send2(t1, g, 0).start())
        when(t, last, last + 1, start_kept)
        when(t1, 0, tiles, lambda: add1(0))
        for g in both:
            give(t1, g, 0, g, 2, last + 1)
        when(t1, last, last + 1, last1)

        t2 = i - 2

        def sum2(t, g, k, n=rows):
            part = pl.ds(0, n)
            return s2_v[t % 2, g, k, part] + r2_v[t % 2, g, k, part]

        def last2():
            last_add1(1)
            got2(last, 1, upper)
            for g in both:
                q_v[last % DO, g, last_part] = sum2(last, g, 1, upper).astype(jnp.bfloat16)
                last_there(g).start()
            each(plain - LATE, plain, got3)
            for g in both:
                each(plain - LATE, plain, lambda t: add3(t, g))
            each(plain - LATE, plain, sent3)
            each(tiles + 3 - LAG, tiles, end_chunks)
            each(max(plain, last + 1 - DO), tiles - 1, pair_sent)
            last_bx().wait_send()
            last_bxz().wait_send()
            add2_here(last - 1)
            last_add1(2)
            got2(last, 0, upper)
            for g in both:
                c_v[pl.ds(g * upper, upper), last_cols(z)] = sum2(last, g, 0, upper).astype(jnp.bfloat16)

        def add2(k):
            got2(t2, k)
            for g in both:
                s3_v[t2 % D3, g, k] = sum2(t2, g, k)

        def add2_there():
            got2(t2, 1)
            for g in both:
                q_v[t2 % DO, g] = sum2(t2, g, 1).astype(jnp.bfloat16)

        def add2_here(t):
            got2(t, 0)
            for g in both:
                c_v[:, tile_cols(t, g)] = sum2(t, g, 0).astype(jnp.bfloat16)

        when(t2, D3, plain - LATE + D3, lambda: sent3(t2 - D3))
        when(t2, plain + DO, last + 1, lambda: pair_sent(t2 - DO))
        when(t2, 0, plain, lambda: add2(1))
        when(t2, plain, tiles, add2_there)
        for g in both:
            take(t2, g, 2, D3, plain - LATE)
            when(t2, 0, plain - LATE, lambda g=g: send3(t2, g).start())
            when(t2, plain, tiles, lambda g=g: pair_there(t2, g).start())
        when(t2, 0, plain, lambda: add2(0))
        when(t2, plain, tiles - 1, lambda: add2_here(t2))
        for g in both:
            give(t2, g, 1, 1 - g, 2, last + 1)
        when(t2, last, last + 1, last2)

        t3 = i - 1 - D3
        when(t3, 0, plain - LATE, lambda: got3(t3))
        for g in both:
            when(t3, 0, plain - LATE, lambda g=g: add3(t3, g))
            give(t3, g, 2, AZ, D3, plain)
        when(t, last - 2, last - 1, start_late)
        when(t, plain - 1, tiles - 1, lambda: fetch_last(t + 1))
        when(t, tiles - 1, tiles, last_fetch)
        return carry

    lax.fori_loop(0, tiles + 3, step, 0)

    each(max(plain, tiles - 1), tiles, pair_sent)
    wait_bytes(r1_v.at[last % 2, :, :, last_part], s1_sem.at[last % 2])
    sent2(last - 1)
    sent2(last, upper)
    wait_bytes(q_v.at[last % DO, :, pl.ds(0, upper)], qs_sem.at[last % DO])
    wait_bytes(c_v.at[:, pl.ds(0, paired * C + W)], qr_sem)


def solution(mesh):
    spec_rows = P(("dp", "tp"), None)

    def local_block(a_rows, b_rows):
        rows, inner = a_rows.shape
        depth, columns = b_rows.shape
        plain, paired = counts(columns)
        tiles = plain + paired
        f32, bf16 = jnp.float32, jnp.bfloat16
        dma = pltpu.SemaphoreType.DMA
        out = pl.pallas_call(
            kernel,
            name="matmul_reduce_scatter",
            out_shape=(
                pltpu.VMEM((rows, columns), bf16),
                jax.ShapeDtypeStruct((tiles + 1, depth, C), bf16),
                jax.ShapeDtypeStruct((paired + 1, depth, C), bf16),
                jax.ShapeDtypeStruct((paired + 1, depth, C), bf16),
                jax.ShapeDtypeStruct((2, rows, 2 * depth), bf16),
            ),
            in_specs=[pl.BlockSpec(memory_space=pl.ANY)] * 2,
            out_specs=(pl.BlockSpec(memory_space=pltpu.VMEM),) + (pl.BlockSpec(memory_space=pl.ANY),) * 4,
            scratch_shapes=[
                pltpu.VMEM((8, rows, 4 * depth), bf16),
                pltpu.VMEM((2, 4 * depth, C), bf16),
                pltpu.VMEM((2, 2, 2, 4, rows, W), f32),
                pltpu.VMEM((2, 2, 4, rows, W), f32),
                pltpu.VMEM((2, 2, 4, rows, W), f32),
                pltpu.VMEM((2, 2, 2, rows, W), f32),
                pltpu.VMEM((D3, 2, 2, rows, W), f32),
                pltpu.VMEM((D3, 2, rows, W), f32),
                pltpu.VMEM((DO, 2, rows, W), bf16),
                dma, dma, dma((RX,)), dma((RX,)), dma((RZ,)), dma((RZ,)), dma((RC,)), dma((max(2 + paired, 14),)), dma((2,)),
                dma((2,)), dma((2, 2)), dma, dma((2,)), dma((2, 2)), dma((D3,)), dma((D3,)), dma((DO,)), dma,
                pltpu.SemaphoreType.REGULAR((3, 2)),
            ],
            compiler_params=pltpu.CompilerParams(
                collective_id=0, has_side_effects=True, vmem_limit_bytes=56 * 1024 * 1024),
            cost_estimate=pl.CostEstimate(
                flops=2 * 8 * rows * 2 * depth * columns, bytes_accessed=6 * depth * columns, transcendentals=0),
        )(a_rows, b_rows)
        return out[0]

    return jax.shard_map(local_block, mesh=mesh, in_specs=(spec_rows, spec_rows), out_specs=spec_rows, check_vma=False)
```

```python
import jax
import jax.numpy as jnp
from jax import lax
from jax.experimental import pallas as pl
from jax.experimental.pallas import tpu as pltpu
from jax.sharding import PartitionSpec as P

MESH = pl.DeviceIdType.MESH
W = 128
C = 2 * W
LOOK = 2
D3 = 6
DO = 6
LATE = 4
AHEAD = 2
LAG = 5
RX, RZ, RC = 2 * LOOK, LOOK + 1, 8
AX, AY, AZ = 0, 1, 2


def bits_of(d):
    return (d // 4, (d // 2) % 2, d % 2)


def counts(columns):
    paired = columns // C // 4
    return columns // C - 2 * paired - 1, paired


def kernel(a_hbm, b_hbm, c_v, bx_hbm, bz_hbm, bxz_hbm, relay,
           head_v, a_v, b_v, p_v, r1_v, s2_v, r2_v, s3_v, r3_v, q_v,
           head_sem, hop_send, own_sem, bx_send, bx_recv, bxz_send, bxz_recv, ch_send, ch_recv, b_sem,
           s1_sem, r1_sem, rk_sem, s2_sem, r2_sem, s3_sem, r3_sem, qs_sem, qr_sem, credit):
    depth, columns = b_hbm.shape
    plain, paired = counts(columns)
    tiles = plain + paired
    rows, upper = a_hbm.shape[0], a_hbm.shape[0] // 2
    half = depth // 2
    chunks = 16 + 2 * paired
    last = plain + paired
    rate = max(114, -(-1600 // plain), -(-100 * (15 + 2 * paired) // (tiles - 1)))

    dp, tp = lax.axis_index("dp"), lax.axis_index("tp")
    core, x, y, z = dp % 2, (dp // 2) % 2, dp // 4, tp

    def flip(v, bit):
        return v + bit - 2 * v * bit

    def device(bits, other=0):
        return {"dp": flip(y, bits[1]) * 4 + flip(x, bits[0]) * 2 + flip(core, other), "tp": flip(z, bits[2])}

    axis_nbr = [device((1, 0, 0)), device((0, 1, 0)), device((0, 0, 1))]
    partner = device((0, 0, 0), 1)

    barrier = pltpu.get_barrier_semaphore()
    for nbr in (*axis_nbr, partner):
        pl.semaphore_signal(barrier, inc=1, device_id=nbr, device_id_type=MESH)

    def send(src, dst, send_sem, recv_sem, to):
        return pltpu.make_async_remote_copy(
            src_ref=src, dst_ref=dst, send_sem=send_sem, recv_sem=recv_sem, device_id=to, device_id_type=MESH)

    def wait_bytes(ref, sem):
        pltpu.make_async_copy(ref, ref, sem).wait()

    def when(t, low, high, fn):
        pl.when(jnp.logical_and(t >= low, t < high))(fn)

    def is_paired(t):
        return (t + tiles - plain) // tiles

    def tile_cols(t, g=None):
        col = t * C + is_paired(t) * ((t - plain) * C + z * C)
        if g is None:
            return pl.ds(pl.multiple_of(col, W), C)
        return pl.ds(pl.multiple_of(col + g * W, W), W)

    def their_cols(q):
        return pl.ds(pl.multiple_of((plain + 2 * q + 1 - z) * C, W), C)

    def last_cols(side):
        return pl.ds(pl.multiple_of((plain + 2 * paired) * C + side * W, W), W)

    def a_cols(bits, h):
        to = device(bits, h)
        return a_hbm.at[:, pl.ds(pl.multiple_of((to["dp"] * 2 + to["tp"]) * depth, depth), depth)]

    def near(d, h):
        return a_v.at[d, :, pl.ds(h * depth, depth)]

    def far(d, h):
        return a_v.at[d, :, pl.ds((2 + h) * depth, depth)]

    def held(i, h):
        return relay.at[i, :, pl.ds(h * depth, depth)]

    def hop(n, h, src, dst, axis):
        return send(src, dst, hop_send, ch_recv.at[-n if n < 0 else 4 + 2 * n + h], axis_nbr[axis])

    both = range(2)
    xy_far1 = [hop(0, h, a_cols((1, 1, 1), h), held(0, h), AX) for h in both]
    xy_near1 = [hop(1, h, a_cols((1, 1, 0), h), held(1, h), AX) for h in both]
    x_far = [hop(2, h, a_cols((1, 0, 1), h), far(4, h), AX) for h in both]
    y_far = [hop(3, h, a_cols((0, 1, 1), h), far(2, h), AY) for h in both]
    xy_far2 = [hop(4, h, held(0, h), far(6, h), AY) for h in both]
    z_own = hop(-1, 1, a_cols((0, 0, 1), 1), near(1, 1), AZ)
    z_y = [hop(-1, h, far(2, h), near(3, h), AZ) for h in both]
    xy_near2 = [hop(-2, h, held(1, h), near(6, h), AY) for h in both]
    z_xy = [hop(-2, h, far(6, h), near(7, h), AZ) for h in both]
    x_near = [hop(-3, h, a_cols((1, 0, 0), h), near(4, h), AX) for h in both]
    y_near = [hop(-3, h, a_cols((0, 1, 0), h), near(2, h), AY) for h in both]
    z_x = [hop(-3, h, far(4, h), near(5, h), AZ) for h in both]
    hops = 24

    head = rows // 8
    openers = ((0, a_cols((1, 1, 1), 0), held(0, 0), AX), (3, a_cols((0, 1, 1), 0), far(2, 0), AY),
               (-1, a_cols((0, 0, 1), 0), near(1, 0), AZ))
    loads = [pltpu.make_async_copy(src.at[pl.ds(0, head)], head_v.at[i], head_sem) for i, (_, src, _, _) in enumerate(openers)]
    heads = [hop(n, 0, head_v.at[i], dst.at[pl.ds(0, head)], axis) for i, (n, _, dst, axis) in enumerate(openers)]
    tails = [hop(n, 0, src.at[pl.ds(head, rows - head)], dst.at[pl.ds(head, rows - head)], axis) for n, src, dst, axis in openers]

    def end_group(n, copies):
        wait_bytes(a_v.at[pl.ds(0, copies // 2), :, pl.ds(0, 2 * depth)], ch_recv.at[n])

    own = [pltpu.make_async_copy(a_cols((0, 0, 0), h), near(0, h), own_sem) for h in both]
    own += [pltpu.make_async_copy(a_cols((0, 0, 1), h), far(0, h), own_sem) for h in both]

    def a_chunk(n):
        d, k = (n // 4) * 2, n % 4
        return send(a_v.at[d, :, pl.ds(pl.multiple_of(k * half, half), half)],
                    a_v.at[d + 1, :, pl.ds(pl.multiple_of(2 * depth + k * half, half), half)],
                    ch_send.at[n % RC], ch_recv.at[0], axis_nbr[AZ])

    def b_chunk(q, h):
        rows = pl.ds(pl.multiple_of(h * half, half), half)
        n = 16 + 2 * q + h
        return send(b_hbm.at[rows, their_cols(q)], bz_hbm.at[q, rows], ch_send.at[n % RC], ch_recv.at[1 + q], axis_nbr[AZ])

    def last_chunk():
        return send(b_hbm.at[:, last_cols(1 - z)], bz_hbm.at[paired, :, 0:W], ch_send.at[chunks % RC], ch_recv.at[1 + paired], axis_nbr[AZ])

    def start_chunks(i):
        def body(n, carry):
            when(n, 0, 16, lambda: a_chunk(n).start())
            when(n, 16, chunks, lambda: b_chunk((n - 16) // 2, (n - 16) % 2).start())
            when(n, chunks, chunks + 1, lambda: last_chunk().start())
            return carry

        lax.fori_loop(rate * i // 100 + AHEAD, rate * (i + 1) // 100 + AHEAD, body, 0)

    def end_chunks(i):
        def body(n, carry):
            when(n, 0, 16, lambda: a_chunk(n).wait_send())
            when(n, 16, chunks, lambda: b_chunk((n - 16) // 2, (n - 16) % 2).wait_send())
            when(n, chunks, chunks + 1, lambda: last_chunk().wait_send())
            return carry

        lax.fori_loop(rate * i // 100 + AHEAD, rate * (i + 1) // 100 + AHEAD, body, 0)

    def bx_copy(t):
        return send(b_hbm.at[:, tile_cols(t)], bx_hbm.at[t], bx_send.at[t % RX], bx_recv.at[t % RX], partner)

    def bxz_copy(q):
        return send(bz_hbm.at[q], bxz_hbm.at[q], bxz_send.at[q % RZ], bxz_recv.at[q % RZ], partner)

    def last_bx():
        return send(b_hbm.at[:, last_cols(z)], bx_hbm.at[last, :, 0:W], bx_send.at[last % RX], bx_recv.at[last % RX], partner)

    def last_bxz():
        return send(bz_hbm.at[paired, :, 0:W], bxz_hbm.at[paired, :, 0:W], bxz_send.at[paired % RZ], bxz_recv.at[paired % RZ], partner)

    def last_piece(k):
        src = (b_hbm.at[:, last_cols(z)], bx_hbm.at[last, :, 0:W], bz_hbm.at[paired, :, 0:W], bxz_hbm.at[paired, :, 0:W])[k]
        return pltpu.make_async_copy(src, b_v.at[last % 2, pl.ds(k * depth, depth), 0:W], b_sem.at[last % 2])

    def b_piece(t, k):
        src = (b_hbm.at[:, tile_cols(t)], bx_hbm.at[t], bz_hbm.at[t - plain], bxz_hbm.at[t - plain])[k]
        return pltpu.make_async_copy(src, b_v.at[t % 2, pl.ds(k * depth, depth)], b_sem.at[t % 2])

    def fetch_near(t):
        b_piece(t, 0).start()
        bx_copy(t).wait_recv()
        b_piece(t, 1).start()

    def fetch_far(t):
        wait_bytes(bz_hbm.at[t - plain], ch_recv.at[1 + t - plain])
        bxz_copy(t - plain).start()
        b_piece(t, 2).start()

    def fetch_last(t):
        bxz_copy(t - plain).wait_recv()
        b_piece(t, 3).start()

    def last_near():
        last_piece(0).start()
        last_bx().wait_recv()
        last_piece(1).start()

    def last_far():
        last_chunk().wait_recv()
        last_bxz().start()
        last_piece(2).start()

    def last_fetch():
        last_bxz().wait_recv()
        last_piece(3).start()

    def partial(t, d, k):
        s = t % 2
        dx, dy, dz = bits_of(d)
        part = jnp.dot(a_v[d, :, 0:k * depth], b_v[s, 0:k * depth], preferred_element_type=jnp.float32)
        p_v[s, 0, dx, dy * 2 + dz] = part[:, 0:W]
        p_v[s, 1, dy, dx * 2 + dz] = part[:, W:C]

    def last_partials():
        s = last % 2

        def body(d, carry):
            dx, dy, dz = bits_of(d)
            part = jnp.dot(a_v[d], b_v[s, :, 0:W], preferred_element_type=jnp.float32)
            p_v[s, 0, dx, dy * 2 + dz, 0:upper] = part[0:upper]
            p_v[s, 1, dy, dx * 2 + dz, 0:upper] = part[upper:rows]
            return carry

        lax.fori_loop(0, 8, body, 0)

    def partials(t, k, n=8, order=lambda j: j):
        def body(j, carry):
            partial(t, order(j), k)
            return carry

        lax.fori_loop(0, n, body, 0)

    def first_two(n, order):
        def body(j, carry):
            partial(j // n, order(j % n), 2)
            return carry

        lax.fori_loop(0, 2 * n, body, 0)

    def send1(t, g, k):
        s, blocks = t % 2, pl.ds(2 * k, 2)
        return send(p_v.at[s, g, 1, blocks], r1_v.at[s, g, blocks], s1_sem.at[s], r1_sem.at[s, k], axis_nbr[g])

    def got1(t, k):
        wait_bytes(r1_v.at[t % 2, :, pl.ds(2 * k, 2)], r1_sem.at[t % 2, k])

    def sent1(t):
        wait_bytes(r1_v.at[t % 2], s1_sem.at[t % 2])

    def send2(t, g, k, n=rows):
        s, part = t % 2, pl.ds(0, n)
        return send(s2_v.at[s, g, 2 + k, part], r2_v.at[s, g, k, part], s2_sem.at[s], r2_sem.at[s, k], axis_nbr[1 - g])

    def got2(t, k, n=rows):
        wait_bytes(r2_v.at[t % 2, :, k, pl.ds(0, n)], r2_sem.at[t % 2, k])

    def sent2(t, n=rows):
        wait_bytes(r2_v.at[t % 2, :, :, pl.ds(0, n)], s2_sem.at[t % 2])

    pieces = (pl.ds(2, 2), pl.ds(1, 1), pl.ds(0, 1))
    last_part = pl.ds(0, upper)

    def last_sem(k):
        return (r1_sem.at[last % 2, 1], rk_sem, r1_sem.at[last % 2, 0])[k]

    def last_send1(g, k):
        s = last % 2
        return send(p_v.at[s, g, 1, pieces[k], last_part], r1_v.at[s, g, pieces[k], last_part],
                    s1_sem.at[s], last_sem(k), axis_nbr[g])

    def last_add1(k):
        s = last % 2
        wait_bytes(r1_v.at[s, :, pieces[k], last_part], last_sem(k))
        for g in both:
            s2_v[s, g, pieces[k], last_part] = p_v[s, g, 0, pieces[k], last_part] + r1_v[s, g, pieces[k], last_part]

    def send3(t, g):
        s = t % D3
        return send(s3_v.at[s, g, 1], r3_v.at[s, g], s3_sem.at[s], r3_sem.at[s], axis_nbr[AZ])

    def pair_there(t, g):
        s = t % DO
        return send(q_v.at[s, g], c_v.at[:, tile_cols(t, g)], qs_sem.at[s], qr_sem, axis_nbr[AZ])

    def last_there(g):
        s = last % DO
        return send(q_v.at[s, g, pl.ds(0, upper)], c_v.at[pl.ds(g * upper, upper), last_cols(z)],
                    qs_sem.at[s], qr_sem, axis_nbr[AZ])

    def sent3(t):
        wait_bytes(r3_v.at[t % D3], s3_sem.at[t % D3])

    def got3(t):
        wait_bytes(r3_v.at[t % D3], r3_sem.at[t % D3])

    def pair_sent(t):
        wait_bytes(q_v.at[t % DO], qs_sem.at[t % DO])

    def take(t, g, phase, slots, high):
        when(t, slots, high, lambda: pl.semaphore_wait(credit.at[phase, g], 1))

    def give(t, g, phase, axis, slots, high):
        when(t, 0, high - slots, lambda: pl.semaphore_signal(
            credit.at[phase, g], inc=1, device_id=axis_nbr[axis], device_id_type=MESH))

    for copy in loads:
        copy.start()
    pl.semaphore_wait(barrier, 4)
    wait_bytes(head_v, head_sem)
    for copy in heads + tails:
        copy.start()
    for copy in (xy_far1[1], y_far[1], z_own, *xy_near1, *x_far, *x_near):
        copy.start()
    for copy in own:
        copy.start()
    for t in range(min(LOOK, tiles)):
        bx_copy(t).start()
    for t in range(2):
        fetch_near(t)
    for h in both:
        y_far[h].wait_recv()
        z_y[h].start()
        xy_far1[h].wait_recv()
        xy_far2[h].start()
    for h in both:
        xy_near1[h].wait_recv()
        xy_near2[h].start()
        xy_far2[h].wait_recv()
        z_xy[h].start()
    for copy in y_near:
        copy.start()
    for t in range(2):
        wait_bytes(b_v.at[t, pl.ds(0, 2 * depth)], b_sem.at[t])
    wait_bytes(a_v.at[0], own_sem)
    end_group(1, 4)
    first_two(3, lambda j: j + j // 2)
    for h in both:
        x_far[h].wait_recv()
        z_x[h].start()
    for n in range(AHEAD):
        a_chunk(n).start()
    end_group(2, 4)
    first_two(2, lambda j: 6 + j)
    for t in range(2):
        for g in both:
            send1(t, g, 1).start()
    end_group(3, 6)

    def last_three(j):
        return 2 + (3 * j + 1) // 2

    def add3(t, g):
        c_v[:, tile_cols(t, g)] = (s3_v[t % D3, g, 0] + r3_v[t % D3, g]).astype(jnp.bfloat16)

    def start_late():
        def body(t, carry):
            for g in both:
                when(t, D3, plain, lambda g=g: pl.semaphore_wait(credit.at[2, g], 1))
                send3(t, g).start()
            return carry

        lax.fori_loop(plain - LATE, plain, body, 0)

    def each(low, high, fn):
        def body(n, carry):
            fn(n)
            return carry

        lax.fori_loop(low, high, body, 0)

    def end_hops():
        wait_bytes(a_v.at[pl.ds(0, hops // 4)], hop_send)
        for n in range(AHEAD):
            a_chunk(n).wait_send()

    def step(i, carry):
        t = i
        when(t, 0, tiles, lambda: start_chunks(t))
        when(t, LAG, tiles + 3, lambda: end_chunks(t - LAG))
        when(t, 1, tiles + 1, lambda: bx_copy(t - 1).wait_send())
        when(t, plain + 1, tiles + 1, lambda: bxz_copy(t - 1 - plain).wait_send())
        when(t, LAG, LAG + 1, end_hops)
        when(t, 0, tiles - LOOK, lambda: bx_copy(t + LOOK).start())
        when(t, tiles - LOOK, tiles - LOOK + 1, lambda: last_bx().start())
        when(t, 1, tiles - 1, lambda: fetch_near(t + 1))
        when(t, tiles - 1, tiles, last_near)
        when(t, 2, tiles + 2, lambda: sent1(t - 2))

        def wait_b(pieces):
            wait_bytes(b_v.at[t % 2, pl.ds(0, pieces * depth)], b_sem.at[t % 2])

        def near_products():
            wait_b(2)
            partials(t, 2)

        def all_products():
            wait_b(4)
            partials(t, 4)

        def last_products():
            wait_bytes(b_v.at[last % 2, :, 0:W], b_sem.at[last % 2])
            last_partials()

            for g in both:
                pl.semaphore_wait(credit.at[0, g], 1)
                last_send1(g, 0).start()

        def start_kept():
            for g in both:
                last_send1(g, 1).start()

        def wait_far():
            wait_bytes(a_v.at[pl.ds(0, 4), :, pl.ds(2 * depth, 2 * depth)], ch_recv.at[0])

        when(t, 0, 2, lambda: partials(t, 2, 3, last_three))
        when(t, 2, plain, near_products)
        when(t, plain, plain + 1, wait_far)
        when(t, plain, tiles, all_products)
        when(t, last, last + 1, last_products)
        for g in both:
            take(t, g, 0, 2, tiles)
            when(t, 2, tiles, lambda g=g: send1(t, g, 1).start())
        for g in both:
            when(t, 0, tiles, lambda g=g: send1(t, g, 0).start())
        when(t, plain - 1, tiles - 1, lambda: fetch_far(t + 1))
        when(t, tiles - 1, tiles, last_far)

        t1 = i - 1

        def add1(k):
            s, blocks = t1 % 2, pl.ds(2 * k, 2)
            got1(t1, k)
            for g in both:
                s2_v[s, g, blocks] = p_v[s, g, 0, blocks] + r1_v[s, g, blocks]

        def last1():
            last_add1(0)
            for g in both:
                pl.semaphore_wait(credit.at[1, g], 1)
                send2(last, g, 1, upper).start()
            for g in both:
                send2(last - 1, g, 0).start()
            for g in both:
                last_send1(g, 2).start()
            for g in both:
                send2(last, g, 0, upper).start()

        when(t1, 2, tiles + 1, lambda: sent2(t1 - 2))
        when(t1, 0, tiles, lambda: add1(1))
        for g in both:
            take(t1, g, 1, 2, tiles)
            when(t1, 0, tiles, lambda g=g: send2(t1, g, 1).start())
            when(t1, 0, tiles - 1, lambda g=g: send2(t1, g, 0).start())
        when(t, last, last + 1, start_kept)
        when(t1, 0, tiles, lambda: add1(0))
        for g in both:
            give(t1, g, 0, g, 2, last + 1)
        when(t1, last, last + 1, last1)

        t2 = i - 2

        def sum2(t, g, k, n=rows):
            part = pl.ds(0, n)
            return s2_v[t % 2, g, k, part] + r2_v[t % 2, g, k, part]

        def last2():
            last_add1(1)
            got2(last, 1, upper)
            for g in both:
                q_v[last % DO, g, last_part] = sum2(last, g, 1, upper).astype(jnp.bfloat16)
                last_there(g).start()
            each(plain - LATE, plain, got3)
            for g in both:
                each(plain - LATE, plain, lambda t: add3(t, g))
            each(plain - LATE, plain, sent3)
            each(tiles + 3 - LAG, tiles, end_chunks)
            each(max(plain, last + 1 - DO), tiles - 1, pair_sent)
            last_bx().wait_send()
            last_bxz().wait_send()
            add2_here(last - 1)
            last_add1(2)
            got2(last, 0, upper)
            for g in both:
                c_v[pl.ds(g * upper, upper), last_cols(z)] = sum2(last, g, 0, upper).astype(jnp.bfloat16)

        def add2(k):
            got2(t2, k)
            for g in both:
                s3_v[t2 % D3, g, k] = sum2(t2, g, k)

        def add2_there():
            got2(t2, 1)
            for g in both:
                q_v[t2 % DO, g] = sum2(t2, g, 1).astype(jnp.bfloat16)

        def add2_here(t):
            got2(t, 0)
            for g in both:
                c_v[:, tile_cols(t, g)] = sum2(t, g, 0).astype(jnp.bfloat16)

        when(t2, D3, plain - LATE + D3, lambda: sent3(t2 - D3))
        when(t2, plain + DO, last + 1, lambda: pair_sent(t2 - DO))
        when(t2, 0, plain, lambda: add2(1))
        when(t2, plain, tiles, add2_there)
        for g in both:
            take(t2, g, 2, D3, plain - LATE)
            when(t2, 0, plain - LATE, lambda g=g: send3(t2, g).start())
            when(t2, plain, tiles, lambda g=g: pair_there(t2, g).start())
        when(t2, 0, plain, lambda: add2(0))
        when(t2, plain, tiles - 1, lambda: add2_here(t2))
        for g in both:
            give(t2, g, 1, 1 - g, 2, last + 1)
        when(t2, last, last + 1, last2)

        t3 = i - 1 - D3
        when(t3, 0, plain - LATE, lambda: got3(t3))
        for g in both:
            when(t3, 0, plain - LATE, lambda g=g: add3(t3, g))
            give(t3, g, 2, AZ, D3, plain)
        when(t, last - 2, last - 1, start_late)
        when(t, plain - 1, tiles - 1, lambda: fetch_last(t + 1))
        when(t, tiles - 1, tiles, last_fetch)
        return carry

    lax.fori_loop(0, tiles + 3, step, 0)

    each(max(plain, tiles - 1), tiles, pair_sent)
    wait_bytes(r1_v.at[last % 2, :, :, last_part], s1_sem.at[last % 2])
    sent2(last - 1)
    sent2(last, upper)
    wait_bytes(q_v.at[last % DO, :, pl.ds(0, upper)], qs_sem.at[last % DO])
    wait_bytes(c_v.at[:, pl.ds(0, paired * C + W)], qr_sem)


def solution(mesh):
    spec_rows = P(("dp", "tp"), None)

    def local_block(a_rows, b_rows):
        rows, inner = a_rows.shape
        depth, columns = b_rows.shape
        plain, paired = counts(columns)
        tiles = plain + paired
        f32, bf16 = jnp.float32, jnp.bfloat16
        dma = pltpu.SemaphoreType.DMA
        out = pl.pallas_call(
            kernel,
            name="matmul_reduce_scatter",
            out_shape=(
                pltpu.VMEM((rows, columns), bf16),
                jax.ShapeDtypeStruct((tiles + 1, depth, C), bf16),
                jax.ShapeDtypeStruct((paired + 1, depth, C), bf16),
                jax.ShapeDtypeStruct((paired + 1, depth, C), bf16),
                jax.ShapeDtypeStruct((2, rows, 2 * depth), bf16),
            ),
            in_specs=[pl.BlockSpec(memory_space=pl.ANY)] * 2,
            out_specs=(pl.BlockSpec(memory_space=pltpu.VMEM),) + (pl.BlockSpec(memory_space=pl.ANY),) * 4,
            scratch_shapes=[
                pltpu.VMEM((3, rows // 8, depth), bf16),
                pltpu.VMEM((8, rows, 4 * depth), bf16),
                pltpu.VMEM((2, 4 * depth, C), bf16),
                pltpu.VMEM((2, 2, 2, 4, rows, W), f32),
                pltpu.VMEM((2, 2, 4, rows, W), f32),
                pltpu.VMEM((2, 2, 4, rows, W), f32),
                pltpu.VMEM((2, 2, 2, rows, W), f32),
                pltpu.VMEM((D3, 2, 2, rows, W), f32),
                pltpu.VMEM((D3, 2, rows, W), f32),
                pltpu.VMEM((DO, 2, rows, W), bf16),
                dma, dma, dma, dma((RX,)), dma((RX,)), dma((RZ,)), dma((RZ,)), dma((RC,)), dma((max(2 + paired, 14),)), dma((2,)),
                dma((2,)), dma((2, 2)), dma, dma((2,)), dma((2, 2)), dma((D3,)), dma((D3,)), dma((DO,)), dma,
                pltpu.SemaphoreType.REGULAR((3, 2)),
            ],
            compiler_params=pltpu.CompilerParams(
                collective_id=0, has_side_effects=True, vmem_limit_bytes=56 * 1024 * 1024),
            cost_estimate=pl.CostEstimate(
                flops=2 * 8 * rows * 2 * depth * columns, bytes_accessed=6 * depth * columns, transcendentals=0),
        )(a_rows, b_rows)
        return out[0]

    return jax.shard_map(local_block, mesh=mesh, in_specs=(spec_rows, spec_rows), out_specs=spec_rows, check_vma=False)
```

```python
import jax
import jax.numpy as jnp
from jax import lax
from jax.experimental import pallas as pl
from jax.experimental.pallas import tpu as pltpu
from jax.sharding import PartitionSpec as P

MESH = pl.DeviceIdType.MESH
W = 128
C = 2 * W
LOOK = 2
D3 = 6
DO = 5
LATE = 4
AHEAD = 2
LAG = 5
RX, RZ = 2 * LOOK - 1, LOOK
AX, AY, AZ = 0, 1, 2


def bits_of(d):
    return (d // 4, (d // 2) % 2, d % 2)


def counts(columns):
    paired = columns // C // 4
    return columns // C - 2 * paired - 1, paired


def pace(columns):
    plain, paired = counts(columns)
    return max(114, -(-1600 // plain), -(-100 * (15 + 2 * paired) // (plain + paired - 1)))


def kernel(a_hbm, b_hbm, c_v, bx_hbm, bz_hbm, bxz_hbm, relay,
           a_v, b_v, p_v, r1_v, s2_v, r2_v, s3_v, r3_v, q_v,
            bx_send, bx_recv, bxz_send, bxz_recv, ch_send, ch_recv, b_sem,
           s1_sem, r1_sem, s2_sem, r2_sem, s3_sem, r3_sem, qs_sem, qr_sem, credit):
    depth, columns = b_hbm.shape
    plain, paired = counts(columns)
    tiles = plain + paired
    rows, upper = a_hbm.shape[0], a_hbm.shape[0] // 2
    half = depth // 2
    chunks = 16 + 2 * paired
    last = plain + paired
    rate = pace(columns)
    ring = 5 * rate // 100 + 2

    dp, tp = lax.axis_index("dp"), lax.axis_index("tp")
    core, x, y, z = dp % 2, (dp // 2) % 2, dp // 4, tp

    def flip(v, bit):
        return v + bit - 2 * v * bit

    def device(bits, other=0):
        return {"dp": flip(y, bits[1]) * 4 + flip(x, bits[0]) * 2 + flip(core, other), "tp": flip(z, bits[2])}

    axis_nbr = [device((1, 0, 0)), device((0, 1, 0)), device((0, 0, 1))]
    partner = device((0, 0, 0), 1)

    barrier = pltpu.get_barrier_semaphore()
    for nbr in (*axis_nbr, partner):
        pl.semaphore_signal(barrier, inc=1, device_id=nbr, device_id_type=MESH)

    def send(src, dst, send_sem, recv_sem, to):
        return pltpu.make_async_remote_copy(
            src_ref=src, dst_ref=dst, send_sem=send_sem, recv_sem=recv_sem, device_id=to, device_id_type=MESH)

    def wait_bytes(ref, sem):
        pltpu.make_async_copy(ref, ref, sem).wait()

    def when(t, low, high, fn):
        pl.when(jnp.logical_and(t >= low, t < high))(fn)

    def is_paired(t):
        return (t + tiles - plain) // tiles

    def tile_cols(t, g=None):
        col = t * C + is_paired(t) * ((t - plain) * C + z * C)
        if g is None:
            return pl.ds(pl.multiple_of(col, W), C)
        return pl.ds(pl.multiple_of(col + g * W, W), W)

    def their_cols(q):
        return pl.ds(pl.multiple_of((plain + 2 * q + 1 - z) * C, W), C)

    def last_cols(side):
        return pl.ds(pl.multiple_of((plain + 2 * paired) * C + side * W, W), W)

    def a_cols(bits, h):
        to = device(bits, h)
        return a_hbm.at[:, pl.ds(pl.multiple_of((to["dp"] * 2 + to["tp"]) * depth, depth), depth)]

    def near(d, h):
        return a_v.at[d, :, pl.ds(h * depth, depth)]

    def far(d, h):
        return a_v.at[d, :, pl.ds((2 + h) * depth, depth)]

    def held(i, h):
        return relay.at[i, :, pl.ds(h * depth, depth)]

    def hop(n, h, src, dst, axis):
        return send(src, dst, qr_sem, ch_recv.at[-n if n < 0 else 4 + 2 * n + h], axis_nbr[axis])

    both = range(2)
    xy_far1 = [hop(0, h, a_cols((1, 1, 1), h), held(0, h), AX) for h in both]
    xy_near1 = [hop(1, h, a_cols((1, 1, 0), h), held(1, h), AX) for h in both]
    x_far = [hop(2, h, a_cols((1, 0, 1), h), far(4, h), AX) for h in both]
    y_far = [hop(3, h, a_cols((0, 1, 1), h), far(2, h), AY) for h in both]
    xy_far2 = [hop(4, h, held(0, h), far(6, h), AY) for h in both]
    z_own = [hop(-1, h, a_cols((0, 0, 1), h), near(1, h), AZ) for h in both]
    z_y = [hop(-1, h, far(2, h), near(3, h), AZ) for h in both]
    xy_near2 = [hop(-2, h, held(1, h), near(6, h), AY) for h in both]
    z_xy = [hop(-2, h, far(6, h), near(7, h), AZ) for h in both]
    x_near = [hop(-3, h, a_cols((1, 0, 0), h), near(4, h), AX) for h in both]
    y_near = [hop(-3, h, a_cols((0, 1, 0), h), near(2, h), AY) for h in both]
    z_x = [hop(-3, h, far(4, h), near(5, h), AZ) for h in both]
    hops = 24

    def end_group(n, copies):
        wait_bytes(a_v.at[pl.ds(0, copies // 2), :, pl.ds(0, 2 * depth)], ch_recv.at[n])

    own = [pltpu.make_async_copy(a_cols((0, 0, 0), h), near(0, h), ch_recv.at[14]) for h in both]
    own += [pltpu.make_async_copy(a_cols((0, 0, 1), h), far(0, h), ch_recv.at[14]) for h in both]

    def a_chunk(n):
        d, k = (n // 4) * 2, n % 4
        return send(a_v.at[d, :, pl.ds(pl.multiple_of(k * half, half), half)],
                    a_v.at[d + 1, :, pl.ds(pl.multiple_of(2 * depth + k * half, half), half)],
                    ch_send.at[n % ring], ch_recv.at[0], axis_nbr[AZ])

    def b_chunk(q, h):
        rows = pl.ds(pl.multiple_of(h * half, half), half)
        n = 16 + 2 * q + h
        return send(b_hbm.at[rows, their_cols(q)], bz_hbm.at[q, rows], ch_send.at[n % ring], ch_recv.at[1 + q], axis_nbr[AZ])

    def last_chunk():
        return send(b_hbm.at[:, last_cols(1 - z)], bz_hbm.at[paired, :, 0:W], ch_send.at[chunks % ring], ch_recv.at[1 + paired], axis_nbr[AZ])

    def start_chunks(i):
        def body(n, carry):
            when(n, 0, 16, lambda: a_chunk(n).start())
            when(n, 16, chunks, lambda: b_chunk((n - 16) // 2, (n - 16) % 2).start())
            when(n, chunks, chunks + 1, lambda: last_chunk().start())
            return carry

        lax.fori_loop(rate * i // 100 + AHEAD, rate * (i + 1) // 100 + AHEAD, body, 0)

    def end_chunks(i):
        def body(n, carry):
            when(n, 0, 16, lambda: a_chunk(n).wait_send())
            when(n, 16, chunks, lambda: b_chunk((n - 16) // 2, (n - 16) % 2).wait_send())
            when(n, chunks, chunks + 1, lambda: last_chunk().wait_send())
            return carry

        lax.fori_loop(rate * i // 100 + AHEAD, rate * (i + 1) // 100 + AHEAD, body, 0)

    def bx_copy(t):
        return send(b_hbm.at[:, tile_cols(t)], bx_hbm.at[t], bx_send.at[t % 2], bx_recv.at[t % RX], partner)

    def bxz_copy(q):
        return send(bz_hbm.at[q], bxz_hbm.at[q], bxz_send, bxz_recv.at[q % RZ], partner)

    def last_bx():
        return send(b_hbm.at[:, last_cols(z)], bx_hbm.at[last, :, 0:W], bx_send.at[last % 2], bx_recv.at[last % RX], partner)

    def last_bxz():
        return send(bz_hbm.at[paired, :, 0:W], bxz_hbm.at[paired, :, 0:W], bxz_send, bxz_recv.at[paired % RZ], partner)

    def last_piece(k):
        src = (b_hbm.at[:, last_cols(z)], bx_hbm.at[last, :, 0:W], bz_hbm.at[paired, :, 0:W], bxz_hbm.at[paired, :, 0:W])[k]
        return pltpu.make_async_copy(src, b_v.at[last % 2, pl.ds(k * depth, depth), 0:W], b_sem.at[last % 2])

    def b_piece(t, k):
        src = (b_hbm.at[:, tile_cols(t)], bx_hbm.at[t], bz_hbm.at[t - plain], bxz_hbm.at[t - plain])[k]
        return pltpu.make_async_copy(src, b_v.at[t % 2, pl.ds(k * depth, depth)], b_sem.at[t % 2])

    def fetch_near(t):
        b_piece(t, 0).start()
        bx_copy(t).wait_recv()
        b_piece(t, 1).start()

    def fetch_far(t):
        wait_bytes(bz_hbm.at[t - plain], ch_recv.at[1 + t - plain])
        bxz_copy(t - plain).start()
        b_piece(t, 2).start()

    def fetch_last(t):
        bxz_copy(t - plain).wait_recv()
        b_piece(t, 3).start()

    def last_near():
        last_piece(0).start()
        last_bx().wait_recv()
        last_piece(1).start()

    def last_far():
        last_chunk().wait_recv()
        last_bxz().start()
        last_piece(2).start()

    def last_fetch():
        last_bxz().wait_recv()
        last_piece(3).start()

    def partial(t, d, k):
        s = t % 2
        dx, dy, dz = bits_of(d)
        part = jnp.dot(a_v[d, :, 0:k * depth], b_v[s, 0:k * depth], preferred_element_type=jnp.float32)
        p_v[s, 0, dx, dy * 2 + dz] = part[:, 0:W]
        p_v[s, 1, dy, dx * 2 + dz] = part[:, W:C]

    def last_partials():
        s = last % 2

        def body(d, carry):
            dx, dy, dz = bits_of(d)
            part = jnp.dot(a_v[d], b_v[s, :, 0:W], preferred_element_type=jnp.float32)
            p_v[s, 0, dx, dy * 2 + dz, 0:upper] = part[0:upper]
            p_v[s, 1, dy, dx * 2 + dz, 0:upper] = part[upper:rows]
            return carry

        lax.fori_loop(0, 8, body, 0)

    def partials(t, k, n=8, order=lambda j: j):
        def body(j, carry):
            partial(t, order(j), k)
            return carry

        lax.fori_loop(0, n, body, 0)

    def first_two(n, order):
        def body(j, carry):
            partial(j // n, order(j % n), 2)
            return carry

        lax.fori_loop(0, 2 * n, body, 0)

    def send1(t, g, k):
        s, blocks = t % 2, pl.ds(2 * k, 2)
        return send(p_v.at[s, g, 1, blocks], r1_v.at[s, g, blocks], s1_sem.at[s], r1_sem.at[s, k], axis_nbr[g])

    def got1(t, k):
        wait_bytes(r1_v.at[t % 2, :, pl.ds(2 * k, 2)], r1_sem.at[t % 2, k])

    def sent1(t):
        wait_bytes(r1_v.at[t % 2], s1_sem.at[t % 2])

    def send2(t, g, k, n=rows):
        s, part = t % 2, pl.ds(0, n)
        return send(s2_v.at[s, g, 2 + k, part], r2_v.at[s, g, k, part], s2_sem.at[s], r2_sem.at[s, k], axis_nbr[1 - g])

    def got2(t, k, n=rows):
        wait_bytes(r2_v.at[t % 2, :, k, pl.ds(0, n)], r2_sem.at[t % 2, k])

    def sent2(t, n=rows):
        wait_bytes(r2_v.at[t % 2, :, :, pl.ds(0, n)], s2_sem.at[t % 2])

    pieces = (pl.ds(2, 2), pl.ds(1, 1), pl.ds(0, 1))
    last_part = pl.ds(0, upper)

    def last_sem(k):
        return (r1_sem.at[last % 2, 1], ch_recv.at[1], r1_sem.at[last % 2, 0])[k]

    def last_send1(g, k):
        s = last % 2
        return send(p_v.at[s, g, 1, pieces[k], last_part], r1_v.at[s, g, pieces[k], last_part],
                    s1_sem.at[s], last_sem(k), axis_nbr[g])

    def last_add1(k):
        s = last % 2
        wait_bytes(r1_v.at[s, :, pieces[k], last_part], last_sem(k))
        for g in both:
            s2_v[s, g, pieces[k], last_part] = p_v[s, g, 0, pieces[k], last_part] + r1_v[s, g, pieces[k], last_part]

    def send3(t, g):
        s = t % D3
        return send(s3_v.at[s, g, 1], r3_v.at[s, g], s3_sem.at[s], r3_sem.at[s], axis_nbr[AZ])

    def pair_there(t, g):
        s = t % DO
        return send(q_v.at[s, g], c_v.at[:, tile_cols(t, g)], qs_sem.at[s], qr_sem, axis_nbr[AZ])

    def last_there(g):
        s = last % DO
        return send(q_v.at[s, g, pl.ds(0, upper)], c_v.at[pl.ds(g * upper, upper), last_cols(z)],
                    qs_sem.at[s], qr_sem, axis_nbr[AZ])

    def sent3(t):
        wait_bytes(r3_v.at[t % D3], s3_sem.at[t % D3])

    def got3(t):
        wait_bytes(r3_v.at[t % D3], r3_sem.at[t % D3])

    def pair_sent(t):
        wait_bytes(q_v.at[t % DO], qs_sem.at[t % DO])

    def take(t, g, phase, slots, high):
        when(t, slots, high, lambda: pl.semaphore_wait(credit.at[2 * phase + g], 1))

    def give(t, g, phase, axis, slots, high):
        when(t, 0, high - slots, lambda: pl.semaphore_signal(
            credit.at[2 * phase + g], inc=1, device_id=axis_nbr[axis], device_id_type=MESH))

    for copy in own:
        copy.start()
    pl.semaphore_wait(barrier, 4)
    for group in (xy_far1, y_far, z_own, xy_near1, x_far, x_near):
        for copy in group:
            copy.start()
    for t in range(min(LOOK, tiles)):
        bx_copy(t).start()
    for t in range(2):
        fetch_near(t)
    for h in both:
        y_far[h].wait_recv()
        z_y[h].start()
        xy_far1[h].wait_recv()
        xy_far2[h].start()
    for h in both:
        xy_near1[h].wait_recv()
        xy_near2[h].start()
        xy_far2[h].wait_recv()
        z_xy[h].start()
    for copy in y_near:
        copy.start()
    for t in range(2):
        wait_bytes(b_v.at[t, pl.ds(0, 2 * depth)], b_sem.at[t])
    wait_bytes(a_v.at[0], ch_recv.at[14])
    end_group(1, 4)
    first_two(3, lambda j: j + j // 2)
    for h in both:
        x_far[h].wait_recv()
        z_x[h].start()
    for n in range(AHEAD):
        a_chunk(n).start()
    end_group(2, 4)
    first_two(2, lambda j: 6 + j)
    for t in range(2):
        for g in both:
            send1(t, g, 1).start()
    end_group(3, 6)

    def last_three(j):
        return 2 + (3 * j + 1) // 2

    def add3(t, g):
        c_v[:, tile_cols(t, g)] = (s3_v[t % D3, g, 0] + r3_v[t % D3, g]).astype(jnp.bfloat16)

    def start_late():
        def body(t, carry):
            take(t, 0, 2, D3, plain)
            for g in both:
                send3(t, g).start()
            return carry

        lax.fori_loop(plain - LATE, plain, body, 0)

    def each(low, high, fn):
        def body(n, carry):
            fn(n)
            return carry

        lax.fori_loop(low, high, body, 0)

    def end_hops():
        wait_bytes(a_v.at[pl.ds(0, hops // 4)], qr_sem)
        for n in range(AHEAD):
            a_chunk(n).wait_send()

    def step(i, carry):
        t = i
        when(t, LAG, LAG + 1, end_hops)
        when(t, LAG, tiles + 3, lambda: end_chunks(t - LAG))
        when(t, 0, tiles, lambda: start_chunks(t))
        when(t, 1, tiles - 1, lambda: fetch_near(t + 1))
        when(t, tiles - 1, tiles, last_near)
        when(t, 0, 1, lambda: bx_copy(0).wait_send())
        when(t, 0, tiles - 1, lambda: bx_copy(t + 1).wait_send())
        when(t, tiles - 1, tiles, lambda: last_bx().wait_send())
        when(t, plain, tiles, lambda: bxz_copy(t - plain).wait_send())
        when(t, 0, tiles - LOOK, lambda: bx_copy(t + LOOK).start())
        when(t, tiles - LOOK, tiles - LOOK + 1, lambda: last_bx().start())
        when(t, 2, tiles + 2, lambda: sent1(t - 2))

        def wait_b(pieces):
            wait_bytes(b_v.at[t % 2, pl.ds(0, pieces * depth)], b_sem.at[t % 2])

        def near_products():
            wait_b(2)
            partials(t, 2)

        def all_products():
            wait_b(4)
            partials(t, 4)

        def last_products():
            wait_bytes(b_v.at[last % 2, :, 0:W], b_sem.at[last % 2])
            last_partials()

            for g in both:
                pl.semaphore_wait(credit.at[g], 1)
                last_send1(g, 0).start()

        def start_kept():
            for g in both:
                last_send1(g, 1).start()

        def wait_far():
            wait_bytes(a_v.at[pl.ds(0, 4), :, pl.ds(2 * depth, 2 * depth)], ch_recv.at[0])

        when(t, 0, 2, lambda: partials(t, 2, 3, last_three))
        when(t, 2, plain, near_products)
        when(t, plain, plain + 1, wait_far)
        when(t, plain, tiles, all_products)
        when(t, last, last + 1, last_products)
        for g in both:
            take(t, g, 0, 2, tiles)
            when(t, 2, tiles, lambda g=g: send1(t, g, 1).start())
        for g in both:
            when(t, 0, tiles, lambda g=g: send1(t, g, 0).start())
        when(t, plain - 1, tiles - 1, lambda: fetch_far(t + 1))
        when(t, tiles - 1, tiles, last_far)

        t1 = i - 1

        def add1(k):
            s, blocks = t1 % 2, pl.ds(2 * k, 2)
            got1(t1, k)
            for g in both:
                s2_v[s, g, blocks] = p_v[s, g, 0, blocks] + r1_v[s, g, blocks]

        def last1():
            last_add1(0)
            for g in both:
                pl.semaphore_wait(credit.at[2 + g], 1)
                send2(last, g, 1, upper).start()
            for g in both:
                send2(last - 1, g, 0).start()
            for g in both:
                last_send1(g, 2).start()
            for g in both:
                send2(last, g, 0, upper).start()

        when(t1, 2, tiles + 1, lambda: sent2(t1 - 2))
        when(t1, 0, tiles, lambda: add1(1))
        for g in both:
            take(t1, g, 1, 2, tiles)
            when(t1, 0, tiles, lambda g=g: send2(t1, g, 1).start())
            when(t1, 0, tiles - 1, lambda g=g: send2(t1, g, 0).start())
        when(t, last, last + 1, start_kept)
        when(t1, 0, tiles, lambda: add1(0))
        for g in both:
            give(t1, g, 0, g, 2, last + 1)
        when(t1, last, last + 1, last1)

        t2 = i - 2

        def sum2(t, g, k, n=rows):
            part = pl.ds(0, n)
            return s2_v[t % 2, g, k, part] + r2_v[t % 2, g, k, part]

        def last2():
            last_add1(1)
            got2(last, 1, upper)
            for g in both:
                q_v[last % DO, g, last_part] = sum2(last, g, 1, upper).astype(jnp.bfloat16)
                last_there(g).start()
            each(plain - LATE, plain, got3)
            for g in both:
                each(plain - LATE, plain, lambda t: add3(t, g))
            each(plain - LATE, plain, sent3)
            each(tiles + 3 - LAG, tiles, end_chunks)
            each(max(plain, last + 1 - DO), tiles - 1, pair_sent)
            last_bxz().wait_send()
            add2_here(last - 1)
            last_add1(2)
            got2(last, 0, upper)
            for g in both:
                c_v[pl.ds(g * upper, upper), last_cols(z)] = sum2(last, g, 0, upper).astype(jnp.bfloat16)

        def add2(k):
            got2(t2, k)
            for g in both:
                s3_v[t2 % D3, g, k] = sum2(t2, g, k)

        def add2_there():
            got2(t2, 1)
            for g in both:
                q_v[t2 % DO, g] = sum2(t2, g, 1).astype(jnp.bfloat16)

        def add2_here(t):
            got2(t, 0)
            for g in both:
                c_v[:, tile_cols(t, g)] = sum2(t, g, 0).astype(jnp.bfloat16)

        when(t2, D3, plain - LATE + D3, lambda: sent3(t2 - D3))
        when(t2, plain + DO, last + 1, lambda: pair_sent(t2 - DO))
        when(t2, 0, plain, lambda: add2(1))
        when(t2, plain, tiles, add2_there)
        take(t2, 0, 2, D3, plain - LATE)
        for g in both:
            when(t2, 0, plain - LATE, lambda g=g: send3(t2, g).start())
            when(t2, plain, tiles, lambda g=g: pair_there(t2, g).start())
        when(t2, 0, plain, lambda: add2(0))
        when(t2, plain, tiles - 1, lambda: add2_here(t2))
        for g in both:
            give(t2, g, 1, 1 - g, 2, last + 1)
        when(t2, last, last + 1, last2)

        t3 = i - 1 - D3
        when(t3, 0, plain - LATE, lambda: got3(t3))
        for g in both:
            when(t3, 0, plain - LATE, lambda g=g: add3(t3, g))
        give(t3, 0, 2, AZ, D3, plain)
        when(t, last - 2, last - 1, start_late)
        when(t, plain - 1, tiles - 1, lambda: fetch_last(t + 1))
        when(t, tiles - 1, tiles, last_fetch)
        return carry

    lax.fori_loop(0, tiles + 3, step, 0)

    each(max(plain, tiles - 1), tiles, pair_sent)
    wait_bytes(r1_v.at[last % 2, :, :, last_part], s1_sem.at[last % 2])
    sent2(last - 1)
    sent2(last, upper)
    wait_bytes(q_v.at[last % DO, :, pl.ds(0, upper)], qs_sem.at[last % DO])
    wait_bytes(c_v.at[:, pl.ds(0, paired * C + W)], qr_sem)


def solution(mesh):
    spec_rows = P(("dp", "tp"), None)

    def local_block(a_rows, b_rows):
        rows, inner = a_rows.shape
        depth, columns = b_rows.shape
        plain, paired = counts(columns)
        tiles = plain + paired
        f32, bf16 = jnp.float32, jnp.bfloat16
        dma = pltpu.SemaphoreType.DMA
        out = pl.pallas_call(
            kernel,
            name="matmul_reduce_scatter",
            out_shape=(
                pltpu.VMEM((rows, columns), bf16),
                jax.ShapeDtypeStruct((tiles + 1, depth, C), bf16),
                jax.ShapeDtypeStruct((paired + 1, depth, C), bf16),
                jax.ShapeDtypeStruct((paired + 1, depth, C), bf16),
                jax.ShapeDtypeStruct((2, rows, 2 * depth), bf16),
            ),
            in_specs=[pl.BlockSpec(memory_space=pl.ANY)] * 2,
            out_specs=(pl.BlockSpec(memory_space=pltpu.VMEM),) + (pl.BlockSpec(memory_space=pl.ANY),) * 4,
            scratch_shapes=[
                pltpu.VMEM((8, rows, 4 * depth), bf16),
                pltpu.VMEM((2, 4 * depth, C), bf16),
                pltpu.VMEM((2, 2, 2, 4, rows, W), f32),
                pltpu.VMEM((2, 2, 4, rows, W), f32),
                pltpu.VMEM((2, 2, 4, rows, W), f32),
                pltpu.VMEM((2, 2, 2, rows, W), f32),
                pltpu.VMEM((D3, 2, 2, rows, W), f32),
                pltpu.VMEM((D3, 2, rows, W), f32),
                pltpu.VMEM((DO, 2, rows, W), bf16),
                dma((2,)), dma((RX,)), dma, dma((RZ,)), dma((5 * pace(columns) // 100 + 2,)), dma((max(2 + paired, 15),)), dma((2,)),
                dma((2,)), dma((2, 2)), dma((2,)), dma((2, 2)), dma((D3,)), dma((D3,)), dma((DO,)), dma,
                pltpu.SemaphoreType.REGULAR((5,)),
            ],
            compiler_params=pltpu.CompilerParams(
                collective_id=0, has_side_effects=True, vmem_limit_bytes=56 * 1024 * 1024),
            cost_estimate=pl.CostEstimate(
                flops=2 * 8 * rows * 2 * depth * columns, bytes_accessed=6 * depth * columns, transcendentals=0),
        )(a_rows, b_rows)
        return out[0]

    return jax.shard_map(local_block, mesh=mesh, in_specs=(spec_rows, spec_rows), out_specs=spec_rows, check_vma=False)
```

```python
import jax
import jax.numpy as jnp
from jax import lax
from jax.experimental import pallas as pl
from jax.experimental.pallas import tpu as pltpu
from jax.sharding import PartitionSpec as P

MESH = pl.DeviceIdType.MESH
W = 128
C = 2 * W
LOOK = 2
D3 = 6
DO = 5
LATE = 4
AHEAD = 2
LAG = 5
RX, RZ = 2 * LOOK - 1, LOOK
AX, AY, AZ = 0, 1, 2


def bits_of(d):
    return (d // 4, (d // 2) % 2, d % 2)


def counts(columns):
    paired = columns // C // 4
    return columns // C - 2 * paired - 1, paired


def pace(columns):
    plain, paired = counts(columns)
    return max(114, -(-1600 // plain), -(-100 * (15 + 2 * paired) // (plain + paired - 1)))


def kernel(a_hbm, b_hbm, c_v, bx_hbm, bz_hbm, bxz_hbm, relay,
           a_v, b_v, p_v, r1_v, s2_v, r2_v, s3_v, r3_v, q_v,
            bx_send, bx_recv, bxz_send, bxz_recv, ch_send, ch_recv, b_sem,
           s1_sem, r1_sem, s2_sem, r2_sem, s3_sem, r3_sem, qs_sem, qr_sem, credit):
    depth, columns = b_hbm.shape
    plain, paired = counts(columns)
    tiles = plain + paired
    rows, upper = a_hbm.shape[0], a_hbm.shape[0] // 2
    half = depth // 2
    chunks = 16 + 2 * paired
    last = plain + paired
    rate = pace(columns)
    ring = 5 * rate // 100 + 2

    dp, tp = lax.axis_index("dp"), lax.axis_index("tp")
    core, x, y, z = dp % 2, (dp // 2) % 2, dp // 4, tp

    def flip(v, bit):
        return v + bit - 2 * v * bit

    def device(bits, other=0):
        return {"dp": flip(y, bits[1]) * 4 + flip(x, bits[0]) * 2 + flip(core, other), "tp": flip(z, bits[2])}

    axis_nbr = [device((1, 0, 0)), device((0, 1, 0)), device((0, 0, 1))]
    partner = device((0, 0, 0), 1)

    barrier = pltpu.get_barrier_semaphore()
    for nbr in (*axis_nbr, partner):
        pl.semaphore_signal(barrier, inc=1, device_id=nbr, device_id_type=MESH)

    def send(src, dst, send_sem, recv_sem, to):
        return pltpu.make_async_remote_copy(
            src_ref=src, dst_ref=dst, send_sem=send_sem, recv_sem=recv_sem, device_id=to, device_id_type=MESH)

    def wait_bytes(ref, sem):
        pltpu.make_async_copy(ref, ref, sem).wait()

    def when(t, low, high, fn):
        pl.when(jnp.logical_and(t >= low, t < high))(fn)

    def is_paired(t):
        return (t + tiles - plain) // tiles

    def tile_cols(t, g=None):
        col = t * C + is_paired(t) * ((t - plain) * C + z * C)
        if g is None:
            return pl.ds(pl.multiple_of(col, W), C)
        return pl.ds(pl.multiple_of(col + g * W, W), W)

    def their_cols(q):
        return pl.ds(pl.multiple_of((plain + 2 * q + 1 - z) * C, W), C)

    def last_cols(side):
        return pl.ds(pl.multiple_of((plain + 2 * paired) * C + side * W, W), W)

    def a_cols(bits, h):
        to = device(bits, h)
        return a_hbm.at[:, pl.ds(pl.multiple_of((to["dp"] * 2 + to["tp"]) * depth, depth), depth)]

    def near(d, h):
        return a_v.at[d, :, pl.ds(h * depth, depth)]

    def far(d, h):
        return a_v.at[d, :, pl.ds((2 + h) * depth, depth)]

    def held(i, h):
        return relay.at[i, :, pl.ds(h * depth, depth)]

    def hop(n, h, src, dst, axis):
        return send(src, dst, qr_sem, ch_recv.at[-n if n < 0 else 4 + 2 * n + h], axis_nbr[axis])

    both = range(2)
    xy_far1 = [hop(0, h, a_cols((1, 1, 1), h), held(0, h), AX) for h in both]
    xy_near1 = [hop(1, h, a_cols((1, 1, 0), h), held(1, h), AX) for h in both]
    x_far = [hop(2, h, a_cols((1, 0, 1), h), far(4, h), AX) for h in both]
    y_far = [hop(3, h, a_cols((0, 1, 1), h), far(2, h), AY) for h in both]
    xy_far2 = [hop(4, h, held(0, h), far(6, h), AY) for h in both]
    z_own = [hop(-1, h, a_cols((0, 0, 1), h), near(1, h), AZ) for h in both]
    z_y = [hop(-1, h, far(2, h), near(3, h), AZ) for h in both]
    xy_near2 = [hop(-2, h, held(1, h), near(6, h), AY) for h in both]
    z_xy = [hop(-2, h, far(6, h), near(7, h), AZ) for h in both]
    x_near = [hop(-3, h, a_cols((1, 0, 0), h), near(4, h), AX) for h in both]
    y_near = [hop(-3, h, a_cols((0, 1, 0), h), near(2, h), AY) for h in both]
    z_x = [hop(-3, h, far(4, h), near(5, h), AZ) for h in both]
    hops = 24

    def end_group(n, copies):
        wait_bytes(a_v.at[pl.ds(0, copies // 2), :, pl.ds(0, 2 * depth)], ch_recv.at[n])

    own = [pltpu.make_async_copy(a_cols((0, 0, 0), h), near(0, h), ch_recv.at[14]) for h in both]
    own += [pltpu.make_async_copy(a_cols((0, 0, 1), h), far(0, h), ch_recv.at[14]) for h in both]

    def a_chunk(n):
        d, k = (n // 4) * 2, n % 4
        return send(a_v.at[d, :, pl.ds(pl.multiple_of(k * half, half), half)],
                    a_v.at[d + 1, :, pl.ds(pl.multiple_of(2 * depth + k * half, half), half)],
                    ch_send.at[n % ring], ch_recv.at[0], axis_nbr[AZ])

    def b_chunk(q, h):
        rows = pl.ds(pl.multiple_of(h * half, half), half)
        n = 16 + 2 * q + h
        return send(b_hbm.at[rows, their_cols(q)], bz_hbm.at[q, rows], ch_send.at[n % ring], ch_recv.at[1 + q], axis_nbr[AZ])

    def last_chunk():
        return send(b_hbm.at[:, last_cols(1 - z)], bz_hbm.at[paired, :, 0:W], ch_send.at[chunks % ring], ch_recv.at[1 + paired], axis_nbr[AZ])

    def start_chunks(i):
        def body(n, carry):
            when(n, 0, 16, lambda: a_chunk(n).start())
            when(n, 16, chunks, lambda: b_chunk((n - 16) // 2, (n - 16) % 2).start())
            when(n, chunks, chunks + 1, lambda: last_chunk().start())
            return carry

        lax.fori_loop(rate * i // 100 + AHEAD, rate * (i + 1) // 100 + AHEAD, body, 0)

    def end_chunks(i):
        def body(n, carry):
            when(n, 0, 16, lambda: a_chunk(n).wait_send())
            when(n, 16, chunks, lambda: b_chunk((n - 16) // 2, (n - 16) % 2).wait_send())
            when(n, chunks, chunks + 1, lambda: last_chunk().wait_send())
            return carry

        lax.fori_loop(rate * i // 100 + AHEAD, rate * (i + 1) // 100 + AHEAD, body, 0)

    def bx_copy(t):
        return send(b_hbm.at[:, tile_cols(t)], bx_hbm.at[t], bx_send.at[t % 2], bx_recv.at[t % RX], partner)

    def bxz_copy(q):
        return send(bz_hbm.at[q], bxz_hbm.at[q], bxz_send, bxz_recv.at[q % RZ], partner)

    def last_bx():
        return send(b_hbm.at[:, last_cols(z)], bx_hbm.at[last, :, 0:W], bx_send.at[last % 2], bx_recv.at[last % RX], partner)

    def last_bxz():
        return send(bz_hbm.at[paired, :, 0:W], bxz_hbm.at[paired, :, 0:W], bxz_send, bxz_recv.at[paired % RZ], partner)

    def last_piece(k):
        src = (b_hbm.at[:, last_cols(z)], bx_hbm.at[last, :, 0:W], bz_hbm.at[paired, :, 0:W], bxz_hbm.at[paired, :, 0:W])[k]
        return pltpu.make_async_copy(src, b_v.at[last % 2, pl.ds(k * depth, depth), 0:W], b_sem.at[last % 2])

    def b_piece(t, k):
        src = (b_hbm.at[:, tile_cols(t)], bx_hbm.at[t], bz_hbm.at[t - plain], bxz_hbm.at[t - plain])[k]
        return pltpu.make_async_copy(src, b_v.at[t % 2, pl.ds(k * depth, depth)], b_sem.at[t % 2])

    def fetch_near(t):
        b_piece(t, 0).start()
        bx_copy(t).wait_recv()
        b_piece(t, 1).start()

    def fetch_far(t):
        wait_bytes(bz_hbm.at[t - plain], ch_recv.at[1 + t - plain])
        bxz_copy(t - plain).start()
        b_piece(t, 2).start()

    def fetch_last(t):
        bxz_copy(t - plain).wait_recv()
        b_piece(t, 3).start()

    def last_near():
        last_piece(0).start()
        last_bx().wait_recv()
        last_piece(1).start()

    def last_far():
        last_chunk().wait_recv()
        last_bxz().start()
        last_piece(2).start()

    def last_fetch():
        last_bxz().wait_recv()
        last_piece(3).start()

    def partial(t, d, k):
        s = t % 2
        dx, dy, dz = bits_of(d)
        part = jnp.dot(a_v[d, :, 0:k * depth], b_v[s, 0:k * depth], preferred_element_type=jnp.float32)
        p_v[s, 0, dx, dy * 2 + dz] = part[:, 0:W]
        p_v[s, 1, dy, dx * 2 + dz] = part[:, W:C]

    def last_partials():
        s = last % 2

        def body(d, carry):
            dx, dy, dz = bits_of(d)
            part = jnp.dot(a_v[d], b_v[s, :, 0:W], preferred_element_type=jnp.float32)
            p_v[s, 0, dx, dy * 2 + dz, 0:upper] = part[0:upper]
            p_v[s, 1, dy, dx * 2 + dz, 0:upper] = part[upper:rows]
            return carry

        lax.fori_loop(0, 8, body, 0)

    def partials(t, k, n=8, order=lambda j: j):
        def body(j, carry):
            partial(t, order(j), k)
            return carry

        lax.fori_loop(0, n, body, 0)

    def first_two(n, order):
        def body(j, carry):
            partial(j // n, order(j % n), 2)
            return carry

        lax.fori_loop(0, 2 * n, body, 0)

    def send1(t, g, k):
        s, blocks = t % 2, pl.ds(2 * k, 2)
        return send(p_v.at[s, g, 1, blocks], r1_v.at[s, g, blocks], s1_sem.at[s], r1_sem.at[s, k], axis_nbr[g])

    def got1(t, k):
        wait_bytes(r1_v.at[t % 2, :, pl.ds(2 * k, 2)], r1_sem.at[t % 2, k])

    def sent1(t):
        wait_bytes(r1_v.at[t % 2], s1_sem.at[t % 2])

    def send2(t, g, k, n=rows):
        s, part = t % 2, pl.ds(0, n)
        return send(s2_v.at[s, g, 2 + k, part], r2_v.at[s, g, k, part], s2_sem.at[s], r2_sem.at[s, k], axis_nbr[1 - g])

    def got2(t, k, n=rows):
        wait_bytes(r2_v.at[t % 2, :, k, pl.ds(0, n)], r2_sem.at[t % 2, k])

    def sent2(t, n=rows):
        wait_bytes(r2_v.at[t % 2, :, :, pl.ds(0, n)], s2_sem.at[t % 2])

    pieces = (pl.ds(2, 2), pl.ds(1, 1), pl.ds(0, 1))
    last_part = pl.ds(0, upper)

    def last_sem(k):
        return (r1_sem.at[last % 2, 1], ch_recv.at[1], r1_sem.at[last % 2, 0])[k]

    def last_send1(g, k):
        s = last % 2
        return send(p_v.at[s, g, 1, pieces[k], last_part], r1_v.at[s, g, pieces[k], last_part],
                    s1_sem.at[s], last_sem(k), axis_nbr[g])

    def last_add1(k):
        s = last % 2
        wait_bytes(r1_v.at[s, :, pieces[k], last_part], last_sem(k))
        for g in both:
            s2_v[s, g, pieces[k], last_part] = p_v[s, g, 0, pieces[k], last_part] + r1_v[s, g, pieces[k], last_part]

    def send3(t, g):
        s = t % D3
        return send(s3_v.at[s, g, 1], r3_v.at[s, g], s3_sem.at[s], r3_sem.at[s], axis_nbr[AZ])

    def pair_there(t, g):
        s = t % DO
        return send(q_v.at[s, g], c_v.at[:, tile_cols(t, g)], qs_sem.at[s], qr_sem, axis_nbr[AZ])

    def last_there(g):
        s = last % DO
        return send(q_v.at[s, g, pl.ds(0, upper)], c_v.at[pl.ds(g * upper, upper), last_cols(z)],
                    qs_sem.at[s], qr_sem, axis_nbr[AZ])

    def sent3(t):
        wait_bytes(r3_v.at[t % D3], s3_sem.at[t % D3])

    def got3(t):
        wait_bytes(r3_v.at[t % D3], r3_sem.at[t % D3])

    def pair_sent(t):
        wait_bytes(q_v.at[t % DO], qs_sem.at[t % DO])

    def take(t, g, phase, slots, high):
        when(t, slots, high, lambda: pl.semaphore_wait(credit.at[2 * phase + g], 1))

    def give(t, g, phase, axis, slots, high):
        when(t, 0, high - slots, lambda: pl.semaphore_signal(
            credit.at[2 * phase + g], inc=1, device_id=axis_nbr[axis], device_id_type=MESH))

    for copy in own:
        copy.start()
    pl.semaphore_wait(barrier, 4)
    for group in (xy_far1, y_far, z_own, xy_near1, x_far, x_near):
        for copy in group:
            copy.start()
    for t in range(min(LOOK, tiles)):
        bx_copy(t).start()
    for t in range(2):
        fetch_near(t)
    for h in both:
        y_far[h].wait_recv()
        z_y[h].start()
        xy_far1[h].wait_recv()
        xy_far2[h].start()
    for h in both:
        xy_near1[h].wait_recv()
        xy_near2[h].start()
        xy_far2[h].wait_recv()
        z_xy[h].start()
    for copy in y_near:
        copy.start()
    for t in range(2):
        wait_bytes(b_v.at[t, pl.ds(0, 2 * depth)], b_sem.at[t])
    wait_bytes(a_v.at[0], ch_recv.at[14])
    end_group(1, 4)
    first_two(3, lambda j: j + j // 2)
    for h in both:
        x_far[h].wait_recv()
        z_x[h].start()
    for n in range(AHEAD):
        a_chunk(n).start()
    end_group(2, 4)
    first_two(2, lambda j: 6 + j)
    for t in range(2):
        for g in both:
            send1(t, g, 1).start()
    end_group(3, 6)

    def last_three(j):
        return 2 + (3 * j + 1) // 2

    def add3(t, g):
        c_v[:, tile_cols(t, g)] = (s3_v[t % D3, g, 0] + r3_v[t % D3, g]).astype(jnp.bfloat16)

    def start_late():
        def body(t, carry):
            take(t, 0, 2, D3, plain)
            for g in both:
                send3(t, g).start()
            return carry

        lax.fori_loop(plain - LATE, plain, body, 0)

    def each(low, high, fn):
        def body(n, carry):
            fn(n)
            return carry

        lax.fori_loop(low, high, body, 0)

    def end_hops():
        wait_bytes(a_v.at[pl.ds(0, hops // 4)], qr_sem)
        for n in range(AHEAD):
            a_chunk(n).wait_send()

    def step(i, carry):
        t = i
        when(t, LAG, LAG + 1, end_hops)
        when(t, LAG, tiles + 3, lambda: end_chunks(t - LAG))
        when(t, 0, tiles, lambda: start_chunks(t))
        when(t, 1, tiles - 1, lambda: fetch_near(t + 1))
        when(t, tiles - 1, tiles, last_near)
        when(t, 0, 1, lambda: bx_copy(0).wait_send())
        when(t, 0, tiles - 1, lambda: bx_copy(t + 1).wait_send())
        when(t, tiles - 1, tiles, lambda: last_bx().wait_send())
        when(t, plain, tiles, lambda: bxz_copy(t - plain).wait_send())
        when(t, 0, tiles - LOOK, lambda: bx_copy(t + LOOK).start())
        when(t, tiles - LOOK, tiles - LOOK + 1, lambda: last_bx().start())
        when(t, 2, tiles + 2, lambda: sent1(t - 2))

        def wait_b(pieces):
            wait_bytes(b_v.at[t % 2, pl.ds(0, pieces * depth)], b_sem.at[t % 2])

        def near_products():
            wait_b(2)
            partials(t, 2)

        def all_products():
            wait_b(4)
            partials(t, 4)

        def last_products():
            wait_bytes(b_v.at[last % 2, :, 0:W], b_sem.at[last % 2])
            last_partials()

            for g in both:
                pl.semaphore_wait(credit.at[g], 1)
                last_send1(g, 0).start()

        def start_kept():
            for g in both:
                last_send1(g, 1).start()

        def wait_far():
            wait_bytes(a_v.at[pl.ds(0, 4), :, pl.ds(2 * depth, 2 * depth)], ch_recv.at[0])

        when(t, 0, 2, lambda: partials(t, 2, 3, last_three))
        when(t, 2, plain, near_products)
        when(t, plain, plain + 1, wait_far)
        when(t, plain, tiles, all_products)
        when(t, last, last + 1, last_products)
        for g in both:
            take(t, g, 0, 2, tiles)
            when(t, 2, tiles, lambda g=g: send1(t, g, 1).start())
        for g in both:
            when(t, 0, tiles, lambda g=g: send1(t, g, 0).start())
        when(t, plain - 1, tiles - 1, lambda: fetch_far(t + 1))
        when(t, tiles - 1, tiles, last_far)

        t1 = i - 1

        def add1(k):
            s, blocks = t1 % 2, pl.ds(2 * k, 2)
            got1(t1, k)
            for g in both:
                s2_v[s, g, blocks] = p_v[s, g, 0, blocks] + r1_v[s, g, blocks]

        def last1():
            last_add1(0)
            for g in both:
                pl.semaphore_wait(credit.at[2 + g], 1)
                send2(last, g, 1, upper).start()
            for g in both:
                send2(last - 1, g, 0).start()
            for g in both:
                last_send1(g, 2).start()
            for g in both:
                send2(last, g, 0, upper).start()

        when(t1, 2, tiles + 1, lambda: sent2(t1 - 2))
        when(t1, 0, tiles, lambda: add1(1))
        for g in both:
            take(t1, g, 1, 2, tiles)
            when(t1, 0, tiles, lambda g=g: send2(t1, g, 1).start())
            when(t1, 0, tiles - 1, lambda g=g: send2(t1, g, 0).start())
        when(t, last, last + 1, start_kept)
        when(t1, 0, tiles, lambda: add1(0))
        for g in both:
            give(t1, g, 0, g, 2, last + 1)
        when(t1, last, last + 1, last1)

        t2 = i - 2

        def sum2(t, g, k, n=rows):
            part = pl.ds(0, n)
            return s2_v[t % 2, g, k, part] + r2_v[t % 2, g, k, part]

        def last2():
            last_add1(1)
            got2(last, 1, upper)
            for g in both:
                q_v[last % DO, g, last_part] = sum2(last, g, 1, upper).astype(jnp.bfloat16)
                last_there(g).start()
            each(plain - LATE, plain, got3)
            for g in both:
                each(plain - LATE, plain, lambda t: add3(t, g))
            each(plain - LATE, plain, sent3)
            each(tiles + 3 - LAG, tiles, end_chunks)
            each(max(plain, last + 1 - DO), tiles - 1, pair_sent)
            last_bxz().wait_send()
            add2_here(last - 1)
            last_add1(2)
            pair_sent(last - 1)
            sent2(last - 1)
            wait_bytes(r1_v.at[last % 2, :, :, last_part], s1_sem.at[last % 2])
            wait_bytes(q_v.at[last % DO, :, last_part], qs_sem.at[last % DO])
            wait_bytes(c_v.at[:, pl.ds(0, paired * C + W)], qr_sem)
            got2(last, 0, upper)
            for g in both:
                c_v[pl.ds(g * upper, upper), last_cols(z)] = sum2(last, g, 0, upper).astype(jnp.bfloat16)

        def add2(k):
            got2(t2, k)
            for g in both:
                s3_v[t2 % D3, g, k] = sum2(t2, g, k)

        def add2_there():
            got2(t2, 1)
            for g in both:
                q_v[t2 % DO, g] = sum2(t2, g, 1).astype(jnp.bfloat16)

        def add2_here(t):
            got2(t, 0)
            for g in both:
                c_v[:, tile_cols(t, g)] = sum2(t, g, 0).astype(jnp.bfloat16)

        when(t2, D3, plain - LATE + D3, lambda: sent3(t2 - D3))
        when(t2, plain + DO, last + 1, lambda: pair_sent(t2 - DO))
        when(t2, 0, plain, lambda: add2(1))
        when(t2, plain, tiles, add2_there)
        take(t2, 0, 2, D3, plain - LATE)
        for g in both:
            when(t2, 0, plain - LATE, lambda g=g: send3(t2, g).start())
            when(t2, plain, tiles, lambda g=g: pair_there(t2, g).start())
        when(t2, 0, plain, lambda: add2(0))
        when(t2, plain, tiles - 1, lambda: add2_here(t2))
        for g in both:
            give(t2, g, 1, 1 - g, 2, last + 1)
        when(t2, last, last + 1, last2)

        t3 = i - 1 - D3
        when(t3, 0, plain - LATE, lambda: got3(t3))
        for g in both:
            when(t3, 0, plain - LATE, lambda g=g: add3(t3, g))
        give(t3, 0, 2, AZ, D3, plain)
        when(t, last - 2, last - 1, start_late)
        when(t, plain - 1, tiles - 1, lambda: fetch_last(t + 1))
        when(t, tiles - 1, tiles, last_fetch)
        return carry

    lax.fori_loop(0, tiles + 3, step, 0)

    sent2(last, upper)


def solution(mesh):
    spec_rows = P(("dp", "tp"), None)

    def local_block(a_rows, b_rows):
        rows, inner = a_rows.shape
        depth, columns = b_rows.shape
        plain, paired = counts(columns)
        tiles = plain + paired
        f32, bf16 = jnp.float32, jnp.bfloat16
        dma = pltpu.SemaphoreType.DMA
        out = pl.pallas_call(
            kernel,
            name="matmul_reduce_scatter",
            out_shape=(
                pltpu.VMEM((rows, columns), bf16),
                jax.ShapeDtypeStruct((tiles + 1, depth, C), bf16),
                jax.ShapeDtypeStruct((paired + 1, depth, C), bf16),
                jax.ShapeDtypeStruct((paired + 1, depth, C), bf16),
                jax.ShapeDtypeStruct((2, rows, 2 * depth), bf16),
            ),
            in_specs=[pl.BlockSpec(memory_space=pl.ANY)] * 2,
            out_specs=(pl.BlockSpec(memory_space=pltpu.VMEM),) + (pl.BlockSpec(memory_space=pl.ANY),) * 4,
            scratch_shapes=[
                pltpu.VMEM((8, rows, 4 * depth), bf16),
                pltpu.VMEM((2, 4 * depth, C), bf16),
                pltpu.VMEM((2, 2, 2, 4, rows, W), f32),
                pltpu.VMEM((2, 2, 4, rows, W), f32),
                pltpu.VMEM((2, 2, 4, rows, W), f32),
                pltpu.VMEM((2, 2, 2, rows, W), f32),
                pltpu.VMEM((D3, 2, 2, rows, W), f32),
                pltpu.VMEM((D3, 2, rows, W), f32),
                pltpu.VMEM((DO, 2, rows, W), bf16),
                dma((2,)), dma((RX,)), dma, dma((RZ,)), dma((5 * pace(columns) // 100 + 2,)), dma((max(2 + paired, 15),)), dma((2,)),
                dma((2,)), dma((2, 2)), dma((2,)), dma((2, 2)), dma((D3,)), dma((D3,)), dma((DO,)), dma,
                pltpu.SemaphoreType.REGULAR((5,)),
            ],
            compiler_params=pltpu.CompilerParams(
                collective_id=0, has_side_effects=True, vmem_limit_bytes=56 * 1024 * 1024),
            cost_estimate=pl.CostEstimate(
                flops=2 * 8 * rows * 2 * depth * columns, bytes_accessed=6 * depth * columns, transcendentals=0),
        )(a_rows, b_rows)
        return out[0]

    return jax.shard_map(local_block, mesh=mesh, in_specs=(spec_rows, spec_rows), out_specs=spec_rows, check_vma=False)
```
